64 devices in a mesh: dp: 4 (over x, y), tp: 16 (over z, core).
Axes of the slice: x: 2, y: 2, z: 8, core: 2. Of those that a mesh axis runs over, the one named last changes fastest.
The devices are a block of a 4x4x8 slice.
Arguments:
- token_act: bfloat16 [32, 1024, 768], P('dp'), parts along dimension 0
- token_cond: bfloat16 [32, 1024, 384], P('dp'), parts along dimension 0
- pair_bias: bfloat16 [2, 16, 1024, 1024], P(None, 'tp')
- token_mask: int32 [1024], replicated
- ada_scale: float32 [2, 2, 384], replicated
- ada_w: bfloat16 [2, 2, 384, 2, 768], replicated
- ada_bias: float32 [2, 2, 768], replicated
- zero_w: bfloat16 [2, 384, 2, 768], replicated
- zero_b: float32 [2, 2, 768], replicated
- w_qkvg: bfloat16 [2, 768, 4, 768], P(None, None, None, 'tp')
- b_q: float32 [2, 768], P(None, 'tp')
- w_o: bfloat16 [2, 768, 768], P(None, 'tp')
- w_up: bfloat16 [2, 768, 2, 1536], P(None, None, None, 'tp')
- w_down: bfloat16 [2, 1536, 768], P(None, 'tp')
Outputs:
- output: bfloat16 [32, 1024, 768], P('dp'), parts along dimension 0
There are 4 independent parts. The reference program is written for one: setup_inputs(seed, part) draws one part's arguments, and reference() takes and returns one part's arrays. A program takes and returns all parts, laid end to end along the dimension named above; an argument that names none is the same for every part.
All inputs are finite; a program needn't handle non-finite values.
Results may differ from the reference program's by a relative error of at most 0.02.
Values are sent between devices in bfloat16 or wider.
A program may use at most 768 MiB of HBM per device.

```python
import math
import jax
import jax.numpy as jnp
from jax import lax

SAMPLES = 8
TOKENS = 1024
TOKEN_DIM = 768
COND_DIM = 384
NUM_HEADS = 16
HEAD_DIM = 48
HIDDEN_DIM = 1536
BLOCKS = 2

LN_EPS = 1e-5
BIAS_SCALE = math.sqrt(math.log(TOKENS / 4.0))


def layer_norm(values_in):
    row_mean = jnp.mean(values_in, axis=-1, keepdims=True)
    centered = values_in - row_mean
    variance = jnp.mean(centered * centered, axis=-1, keepdims=True)
    return centered * lax.rsqrt(variance + LN_EPS)


def ada_norm(act_f32, cond_normed, scale_vec, weight, bias_vec):
    cond_in = (cond_normed * scale_vec).astype(jnp.bfloat16)
    modulation = jnp.dot(cond_in, weight.reshape(COND_DIM, 2 * TOKEN_DIM), preferred_element_type=jnp.float32)
    modulation = modulation.reshape(-1, 2, TOKEN_DIM)
    return (jax.nn.sigmoid(modulation[:, 0] + bias_vec) * layer_norm(act_f32) + modulation[:, 1]).astype(jnp.bfloat16)


def setup_inputs(seed: int = 0, part: int = 0) -> dict:
    root_key = jax.random.key(seed)
    shared_keys = jax.random.split(root_key, 12)
    part_keys = jax.random.split(jax.random.fold_in(shared_keys[11], part), 2)
    token_act = jax.random.normal(part_keys[0], (SAMPLES, TOKENS, TOKEN_DIM), jnp.float32)
    token_cond = jax.random.normal(part_keys[1], (SAMPLES, TOKENS, COND_DIM), jnp.float32)
    pair_bias = BIAS_SCALE * jax.random.normal(shared_keys[0], (BLOCKS, NUM_HEADS, TOKENS, TOKENS), jnp.float32)
    keep_draw = jax.random.randint(shared_keys[1], (TOKENS,), 0, 4)
    token_mask = jnp.where((keep_draw != 0) | (jnp.arange(TOKENS) == 0), 1, 0).astype(jnp.int32)
    cond_gain = COND_DIM ** -0.5
    width_gain = TOKEN_DIM ** -0.5
    hidden_gain = HIDDEN_DIM ** -0.5
    ada_scale = 1.0 + 0.5 * jax.random.normal(shared_keys[2], (BLOCKS, 2, COND_DIM), jnp.float32)
    ada_w = cond_gain * jax.random.normal(shared_keys[3], (BLOCKS, 2, COND_DIM, 2, TOKEN_DIM), jnp.float32)
    ada_bias = jax.random.normal(shared_keys[4], (BLOCKS, 2, TOKEN_DIM), jnp.float32)
    zero_w = cond_gain * jax.random.normal(shared_keys[5], (BLOCKS, COND_DIM, 2, TOKEN_DIM), jnp.float32)
    zero_b = jax.random.normal(shared_keys[6], (BLOCKS, 2, TOKEN_DIM), jnp.float32)
    w_qkvg = width_gain * jax.random.normal(shared_keys[7], (BLOCKS, TOKEN_DIM, 4, TOKEN_DIM), jnp.float32)
    b_q = jax.random.normal(shared_keys[8], (BLOCKS, TOKEN_DIM), jnp.float32)
    w_o = 2.0 * width_gain * jax.random.normal(shared_keys[9], (BLOCKS, TOKEN_DIM, TOKEN_DIM), jnp.float32)
    up_down = jax.random.split(shared_keys[10], 2)
    w_up = width_gain * jax.random.normal(up_down[0], (BLOCKS, TOKEN_DIM, 2, HIDDEN_DIM), jnp.float32)
    w_down = 2.0 * hidden_gain * jax.random.normal(up_down[1], (BLOCKS, HIDDEN_DIM, TOKEN_DIM), jnp.float32)
    return {
        'token_act': token_act.astype(jnp.bfloat16),
        'token_cond': token_cond.astype(jnp.bfloat16),
        'pair_bias': pair_bias.astype(jnp.bfloat16),
        'token_mask': token_mask,
        'ada_scale': ada_scale,
        'ada_w': ada_w.astype(jnp.bfloat16),
        'ada_bias': ada_bias,
        'zero_w': zero_w.astype(jnp.bfloat16),
        'zero_b': zero_b,
        'w_qkvg': w_qkvg.astype(jnp.bfloat16),
        'b_q': b_q,
        'w_o': w_o.astype(jnp.bfloat16),
        'w_up': w_up.astype(jnp.bfloat16),
        'w_down': w_down.astype(jnp.bfloat16),
    }


def reference(token_act, token_cond, pair_bias, token_mask, ada_scale, ada_w, ada_bias, zero_w, zero_b, w_qkvg, b_q, w_o, w_up, w_down):
    row_count = SAMPLES * TOKENS
    head_shape = (SAMPLES, TOKENS, NUM_HEADS, HEAD_DIM)
    logit_scale = 1.0 / math.sqrt(HEAD_DIM)
    mask_add = (token_mask.astype(jnp.float32) - 1.0) * 1e9
    cond_flat = token_cond.reshape(row_count, COND_DIM)
    cond_normed = layer_norm(cond_flat.astype(jnp.float32))

    def block_step(act_flat, layer_args):
        (layer_scale, layer_ada_w, layer_ada_b, layer_zero_w, layer_zero_b, layer_qkvg, layer_bq, layer_wo, layer_up, layer_down, layer_bias) = layer_args
        out_gates = jax.nn.sigmoid(jnp.dot(cond_flat, layer_zero_w.reshape(COND_DIM, 2 * TOKEN_DIM), preferred_element_type=jnp.float32).reshape(row_count, 2, TOKEN_DIM) + layer_zero_b)
        act_f32 = act_flat.astype(jnp.float32)
        normed = ada_norm(act_f32, cond_normed, layer_scale[0], layer_ada_w[0], layer_ada_b[0])
        projected = jnp.dot(normed, layer_qkvg.reshape(TOKEN_DIM, 4 * TOKEN_DIM), preferred_element_type=jnp.float32).reshape(row_count, 4, TOKEN_DIM)
        query_rows = (projected[:, 0] + layer_bq).astype(jnp.bfloat16).reshape(head_shape)
        key_rows = projected[:, 1].astype(jnp.bfloat16).reshape(head_shape)
        value_rows = projected[:, 2].astype(jnp.bfloat16).reshape(head_shape)
        gate_heads = jax.nn.sigmoid(projected[:, 3])
        bias_f32 = layer_bias.astype(jnp.float32)

        def attend(operands):
            query_one, key_one, value_one = operands
            logits = jnp.einsum('qhc,khc->hqk', query_one.astype(jnp.float32), key_one.astype(jnp.float32)) * logit_scale + bias_f32 + mask_add
            attn_probs = jax.nn.softmax(logits, axis=-1).astype(jnp.bfloat16)
            return jnp.einsum('hqk,khc->qhc', attn_probs.astype(jnp.float32), value_one.astype(jnp.float32))

        mixed_heads = lax.map(attend, (query_rows, key_rows, value_rows)).reshape(row_count, TOKEN_DIM)
        heads_out = (gate_heads * mixed_heads).astype(jnp.bfloat16)
        attn_out = jnp.dot(heads_out, layer_wo, preferred_element_type=jnp.float32).astype(jnp.bfloat16).astype(jnp.float32)
        mid_f32 = (act_f32 + out_gates[:, 0] * attn_out).astype(jnp.bfloat16).astype(jnp.float32)
        normed_mid = ada_norm(mid_f32, cond_normed, layer_scale[1], layer_ada_w[1], layer_ada_b[1])
        hidden_pre = jnp.dot(normed_mid, layer_up.reshape(TOKEN_DIM, 2 * HIDDEN_DIM), preferred_element_type=jnp.float32).reshape(row_count, 2, HIDDEN_DIM)
        hidden = (jax.nn.silu(hidden_pre[:, 0]) * hidden_pre[:, 1]).astype(jnp.bfloat16)
        trans_out = jnp.dot(hidden, layer_down, preferred_element_type=jnp.float32).astype(jnp.bfloat16).astype(jnp.float32)
        act_next = (mid_f32 + out_gates[:, 1] * trans_out).astype(jnp.bfloat16)
        return act_next, None

    layer_stack = (ada_scale, ada_w, ada_bias, zero_w, zero_b, w_qkvg, b_q, w_o, w_up, w_down, pair_bias)
    final_act = lax.scan(block_step, token_act.reshape(row_count, TOKEN_DIM), layer_stack)[0]
    return final_act.reshape(SAMPLES, TOKENS, TOKEN_DIM)
```

```python
import functools
import math

import jax
import jax.numpy as jnp
from jax import lax
from jax.experimental import pallas as pl
from jax.experimental.pallas import tpu as pltpu
from jax.sharding import PartitionSpec as P

LN_EPS = 1e-5
LOG2E = 1.4426950408889634
MESH = pl.DeviceIdType.MESH
BF16 = jnp.bfloat16
F32 = jnp.float32


def _ln(x):
    mean = jnp.mean(x, axis=-1, keepdims=True)
    cen = x - mean
    var = jnp.mean(cen * cen, axis=-1, keepdims=True)
    return cen * lax.rsqrt(var + LN_EPS)


def _sig(x):
    return 0.5 * jnp.tanh(0.5 * x) + 0.5


def _dot(a, b, ca=1, cb=0):
    return lax.dot_general(a, b, (((ca,), (cb,)), ((), ())), preferred_element_type=F32)


def _ada(x_f32, cond_normed, scale, w, bias):
    d = x_f32.shape[-1]
    mod = _dot((cond_normed * scale).astype(BF16), w)
    return (_sig(mod[:, :d] + bias) * _ln(x_f32) + mod[:, d:]).astype(BF16)


def _attn_kernel(first, dims, *refs):
    S, T, D, C, n_tp, hd, hp, layer, q_tile = dims
    if first:
        (x_hbm, cond_hbm, bias_hbm, mask_ref, w_ref, brow_ref, ascale_ref, aw_ref, ab_ref, o_hbm,
         xbuf, cbuf, bias_v, bt, k_s, qt_s, vt_s, gt_s, o_s, ld_sem, cd_sem, b_sem, send_sem, recv_sem) = refs
    else:
        (x_hbm, bias_hbm, mask_ref, w_ref, brow_ref, o_hbm,
         xbuf, bias_v, bt, k_s, qt_s, vt_s, gt_s, o_s, ld_sem, b_sem, send_sem, recv_sem) = refs
    cores = n_tp // S
    half = T // cores
    me = lax.axis_index("tp")
    z = me // cores

    barrier = pltpu.get_barrier_semaphore()
    for i in range(1, n_tp):
        pl.semaphore_signal(barrier, inc=1, device_id={"tp": lax.rem(me + i, n_tp)}, device_id_type=MESH)

    def sample_of(k):
        return lax.rem(z + 1 + k, S)

    def loads(k, slot):
        s = sample_of(k)
        out = [pltpu.make_async_copy(x_hbm.at[s], xbuf.at[slot], ld_sem.at[slot])]
        if first:
            out.append(pltpu.make_async_copy(cond_hbm.at[s], cbuf.at[slot], cd_sem.at[slot]))
        return out

    bias_cp = pltpu.make_async_copy(bias_hbm.at[layer, 0], bias_v, b_sem)
    bias_cp.start()
    for cp in loads(0, 0):
        cp.start()
    mask_add = (mask_ref[...].astype(F32) - 1.0) * 1e9
    qt_s[hp:, :] = jnp.zeros((hp, T), BF16)
    bias_cp.wait()

    def bias_step(i, _):
        r = pl.multiple_of(i * 128, 128)
        rows = (bias_v[pl.ds(r, 128), :].astype(F32) + mask_add) * LOG2E
        bt[:, pl.ds(r, 128)] = rows.T
        return 0

    lax.fori_loop(0, T // 128, bias_step, 0)
    pl.semaphore_wait(barrier, n_tp - 1)

    c1 = LOG2E / math.sqrt(hd)

    def message(k, slot, c):
        dst = sample_of(k) * cores + c
        return dst, pltpu.make_async_remote_copy(
            src_ref=o_s.at[slot, :, pl.ds(c * half, half)], dst_ref=o_hbm.at[me],
            send_sem=send_sem.at[slot, c], recv_sem=recv_sem, device_id={"tp": dst}, device_id_type=MESH)

    def sends(k, slot):
        for c in range(cores):
            dst, cp = message(k, slot, c)

            @pl.when(dst != me)
            def _():
                cp.start()

            @pl.when(dst == me)
            def _():
                pltpu.make_async_copy(o_s.at[slot, :, pl.ds(c * half, half)], o_hbm.at[me], recv_sem).start()

    def wait_sends(k, slot):
        for c in range(cores):
            dst, cp = message(k, slot, c)

            @pl.when(dst != me)
            def _():
                cp.wait_send()

    def step(k, _):
        slot = lax.rem(k, 2)

        @pl.when(k + 1 < S)
        def _():
            for cp in loads(k + 1, 1 - slot):
                cp.start()

        for cp in loads(k, slot):
            cp.wait()

        def proj(i, _):
            r = pl.multiple_of(i * q_tile, q_tile)
            rows = pl.ds(r, q_tile)
            xt = xbuf[slot, rows, :]
            if first:
                cn = _ln(cbuf[slot, rows, :].astype(F32))
                xt = _ada(xt.astype(F32), cn, ascale_ref[...], aw_ref[...], ab_ref[...])
            res = _dot(xt, w_ref[...]) + brow_ref[...]
            k_s[rows, :] = res[:, :2 * hp].astype(BF16)
            rest = res.T
            qt_s[0:hp, rows] = rest[hp:2 * hp].astype(BF16)
            ones = lax.broadcasted_iota(jnp.int32, (hp, q_tile), 0) == hd
            vt_s[:, rows] = jnp.where(ones, 1.0, rest[2 * hp:3 * hp]).astype(BF16)
            gt_s[:, rows] = _sig(rest[3 * hp:3 * hp + hd])
            return 0

        lax.fori_loop(0, T // q_tile, proj, 0)

        @pl.when(k >= 1)
        def _():
            sends(k - 1, 1 - slot)

        @pl.when(k >= 2)
        def _():
            wait_sends(k - 2, slot)

        def attend(i, _):
            r = pl.multiple_of(i * q_tile, q_tile)
            cols = pl.ds(r, q_tile)
            logits = _dot(k_s[...], qt_s[:, cols]) * c1 + bt[:, cols]
            top = jnp.max(logits, axis=0, keepdims=True)
            probs = jnp.exp2(logits - top).astype(BF16)
            mixed = _dot(vt_s[...], probs)
            o_s[slot, :, cols] = (gt_s[:, cols] * (mixed[:hd] / mixed[hd:hd + 1])).astype(BF16)
            return 0

        lax.fori_loop(0, T // q_tile, attend, 0)
        return 0

    lax.fori_loop(0, S, step, 0)
    sends(S - 1, (S - 1) % 2)
    wait_sends(S - 2, S % 2)
    wait_sends(S - 1, (S - 1) % 2)
    pltpu.make_async_copy(o_hbm, o_hbm, recv_sem).wait()


def _attention(layer, n_tp, x, cond, pair_bias, mask_row, w, brow, ada, collective_id):
    S, T, D = x.shape
    first = cond is not None
    hd = w.hd
    hp = w.hp
    C = cond.shape[-1] if first else 0
    q_tile = 256
    cores = n_tp // S
    half = T // cores
    anyspec = pl.BlockSpec(memory_space=pl.ANY)
    vspec = pl.BlockSpec(memory_space=pltpu.VMEM)
    args = [x] + ([cond] if first else []) + [pair_bias, mask_row, w.w, brow] + (list(ada) if first else [])
    specs = [anyspec] + ([anyspec] if first else []) + [anyspec, vspec, vspec, vspec] + ([vspec] * 3 if first else [])
    scratch = [pltpu.VMEM((2, T, D), BF16)] + ([pltpu.VMEM((2, T, C), BF16)] if first else []) + [
        pltpu.VMEM((T, T), BF16), pltpu.VMEM((T, T), F32), pltpu.VMEM((T, 2 * hp), BF16), pltpu.VMEM((2 * hp, T), BF16),
        pltpu.VMEM((hp, T), BF16), pltpu.VMEM((hd, T), F32), pltpu.VMEM((2, hd, T), BF16),
        pltpu.SemaphoreType.DMA((2,))] + ([pltpu.SemaphoreType.DMA((2,))] if first else []) + [
        pltpu.SemaphoreType.DMA, pltpu.SemaphoreType.DMA((2, cores)), pltpu.SemaphoreType.DMA]
    flops = 2 * S * T * (D * 4 * hp + 2 * T * 256 + (2 * C * D if first else 0))
    return pl.pallas_call(
        functools.partial(_attn_kernel, first, (S, T, D, C, n_tp, hd, hp, layer, q_tile)),
        out_shape=jax.ShapeDtypeStruct((n_tp, hd, half), BF16),
        in_specs=specs, out_specs=anyspec, scratch_shapes=scratch,
        cost_estimate=pl.CostEstimate(flops=flops, bytes_accessed=S * T * (D + C) * 2, transcendentals=S * T * T),
        compiler_params=pltpu.CompilerParams(collective_id=collective_id, has_side_effects=True, vmem_limit_bytes=60 << 20),
        name=f"attn{layer}",
    )(*args)


class _W:
    def __init__(self, w, hd, hp):
        self.w, self.hd, self.hp = w, hd, hp


def _mlp_kernel(nxt, dims, *refs):
    R, D, C, n_tp, hd, hu = dims
    if nxt:
        (o_ref, act_hbm, cond_hbm, wall_hbm, zw_ref, zb_ref, sc1_ref, w1_ref, b1_ref, sc2_ref, w2_ref, b2_ref,
         a_out, x_out, act, cond, wall, y_s, h_s, sems) = refs
    else:
        (o_ref, act_hbm, cond_hbm, wall_hbm, zw_ref, zb_ref, sc1_ref, w1_ref, b1_ref,
         a_out, act, cond, wall, y_s, h_s, sems) = refs
    if act_hbm.shape[0] != R:
        row0 = lax.axis_index("tp") * R
        act_src = act_hbm.at[pl.ds(row0, R), :]
    else:
        act_src = act_hbm
    row0 = lax.axis_index("tp") * R
    copies = [pltpu.make_async_copy(cond_hbm.at[pl.ds(row0, R), :], cond, sems.at[0]),
              pltpu.make_async_copy(act_src, act, sems.at[1]),
              pltpu.make_async_copy(wall_hbm, wall, sems.at[2])]
    for cp in copies:
        cp.start()
    copies[0].wait()
    cond_b = cond[...]
    cn = _ln(cond_b.astype(F32))
    gates = _sig(_dot(cond_b, zw_ref[...]) + zb_ref[...])
    copies[1].wait()
    copies[2].wait()
    o_t = o_ref[...].reshape(n_tp * hd, R)
    w_o = wall[:, 0:hd, :].reshape(n_tp * hd, D)
    t = _dot(o_t, w_o, 0, 0).astype(BF16).astype(F32)
    mid = (act[...].astype(F32) + gates[:, :D] * t).astype(BF16).astype(F32)
    y_s[...] = _ada(mid, cn, sc1_ref[...], w1_ref[...], b1_ref[...])
    H = n_tp * hu
    step = 4 * hu
    for j in range(H // step):
        dv = slice(4 * j, 4 * j + 4)
        u1 = _dot(y_s[...], wall[dv, hd + hu:hd + 2 * hu, :].reshape(step, D), 1, 1)
        u2 = _dot(y_s[...], wall[dv, hd + 2 * hu:hd + 3 * hu, :].reshape(step, D), 1, 1)
        h_s[:, j * step:(j + 1) * step] = (u1 * _sig(u1) * u2).astype(BF16)
    r = _dot(h_s[...], wall[:, hd:hd + hu, :].reshape(H, D)).astype(BF16).astype(F32)
    new = (mid + gates[:, D:] * r).astype(BF16)
    a_out[...] = new
    if nxt:
        x_out[...] = _ada(new.astype(F32), cn, sc2_ref[...], w2_ref[...], b2_ref[...])


def _mlp(o, act, cond, wall, zero, ada1, ada2, hd, hu):
    n_tp, _, R = o.shape
    D = act.shape[-1]
    C = cond.shape[-1]
    nxt = ada2 is not None
    anyspec = pl.BlockSpec(memory_space=pl.ANY)
    vspec = pl.BlockSpec(memory_space=pltpu.VMEM)
    args = [o, act, cond, wall, *zero, *ada1] + (list(ada2) if nxt else [])
    specs = [vspec, anyspec, anyspec, anyspec] + [vspec] * (len(args) - 4)
    row = jax.ShapeDtypeStruct((R, D), BF16)
    return pl.pallas_call(
        functools.partial(_mlp_kernel, nxt, (R, D, C, n_tp, hd, hu)),
        out_shape=(row, row) if nxt else row,
        in_specs=specs, out_specs=(vspec, vspec) if nxt else vspec,
        scratch_shapes=[pltpu.VMEM((R, D), BF16), pltpu.VMEM((R, C), BF16), pltpu.VMEM(wall.shape, BF16),
                        pltpu.VMEM((R, D), BF16), pltpu.VMEM((R, n_tp * hu), BF16), pltpu.SemaphoreType.DMA((3,))],
        cost_estimate=pl.CostEstimate(flops=2 * R * D * (D + 3 * n_tp * hu + 6 * C), bytes_accessed=wall.size * 2, transcendentals=R * D),
        compiler_params=pltpu.CompilerParams(vmem_limit_bytes=60 << 20),
        name="mlp" + ("0" if nxt else "1"),
    )(*args)


def solution(mesh):
    n_tp = mesh.shape["tp"]

    def shard_body(token_act, token_cond, pair_bias, token_mask, ada_scale, ada_w, ada_bias, zero_w, zero_b, w_qkvg, b_q, w_o, w_up, w_down):
        S, T, D = token_act.shape
        C = token_cond.shape[-1]
        hd = w_qkvg.shape[-1]
        hp = 64
        hu = w_down.shape[1]
        L = pair_bias.shape[0]
        mask_row = token_mask.reshape(1, T)

        walls = []
        for l in range(L):
            up = jnp.transpose(w_up[l], (1, 2, 0)).reshape(2 * hu, D)
            walls.append(lax.all_gather(jnp.concatenate([w_o[l], w_down[l], up], axis=0), "tp"))

        def qkvg(l):
            w = jnp.pad(w_qkvg[l], ((0, 0), (0, 0), (0, hp - hd)))
            w = jnp.concatenate([w[:, 1], w[:, 0], w[:, 2], w[:, 3]], axis=1)
            brow = jnp.zeros((1, 4 * hp), F32).at[0, hp:hp + hd].set(b_q[l])
            return _W(w, hd, hp), brow

        def ada(l, j):
            return ada_scale[l, j].reshape(1, C), ada_w[l, j].reshape(C, 2 * D), ada_bias[l, j].reshape(1, D)

        def zero(l):
            return zero_w[l].reshape(C, 2 * D), zero_b[l].reshape(1, 2 * D)

        cond_flat = token_cond.reshape(S * T, C)
        act = token_act.reshape(S * T, D)
        x = token_act
        for l in range(L):
            w, brow = qkvg(l)
            o = _attention(l, n_tp, x, token_cond if l == 0 else None, pair_bias, mask_row, w, brow, ada(l, 0), l)
            if l + 1 < L:
                act, x_own = _mlp(o, act, cond_flat, walls[l], zero(l), ada(l, 1), ada(l + 1, 0), hd, hu)
                x = lax.all_gather(x_own, "tp", tiled=True).reshape(S, T, D)
            else:
                act = _mlp(o, act, cond_flat, walls[l], zero(l), ada(l, 1), None, hd, hu)
        return lax.all_gather(act, "tp", tiled=True).reshape(S, T, D)

    everywhere = P()
    in_specs = (P('dp', None, None), P('dp', None, None), P(None, 'tp', None, None), P(None), everywhere, everywhere, everywhere, everywhere, everywhere, P(None, None, None, 'tp'), P(None, 'tp'), P(None, 'tp', None), P(None, None, None, 'tp'), P(None, 'tp', None))
    return jax.shard_map(shard_body, mesh=mesh, in_specs=in_specs, out_specs=P('dp', None, None), check_vma=False)
```

```python
import functools
import math

import jax
import jax.numpy as jnp
from jax import lax
from jax.experimental import pallas as pl
from jax.experimental.pallas import tpu as pltpu
from jax.sharding import PartitionSpec as P

LN_EPS = 1e-5
LOG2E = 1.4426950408889634
MESH = pl.DeviceIdType.MESH
BF16 = jnp.bfloat16
F32 = jnp.float32
HP = 64
QT = 256
ANY = pl.BlockSpec(memory_space=pl.ANY)
VMEM = pl.BlockSpec(memory_space=pltpu.VMEM)


def _ln(x):
    mean = jnp.mean(x, axis=-1, keepdims=True)
    cen = x - mean
    var = jnp.mean(cen * cen, axis=-1, keepdims=True)
    return cen * lax.rsqrt(var + LN_EPS)


def _sig(x):
    return 0.5 * jnp.tanh(0.5 * x) + 0.5


def _dot(a, b, ca=1, cb=0):
    return lax.dot_general(a, b, (((ca,), (cb,)), ((), ())), preferred_element_type=F32)


def _ada(x_f32, cond_normed, scale, w, bias):
    d = x_f32.shape[-1]
    mod = _dot((cond_normed * scale).astype(BF16), w)
    return (_sig(mod[:, :d] + bias) * _ln(x_f32) + mod[:, d:]).astype(BF16)


class Place:
    def __init__(self, n_tp):
        self.n = n_tp
        self.nz = n_tp // 2
        self.me = lax.axis_index("tp")
        self.z = self.me // 2
        self.c = lax.rem(self.me, 2)
        self.partner = self.z * 2 + (1 - self.c)

    def at(self, off):
        return lax.rem(self.z + off + self.nz, self.nz) * 2 + self.c

    def enter(self, everyone):
        barrier = pltpu.get_barrier_semaphore()
        if everyone:
            peers = [lax.rem(self.me + i, self.n) for i in range(1, self.n)]
        else:
            peers = [self.at(1), self.at(-1), self.partner]
        for p in peers:
            pl.semaphore_signal(barrier, inc=1, device_id={"tp": p}, device_id_type=MESH)
        return lambda: pl.semaphore_wait(barrier, len(peers))


class Ring:
    def __init__(self, place, view, recv_sem, send_sem, n_chunk):
        self.p, self.view, self.recv, self.send, self.n_chunk = place, view, recv_sem, send_sem, n_chunk
        self.far = place.nz // 2

    def _push(self, b, ch, dst, src=None):
        v = self.view(b, ch)
        pltpu.make_async_remote_copy(
            src_ref=v if src is None else src, dst_ref=v, send_sem=self.send, recv_sem=self.recv.at[b, ch],
            device_id={"tp": dst}, device_id_type=MESH).start()

    def own(self, ch, src=None):
        p = self.p
        self._push(p.me, ch, p.at(1), src)
        self._push(p.me, ch, p.at(-1), src)
        self._push(p.me, ch, p.partner, src)

    def wait(self, b, ch):
        v = self.view(b, ch)
        pltpu.make_async_copy(v, v, self.recv.at[b, ch]).wait()

    def service(self, h, ch):
        p = self.p
        for sign, core in ((1, 0), (-1, 1)):
            b = p.at(-sign * h)

            @pl.when((h < self.far) | (p.c == core))
            def _():
                self.wait(b, ch)

                @pl.when((h < self.far - 1) | ((h == self.far - 1) & (p.c == core)))
                def _():
                    self._push(b, ch, p.at(sign))

                self._push(b, ch, p.partner)

    def drain(self, whole):
        pltpu.make_async_copy(whole, whole, self.send).wait()


class Attend:
    def __init__(self, n_tp, hd, w, brow, bt, k_s, qt_s, vt_s, gt_s, lg, o_s, x_rows):
        self.__dict__.update(locals())
        self.T = bt.shape[0]

    def project(self):
        T, hd = self.T, self.hd
        tile = QT
        for i in range(T // tile):
            rows = pl.ds(i * tile, tile)
            res = _dot(self.x_rows(i, tile), self.w[...], 1, 1) + self.brow
            self.k_s[rows, :] = res[:, :2 * HP].astype(BF16)
            rest = res.T
            self.qt_s[0:HP, rows] = rest[HP:2 * HP].astype(BF16)
            ones = lax.broadcasted_iota(jnp.int32, (HP, tile), 0) == hd
            self.vt_s[:, rows] = jnp.where(ones, 1.0, rest[2 * HP:3 * HP]).astype(BF16)
            self.gt_s[:, rows] = _sig(rest[3 * HP:3 * HP + hd])

    def attend(self, slot):
        T, hd = self.T, self.hd
        n = T // QT
        c1 = LOG2E / math.sqrt(hd)

        def scores(i):
            cols = pl.ds(i * QT, QT)
            logits = _dot(self.k_s[...], self.qt_s[:, cols]) * c1 + self.bt[:, cols]
            self.lg[i % 2] = logits
            return jnp.max(logits, axis=0, keepdims=True)

        top = scores(0)
        for i in range(n):
            cols = pl.ds(i * QT, QT)
            nxt = scores(i + 1) if i + 1 < n else None
            probs = jnp.exp2(self.lg[i % 2] - top).astype(BF16)
            mixed = _dot(self.vt_s[...], probs)
            self.o_s[slot, :, cols] = (self.gt_s[:, cols] * (mixed[:hd] / mixed[hd:hd + 1])).astype(BF16)
            top = nxt


def _load_bias(bias_v, mask_ref, bt):
    T = bt.shape[0]
    mask_add = (mask_ref[...].astype(F32) - 1.0) * 1e9

    def step(i, _):
        r = pl.multiple_of(i * 128, 128)
        rows = (bias_v[pl.ds(r, 128), :].astype(F32) + mask_add) * LOG2E
        bt[:, pl.ds(r, 128)] = rows.T
        return 0

    lax.fori_loop(0, T // 128, step, 0)


class Exchange:
    def __init__(self, place, o_s, o_hbm, send_sem, recv_sem):
        self.p, self.o_s, self.o_hbm, self.send, self.recv = place, o_s, o_hbm, send_sem, recv_sem
        self.half = o_s.shape[-1] // 2

    def _each(self, sample, slot, remote, local):
        p = self.p
        for c in range(2):
            dst = sample * 2 + c
            src = self.o_s.at[slot, :, pl.ds(c * self.half, self.half)]
            cp = pltpu.make_async_remote_copy(
                src_ref=src, dst_ref=self.o_hbm.at[p.me], send_sem=self.send.at[slot, c], recv_sem=self.recv,
                device_id={"tp": dst}, device_id_type=MESH)

            @pl.when(dst != p.me)
            def _():
                remote(cp)

            @pl.when(dst == p.me)
            def _():
                local(pltpu.make_async_copy(src, self.o_hbm.at[p.me], self.send.at[slot, c]))

    def start(self, sample, slot):
        self._each(sample, slot, lambda cp: cp.start(), lambda cp: cp.start())

    def sent(self, sample, slot):
        self._each(sample, slot, lambda cp: cp.wait_send(), lambda cp: cp.wait())

    def arrived(self):
        rest = self.o_hbm.at[0:self.p.n - 1]
        pltpu.make_async_copy(rest, rest, self.recv).wait()


def _block0_kernel(dims, x_hbm, cond_hbm, bias_hbm, mask_ref, wq_hbm, brow_ref, asc_ref, aw_hbm, ab_ref, wo_hbm, wup_hbm, wdn_hbm,
                   o_hbm, wg_hbm,
                   xbuf, cbuf, bias_v, bt, w_s, aw_s, k_s, qt_s, vt_s, gt_s, lg, o_s, wst,
                   ld_sem, cd_sem, b_sem, q_sem, a_sem, st_sem, wl_sem, o_send, o_recv, w_send, w_recv):
    S, T, D, C, n_tp, hd, hu, L = dims
    p = Place(n_tp)
    entered = p.enter(True)
    rows_w = hd + 3 * hu
    cuts = (0, hd + hu, rows_w)
    stage = []
    for l in range(L):
        for src, lo, hi in ((wo_hbm.at[l], 0, hd), (wup_hbm.at[l, 0], hd, hd + hu), (wup_hbm.at[l, 1], hd + hu, hd + 2 * hu),
                            (wdn_hbm.at[l], hd + 2 * hu, rows_w)):
            stage.append(pltpu.make_async_copy(src, wst.at[l, lo:hi, :], st_sem.at[len(stage)]))
    for cp in stage:
        cp.start()
    sign = 1 - 2 * p.c

    def sample_of(k):
        return lax.rem(p.z + S + sign * (k + 1), S)

    def loads(k, slot):
        s = sample_of(k)
        return [pltpu.make_async_copy(x_hbm.at[s], xbuf.at[slot], ld_sem.at[slot]),
                pltpu.make_async_copy(cond_hbm.at[s], cbuf.at[slot], cd_sem.at[slot])]

    bias_cp = pltpu.make_async_copy(bias_hbm.at[0, 0], bias_v, b_sem)
    bias_cp.start()
    aw_cp = pltpu.make_async_copy(aw_hbm.at[0, 0], aw_s, a_sem)
    aw_cp.start()
    for cp in loads(0, 0):
        cp.start()
    w_s[...] = jnp.zeros_like(w_s)
    qt_s[HP:, :] = jnp.zeros((HP, T), BF16)
    order = (1, 0, 2, 3)
    wq = [pltpu.make_async_copy(wq_hbm.at[0, f], w_s.at[i * HP:i * HP + hd, :], q_sem.at[i]) for i, f in enumerate(order)]
    for cp in wq:
        cp.start()
    for cp in stage:
        cp.wait()
    keep = [pltpu.make_async_copy(wst.at[l], wg_hbm.at[l, p.me], wl_sem.at[l]) for l in range(L)]
    for cp in keep:
        cp.start()
    entered()
    rings = []
    for l in range(L):
        def view(b, ch, l=l):
            return wg_hbm.at[l, b, cuts[ch]:cuts[ch + 1], :]
        ring = Ring(p, view, w_recv.at[l], w_send.at[l], 2)
        rings.append(ring)
        for ch in range(2):
            ring.own(ch, wst.at[l, cuts[ch]:cuts[ch + 1], :])
    bias_cp.wait()
    _load_bias(bias_v, mask_ref, bt)
    for cp in wq:
        cp.wait()
    aw_cp.wait()
    ex = Exchange(p, o_s, o_hbm, o_send, o_recv)

    def service(e):
        per = 2 * L
        for l in range(L):
            for ch in range(2):
                @pl.when(lax.rem(e, per) == 2 * l + ch)
                def _():
                    rings[l].service(e // per + 1, ch)

    def step(k, _):
        slot = lax.rem(k, 2)

        @pl.when(k + 1 < S)
        def _():
            for cp in loads(k + 1, 1 - slot):
                cp.start()

        for cp in loads(k, slot):
            cp.wait()

        def x_rows(i, tile):
            rows = pl.ds(i * tile, tile)
            cn = _ln(cbuf[slot, rows, :].astype(F32))
            return _ada(xbuf[slot, rows, :].astype(F32), cn, asc_ref[0, 0:1, :], aw_s[...], ab_ref[0, 0:1, :])

        at = Attend(n_tp, hd, w_s, brow_ref[0:1, :], bt, k_s, qt_s, vt_s, gt_s, lg, o_s, x_rows)
        at.project()

        @pl.when(k >= 1)
        def _():
            ex.start(sample_of(k - 1), 1 - slot)
            service(2 * k - 2)
            service(2 * k - 1)

        @pl.when(k >= 2)
        def _():
            ex.sent(sample_of(k - 2), slot)

        at.attend(slot)
        return 0

    lax.fori_loop(0, S, step, 0)
    ex.start(sample_of(S - 1), (S - 1) % 2)
    lax.fori_loop(2 * S - 2, 2 * L * (p.nz // 2), lambda e, _: (service(e), 0)[1], 0)
    ex.sent(sample_of(S - 2), S % 2)
    ex.sent(sample_of(S - 1), (S - 1) % 2)

    def other(i, _):
        b = i * 2 + (1 - p.c)
        for ring in rings:
            for ch in range(2):
                ring.wait(b, ch)
        return 0

    lax.fori_loop(0, p.nz, other, 0)
    for l in range(L):
        rings[l].drain(wg_hbm.at[l, 0:n_tp - 1])
        keep[l].wait()
    ex.arrived()


def _block0(x, cond, pair_bias, mask_row, wq, brow, asc, aw, ab, wo, wup, wdn):
    S, T, D = x.shape
    C = cond.shape[-1]
    L, _, hd, _ = wq.shape
    hu = wdn.shape[1]
    n_tp = S * 2
    rows_w = hd + 3 * hu
    half = T // 2
    dma = pltpu.SemaphoreType.DMA
    return pl.pallas_call(
        functools.partial(_block0_kernel, (S, T, D, C, n_tp, hd, hu, L)),
        out_shape=(jax.ShapeDtypeStruct((n_tp, hd, half), BF16), jax.ShapeDtypeStruct((L, n_tp, rows_w, D), BF16)),
        in_specs=[ANY, ANY, ANY, VMEM, ANY, VMEM, VMEM, ANY, VMEM, ANY, ANY, ANY],
        out_specs=(ANY, ANY),
        scratch_shapes=[
            pltpu.VMEM((2, T, D), BF16), pltpu.VMEM((2, T, C), BF16), pltpu.VMEM((T, T), BF16), pltpu.VMEM((T, T), F32),
            pltpu.VMEM((4 * HP, D), BF16), pltpu.VMEM((C, 2 * D), BF16), pltpu.VMEM((T, 2 * HP), BF16), pltpu.VMEM((2 * HP, T), BF16),
            pltpu.VMEM((HP, T), BF16), pltpu.VMEM((hd, T), F32), pltpu.VMEM((2, T, QT), F32), pltpu.VMEM((2, hd, T), BF16),
            pltpu.VMEM((L, rows_w, D), BF16),
            dma((2,)), dma((2,)), dma, dma((4,)), dma, dma((4 * L,)), dma((L,)), dma((2, 2)), dma, dma((L,)), dma((L, n_tp, 2))],
        cost_estimate=pl.CostEstimate(flops=2 * S * T * (D * 4 * HP + 2 * T * 256 + 2 * C * D), bytes_accessed=S * T * (D + C) * 2, transcendentals=S * T * T),
        compiler_params=pltpu.CompilerParams(collective_id=0, has_side_effects=True, vmem_limit_bytes=60 << 20),
        name="block0",
    )(x, cond, pair_bias, mask_row, wq, brow, asc, aw, ab, wo, wup, wdn)


def _transition(dims, half_rows, gates, mod1, cn, o_v, act, wall, y_s, h_s, rows):
    D, n_tp, hd, hu = dims
    w_o = wall[:, 0:hd, :].reshape(n_tp * hd, D)
    o_t = o_v[:, :, rows].reshape(n_tp * hd, half_rows)
    t = _dot(o_t, w_o, 0, 0).astype(BF16).astype(F32)
    mid = (act[rows, :].astype(F32) + gates[:, :D] * t).astype(BF16).astype(F32)
    y_s[...] = mod1(mid)
    step = 4 * hu
    for j in range(n_tp * hu // step):
        dv = slice(4 * j, 4 * j + 4)
        u1 = _dot(y_s[...], wall[dv, hd:hd + hu, :].reshape(step, D), 1, 1)
        u2 = _dot(y_s[...], wall[dv, hd + hu:hd + 2 * hu, :].reshape(step, D), 1, 1)
        h_s[:, j * step:(j + 1) * step] = (u1 * _sig(u1) * u2).astype(BF16)
    r = _dot(h_s[...], wall[:, hd + 2 * hu:hd + 3 * hu, :].reshape(n_tp * hu, D)).astype(BF16).astype(F32)
    return (mid + gates[:, D:] * r).astype(BF16)


def _block1_kernel(dims, o0_hbm, act_hbm, cond_hbm, wg_hbm, zw_ref, zb_ref, asc_ref, aw_hbm, ab_ref, bias_hbm, mask_ref, wq_hbm, brow_ref,
                   a_out, o_hbm,
                   o_v, act, cond, wall, aw_s, y_s, h_s, xg, bias_v, bt, w_s, k_s, qt_s, vt_s, gt_s, lg, o_s,
                   l_sem, q_sem, x_send, x_recv, o_send, o_recv):
    S, T, D, C, n_tp, hd, hu = dims
    p = Place(n_tp)
    entered = p.enter(True)
    R = S * T // n_tp
    row0 = p.me * R
    srcs = [(cond_hbm.at[pl.ds(row0, R), :], cond), (o0_hbm, o_v), (act_hbm.at[pl.ds(row0, R), :], act), (wg_hbm.at[0], wall),
            (aw_hbm.at[0, 1], aw_s.at[0]), (aw_hbm.at[1, 0], aw_s.at[1]), (bias_hbm.at[1, 0], bias_v)]
    cps = [pltpu.make_async_copy(a, b, l_sem.at[i]) for i, (a, b) in enumerate(srcs)]
    for cp in cps:
        cp.start()
    w_s[...] = jnp.zeros_like(w_s)
    qt_s[HP:, :] = jnp.zeros((HP, T), BF16)
    order = (1, 0, 2, 3)
    wq = [pltpu.make_async_copy(wq_hbm.at[1, f], w_s.at[i * HP:i * HP + hd, :], q_sem.at[i]) for i, f in enumerate(order)]
    for cp in wq:
        cp.start()
    for i in (0, 4, 5, 1, 2, 3):
        cps[i].wait()

    def view(b, ch):
        return xg.at[pl.ds(b * R + ch * (R // 2), R // 2), :]

    ring = Ring(p, view, x_recv, x_send, 2)
    tile = R // 2
    for ch in range(2):
        rows = pl.ds(ch * tile, tile)
        cb = cond[rows, :]
        cn = _ln(cb.astype(F32))
        gates = _sig(_dot(cb, zw_ref[0]) + zb_ref[0:1, :])
        mod1 = lambda mid: _ada(mid, cn, asc_ref[0, 1:2, :], aw_s[0], ab_ref[0, 1:2, :])
        new = _transition((D, n_tp, hd, hu), tile, gates, mod1, cn, o_v, act, wall, y_s, h_s, rows)
        a_out[rows, :] = new
        xg[pl.ds(row0 + ch * tile, tile), :] = _ada(new.astype(F32), cn, asc_ref[1, 0:1, :], aw_s[1], ab_ref[1, 0:1, :])
        if ch == 0:
            entered()
        ring.own(ch)
    cps[6].wait()
    _load_bias(bias_v, mask_ref, bt)
    for cp in wq:
        cp.wait()
    ex = Exchange(p, o_s, o_hbm, o_send, o_recv)
    turn = 1 - 2 * p.c

    def sample_of(j):
        h = (j + 1) // 2
        return lax.rem(p.z + S + turn * (1 - 2 * lax.rem(j, 2)) * h, S)

    def step(j, _):
        slot = lax.rem(j, 2)
        ring.service(j // 2 + 1, lax.rem(j, 2))

        @pl.when(j >= 1)
        def _():
            ex.start(sample_of(j - 1), 1 - slot)

        s = sample_of(j)
        for ch in range(2):
            ring.wait(s * 2 + (1 - p.c), ch)

        def x_rows(i, t):
            return xg[pl.ds(pl.multiple_of(s * T, T) + i * t, t), :]

        at = Attend(n_tp, hd, w_s, brow_ref[1:2, :], bt, k_s, qt_s, vt_s, gt_s, lg, o_s, x_rows)
        at.project()

        @pl.when(j >= 2)
        def _():
            ex.sent(sample_of(j - 2), slot)

        at.attend(slot)
        return 0

    lax.fori_loop(0, S, step, 0)
    ex.start(sample_of(S - 1), (S - 1) % 2)
    ex.sent(sample_of(S - 2), S % 2)
    ex.sent(sample_of(S - 1), (S - 1) % 2)
    ring.drain(xg.at[0:(n_tp - 1) * R, :])
    ex.arrived()


def _block1(o0, act, cond, wg, zw, zb, asc, aw, ab, pair_bias, mask_row, wq, brow):
    n_tp, hd, R = o0.shape
    D = act.shape[-1]
    C = cond.shape[-1]
    S = n_tp // 2
    T = 2 * R
    hu = (wg.shape[2] - hd) // 3
    dma = pltpu.SemaphoreType.DMA
    return pl.pallas_call(
        functools.partial(_block1_kernel, (S, T, D, C, n_tp, hd, hu)),
        out_shape=(jax.ShapeDtypeStruct((R, D), BF16), jax.ShapeDtypeStruct((n_tp, hd, R), BF16)),
        in_specs=[ANY, ANY, ANY, ANY, VMEM, VMEM, VMEM, ANY, VMEM, ANY, VMEM, ANY, VMEM],
        out_specs=(VMEM, ANY),
        scratch_shapes=[
            pltpu.VMEM((n_tp, hd, R), BF16), pltpu.VMEM((R, D), BF16), pltpu.VMEM((R, C), BF16), pltpu.VMEM(wg.shape[1:], BF16),
            pltpu.VMEM((2, C, 2 * D), BF16), pltpu.VMEM((R // 2, D), BF16), pltpu.VMEM((R // 2, n_tp * hu), BF16),
            pltpu.VMEM((S * T, D), BF16), pltpu.VMEM((T, T), BF16), pltpu.VMEM((T, T), F32),
            pltpu.VMEM((4 * HP, D), BF16), pltpu.VMEM((T, 2 * HP), BF16), pltpu.VMEM((2 * HP, T), BF16),
            pltpu.VMEM((HP, T), BF16), pltpu.VMEM((hd, T), F32), pltpu.VMEM((2, T, QT), F32), pltpu.VMEM((2, hd, T), BF16),
            dma((7,)), dma((4,)), dma, dma((n_tp, 2)), dma((2, 2)), dma],
        cost_estimate=pl.CostEstimate(flops=2 * S * T * (D * 4 * HP + 2 * T * 256), bytes_accessed=S * T * D * 2, transcendentals=S * T * T),
        compiler_params=pltpu.CompilerParams(collective_id=1, has_side_effects=True, vmem_limit_bytes=62 << 20),
        name="block1",
    )(o0, act, cond, wg, zw, zb, asc, aw, ab, pair_bias, mask_row, wq, brow)


def _last_kernel(dims, o_hbm, act_hbm, cond_hbm, wg_hbm, zw_ref, zb_ref, asc_ref, aw_hbm, ab_ref, out_hbm,
                 o_v, act, cond, wall, aw_s, y_s, h_s, new_s, l_sem, c_sem, x_send, x_recv):
    D, C, n_tp, hd, hu, R = dims
    p = Place(n_tp)
    entered = p.enter(False)
    row0 = p.me * R
    srcs = [(cond_hbm.at[pl.ds(row0, R), :], cond), (o_hbm, o_v), (act_hbm, act), (wg_hbm.at[1], wall), (aw_hbm.at[1, 1], aw_s)]
    cps = [pltpu.make_async_copy(a, b, l_sem.at[i]) for i, (a, b) in enumerate(srcs)]
    for cp in cps:
        cp.start()
    for i in (0, 4, 1, 2, 3):
        cps[i].wait()
    tile = R // 2

    def view(b, ch):
        return out_hbm.at[pl.ds(b * R + ch * tile, tile), :]

    ring = Ring(p, view, x_recv, x_send, 2)
    keep = []
    for ch in range(2):
        rows = pl.ds(ch * tile, tile)
        cb = cond[rows, :]
        cn = _ln(cb.astype(F32))
        gates = _sig(_dot(cb, zw_ref[1]) + zb_ref[1:2, :])
        mod1 = lambda mid: _ada(mid, cn, asc_ref[1, 1:2, :], aw_s[...], ab_ref[1, 1:2, :])
        new_s[rows, :] = _transition((D, n_tp, hd, hu), tile, gates, mod1, cn, o_v, act, wall, y_s, h_s, rows)
        if ch == 0:
            entered()
        ring.own(ch, new_s.at[ch * tile:(ch + 1) * tile, :])
        keep.append(pltpu.make_async_copy(new_s.at[ch * tile:(ch + 1) * tile, :], view(p.me, ch), c_sem.at[ch]))
        keep[-1].start()

    lax.fori_loop(0, p.nz, lambda e, _: (ring.service(e // 2 + 1, lax.rem(e, 2)), 0)[1], 0)

    def other(i, _):
        for ch in range(2):
            ring.wait(i * 2 + (1 - p.c), ch)
        return 0

    lax.fori_loop(0, p.nz, other, 0)
    ring.drain(out_hbm.at[0:(n_tp - 1) * R, :])
    for cp in keep:
        cp.wait()


def _last(o, act, cond, wg, zw, zb, asc, aw, ab):
    n_tp, hd, R = o.shape
    D = act.shape[-1]
    C = cond.shape[-1]
    hu = (wg.shape[2] - hd) // 3
    dma = pltpu.SemaphoreType.DMA
    return pl.pallas_call(
        functools.partial(_last_kernel, (D, C, n_tp, hd, hu, R)),
        out_shape=jax.ShapeDtypeStruct((n_tp * R, D), BF16),
        in_specs=[ANY, ANY, ANY, ANY, VMEM, VMEM, VMEM, ANY, VMEM],
        out_specs=ANY,
        scratch_shapes=[
            pltpu.VMEM((n_tp, hd, R), BF16), pltpu.VMEM((R, D), BF16), pltpu.VMEM((R, C), BF16), pltpu.VMEM(wg.shape[1:], BF16),
            pltpu.VMEM((C, 2 * D), BF16), pltpu.VMEM((R // 2, D), BF16), pltpu.VMEM((R // 2, n_tp * hu), BF16), pltpu.VMEM((R, D), BF16),
            dma((5,)), dma((2,)), dma, dma((n_tp, 2))],
        cost_estimate=pl.CostEstimate(flops=2 * R * D * (D + 3 * n_tp * hu + 4 * C), bytes_accessed=wg.size, transcendentals=R * D),
        compiler_params=pltpu.CompilerParams(collective_id=2, has_side_effects=True, vmem_limit_bytes=60 << 20),
        name="last",
    )(o, act, cond, wg, zw, zb, asc, aw, ab)


def solution(mesh):
    def shard_body(token_act, token_cond, pair_bias, token_mask, ada_scale, ada_w, ada_bias, zero_w, zero_b, w_qkvg, b_q, w_o, w_up, w_down):
        S, T, D = token_act.shape
        C = token_cond.shape[-1]
        hd = w_qkvg.shape[-1]
        L = pair_bias.shape[0]
        mask_row = token_mask.reshape(1, T)
        wq = jnp.transpose(w_qkvg, (0, 2, 3, 1))
        wup = jnp.transpose(w_up, (0, 2, 3, 1))
        brow = jnp.pad(b_q, ((0, 0), (HP, 3 * HP - hd)))
        aw = ada_w.reshape(L, 2, C, 2 * D)
        zw = zero_w.reshape(L, C, 2 * D)
        zb = zero_b.reshape(L, 2 * D)
        act = token_act.reshape(S * T, D)
        cond = token_cond.reshape(S * T, C)
        o0, wg = _block0(token_act, token_cond, pair_bias, mask_row, wq, brow, ada_scale, aw, ada_bias, w_o, wup, w_down)
        a1, o1 = _block1(o0, act, cond, wg, zw, zb, ada_scale, aw, ada_bias, pair_bias, mask_row, wq, brow)
        out = _last(o1, a1, cond, wg, zw, zb, ada_scale, aw, ada_bias)
        return out.reshape(S, T, D)

    everywhere = P()
    in_specs = (P('dp', None, None), P('dp', None, None), P(None, 'tp', None, None), P(None), everywhere, everywhere, everywhere, everywhere, everywhere, P(None, None, None, 'tp'), P(None, 'tp'), P(None, 'tp', None), P(None, None, None, 'tp'), P(None, 'tp', None))
    return jax.shard_map(shard_body, mesh=mesh, in_specs=in_specs, out_specs=P('dp', None, None), check_vma=False)
```

```python
import functools
import math

import jax
import jax.numpy as jnp
from jax import lax
from jax.experimental import pallas as pl
from jax.experimental.pallas import tpu as pltpu
from jax.sharding import PartitionSpec as P

LN_EPS = 1e-5
LOG2E = 1.4426950408889634
MESH = pl.DeviceIdType.MESH
BF16 = jnp.bfloat16
F32 = jnp.float32
HP = 64
QT = 256
ANY = pl.BlockSpec(memory_space=pl.ANY)
VMEM = pl.BlockSpec(memory_space=pltpu.VMEM)
VM0, VM1, VM2 = 40 << 20, 40 << 20, 8 << 20


def _ln(x):
    mean = jnp.mean(x, axis=-1, keepdims=True)
    cen = x - mean
    var = jnp.mean(cen * cen, axis=-1, keepdims=True)
    return cen * lax.rsqrt(var + LN_EPS)


def _sig(x):
    return 0.5 * jnp.tanh(0.5 * x) + 0.5


def _dot(a, b, ca=1, cb=0):
    return lax.dot_general(a, b, (((ca,), (cb,)), ((), ())), preferred_element_type=F32)


def _ada(x_f32, cond_normed, scale, w, bias):
    d = x_f32.shape[-1]
    mod = _dot((cond_normed * scale).astype(BF16), w)
    return (_sig(mod[:, :d] + bias) * _ln(x_f32) + mod[:, d:]).astype(BF16)


class Place:
    def __init__(self, n_tp, n_dp):
        self.n = n_tp
        self.n_dp = n_dp
        self.col = lax.axis_index("dp")
        self.nz = n_tp // 2
        self.me = lax.axis_index("tp")
        self.z = self.me // 2
        self.c = lax.rem(self.me, 2)
        self.partner = self.z * 2 + (1 - self.c)

    def at(self, off):
        return lax.rem(self.z + off + self.nz, self.nz) * 2 + self.c

    def column(self, i):
        return lax.rem(self.col + i, self.n_dp)

    def enter(self, everyone):
        barrier = pltpu.get_barrier_semaphore()
        if everyone:
            peers = [{"tp": lax.rem(self.me + i, self.n)} for i in range(1, self.n)]
            peers += [{"dp": self.column(i), "tp": self.me} for i in range(1, self.n_dp)]
        else:
            peers = [{"tp": t} for t in (self.at(1), self.at(-1), self.partner)]
        for peer in peers:
            pl.semaphore_signal(barrier, inc=1, device_id=peer, device_id_type=MESH)
        return lambda: pl.semaphore_wait(barrier, len(peers))


class Ring:
    def __init__(self, place, view, recv_sem, send_sem, n_chunk):
        self.p, self.view, self.recv, self.send, self.n_chunk = place, view, recv_sem, send_sem, n_chunk
        self.far = place.nz // 2

    def _push(self, b, ch, dst, src=None):
        v = self.view(b, ch)
        pltpu.make_async_remote_copy(
            src_ref=v if src is None else src, dst_ref=v, send_sem=self.send, recv_sem=self.recv.at[b, ch],
            device_id={"tp": dst}, device_id_type=MESH).start()

    def own(self, ch, src=None):
        p = self.p
        self._push(p.me, ch, p.at(1), src)
        self._push(p.me, ch, p.at(-1), src)
        self._push(p.me, ch, p.partner, src)

    def wait(self, b, ch):
        v = self.view(b, ch)
        pltpu.make_async_copy(v, v, self.recv.at[b, ch]).wait()

    def service(self, h, ch):
        p = self.p
        for sign, core in ((1, 0), (-1, 1)):
            b = p.at(-sign * h)

            @pl.when((h < self.far) | (p.c == core))
            def _():
                self.wait(b, ch)

                @pl.when((h < self.far - 1) | ((h == self.far - 1) & (p.c == core)))
                def _():
                    self._push(b, ch, p.at(sign))

                self._push(b, ch, p.partner)

    def drain(self, whole):
        pltpu.make_async_copy(whole, whole, self.send).wait()


class Cross:
    def __init__(self, place, buf, lo, hi, recv_sem, near_sem, far_sem):
        self.p, self.buf, self.lo, self.hi = place, buf, lo, hi
        self.recv, self.near, self.far_sem = recv_sem, near_sem, far_sem
        self.far = place.nz // 2

    def _view(self, b):
        return self.buf.at[b, self.lo:self.hi, :]

    def _push(self, b, dst, sem, src=None):
        v = self._view(b)
        pltpu.make_async_remote_copy(
            src_ref=v if src is None else src, dst_ref=v, send_sem=sem, recv_sem=self.recv.at[b],
            device_id=dst, device_id_type=MESH).start()

    def _mine(self, b):
        return lax.rem(b, self.p.n_dp) == self.p.col

    def own(self, src):
        p = self.p

        @pl.when(self._mine(p.me))
        def _():
            self._push(p.me, {"tp": p.at(1)}, self.far_sem.at[p.z], src)
            self._push(p.me, {"tp": p.at(-1)}, self.far_sem.at[p.z], src)

        self._push(p.me, {"tp": p.partner}, self.near, src)

    def wait(self, b):
        v = self._view(b)
        pltpu.make_async_copy(v, v, self.recv.at[b]).wait()

    def _each(self, h, body):
        p = self.p
        for sign, core in ((1, 0), (-1, 1)):
            b = p.at(-sign * h)

            @pl.when((h < self.far) | (p.c == core))
            def _():
                body(b, sign, (h < self.far - 1) | ((h == self.far - 1) & (p.c == core)))

    def along(self, h):
        p = self.p

        def body(b, sign, onward):
            @pl.when(self._mine(b))
            def _():
                self.wait(b)

                @pl.when(onward)
                def _():
                    self._push(b, {"tp": p.at(sign)}, self.far_sem.at[b // 2])

                for i in range(1, p.n_dp):
                    self._push(b, {"dp": p.column(i), "tp": p.me}, self.far_sem.at[b // 2])
                self._push(b, {"tp": p.partner}, self.near)

        self._each(h, body)

    def across(self, h):
        p = self.p

        def body(b, sign, onward):
            @pl.when(jnp.logical_not(self._mine(b)))
            def _():
                self.wait(b)
                self._push(b, {"tp": p.partner}, self.near)

        self._each(h, body)

    def finish(self):
        p = self.p

        def blocks(k, sem):
            v = self.buf.at[0:k, self.lo:self.hi, :]
            pltpu.make_async_copy(v, v, sem).wait()

        def other(i, _):
            self.wait(i * 2 + (1 - p.c))
            return 0

        lax.fori_loop(0, p.nz, other, 0)
        blocks(p.nz, self.near)

        @pl.when(self._mine(p.me))
        def _():
            blocks(2, self.far_sem.at[p.z])

        def body(b, sign, onward):
            @pl.when(self._mine(b))
            def _():
                @pl.when(onward)
                def _():
                    blocks(p.n_dp, self.far_sem.at[b // 2])

                if p.n_dp > 1:
                    @pl.when(jnp.logical_not(onward))
                    def _():
                        blocks(p.n_dp - 1, self.far_sem.at[b // 2])

        def hop(h, _):
            self._each(h, body)
            return 0

        lax.fori_loop(1, self.far + 1, hop, 0)


class Attend:
    def __init__(self, n_tp, hd, w, brow, bt, k_s, qt_s, vt_s, gt_s, lg, o_s, x_rows):
        self.__dict__.update(locals())
        self.T = bt.shape[0]

    def project(self):
        T, hd = self.T, self.hd
        tile = QT
        for i in range(T // tile):
            rows = pl.ds(i * tile, tile)
            res = _dot(self.x_rows(i, tile), self.w[...], 1, 1) + self.brow
            self.k_s[rows, :] = res[:, :2 * HP].astype(BF16)
            rest = res.T
            self.qt_s[0:HP, rows] = rest[HP:2 * HP].astype(BF16)
            ones = lax.broadcasted_iota(jnp.int32, (HP, tile), 0) == hd
            self.vt_s[:, rows] = jnp.where(ones, 1.0, rest[2 * HP:3 * HP]).astype(BF16)
            self.gt_s[:, rows] = _sig(rest[3 * HP:3 * HP + hd])

    def attend(self, slot):
        T, hd = self.T, self.hd
        n = T // QT
        c1 = LOG2E / math.sqrt(hd)

        def scores(i):
            cols = pl.ds(i * QT, QT)
            logits = _dot(self.k_s[...], self.qt_s[:, cols]) * c1 + self.bt[:, cols]
            self.lg[i % 2] = logits
            return jnp.max(logits, axis=0, keepdims=True)

        top = scores(0)
        for i in range(n):
            cols = pl.ds(i * QT, QT)
            nxt = scores(i + 1) if i + 1 < n else None
            probs = jnp.exp2(self.lg[i % 2] - top).astype(BF16)
            mixed = _dot(self.vt_s[...], probs)
            self.o_s[slot, :, cols] = (self.gt_s[:, cols] * (mixed[:hd] / mixed[hd:hd + 1])).astype(BF16)
            top = nxt


def _load_bias(bias_v, mask_ref, bt):
    T = bt.shape[0]
    mask_add = (mask_ref[...].astype(F32) - 1.0) * 1e9

    def step(i, _):
        r = pl.multiple_of(i * 128, 128)
        rows = (bias_v[pl.ds(r, 128), :].astype(F32) + mask_add) * LOG2E
        bt[:, pl.ds(r, 128)] = rows.T
        return 0

    lax.fori_loop(0, T // 128, step, 0)


class Exchange:
    def __init__(self, place, o_s, o_hbm, send_sem, recv_sem):
        self.p, self.o_s, self.o_hbm, self.send, self.recv = place, o_s, o_hbm, send_sem, recv_sem
        self.half = o_s.shape[-1] // 2

    def _each(self, sample, slot, remote, local):
        p = self.p
        for c in range(2):
            dst = sample * 2 + c
            src = self.o_s.at[slot, :, pl.ds(c * self.half, self.half)]
            cp = pltpu.make_async_remote_copy(
                src_ref=src, dst_ref=self.o_hbm.at[p.me], send_sem=self.send.at[slot, c], recv_sem=self.recv,
                device_id={"tp": dst}, device_id_type=MESH)

            @pl.when(dst != p.me)
            def _():
                remote(cp)

            @pl.when(dst == p.me)
            def _():
                local(pltpu.make_async_copy(src, self.o_hbm.at[p.me], self.send.at[slot, c]))

    def start(self, sample, slot):
        self._each(sample, slot, lambda cp: cp.start(), lambda cp: cp.start())

    def sent(self, sample, slot):
        self._each(sample, slot, lambda cp: cp.wait_send(), lambda cp: cp.wait())

    def arrived(self):
        rest = self.o_hbm.at[0:self.p.n - 1]
        pltpu.make_async_copy(rest, rest, self.recv).wait()


def _bias_row(bq, hd):
    return jnp.concatenate([jnp.zeros((1, HP), F32), bq, jnp.zeros((1, 3 * HP - hd), F32)], axis=1)


def _flat(raw):
    c, two, d = raw.shape
    return raw[...].reshape(c, two * d)


def _block0_kernel(dims, x_hbm, cond_hbm, bias_hbm, mask_ref, wq_hbm, bq_ref, asc_ref, aw_hbm, ab_ref, zw_hbm, zb_ref, wo_hbm, wup_hbm, wdn_hbm,
                   o_out, wg, gate_out, mod_out, nxt_out,
                   xbuf, cbuf, bias_v, bt, w_s, raw, aw_s, k_s, qt_s, vt_s, gt_s, lg, o_s, wst, cond,
                   ld_sem, cd_sem, b_sem, q_sem, a_sem, st_sem, o_send, o_recv, w_send, w_recv, c_near, c_far, c_recv):
    S, T, D, C, n_tp, n_dp, hd, hu = dims
    p = Place(n_tp, n_dp)
    entered = p.enter(True)
    rows_w = hd + 3 * hu
    cut = hd + hu
    stage = []
    for src, lo, hi in ((wo_hbm.at[0], 0, hd), (wup_hbm.at[0, 0], hd, cut), (wup_hbm.at[0, 1], cut, hd + 2 * hu),
                        (wdn_hbm.at[0], hd + 2 * hu, rows_w)):
        stage.append(pltpu.make_async_copy(src, wst.at[lo:hi, :], st_sem.at[len(stage)]))
    for cp in stage:
        cp.start()
    sign = 1 - 2 * p.c
    R = S * T // n_tp

    def sample_of(k):
        return lax.rem(p.z + S + sign * (k + 1), S)

    def loads(k, slot):
        s = sample_of(k)
        return [pltpu.make_async_copy(x_hbm.at[s], xbuf.at[slot], ld_sem.at[slot]),
                pltpu.make_async_copy(cond_hbm.at[s], cbuf.at[slot], cd_sem.at[slot])]

    raws = [pltpu.make_async_copy(aw_hbm.at[0, 0], raw.at[0], a_sem.at[0]), pltpu.make_async_copy(zw_hbm.at[0], raw.at[1], a_sem.at[1]),
            pltpu.make_async_copy(aw_hbm.at[0, 1], raw.at[2], a_sem.at[2]), pltpu.make_async_copy(aw_hbm.at[1, 0], raw.at[0], a_sem.at[0])]
    bias_cp = pltpu.make_async_copy(bias_hbm.at[0, 0], bias_v, b_sem)
    bias_cp.start()
    raws[0].start()
    for cp in loads(0, 0):
        cp.start()
    w_s[...] = jnp.zeros_like(w_s)
    qt_s[HP:, :] = jnp.zeros((HP, T), BF16)
    order = (1, 0, 2, 3)
    wq = [pltpu.make_async_copy(wq_hbm.at[0, f], w_s.at[i * HP:i * HP + hd, :], q_sem.at[i]) for i, f in enumerate(order)]
    for cp in wq:
        cp.start()
    for cp in stage:
        cp.wait()
    for cp in wq:
        cp.wait()
    for r in (1, 2):
        raws[r].start()
    cond_cp = pltpu.make_async_copy(cond_hbm.at[p.z, pl.ds(p.c * R, R), :], cond, b_sem)
    entered()
    ring = Ring(p, lambda b, ch: wg.at[b, 0:cut, :], w_recv, w_send, 1)
    cross = Cross(p, wg, cut, rows_w, c_recv, c_near, c_far)
    ring.own(0, wst.at[0:cut, :])
    cross.own(wst.at[cut:rows_w, :])
    bias_cp.wait()
    _load_bias(bias_v, mask_ref, bt)
    cond_cp.start()
    raws[0].wait()
    aw_s[...] = _flat(raw.at[0])
    ex = Exchange(p, o_s, o_out, o_send, o_recv)
    brow = _bias_row(bq_ref[0:1, :], hd)

    def step(k, _):
        slot = lax.rem(k, 2)

        @pl.when(k + 1 < S)
        def _():
            for cp in loads(k + 1, 1 - slot):
                cp.start()

        for cp in loads(k, slot):
            cp.wait()

        def x_rows(i, tile):
            rows = pl.ds(i * tile, tile)
            cn = _ln(cbuf[slot, rows, :].astype(F32))
            return _ada(xbuf[slot, rows, :].astype(F32), cn, asc_ref[0, 0:1, :], aw_s[...], ab_ref[0, 0:1, :])

        at = Attend(n_tp, hd, w_s, brow, bt, k_s, qt_s, vt_s, gt_s, lg, o_s, x_rows)
        at.project()

        @pl.when(k >= 1)
        def _():
            ex.start(sample_of(k - 1), 1 - slot)

        @pl.when((k >= 1) & (k <= p.nz // 2))
        def _():
            ring.service(k, 0)
            cross.along(k)

        @pl.when((k >= 3) & (k <= p.nz // 2 + 2))
        def _():
            cross.across(k - 2)

        @pl.when(k >= 2)
        def _():
            ex.sent(sample_of(k - 2), slot)

        at.attend(slot)
        return 0

    lax.fori_loop(0, S, step, 0)
    ex.start(sample_of(S - 1), (S - 1) % 2)
    raws[3].start()
    wg[p.me] = wst[...]
    cond_cp.wait()
    cn = _ln(cond[...].astype(F32))
    raws[1].wait()
    aw_s[...] = _flat(raw.at[1])
    gate_out[...] = _dot(cond[...], aw_s[...])
    for half in range(2):
        cols = slice(half * D, (half + 1) * D)
        gate_out[:, cols] = _sig(gate_out[:, cols] + zb_ref[0, half:half + 1, :])
    for src, cp, l, j, out in ((2, raws[2], 0, 1, mod_out), (0, raws[3], 1, 0, nxt_out)):
        cp.wait()
        aw_s[...] = _flat(raw.at[src])
        out[...] = _dot((cn * asc_ref[l, j:j + 1, :]).astype(BF16), aw_s[...])
        out[:, :D] = _sig(out[:, :D] + ab_ref[l, j:j + 1, :])
    ex.sent(sample_of(S - 2), S % 2)
    ex.sent(sample_of(S - 1), (S - 1) % 2)

    def other(i, _):
        ring.wait(i * 2 + (1 - p.c), 0)
        return 0

    lax.fori_loop(0, p.nz, other, 0)
    ring.drain(wg.at[0:n_tp - 1, 0:cut, :])
    cross.finish()
    ex.arrived()


def _block0(n_dp, x, cond, pair_bias, mask_row, wq, bq, asc, aw, ab, zw, zb, wo, wup, wdn):
    S, T, D = x.shape
    C = cond.shape[-1]
    _, _, hd, _ = wq.shape
    hu = wdn.shape[1]
    n_tp = S * 2
    rows_w = hd + 3 * hu
    R = T // 2
    dma = pltpu.SemaphoreType.DMA
    return pl.pallas_call(
        functools.partial(_block0_kernel, (S, T, D, C, n_tp, n_dp, hd, hu)),
        out_shape=(pltpu.VMEM((n_tp, hd, R), BF16), pltpu.VMEM((n_tp, rows_w, D), BF16),
                   pltpu.VMEM((R, 2 * D), F32), pltpu.VMEM((R, 2 * D), F32), pltpu.VMEM((R, 2 * D), F32)),
        in_specs=[ANY, ANY, ANY, VMEM, ANY, VMEM, VMEM, ANY, VMEM, ANY, VMEM, ANY, ANY, ANY],
        out_specs=(VMEM,) * 5,
        scratch_shapes=[
            pltpu.VMEM((2, T, D), BF16), pltpu.VMEM((2, T, C), BF16), pltpu.VMEM((T, T), BF16), pltpu.VMEM((T, T), F32),
            pltpu.VMEM((4 * HP, D), BF16), pltpu.VMEM((3, C, 2, D), BF16), pltpu.VMEM((C, 2 * D), BF16),
            pltpu.VMEM((T, 2 * HP), BF16), pltpu.VMEM((2 * HP, T), BF16),
            pltpu.VMEM((HP, T), BF16), pltpu.VMEM((hd, T), F32), pltpu.VMEM((2, T, QT), F32), pltpu.VMEM((2, hd, T), BF16),
            pltpu.VMEM((rows_w, D), BF16), pltpu.VMEM((R, C), BF16),
            dma((2,)), dma((2,)), dma, dma((4,)), dma((3,)), dma((4,)), dma((2, 2)), dma, dma, dma((n_tp, 1)),
            dma, dma((S,)), dma((n_tp,))],
        cost_estimate=pl.CostEstimate(flops=2 * S * T * (D * 4 * HP + 2 * T * 256 + 2 * C * D), bytes_accessed=S * T * (D + C) * 2, transcendentals=S * T * T),
        compiler_params=pltpu.CompilerParams(collective_id=0, has_side_effects=True, vmem_limit_bytes=VM0),
        name="block0",
    )(x, cond, pair_bias, mask_row, wq, bq, asc, aw, ab, zw, zb, wo, wup, wdn)


def _transition(dims, tile, gates, mod1, o_v, act, wall, y_s, h_s, rows):
    D, n_tp, hd, hu = dims
    w_o = wall[:, 0:hd, :].reshape(n_tp * hd, D)
    o_t = o_v[:, :, rows].reshape(n_tp * hd, tile)
    t = _dot(o_t, w_o, 0, 0).astype(BF16).astype(F32)
    mid = (act[rows, :].astype(F32) + gates[rows, :D] * t).astype(BF16).astype(F32)
    y_s[...] = (mod1[rows, :D] * _ln(mid) + mod1[rows, D:]).astype(BF16)
    step = 4 * hu
    for j in range(n_tp * hu // step):
        dv = slice(4 * j, 4 * j + 4)
        u1 = _dot(y_s[...], wall[dv, hd:hd + hu, :].reshape(step, D), 1, 1)
        u2 = _dot(y_s[...], wall[dv, hd + hu:hd + 2 * hu, :].reshape(step, D), 1, 1)
        h_s[:, j * step:(j + 1) * step] = (u1 * _sig(u1) * u2).astype(BF16)
    r = _dot(h_s[...], wall[:, hd + 2 * hu:hd + 3 * hu, :].reshape(n_tp * hu, D)).astype(BF16).astype(F32)
    return (mid + gates[rows, D:] * r).astype(BF16)


def _block1_kernel(dims, o0, w0, gate0, mod0, nxt0, act_hbm, cond_hbm, zw_hbm, zb_ref, asc_ref, aw_hbm, ab_ref, bias_hbm, mask_ref, wq_hbm, bq_ref,
                   wo_hbm, wup_hbm, wdn_hbm,
                   w1, gate1, mod1, a_out, o_out, wg,
                   act, cond, raw, aw_s, y_s, h_s, xg, bias_v, bt, w_s, k_s, qt_s, vt_s, gt_s, lg, o_s, wst,
                   l_sem, q_sem, st_sem, wl_sem, x_send, x_recv, o_send, o_recv, c_near, c_far, c_recv):
    S, T, D, C, n_tp, n_dp, hd, hu = dims
    p = Place(n_tp, n_dp)
    entered = p.enter(True)
    R = S * T // n_tp
    row0 = p.me * R
    rows_w = hd + 3 * hu
    stage = []
    for src, lo, hi in ((wo_hbm.at[1], 0, hd), (wup_hbm.at[1, 0], hd, hd + hu), (wup_hbm.at[1, 1], hd + hu, hd + 2 * hu),
                        (wdn_hbm.at[1], hd + 2 * hu, rows_w)):
        stage.append(pltpu.make_async_copy(src, wst.at[lo:hi, :], st_sem.at[len(stage)]))
    for cp in stage:
        cp.start()
    srcs = [(act_hbm.at[pl.ds(row0, R), :], act), (cond_hbm.at[pl.ds(row0, R), :], cond), (bias_hbm.at[1, 0], bias_v),
            (zw_hbm.at[1], raw.at[0]), (aw_hbm.at[1, 1], raw.at[1])]
    cps = [pltpu.make_async_copy(a, b, l_sem.at[i]) for i, (a, b) in enumerate(srcs)]
    for cp in cps:
        cp.start()
    w_s[...] = jnp.zeros_like(w_s)
    qt_s[HP:, :] = jnp.zeros((HP, T), BF16)
    order = (1, 0, 2, 3)
    wq = [pltpu.make_async_copy(wq_hbm.at[1, f], w_s.at[i * HP:i * HP + hd, :], q_sem.at[i]) for i, f in enumerate(order)]
    for cp in wq:
        cp.start()
    for cp in stage:
        cp.wait()
    cross = Cross(p, wg, 0, rows_w, c_recv, c_near, c_far)
    keep = pltpu.make_async_copy(wst, wg.at[p.me], wl_sem)
    keep.start()
    entered()
    cross.own(wst)
    cps[0].wait()
    tile = R // 2
    ring = Ring(p, lambda b, ch: xg.at[pl.ds(b * R + ch * tile, tile), :], x_recv, x_send, 2)
    for ch in range(2):
        rows = pl.ds(ch * tile, tile)
        new = _transition((D, n_tp, hd, hu), tile, gate0, mod0, o0, act, w0, y_s, h_s, rows)
        a_out[rows, :] = new
        xg[pl.ds(row0 + ch * tile, tile), :] = (nxt0[rows, :D] * _ln(new.astype(F32)) + nxt0[rows, D:]).astype(BF16)
        ring.own(ch)
        cross.along(ch + 1)
    cps[2].wait()
    _load_bias(bias_v, mask_ref, bt)
    for cp in wq:
        cp.wait()
    ex = Exchange(p, o_s, o_out, o_send, o_recv)
    brow = _bias_row(bq_ref[1:2, :], hd)
    turn = 1 - 2 * p.c

    def sample_of(j):
        h = (j + 1) // 2
        return lax.rem(p.z + S + turn * (1 - 2 * lax.rem(j, 2)) * h, S)

    def step(j, _):
        slot = lax.rem(j, 2)
        ring.service(j // 2 + 1, lax.rem(j, 2))

        @pl.when(j <= p.nz // 2 - 3)
        def _():
            cross.along(j + 3)

        @pl.when((j >= 1) & (j <= p.nz // 2))
        def _():
            cross.across(j)

        @pl.when(j >= 1)
        def _():
            ex.start(sample_of(j - 1), 1 - slot)

        s = sample_of(j)
        for ch in range(2):
            ring.wait(s * 2 + (1 - p.c), ch)

        def x_rows(i, t):
            return xg[pl.ds(pl.multiple_of(s * T, T) + i * t, t), :]

        at = Attend(n_tp, hd, w_s, brow, bt, k_s, qt_s, vt_s, gt_s, lg, o_s, x_rows)
        at.project()

        @pl.when(j >= 2)
        def _():
            ex.sent(sample_of(j - 2), slot)

        at.attend(slot)

        @pl.when(j == 1)
        def _():
            cps[1].wait()
            cps[3].wait()
            aw_s[...] = _flat(raw.at[0])
            gate1[...] = _dot(cond[...], aw_s[...])
            for half in range(2):
                cols = slice(half * D, (half + 1) * D)
                gate1[:, cols] = _sig(gate1[:, cols] + zb_ref[1, half:half + 1, :])

        @pl.when(j == 3)
        def _():
            cps[4].wait()
            aw_s[...] = _flat(raw.at[1])
            cn = _ln(cond[...].astype(F32))
            mod1[...] = _dot((cn * asc_ref[1, 1:2, :]).astype(BF16), aw_s[...])
            mod1[:, :D] = _sig(mod1[:, :D] + ab_ref[1, 1:2, :])

        @pl.when(j == S - 2)
        def _():
            cross.finish()
            keep.wait()
            pltpu.make_async_copy(wg, w1, wl_sem).start()

        return 0

    lax.fori_loop(0, S, step, 0)
    ex.start(sample_of(S - 1), (S - 1) % 2)
    pltpu.make_async_copy(wg, w1, wl_sem).wait()
    ex.sent(sample_of(S - 2), S % 2)
    ex.sent(sample_of(S - 1), (S - 1) % 2)
    ring.drain(xg.at[0:(n_tp - 1) * R, :])
    ex.arrived()


def _block1(n_dp, o0, w0, gate0, mod0, nxt0, act, cond, zw, zb, asc, aw, ab, pair_bias, mask_row, wq, bq, wo, wup, wdn):
    n_tp, hd, R = o0.shape
    D = act.shape[-1]
    C = cond.shape[-1]
    S = n_tp // 2
    T = 2 * R
    hu = wdn.shape[1]
    rows_w = hd + 3 * hu
    dma = pltpu.SemaphoreType.DMA
    return pl.pallas_call(
        functools.partial(_block1_kernel, (S, T, D, C, n_tp, n_dp, hd, hu)),
        out_shape=(pltpu.VMEM((n_tp, rows_w, D), BF16), pltpu.VMEM((R, 2 * D), F32), pltpu.VMEM((R, 2 * D), F32),
                   pltpu.VMEM((R, D), BF16), pltpu.VMEM((n_tp, hd, R), BF16), pltpu.HBM((n_tp, rows_w, D), BF16)),
        in_specs=[VMEM, VMEM, VMEM, VMEM, VMEM, ANY, ANY, ANY, VMEM, VMEM, ANY, VMEM, ANY, VMEM, ANY, VMEM, ANY, ANY, ANY],
        out_specs=(VMEM, VMEM, VMEM, VMEM, VMEM, pl.BlockSpec(memory_space=pltpu.HBM)),
        input_output_aliases={1: 0, 2: 1, 3: 2},
        scratch_shapes=[
            pltpu.VMEM((R, D), BF16), pltpu.VMEM((R, C), BF16), pltpu.VMEM((2, C, 2, D), BF16), pltpu.VMEM((C, 2 * D), BF16),
            pltpu.VMEM((R // 2, D), BF16), pltpu.VMEM((R // 2, n_tp * hu), BF16),
            pltpu.VMEM((S * T, D), BF16), pltpu.VMEM((T, T), BF16), pltpu.VMEM((T, T), F32),
            pltpu.VMEM((4 * HP, D), BF16), pltpu.VMEM((T, 2 * HP), BF16), pltpu.VMEM((2 * HP, T), BF16),
            pltpu.VMEM((HP, T), BF16), pltpu.VMEM((hd, T), F32), pltpu.VMEM((2, T, QT), F32), pltpu.VMEM((2, hd, T), BF16),
            pltpu.VMEM((rows_w, D), BF16),
            dma((5,)), dma((4,)), dma((4,)), dma, dma, dma((n_tp, 2)), dma((2, 2)), dma, dma, dma((S,)), dma((n_tp,))],
        cost_estimate=pl.CostEstimate(flops=2 * S * T * (D * 4 * HP + 2 * T * 256), bytes_accessed=S * T * D * 2, transcendentals=S * T * T),
        compiler_params=pltpu.CompilerParams(collective_id=1, has_side_effects=True, vmem_limit_bytes=VM1),
        name="block1",
    )(o0, w0, gate0, mod0, nxt0, act, cond, zw, zb, asc, aw, ab, pair_bias, mask_row, wq, bq, wo, wup, wdn)


def _last_kernel(dims, o_v, act, wall, gate, mod, out, y_s, h_s, x_send, x_recv):
    D, n_tp, n_dp, hd, hu, R = dims
    p = Place(n_tp, n_dp)
    entered = p.enter(False)
    tile = R // 2
    ring = Ring(p, lambda b, ch: out.at[pl.ds(b * R + ch * tile, tile), :], x_recv, x_send, 2)
    for ch in range(2):
        rows = pl.ds(ch * tile, tile)
        out[pl.ds(p.me * R + ch * tile, tile), :] = _transition((D, n_tp, hd, hu), tile, gate, mod, o_v, act, wall, y_s, h_s, rows)
        if ch == 0:
            entered()
        ring.own(ch)

    lax.fori_loop(0, p.nz, lambda e, _: (ring.service(e // 2 + 1, lax.rem(e, 2)), 0)[1], 0)

    def other(i, _):
        for ch in range(2):
            ring.wait(i * 2 + (1 - p.c), ch)
        return 0

    lax.fori_loop(0, p.nz, other, 0)
    ring.drain(out.at[0:(n_tp - 1) * R, :])


def _last(n_dp, o, act, w1, gate, mod):
    n_tp, hd, R = o.shape
    D = act.shape[-1]
    hu = (w1.shape[1] - hd) // 3
    dma = pltpu.SemaphoreType.DMA
    return pl.pallas_call(
        functools.partial(_last_kernel, (D, n_tp, n_dp, hd, hu, R)),
        out_shape=pltpu.VMEM((n_tp * R, D), BF16),
        in_specs=[VMEM] * 5, out_specs=VMEM,
        scratch_shapes=[pltpu.VMEM((R // 2, D), BF16), pltpu.VMEM((R // 2, n_tp * hu), BF16), dma, dma((n_tp, 2))],
        cost_estimate=pl.CostEstimate(flops=2 * R * D * (D + 3 * n_tp * hu), bytes_accessed=w1.size, transcendentals=R * D),
        compiler_params=pltpu.CompilerParams(collective_id=2, has_side_effects=True, vmem_limit_bytes=VM2),
        name="last",
    )(o, act, w1, gate, mod)


def _store_kernel(src, dst, sem):
    cp = pltpu.make_async_copy(src, dst, sem)
    cp.start()
    cp.wait()


def _store(x):
    return pl.pallas_call(
        _store_kernel, out_shape=jax.ShapeDtypeStruct(x.shape, x.dtype), in_specs=[VMEM], out_specs=ANY,
        scratch_shapes=[pltpu.SemaphoreType.DMA], compiler_params=pltpu.CompilerParams(vmem_limit_bytes=1 << 20), name="store")(x)


def solution(mesh):
    n_dp = mesh.shape["dp"]

    def shard_body(token_act, token_cond, pair_bias, token_mask, ada_scale, ada_w, ada_bias, zero_w, zero_b, w_qkvg, b_q, w_o, w_up, w_down):
        S, T, D = token_act.shape
        C = token_cond.shape[-1]
        mask_row = token_mask.reshape(1, T)
        wq = jnp.transpose(w_qkvg, (0, 2, 3, 1))
        wup = jnp.transpose(w_up, (0, 2, 3, 1))
        act = token_act.reshape(S * T, D)
        cond = token_cond.reshape(S * T, C)
        o0, w0, gate0, mod0, nxt0 = _block0(n_dp, token_act, token_cond, pair_bias, mask_row, wq, b_q, ada_scale, ada_w, ada_bias, zero_w, zero_b, w_o, wup, w_down)
        o0, w0, gate0, mod0, nxt0 = (pltpu.with_memory_space_constraint(v, pltpu.VMEM) for v in (o0, w0, gate0, mod0, nxt0))
        w1, gate1, mod1, a1, o1, _ = _block1(n_dp, o0, w0, gate0, mod0, nxt0, act, cond, zero_w, zero_b, ada_scale, ada_w, ada_bias, pair_bias, mask_row, wq, b_q, w_o, wup, w_down)
        o1, a1, w1, gate1, mod1 = (pltpu.with_memory_space_constraint(v, pltpu.VMEM) for v in (o1, a1, w1, gate1, mod1))
        out = pltpu.with_memory_space_constraint(_last(n_dp, o1, a1, w1, gate1, mod1), pltpu.VMEM)
        return _store(out).reshape(S, T, D)

    everywhere = P()
    in_specs = (P('dp', None, None), P('dp', None, None), P(None, 'tp', None, None), P(None), everywhere, everywhere, everywhere, everywhere, everywhere, P(None, None, None, 'tp'), P(None, 'tp'), P(None, 'tp', None), P(None, None, None, 'tp'), P(None, 'tp', None))
    return jax.shard_map(shard_body, mesh=mesh, in_specs=in_specs, out_specs=P('dp', None, None), check_vma=False)
```

```python
import functools
import math

import jax
import jax.numpy as jnp
from jax import lax
from jax.experimental import pallas as pl
from jax.experimental.pallas import tpu as pltpu
from jax.sharding import PartitionSpec as P

LN_EPS = 1e-5
LOG2E = 1.4426950408889634
MESH = pl.DeviceIdType.MESH
BF16 = jnp.bfloat16
F32 = jnp.float32
HP = 64
QT = 256
ANY = pl.BlockSpec(memory_space=pl.ANY)
VMEM = pl.BlockSpec(memory_space=pltpu.VMEM)
VM0, VM1, VM2 = 40 << 20, 40 << 20, 8 << 20


def _ln(x):
    mean = jnp.mean(x, axis=-1, keepdims=True)
    cen = x - mean
    var = jnp.mean(cen * cen, axis=-1, keepdims=True)
    return cen * lax.rsqrt(var + LN_EPS)


def _sig(x):
    return 0.5 * jnp.tanh(0.5 * x) + 0.5


def _dot(a, b, ca=1, cb=0):
    return lax.dot_general(a, b, (((ca,), (cb,)), ((), ())), preferred_element_type=F32)


def _ada(x_f32, cond_normed, scale, w, bias):
    d = x_f32.shape[-1]
    mod = _dot((cond_normed * scale).astype(BF16), w)
    return (_sig(mod[:, :d] + bias) * _ln(x_f32) + mod[:, d:]).astype(BF16)


class Place:
    def __init__(self, n_tp, n_dp):
        self.n = n_tp
        self.n_dp = n_dp
        self.col = lax.axis_index("dp")
        self.nz = n_tp // 2
        self.me = lax.axis_index("tp")
        self.z = self.me // 2
        self.c = lax.rem(self.me, 2)
        self.partner = self.z * 2 + (1 - self.c)

    def at(self, off):
        return lax.rem(self.z + off + self.nz, self.nz) * 2 + self.c

    def column(self, i):
        return lax.rem(self.col + i, self.n_dp)

    def enter(self, everyone):
        barrier = pltpu.get_barrier_semaphore()
        if everyone:
            peers = [{"tp": lax.rem(self.me + i, self.n)} for i in range(1, self.n)]
            peers += [{"dp": self.column(i), "tp": self.me} for i in range(1, self.n_dp)]
        else:
            peers = [{"tp": t} for t in (self.at(1), self.at(-1), self.partner)]
        for peer in peers:
            pl.semaphore_signal(barrier, inc=1, device_id=peer, device_id_type=MESH)
        return lambda: pl.semaphore_wait(barrier, len(peers))


class Ring:
    def __init__(self, place, view, recv_sem, send_sem, n_chunk):
        self.p, self.view, self.recv, self.send, self.n_chunk = place, view, recv_sem, send_sem, n_chunk
        self.far = place.nz // 2

    def _push(self, b, ch, dst, src=None):
        v = self.view(b, ch)
        pltpu.make_async_remote_copy(
            src_ref=v if src is None else src, dst_ref=v, send_sem=self.send, recv_sem=self.recv.at[b, ch],
            device_id={"tp": dst}, device_id_type=MESH).start()

    def own(self, ch, src=None):
        p = self.p
        self._push(p.me, ch, p.at(1), src)
        self._push(p.me, ch, p.at(-1), src)
        self._push(p.me, ch, p.partner, src)

    def wait(self, b, ch):
        v = self.view(b, ch)
        pltpu.make_async_copy(v, v, self.recv.at[b, ch]).wait()

    def service(self, h, ch):
        p = self.p
        for sign, core in ((1, 0), (-1, 1)):
            b = p.at(-sign * h)

            @pl.when((h < self.far) | (p.c == core))
            def _():
                self.wait(b, ch)

                @pl.when((h < self.far - 1) | ((h == self.far - 1) & (p.c == core)))
                def _():
                    self._push(b, ch, p.at(sign))

                self._push(b, ch, p.partner)

    def drain(self, whole):
        pltpu.make_async_copy(whole, whole, self.send).wait()


class Cross:
    def __init__(self, place, buf, lo, hi, n_chunk, recv_sem, near_sem, far_sem):
        self.p, self.buf, self.lo, self.hi, self.n_chunk = place, buf, lo, hi, n_chunk
        self.recv, self.near, self.far_sem = recv_sem, near_sem, far_sem
        self.far = place.nz // 2
        self.size = (hi - lo) // n_chunk

    def _view(self, b, ch):
        return self.buf.at[b, self.lo + ch * self.size:self.lo + (ch + 1) * self.size, :]

    def _push(self, b, ch, dst, sem, src=None):
        v = self._view(b, ch)
        pltpu.make_async_remote_copy(
            src_ref=v if src is None else src, dst_ref=v, send_sem=sem, recv_sem=self.recv.at[b, ch],
            device_id=dst, device_id_type=MESH).start()

    def _mine(self, b):
        return lax.rem(b, self.p.n_dp) == self.p.col

    def own(self, src):
        p = self.p
        for ch in range(self.n_chunk):
            part = src.at[self.lo + ch * self.size:self.lo + (ch + 1) * self.size, :]

            @pl.when(self._mine(p.me))
            def _():
                self._push(p.me, ch, {"tp": p.at(1)}, self.far_sem.at[p.z], part)
                self._push(p.me, ch, {"tp": p.at(-1)}, self.far_sem.at[p.z], part)

            self._push(p.me, ch, {"tp": p.partner}, self.near, part)

    def wait(self, b, ch):
        v = self._view(b, ch)
        pltpu.make_async_copy(v, v, self.recv.at[b, ch]).wait()

    def _each(self, h, body):
        p = self.p
        for sign, core in ((1, 0), (-1, 1)):
            b = p.at(-sign * h)

            @pl.when((h < self.far) | (p.c == core))
            def _():
                body(b, sign, (h < self.far - 1) | ((h == self.far - 1) & (p.c == core)))

    def along(self, h, ch):
        p = self.p

        def body(b, sign, onward):
            @pl.when(self._mine(b))
            def _():
                self.wait(b, ch)

                @pl.when(onward)
                def _():
                    self._push(b, ch, {"tp": p.at(sign)}, self.far_sem.at[b // 2])

                for i in range(1, p.n_dp):
                    self._push(b, ch, {"dp": p.column(i), "tp": p.me}, self.far_sem.at[b // 2])
                self._push(b, ch, {"tp": p.partner}, self.near)

        self._each(h, body)

    def across(self, h, ch):
        p = self.p

        def body(b, sign, onward):
            @pl.when(jnp.logical_not(self._mine(b)))
            def _():
                self.wait(b, ch)
                self._push(b, ch, {"tp": p.partner}, self.near)

        self._each(h, body)

    def finish(self):
        p = self.p

        def blocks(k, sem):
            v = self.buf.at[0:k, self.lo:self.hi, :]
            pltpu.make_async_copy(v, v, sem).wait()

        def other(i, _):
            for ch in range(self.n_chunk):
                self.wait(i * 2 + (1 - p.c), ch)
            return 0

        lax.fori_loop(0, p.nz, other, 0)
        blocks(p.nz, self.near)

        @pl.when(self._mine(p.me))
        def _():
            blocks(2, self.far_sem.at[p.z])

        def body(b, sign, onward):
            @pl.when(self._mine(b))
            def _():
                @pl.when(onward)
                def _():
                    blocks(p.n_dp, self.far_sem.at[b // 2])

                if p.n_dp > 1:
                    @pl.when(jnp.logical_not(onward))
                    def _():
                        blocks(p.n_dp - 1, self.far_sem.at[b // 2])

        def hop(h, _):
            self._each(h, body)
            return 0

        lax.fori_loop(1, self.far + 1, hop, 0)


class Attend:
    def __init__(self, n_tp, hd, w, brow, bt, k_s, qt_s, vt_s, gt_s, lg, o_s, x_rows):
        self.__dict__.update(locals())
        self.T = bt.shape[0]

    def project(self):
        T, hd = self.T, self.hd
        tile = QT
        for i in range(T // tile):
            rows = pl.ds(i * tile, tile)
            res = _dot(self.x_rows(i, tile), self.w[...], 1, 1) + self.brow
            self.k_s[rows, :] = res[:, :2 * HP].astype(BF16)
            rest = res.T
            self.qt_s[0:HP, rows] = rest[HP:2 * HP].astype(BF16)
            ones = lax.broadcasted_iota(jnp.int32, (HP, tile), 0) == hd
            self.vt_s[:, rows] = jnp.where(ones, 1.0, rest[2 * HP:3 * HP]).astype(BF16)
            self.gt_s[:, rows] = _sig(rest[3 * HP:3 * HP + hd])

    def attend(self, slot, hook=None):
        T, hd = self.T, self.hd
        n = T // QT
        c1 = LOG2E / math.sqrt(hd)

        def scores(i):
            cols = pl.ds(i * QT, QT)
            logits = _dot(self.k_s[...], self.qt_s[:, cols]) * c1 + self.bt[:, cols]
            self.lg[i % 2] = logits
            return jnp.max(logits, axis=0, keepdims=True)

        top = scores(0)
        if hook is not None:
            hook()
        for i in range(n):
            cols = pl.ds(i * QT, QT)
            nxt = scores(i + 1) if i + 1 < n else None
            probs = jnp.exp2(self.lg[i % 2] - top).astype(BF16)
            mixed = _dot(self.vt_s[...], probs)
            self.o_s[slot, :, cols] = (self.gt_s[:, cols] * (mixed[:hd] / mixed[hd:hd + 1])).astype(BF16)
            top = nxt


def _load_bias(bias_v, mask_ref, bt):
    T = bt.shape[0]
    mask_add = (mask_ref[...].astype(F32) - 1.0) * 1e9

    def step(i, _):
        r = pl.multiple_of(i * 128, 128)
        rows = (bias_v[pl.ds(r, 128), :].astype(F32) + mask_add) * LOG2E
        bt[:, pl.ds(r, 128)] = rows.T
        return 0

    lax.fori_loop(0, T // 128, step, 0)


class Exchange:
    def __init__(self, place, o_s, o_hbm, send_sem, recv_sem):
        self.p, self.o_s, self.o_hbm, self.send, self.recv = place, o_s, o_hbm, send_sem, recv_sem
        self.half = o_s.shape[-1] // 2

    def _each(self, sample, slot, remote, local):
        p = self.p
        for c in range(2):
            dst = sample * 2 + c
            src = self.o_s.at[slot, :, pl.ds(c * self.half, self.half)]
            cp = pltpu.make_async_remote_copy(
                src_ref=src, dst_ref=self.o_hbm.at[p.me], send_sem=self.send.at[slot, c], recv_sem=self.recv,
                device_id={"tp": dst}, device_id_type=MESH)

            @pl.when(dst != p.me)
            def _():
                remote(cp)

            @pl.when(dst == p.me)
            def _():
                local(pltpu.make_async_copy(src, self.o_hbm.at[p.me], self.send.at[slot, c]))

    def start(self, sample, slot):
        self._each(sample, slot, lambda cp: cp.start(), lambda cp: cp.start())

    def sent(self, sample, slot):
        self._each(sample, slot, lambda cp: cp.wait_send(), lambda cp: cp.wait())

    def arrived(self):
        rest = self.o_hbm.at[0:self.p.n - 1]
        pltpu.make_async_copy(rest, rest, self.recv).wait()


def _bias_row(bq, hd):
    return jnp.concatenate([jnp.zeros((1, HP), F32), bq, jnp.zeros((1, 3 * HP - hd), F32)], axis=1)


def _flat(raw):
    c, two, d = raw.shape
    return raw[...].reshape(c, two * d)


def _block0_kernel(dims, x_hbm, cond_hbm, bias_hbm, mask_ref, wq_hbm, bq_ref, asc_ref, aw_hbm, ab_ref, zw_hbm, zb_ref, wo_hbm, wup_hbm, wdn_hbm,
                   o_out, wg, gate_out, mod_out, nxt_out,
                   xraw, craw, xn, bias_v, bt, w_s, raw, aw_s, k_s, qt_s, vt_s, gt_s, lg, o_s, wst, cond,
                   ld_sem, cd_sem, b_sem, q_sem, a_sem, st_sem, o_send, o_recv, n_send, n_recv, n_free, w_send, w_recv, c_near, c_far, c_recv):
    S, T, D, C, n_tp, n_dp, hd, hu, cut, n_chunk = dims
    p = Place(n_tp, n_dp)
    entered = p.enter(True)
    rows_w = hd + 3 * hu
    stage = []
    for src, lo, hi in ((wo_hbm.at[0], 0, hd), (wup_hbm.at[0, 0], hd, hd + hu), (wup_hbm.at[0, 1], hd + hu, hd + 2 * hu),
                        (wdn_hbm.at[0], hd + 2 * hu, rows_w)):
        stage.append(pltpu.make_async_copy(src, wst.at[lo:hi, :], st_sem.at[len(stage)]))
    for cp in stage:
        cp.start()
    R = S * T // n_tp
    mine = pl.ds(p.c * R, R)

    def sample_of(k):
        j = S - 1 - k
        return lax.rem(p.z + S + (1 - 2 * lax.rem(j, 2)) * ((j + 1) // 2), S)

    def loads(k, slot):
        s = sample_of(k)
        return [pltpu.make_async_copy(x_hbm.at[s, mine], xraw.at[slot], ld_sem.at[slot]),
                pltpu.make_async_copy(cond_hbm.at[s, mine], craw.at[slot], cd_sem.at[slot])]

    raws = [pltpu.make_async_copy(aw_hbm.at[0, 0], raw.at[0], a_sem.at[0]), pltpu.make_async_copy(zw_hbm.at[0], raw.at[1], a_sem.at[1]),
            pltpu.make_async_copy(aw_hbm.at[0, 1], raw.at[2], a_sem.at[2]), pltpu.make_async_copy(aw_hbm.at[1, 0], raw.at[0], a_sem.at[0])]
    raws[0].start()
    for k in range(2):
        for cp in loads(k, k):
            cp.start()
    bias_cp = pltpu.make_async_copy(bias_hbm.at[0, 0], bias_v, b_sem)
    bias_cp.start()
    w_s[...] = jnp.zeros_like(w_s)
    qt_s[HP:, :] = jnp.zeros((HP, T), BF16)
    order = (1, 0, 2, 3)
    wq = [pltpu.make_async_copy(wq_hbm.at[0, f], w_s.at[i * HP:i * HP + hd, :], q_sem.at[i]) for i, f in enumerate(order)]
    for cp in wq:
        cp.start()
    for cp in stage:
        cp.wait()
    for cp in wq:
        cp.wait()
    for r in (1, 2):
        raws[r].start()
    cond_cp = pltpu.make_async_copy(cond_hbm.at[p.z, mine], cond, b_sem)
    entered()
    ring = Ring(p, lambda b, ch: wg.at[b, 0:cut, :], w_recv, w_send, 1)
    cross = Cross(p, wg, cut, rows_w, n_chunk, c_recv, c_near, c_far)
    ring.own(0, wst.at[0:cut, :])
    cross.own(wst)

    def half(slot, dst):
        v = xn.at[slot, mine]
        return pltpu.make_async_remote_copy(src_ref=v, dst_ref=v, send_sem=n_send.at[slot], recv_sem=n_recv.at[slot],
                                            device_id={"tp": p.partner}, device_id_type=MESH)

    def normalise(slot):
        tile = 256 if R % 256 == 0 else R
        for i in range(R // tile):
            rows = pl.ds(i * tile, tile)
            cn = _ln(craw[slot, rows, :].astype(F32))
            y = _ada(xraw[slot, rows, :].astype(F32), cn, asc_ref[0, 0:1, :], aw_s[...], ab_ref[0, 0:1, :])
            xn[slot, pl.ds(pl.multiple_of(p.c * R, R) + i * tile, tile), :] = y

    raws[0].wait()
    aw_s[...] = _flat(raw.at[0])
    for cp in loads(0, 0):
        cp.wait()
    normalise(0)
    bias_cp.wait()
    half(0, p.partner).start()
    _load_bias(bias_v, mask_ref, bt)
    cond_cp.start()
    ex = Exchange(p, o_s, o_out, o_send, o_recv)
    brow = _bias_row(bq_ref[0:1, :], hd)

    def step(k, _):
        slot = lax.rem(k, 2)

        @pl.when(k + 2 < S)
        def _():
            for cp in loads(k + 2, slot):
                cp.start()

        v = xn.at[slot, pl.ds((1 - p.c) * R, R)]
        pltpu.make_async_copy(v, v, n_recv.at[slot]).wait()
        half(slot, p.partner).wait_send()
        at = Attend(n_tp, hd, w_s, brow, bt, k_s, qt_s, vt_s, gt_s, lg, o_s, lambda i, tile: xn[slot, pl.ds(i * tile, tile), :])
        at.project()

        @pl.when(k + 2 < S)
        def _():
            pl.semaphore_signal(n_free, inc=1, device_id={"tp": p.partner}, device_id_type=MESH)

        @pl.when(k >= 1)
        def _():
            ex.start(sample_of(k - 1), 1 - slot)

        @pl.when(k + 1 < S)
        def _():
            for cp in loads(k + 1, 1 - slot):
                cp.wait()
            normalise(1 - slot)

            @pl.when(k >= 1)
            def _():
                pl.semaphore_wait(n_free, 1)

        def at_step(when, *events):
            @pl.when(k == when)
            def _():
                for f, *args in events:
                    f(*args)

        chunks = range(n_chunk)
        at_step(1, (ring.service, 1, 0))
        at_step(2, *((cross.along, 1, ch) for ch in chunks))
        at_step(3, (ring.service, 2, 0))
        at_step(4, *((cross.along, 2, ch) for ch in chunks), *((cross.across, 1, ch) for ch in chunks))
        at_step(5, (ring.service, 3, 0))
        at_step(6, *((cross.along, 3, ch) for ch in chunks), *((cross.across, 2, ch) for ch in chunks))
        at_step(7, (ring.service, 4, 0), *((cross.along, 4, ch) for ch in chunks))

        @pl.when(k >= 2)
        def _():
            ex.sent(sample_of(k - 2), slot)

        def hook():
            @pl.when(k + 1 < S)
            def _():
                half(1 - slot, p.partner).start()

        at.attend(slot, hook)
        return 0

    lax.fori_loop(0, S, step, 0)
    ex.start(sample_of(S - 1), (S - 1) % 2)
    raws[3].start()
    for ch in range(n_chunk):
        cross.across(3, ch)
    wg[p.me] = wst[...]
    cond_cp.wait()
    cn = _ln(cond[...].astype(F32))
    raws[1].wait()
    aw_s[...] = _flat(raw.at[1])
    gate_out[...] = _dot(cond[...], aw_s[...])
    for half_d in range(2):
        cols = slice(half_d * D, (half_d + 1) * D)
        gate_out[:, cols] = _sig(gate_out[:, cols] + zb_ref[0, half_d:half_d + 1, :])
    for src, cp, l, j, out in ((2, raws[2], 0, 1, mod_out), (0, raws[3], 1, 0, nxt_out)):
        cp.wait()
        aw_s[...] = _flat(raw.at[src])
        out[...] = _dot((cn * asc_ref[l, j:j + 1, :]).astype(BF16), aw_s[...])
        out[:, :D] = _sig(out[:, :D] + ab_ref[l, j:j + 1, :])
    for ch in range(n_chunk):
        cross.across(4, ch)
    ex.sent(sample_of(S - 2), S % 2)
    ex.sent(sample_of(S - 1), (S - 1) % 2)

    def other(i, _):
        ring.wait(i * 2 + (1 - p.c), 0)
        return 0

    lax.fori_loop(0, p.nz, other, 0)
    ring.drain(wg.at[0:n_tp - 1, 0:cut, :])
    cross.finish()
    ex.arrived()


def _block0(n_dp, x, cond, pair_bias, mask_row, wq, bq, asc, aw, ab, zw, zb, wo, wup, wdn):
    S, T, D = x.shape
    C = cond.shape[-1]
    _, _, hd, _ = wq.shape
    hu = wdn.shape[1]
    n_tp = S * 2
    rows_w = hd + 3 * hu
    R = T // 2
    cut, n_chunk = hd + hu, 2
    dma = pltpu.SemaphoreType.DMA
    return pl.pallas_call(
        functools.partial(_block0_kernel, (S, T, D, C, n_tp, n_dp, hd, hu, cut, n_chunk)),
        out_shape=(pltpu.VMEM((n_tp, hd, R), BF16), pltpu.VMEM((n_tp, rows_w, D), BF16),
                   pltpu.VMEM((R, 2 * D), F32), pltpu.VMEM((R, 2 * D), F32), pltpu.VMEM((R, 2 * D), F32)),
        in_specs=[ANY, ANY, ANY, VMEM, ANY, VMEM, VMEM, ANY, VMEM, ANY, VMEM, ANY, ANY, ANY],
        out_specs=(VMEM,) * 5,
        scratch_shapes=[
            pltpu.VMEM((2, R, D), BF16), pltpu.VMEM((2, R, C), BF16), pltpu.VMEM((2, T, D), BF16), pltpu.VMEM((T, T), BF16), pltpu.VMEM((T, T), F32),
            pltpu.VMEM((4 * HP, D), BF16), pltpu.VMEM((3, C, 2, D), BF16), pltpu.VMEM((C, 2 * D), BF16),
            pltpu.VMEM((T, 2 * HP), BF16), pltpu.VMEM((2 * HP, T), BF16),
            pltpu.VMEM((HP, T), BF16), pltpu.VMEM((hd, T), F32), pltpu.VMEM((2, T, QT), F32), pltpu.VMEM((2, hd, T), BF16),
            pltpu.VMEM((rows_w, D), BF16), pltpu.VMEM((R, C), BF16),
            dma((2,)), dma((2,)), dma, dma((4,)), dma((3,)), dma((4,)), dma((2, 2)), dma, dma((2,)), dma((2,)), pltpu.SemaphoreType.REGULAR,
            dma, dma((n_tp, 1)), dma, dma((S,)), dma((n_tp, n_chunk))],
        cost_estimate=pl.CostEstimate(flops=2 * S * T * (D * 4 * HP + 2 * T * 256 + C * D), bytes_accessed=S * T * (D + C), transcendentals=S * T * T),
        compiler_params=pltpu.CompilerParams(collective_id=0, has_side_effects=True, vmem_limit_bytes=VM0),
        name="block0",
    )(x, cond, pair_bias, mask_row, wq, bq, asc, aw, ab, zw, zb, wo, wup, wdn)


def _transition(dims, tile, gates, mod1, o_v, act, wall, y_s, h_s, rows):
    D, n_tp, hd, hu = dims
    w_o = wall[:, 0:hd, :].reshape(n_tp * hd, D)
    o_t = o_v[:, :, rows].reshape(n_tp * hd, tile)
    t = _dot(o_t, w_o, 0, 0).astype(BF16).astype(F32)
    mid = (act[rows, :].astype(F32) + gates[rows, :D] * t).astype(BF16).astype(F32)
    y_s[...] = (mod1[rows, :D] * _ln(mid) + mod1[rows, D:]).astype(BF16)
    step = 4 * hu
    for j in range(n_tp * hu // step):
        dv = slice(4 * j, 4 * j + 4)
        u1 = _dot(y_s[...], wall[dv, hd:hd + hu, :].reshape(step, D), 1, 1)
        u2 = _dot(y_s[...], wall[dv, hd + hu:hd + 2 * hu, :].reshape(step, D), 1, 1)
        h_s[:, j * step:(j + 1) * step] = (u1 * _sig(u1) * u2).astype(BF16)
    r = _dot(h_s[...], wall[:, hd + 2 * hu:hd + 3 * hu, :].reshape(n_tp * hu, D)).astype(BF16).astype(F32)
    return (mid + gates[rows, D:] * r).astype(BF16)


def _block1_kernel(dims, o0, w0, gate0, mod0, nxt0, act_hbm, cond_hbm, zw_hbm, zb_ref, asc_ref, aw_hbm, ab_ref, bias_hbm, mask_ref, wq_hbm, bq_ref,
                   wo_hbm, wup_hbm, wdn_hbm,
                   w1, gate1, mod1, a_out, o_out, wg,
                   act, cond, raw, aw_s, y_s, h_s, xg, bias_v, bt, w_s, k_s, qt_s, vt_s, gt_s, lg, o_s, wst,
                   l_sem, q_sem, st_sem, wl_sem, x_send, x_recv, o_send, o_recv, c_near, c_far, c_recv):
    S, T, D, C, n_tp, n_dp, hd, hu = dims
    p = Place(n_tp, n_dp)
    entered = p.enter(True)
    R = S * T // n_tp
    row0 = p.me * R
    rows_w = hd + 3 * hu
    stage = []
    for src, lo, hi in ((wo_hbm.at[1], 0, hd), (wup_hbm.at[1, 0], hd, hd + hu), (wup_hbm.at[1, 1], hd + hu, hd + 2 * hu),
                        (wdn_hbm.at[1], hd + 2 * hu, rows_w)):
        stage.append(pltpu.make_async_copy(src, wst.at[lo:hi, :], st_sem.at[len(stage)]))
    for cp in stage:
        cp.start()
    srcs = [(act_hbm.at[pl.ds(row0, R), :], act), (cond_hbm.at[pl.ds(row0, R), :], cond), (bias_hbm.at[1, 0], bias_v),
            (zw_hbm.at[1], raw.at[0]), (aw_hbm.at[1, 1], raw.at[1])]
    cps = [pltpu.make_async_copy(a, b, l_sem.at[i]) for i, (a, b) in enumerate(srcs)]
    for cp in cps:
        cp.start()
    w_s[...] = jnp.zeros_like(w_s)
    qt_s[HP:, :] = jnp.zeros((HP, T), BF16)
    order = (1, 0, 2, 3)
    wq = [pltpu.make_async_copy(wq_hbm.at[1, f], w_s.at[i * HP:i * HP + hd, :], q_sem.at[i]) for i, f in enumerate(order)]
    for cp in wq:
        cp.start()
    for cp in stage:
        cp.wait()
    n_chunk = 3
    cross = Cross(p, wg, 0, rows_w, n_chunk, c_recv, c_near, c_far)
    keep = pltpu.make_async_copy(wst, wg.at[p.me], wl_sem)
    keep.start()
    entered()
    cross.own(wst)
    cps[0].wait()
    tile = R // 2
    ring = Ring(p, lambda b, ch: xg.at[pl.ds(b * R + ch * tile, tile), :], x_recv, x_send, 2)
    for ch in range(2):
        rows = pl.ds(ch * tile, tile)
        new = _transition((D, n_tp, hd, hu), tile, gate0, mod0, o0, act, w0, y_s, h_s, rows)
        a_out[rows, :] = new
        xg[pl.ds(row0 + ch * tile, tile), :] = (nxt0[rows, :D] * _ln(new.astype(F32)) + nxt0[rows, D:]).astype(BF16)
        ring.own(ch)
        for i in range(n_chunk):
            cross.along(ch + 1, i)
    cps[2].wait()
    _load_bias(bias_v, mask_ref, bt)
    for cp in wq:
        cp.wait()
    ex = Exchange(p, o_s, o_out, o_send, o_recv)
    brow = _bias_row(bq_ref[1:2, :], hd)
    turn = 1 - 2 * p.c

    def sample_of(j):
        h = (j + 1) // 2
        return lax.rem(p.z + S + turn * (1 - 2 * lax.rem(j, 2)) * h, S)

    def step(j, _):
        slot = lax.rem(j, 2)
        ring.service(j // 2 + 1, lax.rem(j, 2))

        @pl.when(j <= p.nz // 2 - 3)
        def _():
            for i in range(n_chunk):
                cross.along(j + 3, i)

        @pl.when((j >= 1) & (j <= p.nz // 2))
        def _():
            for i in range(n_chunk):
                cross.across(j, i)

        @pl.when(j >= 1)
        def _():
            ex.start(sample_of(j - 1), 1 - slot)

        s = sample_of(j)
        for ch in range(2):
            ring.wait(s * 2 + (1 - p.c), ch)

        def x_rows(i, t):
            return xg[pl.ds(pl.multiple_of(s * T, T) + i * t, t), :]

        at = Attend(n_tp, hd, w_s, brow, bt, k_s, qt_s, vt_s, gt_s, lg, o_s, x_rows)
        at.project()

        @pl.when(j >= 2)
        def _():
            ex.sent(sample_of(j - 2), slot)

        at.attend(slot)

        @pl.when(j == 1)
        def _():
            cps[1].wait()
            cps[3].wait()
            aw_s[...] = _flat(raw.at[0])
            gate1[...] = _dot(cond[...], aw_s[...])
            for half in range(2):
                cols = slice(half * D, (half + 1) * D)
                gate1[:, cols] = _sig(gate1[:, cols] + zb_ref[1, half:half + 1, :])

        @pl.when(j == 3)
        def _():
            cps[4].wait()
            aw_s[...] = _flat(raw.at[1])
            cn = _ln(cond[...].astype(F32))
            mod1[...] = _dot((cn * asc_ref[1, 1:2, :]).astype(BF16), aw_s[...])
            mod1[:, :D] = _sig(mod1[:, :D] + ab_ref[1, 1:2, :])

        @pl.when(j == S - 2)
        def _():
            cross.finish()
            keep.wait()
            pltpu.make_async_copy(wg, w1, wl_sem).start()

        return 0

    lax.fori_loop(0, S, step, 0)
    ex.start(sample_of(S - 1), (S - 1) % 2)
    pltpu.make_async_copy(wg, w1, wl_sem).wait()
    ex.sent(sample_of(S - 2), S % 2)
    ex.sent(sample_of(S - 1), (S - 1) % 2)
    ring.drain(xg.at[0:(n_tp - 1) * R, :])
    ex.arrived()


def _block1(n_dp, o0, w0, gate0, mod0, nxt0, act, cond, zw, zb, asc, aw, ab, pair_bias, mask_row, wq, bq, wo, wup, wdn):
    n_tp, hd, R = o0.shape
    D = act.shape[-1]
    C = cond.shape[-1]
    S = n_tp // 2
    T = 2 * R
    hu = wdn.shape[1]
    rows_w = hd + 3 * hu
    dma = pltpu.SemaphoreType.DMA
    return pl.pallas_call(
        functools.partial(_block1_kernel, (S, T, D, C, n_tp, n_dp, hd, hu)),
        out_shape=(pltpu.VMEM((n_tp, rows_w, D), BF16), pltpu.VMEM((R, 2 * D), F32), pltpu.VMEM((R, 2 * D), F32),
                   pltpu.VMEM((R, D), BF16), pltpu.VMEM((n_tp, hd, R), BF16), pltpu.HBM((n_tp, rows_w, D), BF16)),
        in_specs=[VMEM, VMEM, VMEM, VMEM, VMEM, ANY, ANY, ANY, VMEM, VMEM, ANY, VMEM, ANY, VMEM, ANY, VMEM, ANY, ANY, ANY],
        out_specs=(VMEM, VMEM, VMEM, VMEM, VMEM, pl.BlockSpec(memory_space=pltpu.HBM)),
        input_output_aliases={1: 0, 2: 1, 3: 2},
        scratch_shapes=[
            pltpu.VMEM((R, D), BF16), pltpu.VMEM((R, C), BF16), pltpu.VMEM((2, C, 2, D), BF16), pltpu.VMEM((C, 2 * D), BF16),
            pltpu.VMEM((R // 2, D), BF16), pltpu.VMEM((R // 2, n_tp * hu), BF16),
            pltpu.VMEM((S * T, D), BF16), pltpu.VMEM((T, T), BF16), pltpu.VMEM((T, T), F32),
            pltpu.VMEM((4 * HP, D), BF16), pltpu.VMEM((T, 2 * HP), BF16), pltpu.VMEM((2 * HP, T), BF16),
            pltpu.VMEM((HP, T), BF16), pltpu.VMEM((hd, T), F32), pltpu.VMEM((2, T, QT), F32), pltpu.VMEM((2, hd, T), BF16),
            pltpu.VMEM((rows_w, D), BF16),
            dma((5,)), dma((4,)), dma((4,)), dma, dma, dma((n_tp, 2)), dma((2, 2)), dma, dma, dma((S,)), dma((n_tp, 3))],
        cost_estimate=pl.CostEstimate(flops=2 * S * T * (D * 4 * HP + 2 * T * 256), bytes_accessed=S * T * D * 2, transcendentals=S * T * T),
        compiler_params=pltpu.CompilerParams(collective_id=1, has_side_effects=True, vmem_limit_bytes=VM1),
        name="block1",
    )(o0, w0, gate0, mod0, nxt0, act, cond, zw, zb, asc, aw, ab, pair_bias, mask_row, wq, bq, wo, wup, wdn)


def _last_kernel(dims, o_v, act, wall, gate, mod, out, y_s, h_s, x_send, x_recv):
    D, n_tp, n_dp, hd, hu, R = dims
    p = Place(n_tp, n_dp)
    entered = p.enter(False)
    tile = R // 2
    ring = Ring(p, lambda b, ch: out.at[pl.ds(b * R + ch * tile, tile), :], x_recv, x_send, 2)
    for ch in range(2):
        rows = pl.ds(ch * tile, tile)
        out[pl.ds(p.me * R + ch * tile, tile), :] = _transition((D, n_tp, hd, hu), tile, gate, mod, o_v, act, wall, y_s, h_s, rows)
        if ch == 0:
            entered()
        ring.own(ch)

    lax.fori_loop(0, p.nz, lambda e, _: (ring.service(e // 2 + 1, lax.rem(e, 2)), 0)[1], 0)

    def other(i, _):
        for ch in range(2):
            ring.wait(i * 2 + (1 - p.c), ch)
        return 0

    lax.fori_loop(0, p.nz, other, 0)
    ring.drain(out.at[0:(n_tp - 1) * R, :])


def _last(n_dp, o, act, w1, gate, mod):
    n_tp, hd, R = o.shape
    D = act.shape[-1]
    hu = (w1.shape[1] - hd) // 3
    dma = pltpu.SemaphoreType.DMA
    return pl.pallas_call(
        functools.partial(_last_kernel, (D, n_tp, n_dp, hd, hu, R)),
        out_shape=pltpu.VMEM((n_tp * R, D), BF16),
        in_specs=[VMEM] * 5, out_specs=VMEM,
        scratch_shapes=[pltpu.VMEM((R // 2, D), BF16), pltpu.VMEM((R // 2, n_tp * hu), BF16), dma, dma((n_tp, 2))],
        cost_estimate=pl.CostEstimate(flops=2 * R * D * (D + 3 * n_tp * hu), bytes_accessed=w1.size, transcendentals=R * D),
        compiler_params=pltpu.CompilerParams(collective_id=2, has_side_effects=True, vmem_limit_bytes=VM2),
        name="last",
    )(o, act, w1, gate, mod)


def _store_kernel(src, dst, sem):
    cp = pltpu.make_async_copy(src, dst, sem)
    cp.start()
    cp.wait()


def _store(x):
    return pl.pallas_call(
        _store_kernel, out_shape=jax.ShapeDtypeStruct(x.shape, x.dtype), in_specs=[VMEM], out_specs=ANY,
        scratch_shapes=[pltpu.SemaphoreType.DMA], compiler_params=pltpu.CompilerParams(vmem_limit_bytes=1 << 20), name="store")(x)


def solution(mesh):
    n_dp = mesh.shape["dp"]

    def shard_body(token_act, token_cond, pair_bias, token_mask, ada_scale, ada_w, ada_bias, zero_w, zero_b, w_qkvg, b_q, w_o, w_up, w_down):
        S, T, D = token_act.shape
        C = token_cond.shape[-1]
        mask_row = token_mask.reshape(1, T)
        wq = jnp.transpose(w_qkvg, (0, 2, 3, 1))
        wup = jnp.transpose(w_up, (0, 2, 3, 1))
        act = token_act.reshape(S * T, D)
        cond = token_cond.reshape(S * T, C)
        o0, w0, gate0, mod0, nxt0 = _block0(n_dp, token_act, token_cond, pair_bias, mask_row, wq, b_q, ada_scale, ada_w, ada_bias, zero_w, zero_b, w_o, wup, w_down)
        o0, w0, gate0, mod0, nxt0 = (pltpu.with_memory_space_constraint(v, pltpu.VMEM) for v in (o0, w0, gate0, mod0, nxt0))
        w1, gate1, mod1, a1, o1, _ = _block1(n_dp, o0, w0, gate0, mod0, nxt0, act, cond, zero_w, zero_b, ada_scale, ada_w, ada_bias, pair_bias, mask_row, wq, b_q, w_o, wup, w_down)
        o1, a1, w1, gate1, mod1 = (pltpu.with_memory_space_constraint(v, pltpu.VMEM) for v in (o1, a1, w1, gate1, mod1))
        out = pltpu.with_memory_space_constraint(_last(n_dp, o1, a1, w1, gate1, mod1), pltpu.VMEM)
        return _store(out).reshape(S, T, D)

    everywhere = P()
    in_specs = (P('dp', None, None), P('dp', None, None), P(None, 'tp', None, None), P(None), everywhere, everywhere, everywhere, everywhere, everywhere, P(None, None, None, 'tp'), P(None, 'tp'), P(None, 'tp', None), P(None, None, None, 'tp'), P(None, 'tp', None))
    return jax.shard_map(shard_body, mesh=mesh, in_specs=in_specs, out_specs=P('dp', None, None), check_vma=False)
```

```python
import functools
import math

import jax
import jax.numpy as jnp
from jax import lax
from jax.experimental import pallas as pl
from jax.experimental.pallas import tpu as pltpu
from jax.sharding import PartitionSpec as P

LN_EPS = 1e-5
LOG2E = 1.4426950408889634
MESH = pl.DeviceIdType.MESH
BF16 = jnp.bfloat16
F32 = jnp.float32
scope = jax.named_scope
HP = 64
QT = 256
ANY = pl.BlockSpec(memory_space=pl.ANY)
VMEM = pl.BlockSpec(memory_space=pltpu.VMEM)
HBM = pl.BlockSpec(memory_space=pltpu.HBM)
VM0, VM1, VM2 = 40 << 20, 40 << 20, 8 << 20


def _ln(x):
    mean = jnp.mean(x, axis=-1, keepdims=True)
    cen = x - mean
    var = jnp.mean(cen * cen, axis=-1, keepdims=True)
    return cen * lax.rsqrt(var + LN_EPS)


def _sig(x):
    return 0.5 * jnp.tanh(0.5 * x) + 0.5


def _dot(a, b, ca=1, cb=0):
    return lax.dot_general(a, b, (((ca,), (cb,)), ((), ())), preferred_element_type=F32)


def _ada(x_f32, cond_normed, scale, w, bias):
    d = x_f32.shape[-1]
    mod = _dot((cond_normed * scale).astype(BF16), w)
    return (_sig(mod[:, :d] + bias) * _ln(x_f32) + mod[:, d:]).astype(BF16)


class Place:
    def __init__(self, n_tp, n_dp):
        self.n = n_tp
        self.n_dp = n_dp
        self.col = lax.axis_index("dp")
        self.nz = n_tp // 2
        self.me = lax.axis_index("tp")
        self.z = self.me // 2
        self.c = lax.rem(self.me, 2)
        self.partner = self.z * 2 + (1 - self.c)

    def at(self, off):
        return lax.rem(self.z + off + self.nz, self.nz) * 2 + self.c

    def column(self, i):
        return lax.rem(self.col + i, self.n_dp)

    def enter(self, everyone):
        barrier = pltpu.get_barrier_semaphore()
        if everyone:
            peers = [{"tp": lax.rem(self.me + i, self.n)} for i in range(1, self.n)]
            peers += [{"dp": self.column(i), "tp": self.me} for i in range(1, self.n_dp)]
        else:
            peers = [{"tp": t} for t in (self.at(1), self.at(-1), self.partner)]
        for peer in peers:
            pl.semaphore_signal(barrier, inc=1, device_id=peer, device_id_type=MESH)
        return lambda: pl.semaphore_wait(barrier, len(peers))


class Ring:
    def __init__(self, place, view, recv_sem, send_sem, n_chunk):
        self.p, self.view, self.recv, self.send, self.n_chunk = place, view, recv_sem, send_sem, n_chunk
        self.far = place.nz // 2

    def _push(self, b, ch, dst, src=None):
        v = self.view(b, ch)
        pltpu.make_async_remote_copy(
            src_ref=v if src is None else src, dst_ref=v, send_sem=self.send, recv_sem=self.recv.at[b, ch],
            device_id={"tp": dst}, device_id_type=MESH).start()

    def own(self, ch, src=None):
        p = self.p
        self._push(p.me, ch, p.at(1), src)
        self._push(p.me, ch, p.at(-1), src)
        self._push(p.me, ch, p.partner, src)

    def wait(self, b, ch):
        v = self.view(b, ch)
        pltpu.make_async_copy(v, v, self.recv.at[b, ch]).wait()

    def service(self, h, ch):
        p = self.p
        for sign, core in ((1, 0), (-1, 1)):
            b = p.at(-sign * h)

            @pl.when((h < self.far) | (p.c == core))
            def _():
                self.wait(b, ch)

                @pl.when((h < self.far - 1) | ((h == self.far - 1) & (p.c == core)))
                def _():
                    self._push(b, ch, p.at(sign))

                self._push(b, ch, p.partner)

    def drain(self, whole):
        pltpu.make_async_copy(whole, whole, self.send).wait()


class Cross:
    def __init__(self, place, buf, lo, hi, n_chunk, recv_sem, near_sem, far_sem, spread=True):
        self.p, self.buf, self.lo, self.hi, self.n_chunk, self.spread = place, buf, lo, hi, n_chunk, spread
        self.recv, self.near, self.far_sem = recv_sem, near_sem, far_sem
        self.far = place.nz // 2
        self.size = (hi - lo) // n_chunk

    def _rows(self, ch):
        return pl.ds(self.lo + ch * self.size, self.size)

    def _push(self, b, ch, dst, sem, src=None):
        v = self.buf.at[b, self._rows(ch), :]
        pltpu.make_async_remote_copy(
            src_ref=v if src is None else src, dst_ref=v, send_sem=sem, recv_sem=self.recv.at[b, ch],
            device_id=dst, device_id_type=MESH).start()

    def _push_over(self, b, ch, plane):
        p = self.p

        @pl.when(plane)
        def _():
            for i in range(1, p.n_dp):
                self._push(b, ch, {"dp": p.column(i), "tp": p.me}, self.far_sem.at[b // 2])

        self._push(b, ch, {"tp": p.partner}, self.near)

    def _mine(self, b):
        return lax.rem(b, self.p.n_dp) == self.p.col

    def own(self, src):
        p = self.p
        for ch in range(self.n_chunk):
            part = src.at[self._rows(ch), :]

            @pl.when(self._mine(p.me))
            def _():
                for off in (1, -1):
                    self._push(p.me, ch, {"tp": p.at(off)}, self.far_sem.at[p.z], part)

            if self.spread:
                self._push(p.me, ch, {"tp": p.partner}, self.near, part)

    def wait(self, b, ch):
        v = self.buf.at[b, self._rows(ch), :]
        pltpu.make_async_copy(v, v, self.recv.at[b, ch]).wait()

    def _each(self, h, body):
        p = self.p
        for sign, core in ((1, 0), (-1, 1)):
            b = p.at(-sign * h)

            @pl.when((h < self.far) | (p.c == core))
            def _():
                body(b, sign, (h < self.far - 1) | ((h == self.far - 1) & (p.c == core)))

    def along(self, h, ch):
        p = self.p

        def body(b, sign, onward):
            @pl.when(self._mine(b))
            def _():
                self.wait(b, ch)

                @pl.when(onward)
                def _():
                    self._push(b, ch, {"tp": p.at(sign)}, self.far_sem.at[b // 2])

                if self.spread:
                    self._push_over(b, ch, True)

        self._each(h, body)

    def hand_on(self):
        p = self.p

        def block(i, _):
            b = i * 2 + p.c

            @pl.when(self._mine(b) | (i == p.z))
            def _():
                for ch in range(self.n_chunk):
                    self._push_over(b, ch, i != p.z)
            return 0

        lax.fori_loop(0, p.nz, block, 0)

    def across(self, h, ch):
        p = self.p

        def body(b, sign, onward):
            @pl.when(jnp.logical_not(self._mine(b)))
            def _():
                self.wait(b, ch)
                self._push(b, ch, {"tp": p.partner}, self.near)

        self._each(h, body)

    def _sent(self, k, sem):
        if k:
            v = self.buf.at[0:k, self.lo:self.hi, :]
            pltpu.make_async_copy(v, v, sem).wait()

    def finish_near(self):
        p = self.p

        def other(i, _):
            for ch in range(self.n_chunk):
                self.wait(i * 2 + (1 - p.c), ch)
            return 0

        lax.fori_loop(0, p.nz, other, 0)
        self._sent(p.nz, self.near)

    def finish_far(self, ring=True):
        p = self.p
        over = p.n_dp - 1 if self.spread else 0
        if ring:
            @pl.when(self._mine(p.me))
            def _():
                self._sent(2, self.far_sem.at[p.z])

        def body(b, sign, onward):
            sem = self.far_sem.at[b // 2]

            @pl.when(self._mine(b))
            def _():
                if not ring:
                    self._sent(over, sem)
                else:
                    @pl.when(onward)
                    def _():
                        self._sent(over + 1, sem)

                    @pl.when(jnp.logical_not(onward))
                    def _():
                        self._sent(over, sem)

        def hop(h, _):
            self._each(h, body)
            return 0

        lax.fori_loop(1, self.far + 1, hop, 0)


def _copy(src, dst, sem):
    cp = pltpu.make_async_copy(src, dst, sem)
    cp.start()
    return cp


def _stage(l, hd, hu, wo_hbm, wup_hbm, wdn_hbm, wst, sem):
    cps, lo = [], 0
    for src, rows in ((wo_hbm.at[l], hd), (wup_hbm.at[l, 0], hu), (wup_hbm.at[l, 1], hu), (wdn_hbm.at[l], hu)):
        cps.append(_copy(src, wst.at[pl.ds(lo, rows), :], sem.at[len(cps)]))
        lo += rows
    return cps


def _stage_qkvg(l, hd, wq_hbm, w_s, sem):
    w_s[...] = jnp.zeros_like(w_s)
    return [_copy(wq_hbm.at[l, f], w_s.at[pl.ds(i * HP, hd), :], sem.at[i]) for i, f in enumerate((1, 0, 2, 3))]


class Attend:
    def __init__(self, n_tp, hd, w, brow, bt, k_s, qt_s, vt_s, gt_s, lg, o_s, x_rows):
        self.__dict__.update(locals())
        self.T = bt.shape[0]

    def project(self):
        T, hd = self.T, self.hd
        tile = QT
        for i in range(T // tile):
            rows = pl.ds(i * tile, tile)
            res = _dot(self.x_rows(i, tile), self.w[...], 1, 1) + self.brow
            self.k_s[rows, :] = res[:, :2 * HP].astype(BF16)
            rest = res.T
            self.qt_s[0:HP, rows] = rest[HP:2 * HP].astype(BF16)
            ones = lax.broadcasted_iota(jnp.int32, (HP, tile), 0) == hd
            self.vt_s[:, rows] = jnp.where(ones, 1.0, rest[2 * HP:3 * HP]).astype(BF16)
            self.gt_s[:, rows] = _sig(rest[3 * HP:3 * HP + hd])

    def attend(self, slot, hook=None):
        T, hd = self.T, self.hd
        n = T // QT
        c1 = LOG2E / math.sqrt(hd)

        def scores(i):
            cols = pl.ds(i * QT, QT)
            logits = _dot(self.k_s[...], self.qt_s[:, cols]) * c1 + self.bt[:, cols]
            self.lg[i % 2] = logits
            return jnp.max(logits, axis=0, keepdims=True)

        top = scores(0)
        if hook is not None:
            hook()
        for i in range(n):
            cols = pl.ds(i * QT, QT)
            nxt = scores(i + 1) if i + 1 < n else None
            probs = jnp.exp2(self.lg[i % 2] - top).astype(BF16)
            mixed = _dot(self.vt_s[...], probs)
            self.o_s[slot, :, cols] = (self.gt_s[:, cols] * (mixed[:hd] / mixed[hd:hd + 1])).astype(BF16)
            top = nxt


def _load_bias(bias_v, mask_ref, bt):
    T = bt.shape[0]
    mask_add = (mask_ref[...].astype(F32) - 1.0) * 1e9

    def step(i, _):
        r = pl.multiple_of(i * 128, 128)
        rows = (bias_v[pl.ds(r, 128), :].astype(F32) + mask_add) * LOG2E
        bt[:, pl.ds(r, 128)] = rows.T
        return 0

    lax.fori_loop(0, T // 128, step, 0)


class Exchange:
    def __init__(self, place, sample_of, o_s, o_out, send_sem, recv_sem):
        self.p, self.sample_of, self.o_s, self.o_out, self.send, self.recv = place, sample_of, o_s, o_out, send_sem, recv_sem
        self.half = o_s.shape[-1] // 2

    def _each(self, k, remote, local):
        p = self.p
        for c in range(2):
            dst = self.sample_of(k) * 2 + c
            src = self.o_s.at[k, :, pl.ds(c * self.half, self.half)]
            sem = self.send.at[k, c]
            cp = pltpu.make_async_remote_copy(
                src_ref=src, dst_ref=self.o_out.at[p.me], send_sem=sem, recv_sem=self.recv,
                device_id={"tp": dst}, device_id_type=MESH)

            @pl.when(dst != p.me)
            def _():
                remote(cp)

            @pl.when(dst == p.me)
            def _():
                local(pltpu.make_async_copy(src, self.o_out.at[p.me], sem))

    def start(self, k):
        self._each(k, lambda cp: cp.start(), lambda cp: cp.start())

    def finish(self):
        def sent(k, _):
            self._each(k, lambda cp: cp.wait_send(), lambda cp: cp.wait())
            return 0

        lax.fori_loop(0, self.o_s.shape[0], sent, 0)
        rest = self.o_out.at[0:self.p.n - 1]
        pltpu.make_async_copy(rest, rest, self.recv).wait()


def _bias_row(bq, hd):
    return jnp.concatenate([jnp.zeros((1, HP), F32), bq, jnp.zeros((1, 3 * HP - hd), F32)], axis=1)


def _gates(out, cond, w, bias):
    d = bias.shape[-1]
    out[...] = _dot(cond, w)
    for j in range(bias.shape[0]):
        cols = pl.ds(j * d, d)
        out[:, cols] = _sig(out[:, cols] + bias[j:j + 1, :])


def _modulation(out, cond_normed, scale, w, bias):
    d = bias.shape[-1]
    out[...] = _dot((cond_normed * scale).astype(BF16), w)
    out[:, :d] = _sig(out[:, :d] + bias)


def _flat(raw):
    c, two, d = raw.shape
    return raw[...].reshape(c, two * d)


def _block0_kernel(dims, x_hbm, cond_hbm, bias_hbm, mask_ref, wq_hbm, bq_ref, asc_ref, aw_hbm, ab_ref, zw_hbm, zb_ref, wo_hbm, wup_hbm, wdn_hbm,
                   o_out, wg, gate_out, mod_out, nxt_out, w1g,
                   bias_v, bt, w_s, k_s, qt_s, vt_s, gt_s, lg, o_s, xraw, craw, xn, raw, aw_s, wst, wst1, cond,
                   ld_sem, cd_sem, b_sem, q_sem, a_sem, st_sem, o_send, o_recv, n_send, n_recv, n_free, w_send, w_recv, c_near, c_far, c_recv,
                   k_sem, d_far, d_recv):
    S, T, D, C, n_tp, n_dp, hd, hu, cut, n_chunk = dims
    p = Place(n_tp, n_dp)
    entered = p.enter(True)
    rows_w = hd + 3 * hu
    stage = _stage(0, hd, hu, wo_hbm, wup_hbm, wdn_hbm, wst, st_sem.at[0])
    stage1 = _stage(1, hd, hu, wo_hbm, wup_hbm, wdn_hbm, wst1, st_sem.at[1])
    R = S * T // n_tp
    mine = pl.ds(p.c * R, R)

    def sample_of(k):
        j = S - 1 - k
        return lax.rem(p.z + S + (1 - 2 * lax.rem(j, 2)) * ((j + 1) // 2), S)

    def loads(k, slot):
        s = sample_of(k)
        return [pltpu.make_async_copy(x_hbm.at[s, mine], xraw.at[slot], ld_sem.at[slot]),
                pltpu.make_async_copy(cond_hbm.at[s, mine], craw.at[slot], cd_sem.at[slot])]

    raws = [pltpu.make_async_copy(aw_hbm.at[0, 0], raw.at[0], a_sem.at[0]), pltpu.make_async_copy(zw_hbm.at[0], raw.at[1], a_sem.at[1]),
            pltpu.make_async_copy(aw_hbm.at[0, 1], raw.at[2], a_sem.at[2]), pltpu.make_async_copy(aw_hbm.at[1, 0], raw.at[0], a_sem.at[0])]
    raws[0].start()
    for k in range(2):
        for cp in loads(k, k):
            cp.start()
    bias_cp = _copy(bias_hbm.at[0, 0], bias_v, b_sem)
    qt_s[HP:, :] = jnp.zeros((HP, T), BF16)
    wq = _stage_qkvg(0, hd, wq_hbm, w_s, q_sem)
    for cp in stage:
        cp.wait()
    for cp in wq:
        cp.wait()
    for r in (1, 2):
        raws[r].start()
    cond_cp = pltpu.make_async_copy(cond_hbm.at[p.z, mine], cond, b_sem)
    entered()
    ring = Ring(p, lambda b, ch: wg.at[b, 0:cut, :], w_recv, w_send, 1)
    cross = Cross(p, wg, cut, rows_w, n_chunk, c_recv, c_near, c_far)
    cross1 = Cross(p, w1g, 0, rows_w, 1, d_recv, None, d_far, spread=False)
    ring.own(0, wst.at[0:cut, :])
    cross.own(wst)

    def half(slot, dst):
        v = xn.at[slot, mine]
        return pltpu.make_async_remote_copy(src_ref=v, dst_ref=v, send_sem=n_send.at[slot], recv_sem=n_recv.at[slot],
                                            device_id={"tp": p.partner}, device_id_type=MESH)

    def normalise(slot):
        tile = 256 if R % 256 == 0 else R
        for i in range(R // tile):
            rows = pl.ds(i * tile, tile)
            cn = _ln(craw[slot, rows, :].astype(F32))
            y = _ada(xraw[slot, rows, :].astype(F32), cn, asc_ref[0, 0:1, :], aw_s[...], ab_ref[0, 0:1, :])
            xn[slot, pl.ds(pl.multiple_of(p.c * R, R) + i * tile, tile), :] = y

    raws[0].wait()
    aw_s[...] = _flat(raw.at[0])
    for cp in loads(0, 0):
        cp.wait()
    normalise(0)
    bias_cp.wait()
    half(0, p.partner).start()
    _load_bias(bias_v, mask_ref, bt)
    cond_cp.start()
    for cp in stage1:
        cp.wait()
    keep = _copy(wst1, w1g.at[p.me], k_sem)
    ex = Exchange(p, sample_of, o_s, o_out, o_send, o_recv)
    brow = _bias_row(bq_ref[0:1, :], hd)
    events = {}

    def plan(when, f, *args):
        events.setdefault((when % 2, when // 2), []).append((f, args))

    for h in range(1, p.nz // 2 + 1):
        plan(2 * h - 2, ring.service, h, 0)
        for ch in range(n_chunk):
            plan(n_chunk * (h - 1) + ch, cross.along, h, ch)
            plan(n_chunk * h + ch + 1, cross.across, h, ch)
        plan(3 * h + 3, cross1.along, h, 0)
    plan(3, cross1.own, wst1)

    def step(k, _):
        slot = lax.rem(k, 2)

        @pl.when(k + 2 < S)
        def _():
            for cp in loads(k + 2, slot):
                cp.start()

        with scope("b0_half"):
            v = xn.at[slot, pl.ds((1 - p.c) * R, R)]
            pltpu.make_async_copy(v, v, n_recv.at[slot]).wait()
            half(slot, p.partner).wait_send()
        at = Attend(n_tp, hd, w_s, brow, bt, k_s, qt_s, vt_s, gt_s, lg, o_s, lambda i, tile: xn[slot, pl.ds(i * tile, tile), :])
        with scope("b0_proj"):
            at.project()

        @pl.when(k + 2 < S)
        def _():
            pl.semaphore_signal(n_free, inc=1, device_id={"tp": p.partner}, device_id_type=MESH)

        @pl.when(k >= 1)
        def _():
            ex.start(k - 1)

        with scope("b0_norm"):
            @pl.when(k + 1 < S)
            def _():
                for cp in loads(k + 1, 1 - slot):
                    cp.wait()
                normalise(1 - slot)

                @pl.when(k >= 1)
                def _():
                    pl.semaphore_wait(n_free, 1)

        def take(part):
            with scope("b0_ev"):
                for (half_step, when), todo in sorted(events.items(), key=lambda e: e[0]):
                    if half_step == part:
                        @pl.when(k == when)
                        def _():
                            for f, args in todo:
                                f(*args)

        take(0)

        def hook():
            @pl.when(k + 1 < S)
            def _():
                half(1 - slot, p.partner).start()

        with scope("b0_att"):
            at.attend(k, hook)
        take(1)
        return 0

    lax.fori_loop(0, S, step, 0)
    ex.start(S - 1)
    raws[3].start()
    with scope("b0_mods"):
        wg[p.me] = wst[...]
        cond_cp.wait()
        cn = _ln(cond[...].astype(F32))
        raws[1].wait()
        aw_s[...] = _flat(raw.at[1])
        _gates(gate_out, cond[...], aw_s[...], zb_ref.at[0])
        for src, cp, l, j, out in ((2, raws[2], 0, 1, mod_out), (0, raws[3], 1, 0, nxt_out)):
            cp.wait()
            aw_s[...] = _flat(raw.at[src])
            _modulation(out, cn, asc_ref[l, j:j + 1, :], aw_s[...], ab_ref[l, j:j + 1, :])
    for (half_step, when), todo in sorted(events.items(), key=lambda e: (e[0][1], e[0][0])):
        if when >= S:
            for f, args in todo:
                f(*args)

    def other(i, _):
        ring.wait(i * 2 + (1 - p.c), 0)
        return 0

    with scope("b0_ring_end"):
        lax.fori_loop(0, p.nz, other, 0)
        ring.drain(wg.at[0:n_tp - 1, 0:cut, :])
    with scope("b0_cross_end"):
        cross.finish_near()
        cross.finish_far()
        cross1.finish_far()
        keep.wait()
    with scope("b0_arr"):
        ex.finish()


def _head_scratch(S, T, D, hd):
    v = pltpu.VMEM
    return [v((T, T), BF16), v((T, T), F32), v((4 * HP, D), BF16), v((T, 2 * HP), BF16), v((2 * HP, T), BF16), v((HP, T), BF16),
            v((hd, T), F32), v((2, T, QT), F32), v((S, hd, T), BF16)]


def _block0(n_dp, x, cond, pair_bias, mask_row, wq, bq, asc, aw, ab, zw, zb, wo, wup, wdn):
    S, T, D = x.shape
    C = cond.shape[-1]
    _, _, hd, _ = wq.shape
    hu = wdn.shape[1]
    n_tp = S * 2
    rows_w = hd + 3 * hu
    R = T // 2
    cut, n_chunk = hd, 3
    dma = pltpu.SemaphoreType.DMA
    return pl.pallas_call(
        functools.partial(_block0_kernel, (S, T, D, C, n_tp, n_dp, hd, hu, cut, n_chunk)),
        out_shape=(pltpu.VMEM((n_tp, hd, R), BF16), pltpu.VMEM((n_tp, rows_w, D), BF16),
                   *[pltpu.VMEM((R, 2 * D), F32)] * 3, pltpu.HBM((n_tp, rows_w, D), BF16)),
        in_specs=[ANY, ANY, ANY, VMEM, ANY, VMEM, VMEM, ANY, VMEM, ANY, VMEM, ANY, ANY, ANY],
        out_specs=(VMEM,) * 5 + (HBM,),
        scratch_shapes=[
            *_head_scratch(S, T, D, hd),
            pltpu.VMEM((2, R, D), BF16), pltpu.VMEM((2, R, C), BF16), pltpu.VMEM((2, T, D), BF16),
            pltpu.VMEM((3, C, 2, D), BF16), pltpu.VMEM((C, 2 * D), BF16), *[pltpu.VMEM((rows_w, D), BF16)] * 2, pltpu.VMEM((R, C), BF16),
            dma((2,)), dma((2,)), dma, dma((4,)), dma((3,)), dma((2, 4)), dma((S, 2)), dma, dma((2,)), dma((2,)), pltpu.SemaphoreType.REGULAR,
            dma, dma((n_tp, 1)), dma, dma((S,)), dma((n_tp, n_chunk)), dma, dma((S,)), dma((n_tp, 1))],
        cost_estimate=pl.CostEstimate(flops=2 * S * T * (D * 4 * HP + 2 * T * 256 + C * D), bytes_accessed=S * T * (D + C), transcendentals=S * T * T),
        compiler_params=pltpu.CompilerParams(collective_id=0, has_side_effects=True, vmem_limit_bytes=VM0),
        name="block0",
    )(x, cond, pair_bias, mask_row, wq, bq, asc, aw, ab, zw, zb, wo, wup, wdn)


def _transition(dims, tile, gates, mod1, o_v, act, wall, y_s, h_s, rows):
    D, n_tp, hd, hu = dims
    w_o = wall[:, 0:hd, :].reshape(n_tp * hd, D)
    o_t = o_v[:, :, rows].reshape(n_tp * hd, tile)
    t = _dot(o_t, w_o, 0, 0).astype(BF16).astype(F32)
    mid = (act[rows, :].astype(F32) + gates[rows, :D] * t).astype(BF16).astype(F32)
    y_s[...] = (mod1[rows, :D] * _ln(mid) + mod1[rows, D:]).astype(BF16)
    step = 4 * hu
    for j in range(n_tp * hu // step):
        dv = slice(4 * j, 4 * j + 4)
        u1 = _dot(y_s[...], wall[dv, hd:hd + hu, :].reshape(step, D), 1, 1)
        u2 = _dot(y_s[...], wall[dv, hd + hu:hd + 2 * hu, :].reshape(step, D), 1, 1)
        h_s[:, j * step:(j + 1) * step] = (u1 * _sig(u1) * u2).astype(BF16)
    r = _dot(h_s[...], wall[:, hd + 2 * hu:hd + 3 * hu, :].reshape(n_tp * hu, D)).astype(BF16).astype(F32)
    return (mid + gates[rows, D:] * r).astype(BF16)


def _block1_kernel(dims, o0, w0, gate0, mod0, nxt0, act_hbm, cond_hbm, zw_hbm, zb_ref, asc_ref, aw_hbm, ab_ref, bias_hbm, mask_ref, wq_hbm, bq_ref, _,
                   w1, gate1, mod1, a_out, o_out, wg,
                   bias_v, bt, w_s, k_s, qt_s, vt_s, gt_s, lg, o_s, act, cond, raw, aw_s, y_s, h_s, xg,
                   l_sem, q_sem, wl_sem, x_send, x_recv, o_send, o_recv, c_near, c_far, c_recv):
    S, T, D, C, n_tp, n_dp, hd, hu = dims
    p = Place(n_tp, n_dp)
    entered = p.enter(True)
    R = S * T // n_tp
    row0 = p.me * R
    rows_w = hd + 3 * hu
    srcs = [(act_hbm.at[pl.ds(row0, R), :], act), (cond_hbm.at[pl.ds(row0, R), :], cond), (bias_hbm.at[1, 0], bias_v),
            (zw_hbm.at[1], raw.at[0]), (aw_hbm.at[1, 1], raw.at[1])]
    cps = [_copy(a, b, l_sem.at[i]) for i, (a, b) in enumerate(srcs)]
    qt_s[HP:, :] = jnp.zeros((HP, T), BF16)
    wq = _stage_qkvg(1, hd, wq_hbm, w_s, q_sem)
    cross = Cross(p, wg, 0, rows_w, 1, c_recv, c_near, c_far)
    cps[0].wait()
    tile = R // 2
    ring = Ring(p, lambda b, ch: xg.at[pl.ds(b * R + ch * tile, tile), :], x_recv, x_send, 2)
    for ch in range(2):
        rows = pl.ds(ch * tile, tile)
        with scope("b1_mlp"):
            new = _transition((D, n_tp, hd, hu), tile, gate0, mod0, o0, act, w0, y_s, h_s, rows)
            a_out[rows, :] = new
            xg[pl.ds(row0 + ch * tile, tile), :] = (nxt0[rows, :D] * _ln(new.astype(F32)) + nxt0[rows, D:]).astype(BF16)
        if ch == 0:
            with scope("b1_enter"):
                entered()
        ring.own(ch)
        if ch == 0:
            cross.hand_on()
    with scope("b1_bias"):
        cps[2].wait()
        _load_bias(bias_v, mask_ref, bt)
    for cp in wq:
        cp.wait()
    brow = _bias_row(bq_ref[1:2, :], hd)
    turn = 1 - 2 * p.c

    def sample_of(j):
        h = (j + 1) // 2
        return lax.rem(p.z + S + turn * (1 - 2 * lax.rem(j, 2)) * h, S)

    ex = Exchange(p, sample_of, o_s, o_out, o_send, o_recv)

    def step(j, _):
        with scope("b1_svc"):
            ring.service(j // 2 + 1, lax.rem(j, 2))

        @pl.when((j >= 2) & (j <= p.nz // 2 + 1))
        def _():
            with scope("b1_x"):
                cross.across(j - 1, 0)

        @pl.when(j >= 1)
        def _():
            ex.start(j - 1)

        s = sample_of(j)
        with scope("b1_half"):
            for ch in range(2):
                ring.wait(s * 2 + (1 - p.c), ch)

        def x_rows(i, t):
            return xg[pl.ds(pl.multiple_of(s * T, T) + i * t, t), :]

        at = Attend(n_tp, hd, w_s, brow, bt, k_s, qt_s, vt_s, gt_s, lg, o_s, x_rows)
        with scope("b1_proj"):
            at.project()

        with scope("b1_att"):
            at.attend(j)

        @pl.when(j == 1)
        def _():
            cps[1].wait()
            cps[3].wait()
            aw_s[...] = _flat(raw.at[0])
            _gates(gate1, cond[...], aw_s[...], zb_ref.at[1])

        @pl.when(j == 3)
        def _():
            cps[4].wait()
            aw_s[...] = _flat(raw.at[1])
            cn = _ln(cond[...].astype(F32))
            _modulation(mod1, cn, asc_ref[1, 1:2, :], aw_s[...], ab_ref[1, 1:2, :])

        with scope("b1_fin"):
            @pl.when(j == S - 2)
            def _():
                cross.finish_near()
                pltpu.make_async_copy(wg, w1, wl_sem).start()

        return 0

    lax.fori_loop(0, S, step, 0)
    ex.start(S - 1)
    cross.finish_far(ring=False)
    pltpu.make_async_copy(wg, w1, wl_sem).wait()
    with scope("b1_drain"):
        ring.drain(xg.at[0:(n_tp - 1) * R, :])
    with scope("b1_arr"):
        ex.finish()


def _block1(n_dp, o0, w0, gate0, mod0, nxt0, act, cond, zw, zb, asc, aw, ab, pair_bias, mask_row, wq, bq, wg):
    n_tp, hd, R = o0.shape
    D = act.shape[-1]
    C = cond.shape[-1]
    S = n_tp // 2
    T = 2 * R
    rows_w = w0.shape[1]
    hu = (rows_w - hd) // 3
    dma = pltpu.SemaphoreType.DMA
    return pl.pallas_call(
        functools.partial(_block1_kernel, (S, T, D, C, n_tp, n_dp, hd, hu)),
        out_shape=(pltpu.VMEM((n_tp, rows_w, D), BF16), pltpu.VMEM((R, 2 * D), F32), pltpu.VMEM((R, 2 * D), F32),
                   pltpu.VMEM((R, D), BF16), pltpu.VMEM((n_tp, hd, R), BF16), pltpu.HBM((n_tp, rows_w, D), BF16)),
        in_specs=[VMEM, VMEM, VMEM, VMEM, VMEM, ANY, ANY, ANY, VMEM, VMEM, ANY, VMEM, ANY, VMEM, ANY, VMEM, HBM],
        out_specs=(VMEM,) * 5 + (HBM,),
        input_output_aliases={1: 0, 2: 1, 3: 2, 16: 5},
        scratch_shapes=[
            *_head_scratch(S, T, D, hd),
            pltpu.VMEM((R, D), BF16), pltpu.VMEM((R, C), BF16), pltpu.VMEM((2, C, 2, D), BF16), pltpu.VMEM((C, 2 * D), BF16),
            pltpu.VMEM((R // 2, D), BF16), pltpu.VMEM((R // 2, n_tp * hu), BF16), pltpu.VMEM((S * T, D), BF16),
            dma((5,)), dma((4,)), dma, dma, dma((n_tp, 2)), dma((S, 2)), dma, dma, dma((S,)), dma((n_tp, 1))],
        cost_estimate=pl.CostEstimate(flops=2 * S * T * (D * 4 * HP + 2 * T * 256), bytes_accessed=S * T * D * 2, transcendentals=S * T * T),
        compiler_params=pltpu.CompilerParams(collective_id=1, has_side_effects=True, vmem_limit_bytes=VM1),
        name="block1",
    )(o0, w0, gate0, mod0, nxt0, act, cond, zw, zb, asc, aw, ab, pair_bias, mask_row, wq, bq, wg)


def _last_kernel(dims, o_v, act, wall, gate, mod, out, y_s, h_s, x_send, x_recv):
    D, n_tp, n_dp, hd, hu, R = dims
    p = Place(n_tp, n_dp)
    entered = p.enter(False)
    tile = R // 2
    ring = Ring(p, lambda b, ch: out.at[pl.ds(b * R + ch * tile, tile), :], x_recv, x_send, 2)
    for ch in range(2):
        rows = pl.ds(ch * tile, tile)
        with scope("l_mlp"):
            out[pl.ds(p.me * R + ch * tile, tile), :] = _transition((D, n_tp, hd, hu), tile, gate, mod, o_v, act, wall, y_s, h_s, rows)
        if ch == 0:
            entered()
        ring.own(ch)

    with scope("l_svc"):
        lax.fori_loop(0, p.nz, lambda e, _: (ring.service(e // 2 + 1, lax.rem(e, 2)), 0)[1], 0)

    def other(i, _):
        for ch in range(2):
            ring.wait(i * 2 + (1 - p.c), ch)
        return 0

    with scope("l_end"):
        lax.fori_loop(0, p.nz, other, 0)
    ring.drain(out.at[0:(n_tp - 1) * R, :])


def _last(n_dp, o, act, w1, gate, mod):
    n_tp, hd, R = o.shape
    D = act.shape[-1]
    hu = (w1.shape[1] - hd) // 3
    dma = pltpu.SemaphoreType.DMA
    return pl.pallas_call(
        functools.partial(_last_kernel, (D, n_tp, n_dp, hd, hu, R)),
        out_shape=pltpu.VMEM((n_tp * R, D), BF16),
        in_specs=[VMEM] * 5, out_specs=VMEM,
        scratch_shapes=[pltpu.VMEM((R // 2, D), BF16), pltpu.VMEM((R // 2, n_tp * hu), BF16), dma, dma((n_tp, 2))],
        cost_estimate=pl.CostEstimate(flops=2 * R * D * (D + 3 * n_tp * hu), bytes_accessed=w1.size, transcendentals=R * D),
        compiler_params=pltpu.CompilerParams(collective_id=2, has_side_effects=True, vmem_limit_bytes=VM2),
        name="last",
    )(o, act, w1, gate, mod)


def _store_kernel(src, dst, sem):
    cp = pltpu.make_async_copy(src, dst, sem)
    cp.start()
    cp.wait()


def _store(x):
    return pl.pallas_call(
        _store_kernel, out_shape=jax.ShapeDtypeStruct(x.shape, x.dtype), in_specs=[VMEM], out_specs=ANY,
        scratch_shapes=[pltpu.SemaphoreType.DMA], compiler_params=pltpu.CompilerParams(vmem_limit_bytes=1 << 20), name="store")(x)


def solution(mesh):
    n_dp = mesh.shape["dp"]

    def shard_body(token_act, token_cond, pair_bias, token_mask, ada_scale, ada_w, ada_bias, zero_w, zero_b, w_qkvg, b_q, w_o, w_up, w_down):
        S, T, D = token_act.shape
        C = token_cond.shape[-1]
        mask_row = token_mask.reshape(1, T)
        wq = jnp.transpose(w_qkvg, (0, 2, 3, 1))
        wup = jnp.transpose(w_up, (0, 2, 3, 1))
        act = token_act.reshape(S * T, D)
        cond = token_cond.reshape(S * T, C)
        o0, w0, gate0, mod0, nxt0, wg = _block0(n_dp, token_act, token_cond, pair_bias, mask_row, wq, b_q, ada_scale, ada_w, ada_bias, zero_w, zero_b, w_o, wup, w_down)
        o0, w0, gate0, mod0, nxt0 = (pltpu.with_memory_space_constraint(v, pltpu.VMEM) for v in (o0, w0, gate0, mod0, nxt0))
        w1, gate1, mod1, a1, o1, _ = _block1(n_dp, o0, w0, gate0, mod0, nxt0, act, cond, zero_w, zero_b, ada_scale, ada_w, ada_bias, pair_bias, mask_row, wq, b_q, wg)
        o1, a1, w1, gate1, mod1 = (pltpu.with_memory_space_constraint(v, pltpu.VMEM) for v in (o1, a1, w1, gate1, mod1))
        out = pltpu.with_memory_space_constraint(_last(n_dp, o1, a1, w1, gate1, mod1), pltpu.VMEM)
        return _store(out).reshape(S, T, D)

    everywhere = P()
    rows, second, fourth = P('dp'), P(None, 'tp'), P(*[None] * 3, 'tp')
    in_specs = (rows, rows, second) + (everywhere,) * 6 + (fourth, second, second, fourth, second)
    return jax.shard_map(shard_body, mesh=mesh, in_specs=in_specs, out_specs=rows, check_vma=False)
```

```python
import functools
import math

import jax
import jax.numpy as jnp
from jax import lax
from jax.experimental import pallas as pl
from jax.experimental.pallas import tpu as pltpu
from jax.sharding import PartitionSpec as P

LN_EPS = 1e-5
LOG2E = 1.4426950408889634
MESH = pl.DeviceIdType.MESH
BF16 = jnp.bfloat16
F32 = jnp.float32
scope = jax.named_scope
HP = 64
QT = 256
ANY = pl.BlockSpec(memory_space=pl.ANY)
VMEM = pl.BlockSpec(memory_space=pltpu.VMEM)
HBM = pl.BlockSpec(memory_space=pltpu.HBM)
VM0, VM1, VM2 = 40 << 20, 40 << 20, 8 << 20


def _ln(x):
    mean = jnp.mean(x, axis=-1, keepdims=True)
    cen = x - mean
    var = jnp.mean(cen * cen, axis=-1, keepdims=True)
    return cen * lax.rsqrt(var + LN_EPS)


def _sig(x):
    return 0.5 * jnp.tanh(0.5 * x) + 0.5


def _dot(a, b, ca=1, cb=0):
    return lax.dot_general(a, b, (((ca,), (cb,)), ((), ())), preferred_element_type=F32)


def _ada(x_f32, cond_normed, scale, w, bias):
    d = x_f32.shape[-1]
    mod = _dot((cond_normed * scale).astype(BF16), w)
    return (_sig(mod[:, :d] + bias) * _ln(x_f32) + mod[:, d:]).astype(BF16)


class Place:
    def __init__(self, n_tp, n_dp):
        self.n = n_tp
        self.n_dp = n_dp
        self.col = lax.axis_index("dp")
        self.nz = n_tp // 2
        self.me = lax.axis_index("tp")
        self.z = self.me // 2
        self.c = lax.rem(self.me, 2)
        self.partner = self.z * 2 + (1 - self.c)

    def at(self, off):
        return lax.rem(self.z + off + self.nz, self.nz) * 2 + self.c

    def column(self, i):
        return lax.rem(self.col + i, self.n_dp)

    def enter(self, everyone):
        barrier = pltpu.get_barrier_semaphore()
        if everyone:
            peers = [{"tp": lax.rem(self.me + i, self.n)} for i in range(1, self.n)]
            peers += [{"dp": self.column(i), "tp": self.me} for i in range(1, self.n_dp)]
        else:
            peers = [{"tp": t} for t in (self.at(1), self.at(-1), self.partner)]
        for peer in peers:
            pl.semaphore_signal(barrier, inc=1, device_id=peer, device_id_type=MESH)
        return lambda: pl.semaphore_wait(barrier, len(peers))


class Ring:
    def __init__(self, place, view, recv_sem, send_sem, right=None):
        self.p, self.view, self.recv, self.send = place, view, recv_sem, send_sem
        self.far = place.nz // 2
        self.right = right or (lambda ch: place.c == 0)

    def _push(self, b, ch, dst, src=None):
        v = self.view(b, ch)
        pltpu.make_async_remote_copy(
            src_ref=v if src is None else src, dst_ref=v, send_sem=self.send, recv_sem=self.recv.at[b, ch],
            device_id={"tp": dst}, device_id_type=MESH).start()

    def own(self, ch, src=None):
        p = self.p
        self._push(p.me, ch, p.at(1), src)
        self._push(p.me, ch, p.at(-1), src)
        self._push(p.me, ch, p.partner, src)

    def wait(self, b, ch):
        v = self.view(b, ch)
        pltpu.make_async_copy(v, v, self.recv.at[b, ch]).wait()

    def service(self, h, ch):
        p = self.p
        right = self.right(ch)
        for sign, far in ((1, right), (-1, jnp.logical_not(right))):
            b = p.at(-sign * h)

            @pl.when((h < self.far) | far)
            def _():
                self.wait(b, ch)

                @pl.when((h < self.far - 1) | ((h == self.far - 1) & far))
                def _():
                    self._push(b, ch, p.at(sign))

                self._push(b, ch, p.partner)

    def drain(self, whole):
        pltpu.make_async_copy(whole, whole, self.send).wait()


class Cross:
    def __init__(self, place, buf, lo, hi, n_chunk, recv_sem, near_sem, far_sem, spread=True):
        self.p, self.buf, self.lo, self.hi, self.n_chunk, self.spread = place, buf, lo, hi, n_chunk, spread
        self.recv, self.near, self.far_sem = recv_sem, near_sem, far_sem
        self.far = place.nz // 2
        self.size = (hi - lo) // n_chunk

    def _rows(self, ch):
        return pl.ds(self.lo + ch * self.size, self.size)

    def _push(self, b, ch, dst, sem, src=None):
        v = self.buf.at[b, self._rows(ch), :]
        pltpu.make_async_remote_copy(
            src_ref=v if src is None else src, dst_ref=v, send_sem=sem, recv_sem=self.recv.at[b, ch],
            device_id=dst, device_id_type=MESH).start()

    def _push_over(self, b, ch, plane):
        p = self.p

        @pl.when(plane)
        def _():
            for i in range(1, p.n_dp):
                self._push(b, ch, {"dp": p.column(i), "tp": p.me}, self.far_sem.at[b // 2])

        self._push(b, ch, {"tp": p.partner}, self.near)

    def _mine(self, b):
        return lax.rem(b, self.p.n_dp) == self.p.col

    def own(self, src):
        p = self.p
        for ch in range(self.n_chunk):
            part = src.at[self._rows(ch), :]

            @pl.when(self._mine(p.me))
            def _():
                for off in (1, -1):
                    self._push(p.me, ch, {"tp": p.at(off)}, self.far_sem.at[p.z], part)

            if self.spread:
                self._push(p.me, ch, {"tp": p.partner}, self.near, part)

    def wait(self, b, ch):
        v = self.buf.at[b, self._rows(ch), :]
        pltpu.make_async_copy(v, v, self.recv.at[b, ch]).wait()

    def _each(self, h, body):
        p = self.p
        for sign, core in ((1, 0), (-1, 1)):
            b = p.at(-sign * h)

            @pl.when((h < self.far) | (p.c == core))
            def _():
                body(b, sign, (h < self.far - 1) | ((h == self.far - 1) & (p.c == core)))

    def along(self, h, ch):
        p = self.p

        def body(b, sign, onward):
            @pl.when(self._mine(b))
            def _():
                self.wait(b, ch)

                @pl.when(onward)
                def _():
                    self._push(b, ch, {"tp": p.at(sign)}, self.far_sem.at[b // 2])

                if self.spread:
                    self._push_over(b, ch, True)

        self._each(h, body)

    def hand_on(self):
        p = self.p

        def block(i, _):
            b = i * 2 + p.c

            @pl.when(self._mine(b) | (i == p.z))
            def _():
                for ch in range(self.n_chunk):
                    self._push_over(b, ch, i != p.z)
            return 0

        lax.fori_loop(0, p.nz, block, 0)

    def across(self, h, ch):
        p = self.p

        def body(b, sign, onward):
            @pl.when(jnp.logical_not(self._mine(b)))
            def _():
                self.wait(b, ch)
                self._push(b, ch, {"tp": p.partner}, self.near)

        self._each(h, body)

    def _sent(self, k, sem):
        if k:
            v = self.buf.at[0:k, self.lo:self.hi, :]
            pltpu.make_async_copy(v, v, sem).wait()

    def finish_near(self):
        p = self.p

        def other(i, _):
            for ch in range(self.n_chunk):
                self.wait(i * 2 + (1 - p.c), ch)
            return 0

        lax.fori_loop(0, p.nz, other, 0)
        self._sent(p.nz, self.near)

    def finish_far(self, ring=True):
        p = self.p
        over = p.n_dp - 1 if self.spread else 0
        if ring:
            @pl.when(self._mine(p.me))
            def _():
                self._sent(2, self.far_sem.at[p.z])

        def body(b, sign, onward):
            sem = self.far_sem.at[b // 2]

            @pl.when(self._mine(b))
            def _():
                if not ring:
                    self._sent(over, sem)
                else:
                    @pl.when(onward)
                    def _():
                        self._sent(over + 1, sem)

                    @pl.when(jnp.logical_not(onward))
                    def _():
                        self._sent(over, sem)

        def hop(h, _):
            self._each(h, body)
            return 0

        lax.fori_loop(1, self.far + 1, hop, 0)


def _copy(src, dst, sem):
    cp = pltpu.make_async_copy(src, dst, sem)
    cp.start()
    return cp


def _stage(l, hd, hu, wo_hbm, wup_hbm, wdn_hbm, wst, sem):
    cps, lo = [], 0
    for src, rows in ((wo_hbm.at[l], hd), (wup_hbm.at[l, 0], hu), (wup_hbm.at[l, 1], hu), (wdn_hbm.at[l], hu)):
        cps.append(_copy(src, wst.at[pl.ds(lo, rows), :], sem.at[len(cps)]))
        lo += rows
    return cps


def _stage_qkvg(l, hd, wq_hbm, w_s, sem):
    w_s[...] = jnp.zeros_like(w_s)
    return [_copy(wq_hbm.at[l, f], w_s.at[pl.ds(i * HP, hd), :], sem.at[i]) for i, f in enumerate((1, 0, 2, 3))]


class Attend:
    def __init__(self, n_tp, hd, w, brow, bt, k_s, qt_s, vt_s, gt_s, lg, o_s, x_rows):
        self.__dict__.update(locals())
        self.T = bt.shape[0]

    def project(self):
        T, hd = self.T, self.hd
        tile = QT
        for i in range(T // tile):
            rows = pl.ds(i * tile, tile)
            res = _dot(self.x_rows(i, tile), self.w[...], 1, 1) + self.brow
            self.k_s[rows, :] = res[:, :2 * HP].astype(BF16)
            rest = res.T
            self.qt_s[0:HP, rows] = rest[HP:2 * HP].astype(BF16)
            ones = lax.broadcasted_iota(jnp.int32, (HP, tile), 0) == hd
            self.vt_s[:, rows] = jnp.where(ones, 1.0, rest[2 * HP:3 * HP]).astype(BF16)
            self.gt_s[:, rows] = _sig(rest[3 * HP:3 * HP + hd])

    def attend(self, slot, hook=None):
        T, hd = self.T, self.hd
        n = T // QT
        c1 = LOG2E / math.sqrt(hd)

        def scores(i):
            cols = pl.ds(i * QT, QT)
            logits = _dot(self.k_s[...], self.qt_s[:, cols]) * c1 + self.bt[:, cols]
            self.lg[i % 2] = logits
            return jnp.max(logits, axis=0, keepdims=True)

        top = scores(0)
        if hook is not None:
            hook()
        for i in range(n):
            cols = pl.ds(i * QT, QT)
            nxt = scores(i + 1) if i + 1 < n else None
            probs = jnp.exp2(self.lg[i % 2] - top).astype(BF16)
            mixed = _dot(self.vt_s[...], probs)
            self.o_s[slot, :, cols] = (self.gt_s[:, cols] * (mixed[:hd] / mixed[hd:hd + 1])).astype(BF16)
            top = nxt


def _load_bias(bias_v, mask_ref, bt):
    T = bt.shape[0]
    mask_add = (mask_ref[...].astype(F32) - 1.0) * 1e9

    def step(i, _):
        r = pl.multiple_of(i * 128, 128)
        rows = (bias_v[pl.ds(r, 128), :].astype(F32) + mask_add) * LOG2E
        bt[:, pl.ds(r, 128)] = rows.T
        return 0

    lax.fori_loop(0, T // 128, step, 0)


class Exchange:
    def __init__(self, place, sample_of, o_s, o_out, send_sem, recv_sem):
        self.p, self.sample_of, self.o_s, self.o_out, self.send, self.recv = place, sample_of, o_s, o_out, send_sem, recv_sem
        self.half = o_s.shape[-1] // 2

    def _each(self, k, remote, local):
        p = self.p
        for c in range(2):
            dst = self.sample_of(k) * 2 + c
            src = self.o_s.at[k, :, pl.ds(c * self.half, self.half)]
            sem = self.send.at[k, c]
            cp = pltpu.make_async_remote_copy(
                src_ref=src, dst_ref=self.o_out.at[p.me], send_sem=sem, recv_sem=self.recv,
                device_id={"tp": dst}, device_id_type=MESH)

            @pl.when(dst != p.me)
            def _():
                remote(cp)

            @pl.when(dst == p.me)
            def _():
                local(pltpu.make_async_copy(src, self.o_out.at[p.me], sem))

    def start(self, k):
        self._each(k, lambda cp: cp.start(), lambda cp: cp.start())

    def finish(self):
        def sent(k, _):
            self._each(k, lambda cp: cp.wait_send(), lambda cp: cp.wait())
            return 0

        lax.fori_loop(0, self.o_s.shape[0], sent, 0)
        rest = self.o_out.at[0:self.p.n - 1]
        pltpu.make_async_copy(rest, rest, self.recv).wait()


def _bias_row(bq, hd):
    return jnp.concatenate([jnp.zeros((1, HP), F32), bq, jnp.zeros((1, 3 * HP - hd), F32)], axis=1)


def _gates(out, cond, w, bias):
    d = bias.shape[-1]
    out[...] = _dot(cond, w)
    for j in range(bias.shape[0]):
        cols = pl.ds(j * d, d)
        out[:, cols] = _sig(out[:, cols] + bias[j:j + 1, :])


def _modulation(out, cond_normed, scale, w, bias):
    d = bias.shape[-1]
    out[...] = _dot((cond_normed * scale).astype(BF16), w)
    out[:, :d] = _sig(out[:, :d] + bias)


def _flat(raw):
    c, two, d = raw.shape
    return raw[...].reshape(c, two * d)


def _block0_kernel(dims, x_hbm, cond_hbm, bias_hbm, mask_ref, wq_hbm, bq_ref, asc_ref, aw_hbm, ab_ref, zw_hbm, zb_ref, wo_hbm, wup_hbm, wdn_hbm,
                   o_out, wg, gate_out, mod_out, nxt_out, w1g,
                   bias_v, bt, w_s, k_s, qt_s, vt_s, gt_s, lg, o_s, xraw, craw, xn, raw, aw_s, wst, wst1, cond,
                   ld_sem, cd_sem, b_sem, q_sem, a_sem, st_sem, o_send, o_recv, n_send, n_recv, n_free, w_send, w_recv, c_near, c_far, c_recv,
                   k_sem, d_far, d_recv):
    S, T, D, C, n_tp, n_dp, hd, hu, cut, n_chunk = dims
    p = Place(n_tp, n_dp)
    entered = p.enter(True)
    rows_w = hd + 3 * hu
    stage = _stage(0, hd, hu, wo_hbm, wup_hbm, wdn_hbm, wst, st_sem.at[0])
    stage1 = _stage(1, hd, hu, wo_hbm, wup_hbm, wdn_hbm, wst1, st_sem.at[1])
    R = S * T // n_tp
    mine = pl.ds(p.c * R, R)

    def sample_of(k):
        j = S - 1 - k
        return lax.rem(p.z + S + (1 - 2 * lax.rem(j, 2)) * ((j + 1) // 2), S)

    def loads(k, slot):
        s = sample_of(k)
        return [pltpu.make_async_copy(x_hbm.at[s, mine], xraw.at[slot], ld_sem.at[slot]),
                pltpu.make_async_copy(cond_hbm.at[s, mine], craw.at[slot], cd_sem.at[slot])]

    raws = [pltpu.make_async_copy(aw_hbm.at[0, 0], raw.at[0], a_sem.at[0]), pltpu.make_async_copy(zw_hbm.at[0], raw.at[1], a_sem.at[1]),
            pltpu.make_async_copy(aw_hbm.at[0, 1], raw.at[2], a_sem.at[2]), pltpu.make_async_copy(aw_hbm.at[1, 0], raw.at[0], a_sem.at[0])]
    raws[0].start()
    for k in range(2):
        for cp in loads(k, k):
            cp.start()
    bias_cp = _copy(bias_hbm.at[0, 0], bias_v, b_sem)
    qt_s[HP:, :] = jnp.zeros((HP, T), BF16)
    wq = _stage_qkvg(0, hd, wq_hbm, w_s, q_sem)
    for cp in stage:
        cp.wait()
    for cp in wq:
        cp.wait()
    for r in (1, 2):
        raws[r].start()
    cond_cp = pltpu.make_async_copy(cond_hbm.at[p.z, mine], cond, b_sem)
    entered()
    ring = Ring(p, lambda b, ch: wg.at[b, 0:cut, :], w_recv, w_send)
    cross = Cross(p, wg, cut, rows_w, n_chunk, c_recv, c_near, c_far)
    cross1 = Cross(p, w1g, 0, rows_w, n_chunk, d_recv, None, d_far, spread=False)
    ring.own(0, wst.at[0:cut, :])
    cross.own(wst)

    def half(slot, dst):
        v = xn.at[slot, mine]
        return pltpu.make_async_remote_copy(src_ref=v, dst_ref=v, send_sem=n_send.at[slot], recv_sem=n_recv.at[slot],
                                            device_id={"tp": p.partner}, device_id_type=MESH)

    def normalise(slot):
        tile = 256 if R % 256 == 0 else R
        for i in range(R // tile):
            rows = pl.ds(i * tile, tile)
            cn = _ln(craw[slot, rows, :].astype(F32))
            y = _ada(xraw[slot, rows, :].astype(F32), cn, asc_ref[0, 0:1, :], aw_s[...], ab_ref[0, 0:1, :])
            xn[slot, pl.ds(pl.multiple_of(p.c * R, R) + i * tile, tile), :] = y

    raws[0].wait()
    aw_s[...] = _flat(raw.at[0])
    for cp in loads(0, 0):
        cp.wait()
    normalise(0)
    bias_cp.wait()
    half(0, p.partner).start()
    _load_bias(bias_v, mask_ref, bt)
    cond_cp.start()
    for cp in stage1:
        cp.wait()
    keep = _copy(wst1, w1g.at[p.me], k_sem)
    ex = Exchange(p, sample_of, o_s, o_out, o_send, o_recv)
    brow = _bias_row(bq_ref[0:1, :], hd)
    events = {}

    def plan(when, f, *args):
        events.setdefault((when % 2, when // 2), []).append((f, args))

    for h in range(1, p.nz // 2 + 1):
        plan(2 * h - 2, ring.service, h, 0)
        for ch in range(n_chunk):
            plan(n_chunk * (h - 1) + ch, cross.along, h, ch)
            plan(n_chunk * h + ch + 1, cross.across, h, ch)
            plan(n_chunk * h + ch + S // 2, cross1.along, h, ch)
    plan(n_chunk, cross1.own, wst1)

    def step(k, _):
        slot = lax.rem(k, 2)

        @pl.when(k + 2 < S)
        def _():
            for cp in loads(k + 2, slot):
                cp.start()

        with scope("b0_half"):
            v = xn.at[slot, pl.ds((1 - p.c) * R, R)]
            pltpu.make_async_copy(v, v, n_recv.at[slot]).wait()
            half(slot, p.partner).wait_send()
        at = Attend(n_tp, hd, w_s, brow, bt, k_s, qt_s, vt_s, gt_s, lg, o_s, lambda i, tile: xn[slot, pl.ds(i * tile, tile), :])
        with scope("b0_proj"):
            at.project()

        @pl.when(k + 2 < S)
        def _():
            pl.semaphore_signal(n_free, inc=1, device_id={"tp": p.partner}, device_id_type=MESH)

        @pl.when(k >= 1)
        def _():
            ex.start(k - 1)

        with scope("b0_norm"):
            @pl.when(k + 1 < S)
            def _():
                for cp in loads(k + 1, 1 - slot):
                    cp.wait()
                normalise(1 - slot)

                @pl.when(k >= 1)
                def _():
                    pl.semaphore_wait(n_free, 1)

        def take(part):
            with scope("b0_ev"):
                for (half_step, when), todo in sorted(events.items(), key=lambda e: e[0]):
                    if half_step == part:
                        @pl.when(k == when)
                        def _():
                            for f, args in todo:
                                f(*args)

        take(0)

        def hook():
            @pl.when(k + 1 < S)
            def _():
                half(1 - slot, p.partner).start()

        with scope("b0_att"):
            at.attend(k, hook)
        take(1)
        return 0

    lax.fori_loop(0, S, step, 0)
    ex.start(S - 1)
    raws[3].start()
    with scope("b0_mods"):
        wg[p.me] = wst[...]
        cond_cp.wait()
        cn = _ln(cond[...].astype(F32))
        raws[1].wait()
        aw_s[...] = _flat(raw.at[1])
        _gates(gate_out, cond[...], aw_s[...], zb_ref.at[0])
        for src, cp, l, j, out in ((2, raws[2], 0, 1, mod_out), (0, raws[3], 1, 0, nxt_out)):
            cp.wait()
            aw_s[...] = _flat(raw.at[src])
            _modulation(out, cn, asc_ref[l, j:j + 1, :], aw_s[...], ab_ref[l, j:j + 1, :])
    for (half_step, when), todo in sorted(events.items(), key=lambda e: (e[0][1], e[0][0])):
        if when >= S:
            for f, args in todo:
                f(*args)

    def other(i, _):
        ring.wait(i * 2 + (1 - p.c), 0)
        return 0

    with scope("b0_ring_end"):
        lax.fori_loop(0, p.nz, other, 0)
        ring.drain(wg.at[0:n_tp - 1, 0:cut, :])
    with scope("b0_cross_end"):
        cross.finish_near()
        cross.finish_far()
        cross1.finish_far()
        keep.wait()
    with scope("b0_arr"):
        ex.finish()


def _head_scratch(S, T, D, hd):
    v = pltpu.VMEM
    return [v((T, T), BF16), v((T, T), F32), v((4 * HP, D), BF16), v((T, 2 * HP), BF16), v((2 * HP, T), BF16), v((HP, T), BF16),
            v((hd, T), F32), v((2, T, QT), F32), v((S, hd, T), BF16)]


def _block0(n_dp, x, cond, pair_bias, mask_row, wq, bq, asc, aw, ab, zw, zb, wo, wup, wdn):
    S, T, D = x.shape
    C = cond.shape[-1]
    _, _, hd, _ = wq.shape
    hu = wdn.shape[1]
    n_tp = S * 2
    rows_w = hd + 3 * hu
    R = T // 2
    cut, n_chunk = hd, 3
    dma = pltpu.SemaphoreType.DMA
    return pl.pallas_call(
        functools.partial(_block0_kernel, (S, T, D, C, n_tp, n_dp, hd, hu, cut, n_chunk)),
        out_shape=(pltpu.VMEM((n_tp, hd, R), BF16), pltpu.VMEM((n_tp, rows_w, D), BF16),
                   *[pltpu.VMEM((R, 2 * D), F32)] * 3, pltpu.HBM((n_tp, rows_w, D), BF16)),
        in_specs=[ANY, ANY, ANY, VMEM, ANY, VMEM, VMEM, ANY, VMEM, ANY, VMEM, ANY, ANY, ANY],
        out_specs=(VMEM,) * 5 + (HBM,),
        scratch_shapes=[
            *_head_scratch(S, T, D, hd),
            pltpu.VMEM((2, R, D), BF16), pltpu.VMEM((2, R, C), BF16), pltpu.VMEM((2, T, D), BF16),
            pltpu.VMEM((3, C, 2, D), BF16), pltpu.VMEM((C, 2 * D), BF16), *[pltpu.VMEM((rows_w, D), BF16)] * 2, pltpu.VMEM((R, C), BF16),
            dma((2,)), dma((2,)), dma, dma((4,)), dma((3,)), dma((2, 4)), dma((S, 2)), dma, dma((2,)), dma((2,)), pltpu.SemaphoreType.REGULAR,
            dma, dma((n_tp, 1)), dma, dma((S,)), dma((n_tp, n_chunk)), dma, dma((S,)), dma((n_tp, n_chunk))],
        cost_estimate=pl.CostEstimate(flops=2 * S * T * (D * 4 * HP + 2 * T * 256 + C * D), bytes_accessed=S * T * (D + C), transcendentals=S * T * T),
        compiler_params=pltpu.CompilerParams(collective_id=0, has_side_effects=True, vmem_limit_bytes=VM0),
        name="block0",
    )(x, cond, pair_bias, mask_row, wq, bq, asc, aw, ab, zw, zb, wo, wup, wdn)


def _transition(dims, tile, gates, mod1, o_v, act, wall, y_s, h_s, rows):
    D, n_tp, hd, hu = dims
    w_o = wall[:, 0:hd, :].reshape(n_tp * hd, D)
    o_t = o_v[:, :, rows].reshape(n_tp * hd, tile)
    t = _dot(o_t, w_o, 0, 0).astype(BF16).astype(F32)
    mid = (act[rows, :].astype(F32) + gates[rows, :D] * t).astype(BF16).astype(F32)
    y_s[...] = (mod1[rows, :D] * _ln(mid) + mod1[rows, D:]).astype(BF16)
    step = 4 * hu
    for j in range(n_tp * hu // step):
        dv = slice(4 * j, 4 * j + 4)
        u1 = _dot(y_s[...], wall[dv, hd:hd + hu, :].reshape(step, D), 1, 1)
        u2 = _dot(y_s[...], wall[dv, hd + hu:hd + 2 * hu, :].reshape(step, D), 1, 1)
        h_s[:, j * step:(j + 1) * step] = (u1 * _sig(u1) * u2).astype(BF16)
    r = _dot(h_s[...], wall[:, hd + 2 * hu:hd + 3 * hu, :].reshape(n_tp * hu, D)).astype(BF16).astype(F32)
    return (mid + gates[rows, D:] * r).astype(BF16)


def _block1_kernel(dims, o0, w0, gate0, mod0, nxt0, act_hbm, cond_hbm, zw_hbm, zb_ref, asc_ref, aw_hbm, ab_ref, bias_hbm, mask_ref, wq_hbm, bq_ref, _,
                   w1, gate1, mod1, a_out, o_out, wg,
                   bias_v, bt, w_s, k_s, qt_s, vt_s, gt_s, lg, o_s, act, cond, raw, aw_s, y_s, h_s, xg,
                   l_sem, q_sem, wl_sem, x_send, x_recv, o_send, o_recv, c_near, c_far, c_recv):
    S, T, D, C, n_tp, n_dp, hd, hu = dims
    p = Place(n_tp, n_dp)
    entered = p.enter(True)
    R = S * T // n_tp
    row0 = p.me * R
    rows_w = hd + 3 * hu
    srcs = [(act_hbm.at[pl.ds(row0, R), :], act), (cond_hbm.at[pl.ds(row0, R), :], cond), (bias_hbm.at[1, 0], bias_v),
            (zw_hbm.at[1], raw.at[0]), (aw_hbm.at[1, 1], raw.at[1])]
    cps = [_copy(a, b, l_sem.at[i]) for i, (a, b) in enumerate(srcs)]
    qt_s[HP:, :] = jnp.zeros((HP, T), BF16)
    wq = _stage_qkvg(1, hd, wq_hbm, w_s, q_sem)
    cross = Cross(p, wg, 0, rows_w, 1, c_recv, c_near, c_far)
    cps[0].wait()
    tile = R // 2
    ring = Ring(p, lambda b, ch: xg.at[pl.ds(b * R + ch * tile, tile), :], x_recv, x_send,
                lambda ch: p.c + ch == 0)
    for ch in range(2):
        rows = pl.ds(ch * tile, tile)
        with scope("b1_mlp"):
            new = _transition((D, n_tp, hd, hu), tile, gate0, mod0, o0, act, w0, y_s, h_s, rows)
            a_out[rows, :] = new
            xg[pl.ds(row0 + ch * tile, tile), :] = (nxt0[rows, :D] * _ln(new.astype(F32)) + nxt0[rows, D:]).astype(BF16)
        if ch == 0:
            with scope("b1_enter"):
                entered()
        ring.own(ch)
        if ch == 0:
            cross.hand_on()
    with scope("b1_bias"):
        cps[2].wait()
        _load_bias(bias_v, mask_ref, bt)
    for cp in wq:
        cp.wait()
    brow = _bias_row(bq_ref[1:2, :], hd)
    turn = 1 - 2 * p.c

    def sample_of(j):
        h = (j + 1) // 2
        return lax.rem(p.z + S + turn * (1 - 2 * lax.rem(j, 2)) * h, S)

    ex = Exchange(p, sample_of, o_s, o_out, o_send, o_recv)

    def step(j, _):
        with scope("b1_svc"):
            ring.service(j // 2 + 1, lax.rem(j, 2))

        @pl.when((j >= 2) & (j <= p.nz // 2 + 1))
        def _():
            with scope("b1_x"):
                cross.across(j - 1, 0)

        @pl.when(j >= 1)
        def _():
            ex.start(j - 1)

        s = sample_of(j)
        with scope("b1_half"):
            for ch in range(2):
                ring.wait(s * 2 + (1 - p.c), ch)

        def x_rows(i, t):
            return xg[pl.ds(pl.multiple_of(s * T, T) + i * t, t), :]

        at = Attend(n_tp, hd, w_s, brow, bt, k_s, qt_s, vt_s, gt_s, lg, o_s, x_rows)
        with scope("b1_proj"):
            at.project()

        with scope("b1_att"):
            at.attend(j)

        @pl.when(j == 1)
        def _():
            cps[1].wait()
            cps[3].wait()
            aw_s[...] = _flat(raw.at[0])
            _gates(gate1, cond[...], aw_s[...], zb_ref.at[1])

        @pl.when(j == 3)
        def _():
            cps[4].wait()
            aw_s[...] = _flat(raw.at[1])
            cn = _ln(cond[...].astype(F32))
            _modulation(mod1, cn, asc_ref[1, 1:2, :], aw_s[...], ab_ref[1, 1:2, :])

        with scope("b1_fin"):
            @pl.when(j == S - 2)
            def _():
                cross.finish_near()
                pltpu.make_async_copy(wg, w1, wl_sem).start()

        return 0

    lax.fori_loop(0, S, step, 0)
    ex.start(S - 1)
    cross.finish_far(ring=False)
    pltpu.make_async_copy(wg, w1, wl_sem).wait()
    with scope("b1_drain"):
        ring.drain(xg.at[0:(n_tp - 1) * R, :])
    with scope("b1_arr"):
        ex.finish()


def _block1(n_dp, o0, w0, gate0, mod0, nxt0, act, cond, zw, zb, asc, aw, ab, pair_bias, mask_row, wq, bq, wg):
    n_tp, hd, R = o0.shape
    D = act.shape[-1]
    C = cond.shape[-1]
    S = n_tp // 2
    T = 2 * R
    rows_w = w0.shape[1]
    hu = (rows_w - hd) // 3
    dma = pltpu.SemaphoreType.DMA
    return pl.pallas_call(
        functools.partial(_block1_kernel, (S, T, D, C, n_tp, n_dp, hd, hu)),
        out_shape=(pltpu.VMEM((n_tp, rows_w, D), BF16), pltpu.VMEM((R, 2 * D), F32), pltpu.VMEM((R, 2 * D), F32),
                   pltpu.VMEM((R, D), BF16), pltpu.VMEM((n_tp, hd, R), BF16), pltpu.HBM((n_tp, rows_w, D), BF16)),
        in_specs=[VMEM, VMEM, VMEM, VMEM, VMEM, ANY, ANY, ANY, VMEM, VMEM, ANY, VMEM, ANY, VMEM, ANY, VMEM, HBM],
        out_specs=(VMEM,) * 5 + (HBM,),
        input_output_aliases={1: 0, 2: 1, 3: 2, 16: 5},
        scratch_shapes=[
            *_head_scratch(S, T, D, hd),
            pltpu.VMEM((R, D), BF16), pltpu.VMEM((R, C), BF16), pltpu.VMEM((2, C, 2, D), BF16), pltpu.VMEM((C, 2 * D), BF16),
            pltpu.VMEM((R // 2, D), BF16), pltpu.VMEM((R // 2, n_tp * hu), BF16), pltpu.VMEM((S * T, D), BF16),
            dma((5,)), dma((4,)), dma, dma, dma((n_tp, 2)), dma((S, 2)), dma, dma, dma((S,)), dma((n_tp, 1))],
        cost_estimate=pl.CostEstimate(flops=2 * S * T * (D * 4 * HP + 2 * T * 256), bytes_accessed=S * T * D * 2, transcendentals=S * T * T),
        compiler_params=pltpu.CompilerParams(collective_id=1, has_side_effects=True, vmem_limit_bytes=VM1),
        name="block1",
    )(o0, w0, gate0, mod0, nxt0, act, cond, zw, zb, asc, aw, ab, pair_bias, mask_row, wq, bq, wg)


def _last_kernel(dims, o_v, act, wall, gate, mod, out, y_s, h_s, x_send, x_recv):
    D, n_tp, n_dp, hd, hu, R = dims
    p = Place(n_tp, n_dp)
    entered = p.enter(False)
    tile = R // 2
    ring = Ring(p, lambda b, ch: out.at[pl.ds(b * R + ch * tile, tile), :], x_recv, x_send)
    for ch in range(2):
        rows = pl.ds(ch * tile, tile)
        with scope("l_mlp"):
            out[pl.ds(p.me * R + ch * tile, tile), :] = _transition((D, n_tp, hd, hu), tile, gate, mod, o_v, act, wall, y_s, h_s, rows)
        if ch == 0:
            entered()
        ring.own(ch)

    with scope("l_svc"):
        lax.fori_loop(0, p.nz, lambda e, _: (ring.service(e // 2 + 1, lax.rem(e, 2)), 0)[1], 0)

    def other(i, _):
        for ch in range(2):
            ring.wait(i * 2 + (1 - p.c), ch)
        return 0

    with scope("l_end"):
        lax.fori_loop(0, p.nz, other, 0)
    ring.drain(out.at[0:(n_tp - 1) * R, :])


def _last(n_dp, o, act, w1, gate, mod):
    n_tp, hd, R = o.shape
    D = act.shape[-1]
    hu = (w1.shape[1] - hd) // 3
    dma = pltpu.SemaphoreType.DMA
    return pl.pallas_call(
        functools.partial(_last_kernel, (D, n_tp, n_dp, hd, hu, R)),
        out_shape=pltpu.VMEM((n_tp * R, D), BF16),
        in_specs=[VMEM] * 5, out_specs=VMEM,
        scratch_shapes=[pltpu.VMEM((R // 2, D), BF16), pltpu.VMEM((R // 2, n_tp * hu), BF16), dma, dma((n_tp, 2))],
        cost_estimate=pl.CostEstimate(flops=2 * R * D * (D + 3 * n_tp * hu), bytes_accessed=w1.size, transcendentals=R * D),
        compiler_params=pltpu.CompilerParams(collective_id=2, has_side_effects=True, vmem_limit_bytes=VM2),
        name="last",
    )(o, act, w1, gate, mod)


def _store_kernel(src, dst, sem):
    cp = pltpu.make_async_copy(src, dst, sem)
    cp.start()
    cp.wait()


def _store(x):
    return pl.pallas_call(
        _store_kernel, out_shape=jax.ShapeDtypeStruct(x.shape, x.dtype), in_specs=[VMEM], out_specs=ANY,
        scratch_shapes=[pltpu.SemaphoreType.DMA], compiler_params=pltpu.CompilerParams(vmem_limit_bytes=1 << 20), name="store")(x)


def solution(mesh):
    n_dp = mesh.shape["dp"]

    def shard_body(token_act, token_cond, pair_bias, token_mask, ada_scale, ada_w, ada_bias, zero_w, zero_b, w_qkvg, b_q, w_o, w_up, w_down):
        S, T, D = token_act.shape
        C = token_cond.shape[-1]
        mask_row = token_mask.reshape(1, T)
        wq = jnp.transpose(w_qkvg, (0, 2, 3, 1))
        wup = jnp.transpose(w_up, (0, 2, 3, 1))
        act = token_act.reshape(S * T, D)
        cond = token_cond.reshape(S * T, C)
        o0, w0, gate0, mod0, nxt0, wg = _block0(n_dp, token_act, token_cond, pair_bias, mask_row, wq, b_q, ada_scale, ada_w, ada_bias, zero_w, zero_b, w_o, wup, w_down)
        o0, w0, gate0, mod0, nxt0 = (pltpu.with_memory_space_constraint(v, pltpu.VMEM) for v in (o0, w0, gate0, mod0, nxt0))
        w1, gate1, mod1, a1, o1, _ = _block1(n_dp, o0, w0, gate0, mod0, nxt0, act, cond, zero_w, zero_b, ada_scale, ada_w, ada_bias, pair_bias, mask_row, wq, b_q, wg)
        o1, a1, w1, gate1, mod1 = (pltpu.with_memory_space_constraint(v, pltpu.VMEM) for v in (o1, a1, w1, gate1, mod1))
        out = pltpu.with_memory_space_constraint(_last(n_dp, o1, a1, w1, gate1, mod1), pltpu.VMEM)
        return _store(out).reshape(S, T, D)

    everywhere = P()
    rows, second, fourth = P('dp'), P(None, 'tp'), P(*[None] * 3, 'tp')
    in_specs = (rows, rows, second) + (everywhere,) * 6 + (fourth, second, second, fourth, second)
    return jax.shard_map(shard_body, mesh=mesh, in_specs=in_specs, out_specs=rows, check_vma=False)
```

```python
import functools
import math

import jax
import jax.numpy as jnp
from jax import lax
from jax.experimental import pallas as pl
from jax.experimental.pallas import tpu as pltpu
from jax.sharding import PartitionSpec as P

LN_EPS = 1e-5
LOG2E = 1.4426950408889634
MESH = pl.DeviceIdType.MESH
BF16 = jnp.bfloat16
F32 = jnp.float32
scope = jax.named_scope
HP = 64
QT = 256
ANY = pl.BlockSpec(memory_space=pl.ANY)
VMEM = pl.BlockSpec(memory_space=pltpu.VMEM)
HBM = pl.BlockSpec(memory_space=pltpu.HBM)
VM = 50 << 20


def _ln(x):
    mean = jnp.mean(x, axis=-1, keepdims=True)
    cen = x - mean
    var = jnp.mean(cen * cen, axis=-1, keepdims=True)
    return cen * lax.rsqrt(var + LN_EPS)


def _sig(x):
    return 0.5 * jnp.tanh(0.5 * x) + 0.5


def _dot(a, b, ca=1, cb=0):
    return lax.dot_general(a, b, (((ca,), (cb,)), ((), ())), preferred_element_type=F32)


def _ada(x_f32, cond_normed, scale, w, bias):
    d = x_f32.shape[-1]
    mod = _dot((cond_normed * scale).astype(BF16), w)
    return (_sig(mod[:, :d] + bias) * _ln(x_f32) + mod[:, d:]).astype(BF16)


class Place:
    def __init__(self, n_tp, n_dp):
        self.n = n_tp
        self.n_dp = n_dp
        self.col = lax.axis_index("dp")
        self.nz = n_tp // 2
        self.me = lax.axis_index("tp")
        self.z = self.me // 2
        self.c = lax.rem(self.me, 2)
        self.partner = self.z * 2 + (1 - self.c)

    def at(self, off):
        return lax.rem(self.z + off + self.nz, self.nz) * 2 + self.c

    def column(self, i):
        return lax.rem(self.col + i, self.n_dp)

    def enter(self):
        barrier = pltpu.get_barrier_semaphore()
        peers = [{"tp": lax.rem(self.me + i, self.n)} for i in range(1, self.n)]
        peers += [{"dp": self.column(i), "tp": self.me} for i in range(1, self.n_dp)]
        for peer in peers:
            pl.semaphore_signal(barrier, inc=1, device_id=peer, device_id_type=MESH)
        return lambda: pl.semaphore_wait(barrier, len(peers))


class Ring:
    def __init__(self, place, view, recv_sem, send_sem, right=None):
        self.p, self.view, self.recv, self.send = place, view, recv_sem, send_sem
        self.far = place.nz // 2
        self.right = right or (lambda ch: place.c == 0)

    def _push(self, b, ch, dst, src=None):
        v = self.view(b, ch)
        pltpu.make_async_remote_copy(
            src_ref=v if src is None else src, dst_ref=v, send_sem=self.send, recv_sem=self.recv.at[b, ch],
            device_id={"tp": dst}, device_id_type=MESH).start()

    def own(self, ch, src=None):
        p = self.p
        self._push(p.me, ch, p.at(1), src)
        self._push(p.me, ch, p.at(-1), src)
        self._push(p.me, ch, p.partner, src)

    def wait(self, b, ch):
        v = self.view(b, ch)
        pltpu.make_async_copy(v, v, self.recv.at[b, ch]).wait()

    def service(self, h, ch):
        p = self.p
        right = self.right(ch)
        for sign, far in ((1, right), (-1, jnp.logical_not(right))):
            b = p.at(-sign * h)

            @pl.when((h < self.far) | far)
            def _():
                self.wait(b, ch)

                @pl.when((h < self.far - 1) | ((h == self.far - 1) & far))
                def _():
                    self._push(b, ch, p.at(sign))

                self._push(b, ch, p.partner)

    def drain(self, whole):
        pltpu.make_async_copy(whole, whole, self.send).wait()


class Cross:
    def __init__(self, place, buf, lo, hi, n_chunk, recv_sem, near_sem, far_sem, spread=True):
        self.p, self.buf, self.lo, self.hi, self.n_chunk, self.spread = place, buf, lo, hi, n_chunk, spread
        self.recv, self.near, self.far_sem = recv_sem, near_sem, far_sem
        self.far = place.nz // 2
        self.size = (hi - lo) // n_chunk

    def _rows(self, ch):
        return pl.ds(self.lo + ch * self.size, self.size)

    def _push(self, b, ch, dst, sem, src=None):
        v = self.buf.at[b, self._rows(ch), :]
        pltpu.make_async_remote_copy(
            src_ref=v if src is None else src, dst_ref=v, send_sem=sem, recv_sem=self.recv.at[b, ch],
            device_id=dst, device_id_type=MESH).start()

    def _push_over(self, b, ch, plane):
        p = self.p

        @pl.when(plane)
        def _():
            for i in range(1, p.n_dp):
                self._push(b, ch, {"dp": p.column(i), "tp": p.me}, self.far_sem.at[b // 2])

        self._push(b, ch, {"tp": p.partner}, self.near)

    def _mine(self, b):
        return lax.rem(b, self.p.n_dp) == self.p.col

    def own(self, src):
        p = self.p
        for ch in range(self.n_chunk):
            part = src.at[self._rows(ch), :]

            @pl.when(self._mine(p.me))
            def _():
                for off in (1, -1):
                    self._push(p.me, ch, {"tp": p.at(off)}, self.far_sem.at[p.z], part)

            if self.spread:
                self._push(p.me, ch, {"tp": p.partner}, self.near, part)

    def wait(self, b, ch):
        v = self.buf.at[b, self._rows(ch), :]
        pltpu.make_async_copy(v, v, self.recv.at[b, ch]).wait()

    def _each(self, h, body):
        p = self.p
        for sign, core in ((1, 0), (-1, 1)):
            b = p.at(-sign * h)

            @pl.when((h < self.far) | (p.c == core))
            def _():
                body(b, sign, (h < self.far - 1) | ((h == self.far - 1) & (p.c == core)))

    def along(self, h, ch):
        p = self.p

        def body(b, sign, onward):
            @pl.when(self._mine(b))
            def _():
                self.wait(b, ch)

                @pl.when(onward)
                def _():
                    self._push(b, ch, {"tp": p.at(sign)}, self.far_sem.at[b // 2])

                if self.spread:
                    self._push_over(b, ch, True)

        self._each(h, body)

    def hand_on(self):
        p = self.p

        def block(i, _):
            b = i * 2 + p.c

            @pl.when(self._mine(b) | (i == p.z))
            def _():
                for ch in range(self.n_chunk):
                    self._push_over(b, ch, i != p.z)
            return 0

        lax.fori_loop(0, p.nz, block, 0)

    def across(self, h, ch):
        p = self.p

        def body(b, sign, onward):
            @pl.when(jnp.logical_not(self._mine(b)))
            def _():
                self.wait(b, ch)
                self._push(b, ch, {"tp": p.partner}, self.near)

        self._each(h, body)

    def _sent(self, k, sem):
        if k:
            v = self.buf.at[0:k, self.lo:self.hi, :]
            pltpu.make_async_copy(v, v, sem).wait()

    def finish_near(self):
        p = self.p

        def other(i, _):
            for ch in range(self.n_chunk):
                self.wait(i * 2 + (1 - p.c), ch)
            return 0

        lax.fori_loop(0, p.nz, other, 0)
        self._sent(p.nz, self.near)

    def finish_far(self, ring=True):
        p = self.p
        over = p.n_dp - 1 if self.spread else 0
        if ring:
            @pl.when(self._mine(p.me))
            def _():
                self._sent(2, self.far_sem.at[p.z])

        def body(b, sign, onward):
            sem = self.far_sem.at[b // 2]

            @pl.when(self._mine(b))
            def _():
                if not ring:
                    self._sent(over, sem)
                else:
                    @pl.when(onward)
                    def _():
                        self._sent(over + 1, sem)

                    @pl.when(jnp.logical_not(onward))
                    def _():
                        self._sent(over, sem)

        def hop(h, _):
            self._each(h, body)
            return 0

        lax.fori_loop(1, self.far + 1, hop, 0)


def _copy(src, dst, sem):
    cp = pltpu.make_async_copy(src, dst, sem)
    cp.start()
    return cp


def _stage(l, hd, hu, wo_hbm, wup_hbm, wdn_hbm, wst, sem):
    cps, lo = [], 0
    for src, rows in ((wo_hbm.at[l], hd), (wup_hbm.at[l, 0], hu), (wup_hbm.at[l, 1], hu), (wdn_hbm.at[l], hu)):
        cps.append(_copy(src, wst.at[pl.ds(lo, rows), :], sem.at[len(cps)]))
        lo += rows
    return cps


def _stage_qkvg(l, hd, wq_hbm, w_s, sem):
    return [_copy(wq_hbm.at[l, f], w_s.at[pl.ds(i * HP, hd), :], sem.at[i]) for i, f in enumerate((1, 0, 2, 3))]


class Attend:
    def __init__(self, n_tp, hd, w, brow, bt, k_s, qt_s, vt_s, gt_s, lg, o_s, x_rows):
        self.__dict__.update(locals())
        self.T = bt.shape[0]

    def project(self):
        T, hd = self.T, self.hd
        tile = QT
        for i in range(T // tile):
            rows = pl.ds(i * tile, tile)
            res = _dot(self.x_rows(i, tile), self.w[...], 1, 1) + self.brow
            self.k_s[rows, :] = res[:, :2 * HP].astype(BF16)
            rest = res.T
            self.qt_s[0:HP, rows] = rest[HP:2 * HP].astype(BF16)
            ones = lax.broadcasted_iota(jnp.int32, (HP, tile), 0) == hd
            self.vt_s[:, rows] = jnp.where(ones, 1.0, rest[2 * HP:3 * HP]).astype(BF16)
            self.gt_s[:, rows] = _sig(rest[3 * HP:3 * HP + hd])

    def attend(self, slot, hook=None):
        T, hd = self.T, self.hd
        n = T // QT
        c1 = LOG2E / math.sqrt(hd)

        def scores(i):
            cols = pl.ds(i * QT, QT)
            logits = _dot(self.k_s[...], self.qt_s[:, cols]) * c1 + self.bt[:, cols]
            self.lg[i % 2] = logits
            return jnp.max(logits, axis=0, keepdims=True)

        top = scores(0)
        if hook is not None:
            hook()
        for i in range(n):
            cols = pl.ds(i * QT, QT)
            nxt = scores(i + 1) if i + 1 < n else None
            probs = jnp.exp2(self.lg[i % 2] - top).astype(BF16)
            mixed = _dot(self.vt_s[...], probs)
            self.o_s[slot, :, cols] = (self.gt_s[:, cols] * (mixed[:hd] / mixed[hd:hd + 1])).astype(BF16)
            top = nxt


def _load_bias(bias_v, mask_ref, bt):
    T = bt.shape[0]
    mask_add = (mask_ref[...].astype(F32) - 1.0) * 1e9

    def step(i, _):
        r = pl.multiple_of(i * 128, 128)
        rows = (bias_v[pl.ds(r, 128), :].astype(F32) + mask_add) * LOG2E
        bt[:, pl.ds(r, 128)] = rows.T
        return 0

    lax.fori_loop(0, T // 128, step, 0)


class Exchange:
    def __init__(self, place, sample_of, o_s, o_out, send_sem, recv_sem):
        self.p, self.sample_of, self.o_s, self.o_out, self.send, self.recv = place, sample_of, o_s, o_out, send_sem, recv_sem
        self.half = o_s.shape[-1] // 2

    def _each(self, k, remote, local):
        p = self.p
        for c in range(2):
            dst = self.sample_of(k) * 2 + c
            src = self.o_s.at[k, :, pl.ds(c * self.half, self.half)]
            sem = self.send.at[k, c]
            cp = pltpu.make_async_remote_copy(
                src_ref=src, dst_ref=self.o_out.at[p.me], send_sem=sem, recv_sem=self.recv,
                device_id={"tp": dst}, device_id_type=MESH)

            @pl.when(dst != p.me)
            def _():
                remote(cp)

            @pl.when(dst == p.me)
            def _():
                local(pltpu.make_async_copy(src, self.o_out.at[p.me], sem))

    def start(self, k):
        self._each(k, lambda cp: cp.start(), lambda cp: cp.start())

    def sent(self):
        def one(k, _):
            self._each(k, lambda cp: cp.wait_send(), lambda cp: cp.wait())
            return 0

        lax.fori_loop(0, self.o_s.shape[0], one, 0)

    def arrived(self):
        rest = self.o_out.at[0:self.p.n - 1]
        pltpu.make_async_copy(rest, rest, self.recv).wait()


def _bias_row(bq, hd):
    return jnp.concatenate([jnp.zeros((1, HP), F32), bq, jnp.zeros((1, 3 * HP - hd), F32)], axis=1)


def _gates(out, cond, w, bias):
    d = bias.shape[-1]
    out[...] = _dot(cond, w)
    for j in range(bias.shape[0]):
        cols = pl.ds(j * d, d)
        out[:, cols] = _sig(out[:, cols] + bias[j:j + 1, :])


def _modulation(out, cond_normed, scale, w, bias):
    d = bias.shape[-1]
    out[...] = _dot((cond_normed * scale).astype(BF16), w)
    out[:, :d] = _sig(out[:, :d] + bias)


def _flat(raw):
    c, two, d = raw.shape
    return raw[...].reshape(c, two * d)


def _transition(dims, tile, gates, mod1, o_v, act, wall, y_s, h_s, rows):
    D, n_tp, hd, hu = dims
    w_o = wall[:, 0:hd, :].reshape(n_tp * hd, D)
    o_t = o_v[:, :, rows].reshape(n_tp * hd, tile)
    t = _dot(o_t, w_o, 0, 0).astype(BF16).astype(F32)
    mid = (act[rows, :].astype(F32) + gates[rows, :D] * t).astype(BF16).astype(F32)
    y_s[...] = (mod1[rows, :D] * _ln(mid) + mod1[rows, D:]).astype(BF16)
    step = 4 * hu
    for j in range(n_tp * hu // step):
        dv = slice(4 * j, 4 * j + 4)
        u1 = _dot(y_s[...], wall[dv, hd:hd + hu, :].reshape(step, D), 1, 1)
        u2 = _dot(y_s[...], wall[dv, hd + hu:hd + 2 * hu, :].reshape(step, D), 1, 1)
        h_s[:, j * step:(j + 1) * step] = (u1 * _sig(u1) * u2).astype(BF16)
    r = _dot(h_s[...], wall[:, hd + 2 * hu:hd + 3 * hu, :].reshape(n_tp * hu, D)).astype(BF16).astype(F32)
    return (mid + gates[rows, D:] * r).astype(BF16)


def _main_kernel(dims, x_hbm, cond_hbm, bias_hbm, mask_ref, wq_hbm, bq_ref, asc_ref, aw_hbm, ab_ref, zw_hbm, zb_ref, wo_hbm, wup_hbm, wdn_hbm,
                 xg, w1g,
                 bias_v, bt, w_s, k_s, qt_s, vt_s, gt_s, lg, o_s, xraw, craw, xn, raw, aw_s, flat_s, wst, wst1, cond, act, y_s, h_s,
                 wall, gate, mod, nxt, o0, o1,
                 ld_sem, cd_sem, b_sem, q_sem, a_sem, st_sem, own_sem, k_sem, n_send, n_recv, n_free,
                 o_send, o_recv, w_send, w_recv, c_near, c_far, c_recv, d_near, d_far, d_recv, x_send, x_recv, r_send, r_recv, ready):
    S, T, D, C, n_tp, n_dp, hd, hu, n_chunk = dims
    p = Place(n_tp, n_dp)
    entered = p.enter()
    far = p.nz // 2
    rows_w = hd + 3 * hu
    R = S * T // n_tp
    row0 = p.me * R
    tile = R // 2
    mine = pl.ds(p.c * R, R)
    stage = [_stage(l, hd, hu, wo_hbm, wup_hbm, wdn_hbm, w, st_sem.at[l]) for l, w in enumerate((wst, wst1))]

    def toward(k):
        j = S - 1 - k
        return lax.rem(p.z + S + (1 - 2 * lax.rem(j, 2)) * ((j + 1) // 2), S)

    def outward(j):
        return lax.rem(p.z + S + (1 - 2 * p.c) * (1 - 2 * lax.rem(j, 2)) * ((j + 1) // 2), S)

    def loads(k, slot):
        s = toward(k)
        return [pltpu.make_async_copy(x_hbm.at[s, mine], xraw.at[slot], ld_sem.at[slot]),
                pltpu.make_async_copy(cond_hbm.at[s, mine], craw.at[slot], cd_sem.at[slot])]

    raw0 = _copy(aw_hbm.at[0, 0], raw.at[0], a_sem.at[0])
    for k in range(2):
        for cp in loads(k, k):
            cp.start()
    bias_cp = _copy(bias_hbm.at[0, 0], bias_v, b_sem)
    w_s[...] = jnp.zeros_like(w_s)
    qt_s[HP:, :] = jnp.zeros((HP, T), BF16)
    wq = _stage_qkvg(0, hd, wq_hbm, w_s, q_sem)
    for cp in stage[0]:
        cp.wait()
    for cp in wq:
        cp.wait()
    raws = [_copy(src, raw.at[i + 1], a_sem.at[i + 1]) for i, src in enumerate((zw_hbm.at[0], aw_hbm.at[0, 1], aw_hbm.at[1, 0]))]
    own = [_copy(cond_hbm.at[p.z, mine], cond, own_sem.at[0]), _copy(x_hbm.at[p.z, mine], act, own_sem.at[1])]
    entered()
    ring_o = Ring(p, lambda b, ch: wall.at[b, 0:hd, :], w_recv, w_send)
    cross = Cross(p, wall, hd, rows_w, n_chunk, c_recv, c_near, c_far)
    cross1 = Cross(p, w1g, 0, rows_w, n_chunk, d_recv, d_near, d_far)
    ring_x = Ring(p, lambda b, ch: xg.at[pl.ds(b * R + ch * tile, tile), :], x_recv, x_send)
    ring_r = Ring(p, lambda b, ch: xg.at[pl.ds(b * R + ch * tile, tile), :], r_recv, r_send)
    ring_o.own(0, wst.at[0:hd, :])
    cross.own(wst)

    def half(slot):
        v = xn.at[slot, mine]
        return pltpu.make_async_remote_copy(src_ref=v, dst_ref=v, send_sem=n_send.at[slot], recv_sem=n_recv.at[slot],
                                            device_id={"tp": p.partner}, device_id_type=MESH)

    def normalise(slot):
        for i in range(2):
            rows = pl.ds(i * tile, tile)
            cn = _ln(craw[slot, rows, :].astype(F32))
            y = _ada(xraw[slot, rows, :].astype(F32), cn, asc_ref[0, 0:1, :], aw_s[...], ab_ref[0, 0:1, :])
            xn[slot, pl.ds(pl.multiple_of(p.c * R, R) + i * tile, tile), :] = y

    raw0.wait()
    aw_s[...] = _flat(raw.at[0])
    for cp in loads(0, 0):
        cp.wait()
    normalise(0)
    bias_cp.wait()
    half(0).start()
    _load_bias(bias_v, mask_ref, bt)
    bias_cp = _copy(bias_hbm.at[1, 0], bias_v, b_sem)
    for cp in stage[1]:
        cp.wait()
    wall[p.me] = wst[...]
    keep = _copy(wst1, w1g.at[p.me], k_sem)

    def gates(l, i):
        raws[i].wait()
        flat_s[...] = _flat(raw.at[i + 1])
        _gates(gate, cond[...], flat_s[...], zb_ref.at[l])

    def modulation(out, l, j, i):
        raws[i].wait()
        flat_s[...] = _flat(raw.at[i + 1])
        cn = _ln(cond[...].astype(F32))
        _modulation(out, cn, asc_ref[l, j:j + 1, :], flat_s[...], ab_ref[l, j:j + 1, :])

    events = {}

    def plan(when, f, *args):
        events.setdefault(when, []).append((f, args))

    def take(step, k):
        for when in sorted(events):
            if when % 2 == step:
                @pl.when(k == when // 2)
                def _():
                    for f, args in events[when]:
                        f(*args)

    for h in range(1, far + 1):
        plan(n_chunk * (h - 1), ring_o.service, h, 0)
        for ch in range(n_chunk):
            plan(n_chunk * (h - 1) + ch, cross.along, h, ch)
            plan(n_chunk * h + ch + 1, cross.across, h, ch)
    for ch in range(n_chunk):
        plan(2 * S - n_chunk + ch, cross1.along, 1, ch)
    plan(2 * S - 2 * n_chunk, cross1.own, wst1)
    for cp in own:
        plan(3, cp.wait)
    plan(5, gates, 0, 0)
    plan(7, modulation, mod, 0, 1, 1)
    plan(9, modulation, nxt, 1, 0, 2)
    ex = [Exchange(p, order, o_s, o, o_send.at[l], o_recv.at[l]) for l, (order, o) in enumerate(((toward, o0), (outward, o1)))]
    brow = [_bias_row(bq_ref[l:l + 1, :], hd) for l in range(2)]
    heads = (n_tp, hd, w_s)
    work = (bt, k_s, qt_s, vt_s, gt_s, lg, o_s)

    def step0(k, _):
        slot = lax.rem(k, 2)

        @pl.when(k + 2 < S)
        def _():
            for cp in loads(k + 2, slot):
                cp.start()

        with scope("a_half"):
            v = xn.at[slot, pl.ds((1 - p.c) * R, R)]
            pltpu.make_async_copy(v, v, n_recv.at[slot]).wait()
            half(slot).wait_send()
        at = Attend(*heads, brow[0], *work, lambda i, t: xn[slot, pl.ds(i * t, t), :])
        at.project()

        @pl.when(k + 2 < S)
        def _():
            pl.semaphore_signal(n_free, inc=1, device_id={"tp": p.partner}, device_id_type=MESH)

        @pl.when(k >= 1)
        def _():
            ex[0].start(k - 1)

        @pl.when(k + 1 < S)
        def _():
            for cp in loads(k + 1, 1 - slot):
                cp.wait()
            normalise(1 - slot)

            @pl.when(k >= 1)
            def _():
                pl.semaphore_wait(n_free, 1)

        with scope("a_ev0"):
            take(0, k)

        def hook():
            @pl.when(k + 1 < S)
            def _():
                half(1 - slot).start()

        with scope("a_att"):
            at.attend(k, hook)
        with scope("a_ev1"):
            take(1, k)
        return 0

    lax.fori_loop(0, S, step0, 0)
    ex[0].start(S - 1)
    wq = _stage_qkvg(1, hd, wq_hbm, w_s, q_sem)
    raws = [_copy(src, raw.at[i + 1], a_sem.at[i + 1]) for i, src in enumerate((zw_hbm.at[1], aw_hbm.at[1, 1]))]
    for when in sorted(events):
        if when >= 2 * S:
            for f, args in events[when]:
                f(*args)

    def other(i, _):
        ring_o.wait(i * 2 + (1 - p.c), 0)
        return 0

    with scope("b_w0"):
        lax.fori_loop(0, p.nz, other, 0)
        cross.finish_near()
    with scope("b_o0"):
        ex[0].sent()
        ex[0].arrived()
    size = (D, n_tp, hd, hu)
    for ch in range(2):
        rows = pl.ds(ch * tile, tile)
        with scope("b_mlp"):
            new = _transition(size, tile, gate, mod, o0, act, wall, y_s, h_s, rows)
            act[rows, :] = new
            xg[pl.ds(row0 + ch * tile, tile), :] = (nxt[rows, :D] * _ln(new.astype(F32)) + nxt[rows, D:]).astype(BF16)
        ring_x.own(ch)
        if ch == 0:
            with scope("b_along"):
                for i in range(n_chunk):
                    cross1.along(2, i)
    bias_cp.wait()
    _load_bias(bias_v, mask_ref, bt)
    for cp in wq:
        cp.wait()
    ring_o.drain(wall.at[0:n_tp - 1, 0:hd, :])
    cross.finish_far()
    keep.wait()
    events = {}
    for ch in range(n_chunk):
        plan(1, cross1.along, far - 1, ch)
        plan(5, cross1.along, far, ch)
        for h in range(1, far + 1):
            plan(2 * h + 3, cross1.across, h, ch)
    plan(3, gates, 1, 0)
    plan(7, modulation, mod, 1, 1, 1)

    def last_weights():
        cross1.finish_near()
        pltpu.make_async_copy(w1g, wall, k_sem).start()

    plan(2 * S - 3, last_weights)

    def step1(j, _):
        with scope("b_svc"):
            ring_x.service(j // 2 + 1, lax.rem(j, 2))

        @pl.when(j >= 1)
        def _():
            ex[1].start(j - 1)

        s = outward(j)
        with scope("b_half"):
            for ch in range(2):
                ring_x.wait(s * 2 + (1 - p.c), ch)
        at = Attend(*heads, brow[1], *work, lambda i, t: xg[pl.ds(pl.multiple_of(s * T, T) + i * t, t), :])
        with scope("b_att"):
            at.project()
            at.attend(j)
        with scope("b_ev"):
            take(1, j)
        return 0

    lax.fori_loop(0, S, step1, 0)
    ex[1].start(S - 1)
    pltpu.make_async_copy(w1g, wall, k_sem).wait()
    cross1.finish_far()
    ring_x.drain(xg.at[0:(n_tp - 1) * R, :])
    for peer in (p.at(1), p.at(-1), p.partner):
        pl.semaphore_signal(ready, inc=1, device_id={"tp": peer}, device_id_type=MESH)
    with scope("c_o1"):
        ex[1].sent()
        ex[1].arrived()
    for ch in range(2):
        rows = pl.ds(ch * tile, tile)
        with scope("c_mlp"):
            xg[pl.ds(row0 + ch * tile, tile), :] = _transition(size, tile, gate, mod, o1, act, wall, y_s, h_s, rows)
        if ch == 0:
            with scope("c_ready"):
                pl.semaphore_wait(ready, 3)
        ring_r.own(ch)
    with scope("c_svc"):
        lax.fori_loop(0, p.nz, lambda e, _: (ring_r.service(e // 2 + 1, lax.rem(e, 2)), 0)[1], 0)

    def rest(i, _):
        for ch in range(2):
            ring_r.wait(i * 2 + (1 - p.c), ch)
        return 0

    with scope("c_end"):
        lax.fori_loop(0, p.nz, rest, 0)
        ring_r.drain(xg.at[0:(n_tp - 1) * R, :])


def _main(n_dp, x, cond, pair_bias, mask_row, wq, bq, asc, aw, ab, zw, zb, wo, wup, wdn):
    S, T, D = x.shape
    C = cond.shape[-1]
    hd, hu = wq.shape[2], wdn.shape[1]
    n_tp = S * 2
    rows_w = hd + 3 * hu
    R = T // 2
    n_chunk = 3
    dma = pltpu.SemaphoreType.DMA
    v = pltpu.VMEM
    pair, blocks, each = dma((2,)), dma((S,)), dma((n_tp, n_chunk))
    halves = dma((n_tp, 2))
    return pl.pallas_call(
        functools.partial(_main_kernel, (S, T, D, C, n_tp, n_dp, hd, hu, n_chunk)),
        out_shape=(v((n_tp * R, D), BF16), pltpu.HBM((n_tp, rows_w, D), BF16)),
        in_specs=[ANY, ANY, ANY, VMEM, ANY, VMEM, VMEM, ANY, VMEM, ANY, VMEM, ANY, ANY, ANY],
        out_specs=(VMEM, HBM),
        scratch_shapes=[
            v((T, T), BF16), v((T, T), F32), v((4 * HP, D), BF16), v((T, 2 * HP), BF16), v((2 * HP, T), BF16), v((HP, T), BF16),
            v((hd, T), F32), v((2, T, QT), F32), v((S, hd, T), BF16),
            v((2, R, D), BF16), v((2, R, C), BF16), v((2, T, D), BF16), v((4, C, 2, D), BF16), *[v((C, 2 * D), BF16)] * 2,
            *[v((rows_w, D), BF16)] * 2, v((R, C), BF16), v((R, D), BF16), v((R // 2, D), BF16), v((R // 2, n_tp * hu), BF16),
            v((n_tp, rows_w, D), BF16), *[v((R, 2 * D), F32)] * 3, *[v((n_tp, hd, R), BF16)] * 2,
            pair, pair, dma, dma((4,)), dma((4,)), dma((2, 4)), pair, dma, pair, pair, pltpu.SemaphoreType.REGULAR,
            dma((2, S, 2)), pair, dma, dma((n_tp, 1)), dma, blocks, each, dma, blocks, each, dma, halves, dma, halves, pltpu.SemaphoreType.REGULAR],
        cost_estimate=pl.CostEstimate(flops=S * T * T * D, bytes_accessed=S * T * D, transcendentals=S * T * T),
        compiler_params=pltpu.CompilerParams(collective_id=0, has_side_effects=True, vmem_limit_bytes=VM),
        name="blocks",
    )(x, cond, pair_bias, mask_row, wq, bq, asc, aw, ab, zw, zb, wo, wup, wdn)


def _store_kernel(src, dst, sem):
    cp = pltpu.make_async_copy(src, dst, sem)
    cp.start()
    cp.wait()


def _store(x):
    return pl.pallas_call(
        _store_kernel, out_shape=jax.ShapeDtypeStruct(x.shape, x.dtype), in_specs=[VMEM], out_specs=ANY,
        scratch_shapes=[pltpu.SemaphoreType.DMA], compiler_params=pltpu.CompilerParams(vmem_limit_bytes=1 << 20), name="store")(x)


def solution(mesh):
    n_dp = mesh.shape["dp"]

    def shard_body(token_act, token_cond, pair_bias, token_mask, ada_scale, ada_w, ada_bias, zero_w, zero_b, w_qkvg, b_q, w_o, w_up, w_down):
        S, T, D = token_act.shape
        mask_row = token_mask.reshape(1, T)
        wq = jnp.transpose(w_qkvg, (0, 2, 3, 1))
        wup = jnp.transpose(w_up, (0, 2, 3, 1))
        out, _ = _main(n_dp, token_act, token_cond, pair_bias, mask_row, wq, b_q, ada_scale, ada_w, ada_bias, zero_w, zero_b, w_o, wup, w_down)
        out = pltpu.with_memory_space_constraint(out, pltpu.VMEM)
        return _store(out).reshape(S, T, D)

    everywhere = P()
    rows, second, fourth = P('dp'), P(None, 'tp'), P(*[None] * 3, 'tp')
    in_specs = (rows, rows, second) + (everywhere,) * 6 + (fourth, second, second, fourth, second)
    return jax.shard_map(shard_body, mesh=mesh, in_specs=in_specs, out_specs=rows, check_vma=False)
```

```python
import functools
import math

import jax
import jax.numpy as jnp
from jax import lax
from jax.experimental import pallas as pl
from jax.experimental.pallas import tpu as pltpu
from jax.sharding import PartitionSpec as P

LN_EPS = 1e-5
LOG2E = 1.4426950408889634
MESH = pl.DeviceIdType.MESH
BF16 = jnp.bfloat16
F32 = jnp.float32
scope = jax.named_scope
HP = 64
QT = 256
ANY = pl.BlockSpec(memory_space=pl.ANY)
VMEM = pl.BlockSpec(memory_space=pltpu.VMEM)
HBM = pl.BlockSpec(memory_space=pltpu.HBM)
VM = 50 << 20


def _ln(x):
    mean = jnp.mean(x, axis=-1, keepdims=True)
    cen = x - mean
    var = jnp.mean(cen * cen, axis=-1, keepdims=True)
    return cen * lax.rsqrt(var + LN_EPS)


def _sig(x):
    return 0.5 * jnp.tanh(0.5 * x) + 0.5


def _dot(a, b, ca=1, cb=0):
    return lax.dot_general(a, b, (((ca,), (cb,)), ((), ())), preferred_element_type=F32)


def _ada(x_f32, cond_normed, scale, w, bias):
    d = x_f32.shape[-1]
    mod = _dot((cond_normed * scale).astype(BF16), w)
    return (_sig(mod[:, :d] + bias) * _ln(x_f32) + mod[:, d:]).astype(BF16)


class Place:
    def __init__(self, n_tp, n_dp):
        self.n = n_tp
        self.n_dp = n_dp
        self.col = lax.axis_index("dp")
        self.nz = n_tp // 2
        self.me = lax.axis_index("tp")
        self.z = self.me // 2
        self.c = lax.rem(self.me, 2)
        self.partner = self.z * 2 + (1 - self.c)

    def at(self, off):
        return lax.rem(self.z + off + self.nz, self.nz) * 2 + self.c

    def column(self, i):
        return lax.rem(self.col + i, self.n_dp)

    def enter(self):
        barrier = pltpu.get_barrier_semaphore()
        peers = [{"tp": lax.rem(self.me + i, self.n)} for i in range(1, self.n)]
        peers += [{"dp": self.column(i), "tp": self.me} for i in range(1, self.n_dp)]
        for peer in peers:
            pl.semaphore_signal(barrier, inc=1, device_id=peer, device_id_type=MESH)
        return lambda: pl.semaphore_wait(barrier, len(peers))


class Ring:
    def __init__(self, place, view, recv_sem, send_sem, right=None):
        self.p, self.view, self.recv, self.send = place, view, recv_sem, send_sem
        self.far = place.nz // 2
        self.right = right or (lambda ch: place.c == 0)

    def _push(self, b, ch, dst, src=None):
        v = self.view(b, ch)
        pltpu.make_async_remote_copy(
            src_ref=v if src is None else src, dst_ref=v, send_sem=self.send, recv_sem=self.recv.at[b, ch],
            device_id={"tp": dst}, device_id_type=MESH).start()

    def own(self, ch, src=None):
        p = self.p
        self._push(p.me, ch, p.at(1), src)
        self._push(p.me, ch, p.at(-1), src)
        self._push(p.me, ch, p.partner, src)

    def wait(self, b, ch):
        v = self.view(b, ch)
        pltpu.make_async_copy(v, v, self.recv.at[b, ch]).wait()

    def service(self, h, ch):
        p = self.p
        right = self.right(ch)
        for sign, far in ((1, right), (-1, jnp.logical_not(right))):
            b = p.at(-sign * h)

            @pl.when((h < self.far) | far)
            def _():
                self.wait(b, ch)

                @pl.when((h < self.far - 1) | ((h == self.far - 1) & far))
                def _():
                    self._push(b, ch, p.at(sign))

                self._push(b, ch, p.partner)

    def drain(self, whole):
        pltpu.make_async_copy(whole, whole, self.send).wait()


class Cross:
    def __init__(self, place, buf, lo, hi, n_chunk, recv_sem, near_sem, far_sem, spread=True):
        self.p, self.buf, self.lo, self.hi, self.n_chunk, self.spread = place, buf, lo, hi, n_chunk, spread
        self.recv, self.near, self.far_sem = recv_sem, near_sem, far_sem
        self.far = place.nz // 2
        self.size = (hi - lo) // n_chunk

    def _rows(self, ch):
        return pl.ds(self.lo + ch * self.size, self.size)

    def _push(self, b, ch, dst, sem, src=None):
        v = self.buf.at[b, self._rows(ch), :]
        pltpu.make_async_remote_copy(
            src_ref=v if src is None else src, dst_ref=v, send_sem=sem, recv_sem=self.recv.at[b, ch],
            device_id=dst, device_id_type=MESH).start()

    def _push_over(self, b, ch, plane):
        p = self.p

        @pl.when(plane)
        def _():
            for i in range(1, p.n_dp):
                self._push(b, ch, {"dp": p.column(i), "tp": p.me}, self.far_sem.at[b // 2])

        self._push(b, ch, {"tp": p.partner}, self.near)

    def _mine(self, b):
        return lax.rem(b, self.p.n_dp) == self.p.col

    def own(self, src):
        p = self.p
        for ch in range(self.n_chunk):
            part = src.at[self._rows(ch), :]

            @pl.when(self._mine(p.me))
            def _():
                for off in (1, -1):
                    self._push(p.me, ch, {"tp": p.at(off)}, self.far_sem.at[p.z], part)

            if self.spread:
                self._push(p.me, ch, {"tp": p.partner}, self.near, part)

    def wait(self, b, ch):
        v = self.buf.at[b, self._rows(ch), :]
        pltpu.make_async_copy(v, v, self.recv.at[b, ch]).wait()

    def _each(self, h, body):
        p = self.p
        for sign, core in ((1, 0), (-1, 1)):
            b = p.at(-sign * h)

            @pl.when((h < self.far) | (p.c == core))
            def _():
                body(b, sign, (h < self.far - 1) | ((h == self.far - 1) & (p.c == core)))

    def along(self, h, ch):
        p = self.p

        def body(b, sign, onward):
            @pl.when(self._mine(b))
            def _():
                self.wait(b, ch)

                @pl.when(onward)
                def _():
                    self._push(b, ch, {"tp": p.at(sign)}, self.far_sem.at[b // 2])

                if self.spread:
                    self._push_over(b, ch, True)

        self._each(h, body)

    def hand_on(self):
        p = self.p

        def block(i, _):
            b = i * 2 + p.c

            @pl.when(self._mine(b) | (i == p.z))
            def _():
                for ch in range(self.n_chunk):
                    self._push_over(b, ch, i != p.z)
            return 0

        lax.fori_loop(0, p.nz, block, 0)

    def across(self, h, ch):
        p = self.p

        def body(b, sign, onward):
            @pl.when(jnp.logical_not(self._mine(b)))
            def _():
                self.wait(b, ch)
                self._push(b, ch, {"tp": p.partner}, self.near)

        self._each(h, body)

    def _sent(self, k, sem):
        if k:
            v = self.buf.at[0:k, self.lo:self.hi, :]
            pltpu.make_async_copy(v, v, sem).wait()

    def finish_near(self):
        p = self.p

        def other(i, _):
            for ch in range(self.n_chunk):
                self.wait(i * 2 + (1 - p.c), ch)
            return 0

        lax.fori_loop(0, p.nz, other, 0)
        self._sent(p.nz, self.near)

    def finish_far(self, ring=True):
        p = self.p
        over = p.n_dp - 1 if self.spread else 0
        if ring:
            @pl.when(self._mine(p.me))
            def _():
                self._sent(2, self.far_sem.at[p.z])

        def body(b, sign, onward):
            sem = self.far_sem.at[b // 2]

            @pl.when(self._mine(b))
            def _():
                if not ring:
                    self._sent(over, sem)
                else:
                    @pl.when(onward)
                    def _():
                        self._sent(over + 1, sem)

                    @pl.when(jnp.logical_not(onward))
                    def _():
                        self._sent(over, sem)

        def hop(h, _):
            self._each(h, body)
            return 0

        lax.fori_loop(1, self.far + 1, hop, 0)


def _copy(src, dst, sem):
    cp = pltpu.make_async_copy(src, dst, sem)
    cp.start()
    return cp


def _stage(l, hd, hu, wo_hbm, wup_hbm, wdn_hbm, wst, sem):
    cps, lo = [], 0
    for src, rows in ((wo_hbm.at[l], hd), (wup_hbm.at[l, 0], hu), (wup_hbm.at[l, 1], hu), (wdn_hbm.at[l], hu)):
        cps.append(_copy(src, wst.at[pl.ds(lo, rows), :], sem.at[len(cps)]))
        lo += rows
    return cps


def _stage_qkvg(l, hd, wq_hbm, w_s, sem):
    return [_copy(wq_hbm.at[l, f], w_s.at[pl.ds(i * HP, hd), :], sem.at[i]) for i, f in enumerate((1, 0, 2, 3))]


class Attend:
    def __init__(self, n_tp, hd, w, brow, bt, k_s, qt_s, vt_s, gt_s, lg, o_s, x_rows):
        self.__dict__.update(locals())
        self.T = bt.shape[0]

    def project(self):
        T, hd = self.T, self.hd
        tile = QT
        for i in range(T // tile):
            rows = pl.ds(i * tile, tile)
            res = _dot(self.x_rows(i, tile), self.w[...], 1, 1) + self.brow
            self.k_s[rows, :] = res[:, :2 * HP].astype(BF16)
            rest = res.T
            self.qt_s[0:HP, rows] = rest[HP:2 * HP].astype(BF16)
            ones = lax.broadcasted_iota(jnp.int32, (HP, tile), 0) == hd
            self.vt_s[:, rows] = jnp.where(ones, 1.0, rest[2 * HP:3 * HP]).astype(BF16)
            self.gt_s[:, rows] = _sig(rest[3 * HP:3 * HP + hd])

    def attend(self, slot, hook=None):
        T, hd = self.T, self.hd
        n = T // QT
        c1 = LOG2E / math.sqrt(hd)

        def scores(i):
            cols = pl.ds(i * QT, QT)
            logits = _dot(self.k_s[...], self.qt_s[:, cols]) * c1 + self.bt[:, cols]
            self.lg[i % 2] = logits
            return jnp.max(logits, axis=0, keepdims=True)

        top = scores(0)
        if hook is not None:
            hook()
        for i in range(n):
            cols = pl.ds(i * QT, QT)
            nxt = scores(i + 1) if i + 1 < n else None
            probs = jnp.exp2(self.lg[i % 2] - top).astype(BF16)
            mixed = _dot(self.vt_s[...], probs)
            self.o_s[slot, :, cols] = (self.gt_s[:, cols] * (mixed[:hd] / mixed[hd:hd + 1])).astype(BF16)
            top = nxt


def _load_bias(bias_v, mask_ref, bt):
    T = bt.shape[0]
    mask_add = (mask_ref[...].astype(F32) - 1.0) * 1e9

    def step(i, _):
        r = pl.multiple_of(i * 128, 128)
        rows = (bias_v[pl.ds(r, 128), :].astype(F32) + mask_add) * LOG2E
        bt[:, pl.ds(r, 128)] = rows.T
        return 0

    lax.fori_loop(0, T // 128, step, 0)


class Exchange:
    def __init__(self, place, sample_of, o_s, o_out, send_sem, recv_sem):
        self.p, self.sample_of, self.o_s, self.o_out, self.send, self.recv = place, sample_of, o_s, o_out, send_sem, recv_sem
        self.half = o_s.shape[-1] // 2

    def _each(self, k, remote, local):
        p = self.p
        for c in range(2):
            dst = self.sample_of(k) * 2 + c
            src = self.o_s.at[k, :, pl.ds(c * self.half, self.half)]
            sem = self.send.at[k, c]
            cp = pltpu.make_async_remote_copy(
                src_ref=src, dst_ref=self.o_out.at[p.me], send_sem=sem, recv_sem=self.recv,
                device_id={"tp": dst}, device_id_type=MESH)

            @pl.when(dst != p.me)
            def _():
                remote(cp)

            @pl.when(dst == p.me)
            def _():
                local(pltpu.make_async_copy(src, self.o_out.at[p.me], sem))

    def start(self, k):
        self._each(k, lambda cp: cp.start(), lambda cp: cp.start())

    def sent(self):
        def one(k, _):
            self._each(k, lambda cp: cp.wait_send(), lambda cp: cp.wait())
            return 0

        lax.fori_loop(0, self.o_s.shape[0], one, 0)

    def arrived(self):
        rest = self.o_out.at[0:self.p.n - 1]
        pltpu.make_async_copy(rest, rest, self.recv).wait()


def _bias_row(bq, hd):
    return jnp.concatenate([jnp.zeros((1, HP), F32), bq, jnp.zeros((1, 3 * HP - hd), F32)], axis=1)


def _gates(out, cond, w, bias):
    d = bias.shape[-1]
    out[...] = _dot(cond, w)
    for j in range(bias.shape[0]):
        cols = pl.ds(j * d, d)
        out[:, cols] = _sig(out[:, cols] + bias[j:j + 1, :])


def _modulation(out, cond_normed, scale, w, bias):
    d = bias.shape[-1]
    out[...] = _dot((cond_normed * scale).astype(BF16), w)
    out[:, :d] = _sig(out[:, :d] + bias)


def _flat(raw):
    c, two, d = raw.shape
    return raw[...].reshape(c, two * d)


def _transition(dims, tile, gates, mod1, o_v, act, wall, y_s, h_s, rows):
    D, n_tp, hd, hu = dims
    w_o = wall[:, 0:hd, :].reshape(n_tp * hd, D)
    o_t = o_v[:, :, rows].reshape(n_tp * hd, tile)
    t = _dot(o_t, w_o, 0, 0).astype(BF16).astype(F32)
    mid = (act[rows, :].astype(F32) + gates[rows, :D] * t).astype(BF16).astype(F32)
    y_s[...] = (mod1[rows, :D] * _ln(mid) + mod1[rows, D:]).astype(BF16)
    step = 4 * hu
    for j in range(n_tp * hu // step):
        dv = slice(4 * j, 4 * j + 4)
        u1 = _dot(y_s[...], wall[dv, hd:hd + hu, :].reshape(step, D), 1, 1)
        u2 = _dot(y_s[...], wall[dv, hd + hu:hd + 2 * hu, :].reshape(step, D), 1, 1)
        h_s[:, j * step:(j + 1) * step] = (u1 * _sig(u1) * u2).astype(BF16)
    r = _dot(h_s[...], wall[:, hd + 2 * hu:hd + 3 * hu, :].reshape(n_tp * hu, D)).astype(BF16).astype(F32)
    return (mid + gates[rows, D:] * r).astype(BF16)


def _main_kernel(dims, x_hbm, cond_hbm, bias_hbm, mask_ref, wq_hbm, bq_ref, asc_ref, aw_hbm, ab_ref, zw_hbm, zb_ref, wo_hbm, wup_hbm, wdn_hbm,
                 xg, w1g,
                 bias_v, bt, w_s, k_s, qt_s, vt_s, gt_s, lg, o_s, xraw, craw, xn, raw, aw_s, flat_s, wst, wst1, cond, act, y_s, h_s,
                 wall, gate, mod, nxt, o0, o1,
                 ld_sem, cd_sem, b_sem, q_sem, a_sem, st_sem, own_sem, k_sem, n_send, n_recv, n_free,
                 o_send, o_recv, w_send, w_recv, c_near, c_far, c_recv, d_near, d_far, d_recv, x_send, x_recv, r_send, r_recv, ready):
    S, T, D, C, n_tp, n_dp, hd, hu, n_chunk, n_tile = dims
    p = Place(n_tp, n_dp)
    entered = p.enter()
    far = p.nz // 2
    rows_w = hd + 3 * hu
    cut = 2 * hd
    R = S * T // n_tp
    row0 = p.me * R
    tile = R // n_tile
    mine = pl.ds(p.c * R, R)
    stage = [_stage(l, hd, hu, wo_hbm, wup_hbm, wdn_hbm, w, st_sem.at[l]) for l, w in enumerate((wst, wst1))]

    def toward(k):
        j = S - 1 - k
        return lax.rem(p.z + S + (1 - 2 * lax.rem(j, 2)) * ((j + 1) // 2), S)

    def outward(j):
        return lax.rem(p.z + S + (1 - 2 * p.c) * (1 - 2 * lax.rem(j, 2)) * ((j + 1) // 2), S)

    def loads(k, slot):
        s = toward(k)
        return [pltpu.make_async_copy(x_hbm.at[s, mine], xraw.at[slot], ld_sem.at[slot]),
                pltpu.make_async_copy(cond_hbm.at[s, mine], craw.at[slot], cd_sem.at[slot])]

    raw0 = _copy(aw_hbm.at[0, 0], raw.at[0], a_sem.at[0])
    for k in range(2):
        for cp in loads(k, k):
            cp.start()
    bias_cp = _copy(bias_hbm.at[0, 0], bias_v, b_sem)
    w_s[...] = jnp.zeros_like(w_s)
    qt_s[HP:, :] = jnp.zeros((HP, T), BF16)
    wq = _stage_qkvg(0, hd, wq_hbm, w_s, q_sem)
    for cp in stage[0]:
        cp.wait()
    for cp in wq:
        cp.wait()
    raws = [_copy(src, raw.at[i + 1], a_sem.at[i + 1]) for i, src in enumerate((zw_hbm.at[0], aw_hbm.at[0, 1], aw_hbm.at[1, 0]))]
    own = [_copy(cond_hbm.at[p.z, mine], cond, own_sem.at[0]), _copy(x_hbm.at[p.z, mine], act, own_sem.at[1])]
    entered()
    ring_o = Ring(p, lambda b, ch: wall.at[b, 0:cut, :], w_recv, w_send)
    cross = Cross(p, wall, cut, rows_w, n_chunk, c_recv, c_near, c_far)
    cross1 = Cross(p, w1g, 0, rows_w, n_chunk, d_recv, d_near, d_far)
    ring_x = Ring(p, lambda b, ch: xg.at[pl.ds(b * R + ch * tile, tile), :], x_recv, x_send)
    ring_r = Ring(p, lambda b, ch: xg.at[pl.ds(b * R + ch * tile, tile), :], r_recv, r_send)
    ring_o.own(0, wst.at[0:cut, :])
    cross.own(wst)

    def half(slot):
        v = xn.at[slot, mine]
        return pltpu.make_async_remote_copy(src_ref=v, dst_ref=v, send_sem=n_send.at[slot], recv_sem=n_recv.at[slot],
                                            device_id={"tp": p.partner}, device_id_type=MESH)

    def normalise(slot):
        big = R // 2
        for i in range(2):
            rows = pl.ds(i * big, big)
            cn = _ln(craw[slot, rows, :].astype(F32))
            y = _ada(xraw[slot, rows, :].astype(F32), cn, asc_ref[0, 0:1, :], aw_s[...], ab_ref[0, 0:1, :])
            xn[slot, pl.ds(pl.multiple_of(p.c * R, R) + i * big, big), :] = y

    raw0.wait()
    aw_s[...] = _flat(raw.at[0])
    for cp in loads(0, 0):
        cp.wait()
    normalise(0)
    bias_cp.wait()
    half(0).start()
    _load_bias(bias_v, mask_ref, bt)
    bias_cp = _copy(bias_hbm.at[1, 0], bias_v, b_sem)
    for cp in stage[1]:
        cp.wait()
    wall[p.me] = wst[...]
    keep = _copy(wst1, w1g.at[p.me], k_sem)

    def gates(l, i):
        raws[i].wait()
        flat_s[...] = _flat(raw.at[i + 1])
        _gates(gate, cond[...], flat_s[...], zb_ref.at[l])

    def modulation(out, l, j, i):
        raws[i].wait()
        flat_s[...] = _flat(raw.at[i + 1])
        cn = _ln(cond[...].astype(F32))
        _modulation(out, cn, asc_ref[l, j:j + 1, :], flat_s[...], ab_ref[l, j:j + 1, :])

    events = {}

    def plan(when, f, *args):
        events.setdefault(when, []).append((f, args))

    def take(step, k):
        for when in sorted(events):
            if when % 2 == step:
                @pl.when(k == when // 2)
                def _():
                    for f, args in events[when]:
                        f(*args)

    first, over = (0, 4, 7, 10), (4, 8, 11, 14)
    for h in range(1, far + 1):
        plan(first[h - 1] + 1, ring_o.service, h, 0)
        for ch in range(n_chunk):
            plan(first[h - 1] + ch, cross.along, h, ch)
            plan(over[h - 1] + ch, cross.across, h, ch)
    for ch in range(n_chunk):
        plan(2 * S + 1, cross1.along, 1, ch)
    plan(11, cross1.own, wst1)
    for cp in own:
        plan(3, cp.wait)
    plan(5, gates, 0, 0)
    plan(7, modulation, mod, 0, 1, 1)
    plan(9, modulation, nxt, 1, 0, 2)
    ex = [Exchange(p, order, o_s, o, o_send.at[l], o_recv.at[l]) for l, (order, o) in enumerate(((toward, o0), (outward, o1)))]
    brow = [_bias_row(bq_ref[l:l + 1, :], hd) for l in range(2)]
    heads = (n_tp, hd, w_s)
    work = (bt, k_s, qt_s, vt_s, gt_s, lg, o_s)

    def step0(k, _):
        slot = lax.rem(k, 2)

        @pl.when(k + 2 < S)
        def _():
            for cp in loads(k + 2, slot):
                cp.start()

        with scope("a_half"):
            v = xn.at[slot, pl.ds((1 - p.c) * R, R)]
            pltpu.make_async_copy(v, v, n_recv.at[slot]).wait()
            half(slot).wait_send()
        at = Attend(*heads, brow[0], *work, lambda i, t: xn[slot, pl.ds(i * t, t), :])
        at.project()

        @pl.when(k + 2 < S)
        def _():
            pl.semaphore_signal(n_free, inc=1, device_id={"tp": p.partner}, device_id_type=MESH)

        @pl.when(k >= 1)
        def _():
            ex[0].start(k - 1)

        @pl.when(k + 1 < S)
        def _():
            for cp in loads(k + 1, 1 - slot):
                cp.wait()
            normalise(1 - slot)

            @pl.when(k >= 1)
            def _():
                pl.semaphore_wait(n_free, 1)

        with scope("a_ev0"):
            take(0, k)

        def hook():
            @pl.when(k + 1 < S)
            def _():
                half(1 - slot).start()

        with scope("a_att"):
            at.attend(k, hook)
        with scope("a_ev1"):
            take(1, k)
        return 0

    lax.fori_loop(0, S, step0, 0)
    ex[0].start(S - 1)
    wq = _stage_qkvg(1, hd, wq_hbm, w_s, q_sem)
    raws = [_copy(src, raw.at[i + 1], a_sem.at[i + 1]) for i, src in enumerate((zw_hbm.at[1], aw_hbm.at[1, 1]))]
    for when in sorted(events):
        if when >= 2 * S:
            for f, args in events[when]:
                f(*args)

    def other(i, _):
        ring_o.wait(i * 2 + (1 - p.c), 0)
        return 0

    with scope("b_w0"):
        lax.fori_loop(0, p.nz, other, 0)
        cross.finish_near()
    with scope("b_o0"):
        ex[0].sent()
        ex[0].arrived()
    size = (D, n_tp, hd, hu)

    def tile0(ch, _):
        rows = pl.ds(pl.multiple_of(ch * tile, tile), tile)
        with scope("b_mlp"):
            new = _transition(size, tile, gate, mod, o0, act, wall, y_s, h_s, rows)
            act[rows, :] = new
            xg[pl.ds(pl.multiple_of(row0 + ch * tile, tile), tile), :] = (nxt[rows, :D] * _ln(new.astype(F32)) + nxt[rows, D:]).astype(BF16)
        ring_x.own(ch)

        @pl.when(ch == 1)
        def _():
            with scope("b_along"):
                for i in range(n_chunk):
                    cross1.along(2, i)
        return 0

    lax.fori_loop(0, n_tile, tile0, 0)
    bias_cp.wait()
    _load_bias(bias_v, mask_ref, bt)
    for cp in wq:
        cp.wait()
    ring_o.drain(wall.at[0:n_tp - 1, 0:cut, :])
    cross.finish_far()
    keep.wait()
    events = {}
    for ch in range(n_chunk):
        plan(3, cross1.along, far - 1, ch)
        plan(9, cross1.along, far, ch)
        for h in range(1, far + 1):
            plan(2 * h + 5, cross1.across, h, ch)
    plan(1, gates, 1, 0)
    plan(5, modulation, mod, 1, 1, 1)

    def last_weights():
        cross1.finish_near()
        pltpu.make_async_copy(w1g, wall, k_sem).start()

    plan(2 * S - 3, last_weights)

    def step1(j, _):
        with scope("b_svc"):
            for i in range(n_tile // 2):
                ring_x.service(j // 2 + 1, lax.rem(j, 2) * (n_tile // 2) + i)

        @pl.when(j >= 1)
        def _():
            ex[1].start(j - 1)

        s = outward(j)
        with scope("b_half"):
            for ch in range(n_tile):
                ring_x.wait(s * 2 + (1 - p.c), ch)
        at = Attend(*heads, brow[1], *work, lambda i, t: xg[pl.ds(pl.multiple_of(s * T, T) + i * t, t), :])
        with scope("b_att"):
            at.project()
            at.attend(j)
        with scope("b_ev"):
            take(1, j)
        return 0

    lax.fori_loop(0, S, step1, 0)
    ex[1].start(S - 1)
    pltpu.make_async_copy(w1g, wall, k_sem).wait()
    cross1.finish_far()
    ring_x.drain(xg.at[0:(n_tp - 1) * R, :])
    for peer in (p.at(1), p.at(-1), p.partner):
        pl.semaphore_signal(ready, inc=1, device_id={"tp": peer}, device_id_type=MESH)
    with scope("c_o1"):
        ex[1].sent()
        ex[1].arrived()
    def tile1(ch, _):
        rows = pl.ds(pl.multiple_of(ch * tile, tile), tile)
        with scope("c_mlp"):
            xg[pl.ds(pl.multiple_of(row0 + ch * tile, tile), tile), :] = _transition(size, tile, gate, mod, o1, act, wall, y_s, h_s, rows)

        @pl.when(ch == 0)
        def _():
            with scope("c_ready"):
                pl.semaphore_wait(ready, 3)

        ring_r.own(ch)
        return 0

    lax.fori_loop(0, n_tile, tile1, 0)
    with scope("c_svc"):
        lax.fori_loop(0, far * n_tile, lambda e, _: (ring_r.service(e // n_tile + 1, lax.rem(e, n_tile)), 0)[1], 0)

    def rest(i, _):
        for ch in range(n_tile):
            ring_r.wait(i * 2 + (1 - p.c), ch)
        return 0

    with scope("c_end"):
        lax.fori_loop(0, p.nz, rest, 0)
        ring_r.drain(xg.at[0:(n_tp - 1) * R, :])


def _main(n_dp, x, cond, pair_bias, mask_row, wq, bq, asc, aw, ab, zw, zb, wo, wup, wdn):
    S, T, D = x.shape
    C = cond.shape[-1]
    hd, hu = wq.shape[2], wdn.shape[1]
    n_tp = S * 2
    rows_w = hd + 3 * hu
    R = T // 2
    n_chunk = 3
    dma = pltpu.SemaphoreType.DMA
    v = pltpu.VMEM
    pair, blocks, each = dma((2,)), dma((S,)), dma((n_tp, n_chunk))
    n_tile = 4
    tiles = dma((n_tp, n_tile))
    return pl.pallas_call(
        functools.partial(_main_kernel, (S, T, D, C, n_tp, n_dp, hd, hu, n_chunk, n_tile)),
        out_shape=(v((n_tp * R, D), BF16), pltpu.HBM((n_tp, rows_w, D), BF16)),
        in_specs=[ANY, ANY, ANY, VMEM, ANY, VMEM, VMEM, ANY, VMEM, ANY, VMEM, ANY, ANY, ANY],
        out_specs=(VMEM, HBM),
        scratch_shapes=[
            v((T, T), BF16), v((T, T), F32), v((4 * HP, D), BF16), v((T, 2 * HP), BF16), v((2 * HP, T), BF16), v((HP, T), BF16),
            v((hd, T), F32), v((2, T, QT), F32), v((S, hd, T), BF16),
            v((2, R, D), BF16), v((2, R, C), BF16), v((2, T, D), BF16), v((4, C, 2, D), BF16), *[v((C, 2 * D), BF16)] * 2,
            *[v((rows_w, D), BF16)] * 2, v((R, C), BF16), v((R, D), BF16), v((R // n_tile, D), BF16), v((R // n_tile, n_tp * hu), BF16),
            v((n_tp, rows_w, D), BF16), *[v((R, 2 * D), F32)] * 3, *[v((n_tp, hd, R), BF16)] * 2,
            pair, pair, dma, dma((4,)), dma((4,)), dma((2, 4)), pair, dma, pair, pair, pltpu.SemaphoreType.REGULAR,
            dma((2, S, 2)), pair, dma, dma((n_tp, 1)), dma, blocks, each, dma, blocks, each, dma, tiles, dma, tiles, pltpu.SemaphoreType.REGULAR],
        cost_estimate=pl.CostEstimate(flops=S * T * T * D, bytes_accessed=S * T * D, transcendentals=S * T * T),
        compiler_params=pltpu.CompilerParams(collective_id=0, has_side_effects=True, vmem_limit_bytes=VM),
        name="blocks",
    )(x, cond, pair_bias, mask_row, wq, bq, asc, aw, ab, zw, zb, wo, wup, wdn)


def _store_kernel(src, dst, sem):
    cp = pltpu.make_async_copy(src, dst, sem)
    cp.start()
    cp.wait()


def _store(x):
    return pl.pallas_call(
        _store_kernel, out_shape=jax.ShapeDtypeStruct(x.shape, x.dtype), in_specs=[VMEM], out_specs=ANY,
        scratch_shapes=[pltpu.SemaphoreType.DMA], compiler_params=pltpu.CompilerParams(vmem_limit_bytes=1 << 20), name="store")(x)


def solution(mesh):
    n_dp = mesh.shape["dp"]

    def shard_body(token_act, token_cond, pair_bias, token_mask, ada_scale, ada_w, ada_bias, zero_w, zero_b, w_qkvg, b_q, w_o, w_up, w_down):
        S, T, D = token_act.shape
        mask_row = token_mask.reshape(1, T)
        wq = jnp.transpose(w_qkvg, (0, 2, 3, 1))
        wup = jnp.transpose(w_up, (0, 2, 3, 1))
        out, _ = _main(n_dp, token_act, token_cond, pair_bias, mask_row, wq, b_q, ada_scale, ada_w, ada_bias, zero_w, zero_b, w_o, wup, w_down)
        out = pltpu.with_memory_space_constraint(out, pltpu.VMEM)
        return _store(out).reshape(S, T, D)

    everywhere = P()
    rows, second, fourth = P('dp'), P(None, 'tp'), P(*[None] * 3, 'tp')
    in_specs = (rows, rows, second) + (everywhere,) * 6 + (fourth, second, second, fourth, second)
    return jax.shard_map(shard_body, mesh=mesh, in_specs=in_specs, out_specs=rows, check_vma=False)
```

```python
import functools
import math

import jax
import jax.numpy as jnp
from jax import lax
from jax.experimental import pallas as pl
from jax.experimental.pallas import tpu as pltpu
from jax.sharding import PartitionSpec as P

LN_EPS = 1e-5
LOG2E = 1.4426950408889634
MESH = pl.DeviceIdType.MESH
BF16 = jnp.bfloat16
F32 = jnp.float32
scope = jax.named_scope
HP = 64
QT = 256
ANY = pl.BlockSpec(memory_space=pl.ANY)
VMEM = pl.BlockSpec(memory_space=pltpu.VMEM)
HBM = pl.BlockSpec(memory_space=pltpu.HBM)
VM = 50 << 20


def _ln(x):
    mean = jnp.mean(x, axis=-1, keepdims=True)
    cen = x - mean
    var = jnp.mean(cen * cen, axis=-1, keepdims=True)
    return cen * lax.rsqrt(var + LN_EPS)


def _sig(x):
    return 0.5 * jnp.tanh(0.5 * x) + 0.5


def _dot(a, b, ca=1, cb=0):
    return lax.dot_general(a, b, (((ca,), (cb,)), ((), ())), preferred_element_type=F32)


def _ada(x_f32, cond_normed, scale, w, bias):
    d = x_f32.shape[-1]
    mod = _dot((cond_normed * scale).astype(BF16), w)
    return (_sig(mod[:, :d] + bias) * _ln(x_f32) + mod[:, d:]).astype(BF16)


class Place:
    def __init__(self, n_tp, n_dp):
        self.n = n_tp
        self.n_dp = n_dp
        self.col = lax.axis_index("dp")
        self.nz = n_tp // 2
        self.me = lax.axis_index("tp")
        self.z = self.me // 2
        self.c = lax.rem(self.me, 2)
        self.partner = self.z * 2 + (1 - self.c)

    def at(self, off):
        return lax.rem(self.z + off + self.nz, self.nz) * 2 + self.c

    def column(self, i):
        return lax.rem(self.col + i, self.n_dp)

    def enter(self):
        barrier = pltpu.get_barrier_semaphore()
        peers = [{"tp": lax.rem(self.me + i, self.n)} for i in range(1, self.n)]
        peers += [{"dp": self.column(i), "tp": self.me} for i in range(1, self.n_dp)]
        for peer in peers:
            pl.semaphore_signal(barrier, inc=1, device_id=peer, device_id_type=MESH)
        return lambda: pl.semaphore_wait(barrier, len(peers))


class Ring:
    def __init__(self, place, view, recv_sem, send_sem, right=None):
        self.p, self.view, self.recv, self.send = place, view, recv_sem, send_sem
        self.far = place.nz // 2
        self.right = right or (lambda ch: place.c == 0)

    def _push(self, b, ch, dst, src=None):
        v = self.view(b, ch)
        pltpu.make_async_remote_copy(
            src_ref=v if src is None else src, dst_ref=v, send_sem=self.send, recv_sem=self.recv.at[b, ch],
            device_id={"tp": dst}, device_id_type=MESH).start()

    def own(self, ch, src=None):
        p = self.p
        self._push(p.me, ch, p.at(1), src)
        self._push(p.me, ch, p.at(-1), src)
        self._push(p.me, ch, p.partner, src)

    def wait(self, b, ch):
        v = self.view(b, ch)
        pltpu.make_async_copy(v, v, self.recv.at[b, ch]).wait()

    def service(self, h, ch):
        p = self.p
        right = self.right(ch)
        for sign, far in ((1, right), (-1, jnp.logical_not(right))):
            b = p.at(-sign * h)

            @pl.when((h < self.far) | far)
            def _():
                self.wait(b, ch)

                @pl.when((h < self.far - 1) | ((h == self.far - 1) & far))
                def _():
                    self._push(b, ch, p.at(sign))

                self._push(b, ch, p.partner)

    def drain(self, whole):
        pltpu.make_async_copy(whole, whole, self.send).wait()


class Cross:
    def __init__(self, place, buf, lo, hi, n_chunk, recv_sem, near_sem, far_sem, spread=True):
        self.p, self.buf, self.lo, self.hi, self.n_chunk, self.spread = place, buf, lo, hi, n_chunk, spread
        self.recv, self.near, self.far_sem = recv_sem, near_sem, far_sem
        self.far = place.nz // 2
        self.size = (hi - lo) // n_chunk

    def _rows(self, ch):
        return pl.ds(self.lo + ch * self.size, self.size)

    def _push(self, b, ch, dst, sem, src=None):
        v = self.buf.at[b, self._rows(ch), :]
        pltpu.make_async_remote_copy(
            src_ref=v if src is None else src, dst_ref=v, send_sem=sem, recv_sem=self.recv.at[b, ch],
            device_id=dst, device_id_type=MESH).start()

    def _push_over(self, b, ch, plane):
        p = self.p

        @pl.when(plane)
        def _():
            for i in range(1, p.n_dp):
                self._push(b, ch, {"dp": p.column(i), "tp": p.me}, self.far_sem.at[b // 2])

        self._push(b, ch, {"tp": p.partner}, self.near)

    def _mine(self, b):
        return lax.rem(b, self.p.n_dp) == self.p.col

    def own(self, src):
        p = self.p
        for ch in range(self.n_chunk):
            part = src.at[self._rows(ch), :]

            @pl.when(self._mine(p.me))
            def _():
                for off in (1, -1):
                    self._push(p.me, ch, {"tp": p.at(off)}, self.far_sem.at[p.z], part)

            if self.spread:
                self._push(p.me, ch, {"tp": p.partner}, self.near, part)

    def wait(self, b, ch):
        v = self.buf.at[b, self._rows(ch), :]
        pltpu.make_async_copy(v, v, self.recv.at[b, ch]).wait()

    def _each(self, h, body):
        p = self.p
        for sign, core in ((1, 0), (-1, 1)):
            b = p.at(-sign * h)

            @pl.when((h < self.far) | (p.c == core))
            def _():
                body(b, sign, (h < self.far - 1) | ((h == self.far - 1) & (p.c == core)))

    def along(self, h, ch):
        p = self.p

        def body(b, sign, onward):
            @pl.when(self._mine(b))
            def _():
                self.wait(b, ch)

                @pl.when(onward)
                def _():
                    self._push(b, ch, {"tp": p.at(sign)}, self.far_sem.at[b // 2])

                if self.spread:
                    self._push_over(b, ch, True)

        self._each(h, body)

    def hand_on(self):
        p = self.p

        def block(i, _):
            b = i * 2 + p.c

            @pl.when(self._mine(b) | (i == p.z))
            def _():
                for ch in range(self.n_chunk):
                    self._push_over(b, ch, i != p.z)
            return 0

        lax.fori_loop(0, p.nz, block, 0)

    def across(self, h, ch):
        p = self.p

        def body(b, sign, onward):
            @pl.when(jnp.logical_not(self._mine(b)))
            def _():
                self.wait(b, ch)
                self._push(b, ch, {"tp": p.partner}, self.near)

        self._each(h, body)

    def _sent(self, k, sem):
        if k:
            v = self.buf.at[0:k, self.lo:self.hi, :]
            pltpu.make_async_copy(v, v, sem).wait()

    def finish_near(self):
        p = self.p

        def other(i, _):
            for ch in range(self.n_chunk):
                self.wait(i * 2 + (1 - p.c), ch)
            return 0

        lax.fori_loop(0, p.nz, other, 0)
        self._sent(p.nz, self.near)

    def finish_far(self, ring=True):
        p = self.p
        over = p.n_dp - 1 if self.spread else 0
        if ring:
            @pl.when(self._mine(p.me))
            def _():
                self._sent(2, self.far_sem.at[p.z])

        def body(b, sign, onward):
            sem = self.far_sem.at[b // 2]

            @pl.when(self._mine(b))
            def _():
                if not ring:
                    self._sent(over, sem)
                else:
                    @pl.when(onward)
                    def _():
                        self._sent(over + 1, sem)

                    @pl.when(jnp.logical_not(onward))
                    def _():
                        self._sent(over, sem)

        def hop(h, _):
            self._each(h, body)
            return 0

        lax.fori_loop(1, self.far + 1, hop, 0)


def _copy(src, dst, sem):
    cp = pltpu.make_async_copy(src, dst, sem)
    cp.start()
    return cp


def _stage(l, hd, hu, wo_hbm, wup_hbm, wdn_hbm, wst, sem):
    cps, lo = [], 0
    for src, rows in ((wo_hbm.at[l], hd), (wup_hbm.at[l, 0], hu), (wup_hbm.at[l, 1], hu), (wdn_hbm.at[l], hu)):
        cps.append(_copy(src, wst.at[pl.ds(lo, rows), :], sem.at[len(cps)]))
        lo += rows
    return cps


def _stage_qkvg(l, hd, wq_hbm, w_s, sem):
    return [_copy(wq_hbm.at[l, f], w_s.at[pl.ds(i * HP, hd), :], sem.at[i]) for i, f in enumerate((1, 0, 2, 3))]


class Attend:
    def __init__(self, n_tp, hd, w, brow, bt, k_s, qt_s, vt_s, gt_s, lg, o_s, x_rows):
        self.__dict__.update(locals())
        self.T = bt.shape[0]

    def project(self):
        T, hd = self.T, self.hd
        tile = QT
        for i in range(T // tile):
            rows = pl.ds(i * tile, tile)
            res = _dot(self.x_rows(i, tile), self.w[...], 1, 1) + self.brow
            self.k_s[rows, :] = res[:, :2 * HP].astype(BF16)
            rest = res.T
            self.qt_s[0:HP, rows] = rest[HP:2 * HP].astype(BF16)
            ones = lax.broadcasted_iota(jnp.int32, (HP, tile), 0) == hd
            self.vt_s[:, rows] = jnp.where(ones, 1.0, rest[2 * HP:3 * HP]).astype(BF16)
            self.gt_s[:, rows] = _sig(rest[3 * HP:3 * HP + hd])

    def attend(self, slot, hook=None):
        T, hd = self.T, self.hd
        n = T // QT
        c1 = LOG2E / math.sqrt(hd)

        def scores(i):
            cols = pl.ds(i * QT, QT)
            logits = _dot(self.k_s[...], self.qt_s[:, cols]) * c1 + self.bt[:, cols]
            self.lg[i % 2] = logits
            return jnp.max(logits, axis=0, keepdims=True)

        top = scores(0)
        if hook is not None:
            hook()
        for i in range(n):
            cols = pl.ds(i * QT, QT)
            nxt = scores(i + 1) if i + 1 < n else None
            probs = jnp.exp2(self.lg[i % 2] - top).astype(BF16)
            mixed = _dot(self.vt_s[...], probs)
            self.o_s[slot, :, cols] = (self.gt_s[:, cols] * (mixed[:hd] / mixed[hd:hd + 1])).astype(BF16)
            top = nxt


def _load_bias(bias_v, mask_ref, bt):
    T = bt.shape[0]
    mask_add = (mask_ref[...].astype(F32) - 1.0) * 1e9

    def step(i, _):
        r = pl.multiple_of(i * 128, 128)
        rows = (bias_v[pl.ds(r, 128), :].astype(F32) + mask_add) * LOG2E
        bt[:, pl.ds(r, 128)] = rows.T
        return 0

    lax.fori_loop(0, T // 128, step, 0)


class Exchange:
    def __init__(self, place, sample_of, o_s, o_out, send_sem, recv_sem):
        self.p, self.sample_of, self.o_s, self.o_out, self.send, self.recv = place, sample_of, o_s, o_out, send_sem, recv_sem
        self.half = o_s.shape[-1] // 2

    def _each(self, k, remote, local):
        p = self.p
        for c in range(2):
            dst = self.sample_of(k) * 2 + c
            src = self.o_s.at[k, :, pl.ds(c * self.half, self.half)]
            sem = self.send.at[k, c]
            cp = pltpu.make_async_remote_copy(
                src_ref=src, dst_ref=self.o_out.at[p.me], send_sem=sem, recv_sem=self.recv,
                device_id={"tp": dst}, device_id_type=MESH)

            @pl.when(dst != p.me)
            def _():
                remote(cp)

            @pl.when(dst == p.me)
            def _():
                local(pltpu.make_async_copy(src, self.o_out.at[p.me], sem))

    def start(self, k):
        self._each(k, lambda cp: cp.start(), lambda cp: cp.start())

    def sent(self):
        def one(k, _):
            self._each(k, lambda cp: cp.wait_send(), lambda cp: cp.wait())
            return 0

        lax.fori_loop(0, self.o_s.shape[0], one, 0)

    def arrived(self):
        rest = self.o_out.at[0:self.p.n - 1]
        pltpu.make_async_copy(rest, rest, self.recv).wait()


def _bias_row(bq, hd):
    return jnp.concatenate([jnp.zeros((1, HP), F32), bq, jnp.zeros((1, 3 * HP - hd), F32)], axis=1)


def _gates(out, cond, w, bias):
    d = bias.shape[-1]
    out[...] = _dot(cond, w)
    for j in range(bias.shape[0]):
        cols = pl.ds(j * d, d)
        out[:, cols] = _sig(out[:, cols] + bias[j:j + 1, :])


def _modulation(out, cond_normed, scale, w, bias):
    d = bias.shape[-1]
    out[...] = _dot((cond_normed * scale).astype(BF16), w)
    out[:, :d] = _sig(out[:, :d] + bias)


def _flat(raw):
    c, two, d = raw.shape
    return raw[...].reshape(c, two * d)


def _transition(dims, tile, gates, mod1, o_v, act, wall, y_s, h_s, rows):
    D, n_tp, hd, hu = dims
    w_o = wall[:, 0:hd, :].reshape(n_tp * hd, D)
    o_t = o_v[:, :, rows].reshape(n_tp * hd, tile)
    t = _dot(o_t, w_o, 0, 0).astype(BF16).astype(F32)
    mid = (act[rows, :].astype(F32) + gates[rows, :D] * t).astype(BF16).astype(F32)
    y_s[...] = (mod1[rows, :D] * _ln(mid) + mod1[rows, D:]).astype(BF16)
    step = 4 * hu
    for j in range(n_tp * hu // step):
        dv = slice(4 * j, 4 * j + 4)
        u1 = _dot(y_s[...], wall[dv, hd:hd + hu, :].reshape(step, D), 1, 1)
        u2 = _dot(y_s[...], wall[dv, hd + hu:hd + 2 * hu, :].reshape(step, D), 1, 1)
        h_s[:, j * step:(j + 1) * step] = (u1 * _sig(u1) * u2).astype(BF16)
    r = _dot(h_s[...], wall[:, hd + 2 * hu:hd + 3 * hu, :].reshape(n_tp * hu, D)).astype(BF16).astype(F32)
    return (mid + gates[rows, D:] * r).astype(BF16)


def _main_kernel(dims, x_hbm, cond_hbm, bias_hbm, mask_ref, wq_hbm, bq_ref, asc_ref, aw_hbm, ab_ref, zw_hbm, zb_ref, wo_hbm, wup_hbm, wdn_hbm,
                 xg, w1g,
                 bias_v, bt, w_s, k_s, qt_s, vt_s, gt_s, lg, o_s, xraw, craw, xn, raw, aw_s, flat_s, wst, wst1, cond, act, y_s, h_s,
                 wall, gate, mod, nxt, o0, o1,
                 ld_sem, cd_sem, b_sem, q_sem, a_sem, st_sem, own_sem, k_sem, n_send, n_recv, n_free,
                 o_send, o_recv, w_send, w_recv, c_near, c_far, c_recv, d_near, d_far, d_recv, x_send, x_recv, r_send, r_recv, ready):
    S, T, D, C, n_tp, n_dp, hd, hu, n_chunk, n_tile = dims
    p = Place(n_tp, n_dp)
    entered = p.enter()
    far = p.nz // 2
    rows_w = hd + 3 * hu
    cut = 2 * hd
    R = S * T // n_tp
    row0 = p.me * R
    tile = R // n_tile
    mine = pl.ds(p.c * R, R)
    stage = [_stage(l, hd, hu, wo_hbm, wup_hbm, wdn_hbm, w, st_sem.at[l]) for l, w in enumerate((wst, wst1))]

    def toward(k):
        late, own = k // far, k // (S - 1)
        j = (1 - late) * (k + 1) + (late - own) * (S + far - 1 - k)
        return lax.rem(p.z + S + (1 - 2 * lax.rem(j, 2)) * ((j + 1) // 2), S)

    def outward(j):
        return lax.rem(p.z + S + (1 - 2 * p.c) * (1 - 2 * lax.rem(j, 2)) * ((j + 1) // 2), S)

    def loads(k, slot):
        s = toward(k)
        return [pltpu.make_async_copy(x_hbm.at[s, mine], xraw.at[slot], ld_sem.at[slot]),
                pltpu.make_async_copy(cond_hbm.at[s, mine], craw.at[slot], cd_sem.at[slot])]

    raw0 = _copy(aw_hbm.at[0, 0], raw.at[0], a_sem.at[0])
    for k in range(2):
        for cp in loads(k, k):
            cp.start()
    bias_cp = _copy(bias_hbm.at[0, 0], bias_v, b_sem)
    w_s[...] = jnp.zeros_like(w_s)
    qt_s[HP:, :] = jnp.zeros((HP, T), BF16)
    wq = _stage_qkvg(0, hd, wq_hbm, w_s, q_sem)
    for cp in stage[0]:
        cp.wait()
    for cp in wq:
        cp.wait()
    raws = [_copy(src, raw.at[i + 1], a_sem.at[i + 1]) for i, src in enumerate((zw_hbm.at[0], aw_hbm.at[0, 1], aw_hbm.at[1, 0]))]
    own = [_copy(cond_hbm.at[p.z, mine], cond, own_sem.at[0]), _copy(x_hbm.at[p.z, mine], act, own_sem.at[1])]
    entered()
    ring_o = Ring(p, lambda b, ch: wall.at[b, 0:cut, :], w_recv, w_send)
    cross = Cross(p, wall, cut, rows_w, n_chunk, c_recv, c_near, c_far)
    cross1 = Cross(p, w1g, 0, rows_w, n_chunk, d_recv, d_near, d_far)
    ring_x = Ring(p, lambda b, ch: xg.at[pl.ds(b * R + ch * tile, tile), :], x_recv, x_send)
    ring_r = Ring(p, lambda b, ch: xg.at[pl.ds(b * R + ch * tile, tile), :], r_recv, r_send)
    ring_o.own(0, wst.at[0:cut, :])
    cross.own(wst)

    def half(slot):
        v = xn.at[slot, mine]
        return pltpu.make_async_remote_copy(src_ref=v, dst_ref=v, send_sem=n_send.at[slot], recv_sem=n_recv.at[slot],
                                            device_id={"tp": p.partner}, device_id_type=MESH)

    def normalise(slot):
        big = R // 2
        for i in range(2):
            rows = pl.ds(i * big, big)
            cn = _ln(craw[slot, rows, :].astype(F32))
            y = _ada(xraw[slot, rows, :].astype(F32), cn, asc_ref[0, 0:1, :], aw_s[...], ab_ref[0, 0:1, :])
            xn[slot, pl.ds(pl.multiple_of(p.c * R, R) + i * big, big), :] = y

    raw0.wait()
    aw_s[...] = _flat(raw.at[0])
    for cp in loads(0, 0):
        cp.wait()
    normalise(0)
    bias_cp.wait()
    half(0).start()
    _load_bias(bias_v, mask_ref, bt)
    bias_cp = _copy(bias_hbm.at[1, 0], bias_v, b_sem)
    for cp in stage[1]:
        cp.wait()
    wall[p.me] = wst[...]
    keep = _copy(wst1, w1g.at[p.me], k_sem)

    def gates(l, i):
        raws[i].wait()
        flat_s[...] = _flat(raw.at[i + 1])
        _gates(gate, cond[...], flat_s[...], zb_ref.at[l])

    def modulation(out, l, j, i):
        raws[i].wait()
        flat_s[...] = _flat(raw.at[i + 1])
        cn = _ln(cond[...].astype(F32))
        _modulation(out, cn, asc_ref[l, j:j + 1, :], flat_s[...], ab_ref[l, j:j + 1, :])

    events = {}

    def plan(when, f, *args):
        events.setdefault(when, []).append((f, args))

    def take(step, k):
        for when in sorted(events):
            if when % 2 == step:
                @pl.when(k == when // 2)
                def _():
                    for f, args in events[when]:
                        f(*args)

    first, over, first1 = (0, 4, 7, 10), (4, 8, 11, 14), (8, 11, 14)
    for h in range(1, far + 1):
        plan(first[h - 1] + 1, ring_o.service, h, 0)
        for ch in range(n_chunk):
            plan(first[h - 1] + ch, cross.along, h, ch)
            plan(over[h - 1] + ch, cross.across, h, ch)
    for h in range(1, far):
        for ch in range(n_chunk):
            plan(first1[h - 1] + (ch + 1) // 2, cross1.along, h, ch)
    plan(n_chunk + 1, cross1.own, wst1)
    for cp in own:
        plan(3, cp.wait)
    plan(5, gates, 0, 0)
    plan(7, modulation, mod, 0, 1, 1)
    plan(9, modulation, nxt, 1, 0, 2)
    ex = [Exchange(p, order, o_s, o, o_send.at[l], o_recv.at[l]) for l, (order, o) in enumerate(((toward, o0), (outward, o1)))]
    brow = [_bias_row(bq_ref[l:l + 1, :], hd) for l in range(2)]
    heads = (n_tp, hd, w_s)
    work = (bt, k_s, qt_s, vt_s, gt_s, lg, o_s)

    def step0(k, _):
        slot = lax.rem(k, 2)

        @pl.when(k + 2 < S)
        def _():
            for cp in loads(k + 2, slot):
                cp.start()

        with scope("a_half"):
            v = xn.at[slot, pl.ds((1 - p.c) * R, R)]
            pltpu.make_async_copy(v, v, n_recv.at[slot]).wait()
            half(slot).wait_send()
        at = Attend(*heads, brow[0], *work, lambda i, t: xn[slot, pl.ds(i * t, t), :])
        at.project()

        @pl.when(k + 2 < S)
        def _():
            pl.semaphore_signal(n_free, inc=1, device_id={"tp": p.partner}, device_id_type=MESH)

        @pl.when(k >= 1)
        def _():
            ex[0].start(k - 1)

        @pl.when(k + 1 < S)
        def _():
            for cp in loads(k + 1, 1 - slot):
                cp.wait()
            normalise(1 - slot)

            @pl.when(k >= 1)
            def _():
                pl.semaphore_wait(n_free, 1)

        with scope("a_ev0"):
            take(0, k)

        def hook():
            @pl.when(k + 1 < S)
            def _():
                half(1 - slot).start()

        with scope("a_att"):
            at.attend(k, hook)
        with scope("a_ev1"):
            take(1, k)
        return 0

    lax.fori_loop(0, S, step0, 0)
    ex[0].start(S - 1)
    wq = _stage_qkvg(1, hd, wq_hbm, w_s, q_sem)
    raws = [_copy(src, raw.at[i + 1], a_sem.at[i + 1]) for i, src in enumerate((zw_hbm.at[1], aw_hbm.at[1, 1]))]
    for when in sorted(events):
        if when >= 2 * S:
            for f, args in events[when]:
                f(*args)

    def other(i, _):
        ring_o.wait(i * 2 + (1 - p.c), 0)
        return 0

    with scope("b_w0"):
        lax.fori_loop(0, p.nz, other, 0)
        cross.finish_near()
    with scope("b_o0"):
        ex[0].sent()
        ex[0].arrived()
    size = (D, n_tp, hd, hu)

    def tile0(ch, _):
        rows = pl.ds(pl.multiple_of(ch * tile, tile), tile)
        with scope("b_mlp"):
            new = _transition(size, tile, gate, mod, o0, act, wall, y_s, h_s, rows)
            act[rows, :] = new
            xg[pl.ds(pl.multiple_of(row0 + ch * tile, tile), tile), :] = (nxt[rows, :D] * _ln(new.astype(F32)) + nxt[rows, D:]).astype(BF16)
        ring_x.own(ch)

        @pl.when(ch == 1)
        def _():
            with scope("b_along"):
                for i in range(n_chunk):
                    cross1.along(far, i)
        return 0

    lax.fori_loop(0, n_tile, tile0, 0)
    bias_cp.wait()
    _load_bias(bias_v, mask_ref, bt)
    for cp in wq:
        cp.wait()
    ring_o.drain(wall.at[0:n_tp - 1, 0:cut, :])
    cross.finish_far()
    keep.wait()
    events = {}
    for ch in range(n_chunk):
        for h in range(1, far + 1):
            plan(2 * h + 5, cross1.across, h, ch)
    plan(1, gates, 1, 0)
    plan(5, modulation, mod, 1, 1, 1)

    def last_weights():
        cross1.finish_near()
        pltpu.make_async_copy(w1g, wall, k_sem).start()

    plan(2 * S - 3, last_weights)

    def step1(j, _):
        with scope("b_svc"):
            for i in range(n_tile // 2):
                ring_x.service(j // 2 + 1, lax.rem(j, 2) * (n_tile // 2) + i)

        @pl.when(j >= 1)
        def _():
            ex[1].start(j - 1)

        s = outward(j)
        with scope("b_half"):
            for ch in range(n_tile):
                ring_x.wait(s * 2 + (1 - p.c), ch)
        at = Attend(*heads, brow[1], *work, lambda i, t: xg[pl.ds(pl.multiple_of(s * T, T) + i * t, t), :])
        with scope("b_att"):
            at.project()
            at.attend(j)
        with scope("b_ev"):
            take(1, j)
        return 0

    lax.fori_loop(0, S, step1, 0)
    ex[1].start(S - 1)
    pltpu.make_async_copy(w1g, wall, k_sem).wait()
    cross1.finish_far()
    ring_x.drain(xg.at[0:(n_tp - 1) * R, :])
    for peer in (p.at(1), p.at(-1), p.partner):
        pl.semaphore_signal(ready, inc=1, device_id={"tp": peer}, device_id_type=MESH)
    with scope("c_o1"):
        ex[1].sent()
        ex[1].arrived()
    def tile1(ch, _):
        rows = pl.ds(pl.multiple_of(ch * tile, tile), tile)
        with scope("c_mlp"):
            xg[pl.ds(pl.multiple_of(row0 + ch * tile, tile), tile), :] = _transition(size, tile, gate, mod, o1, act, wall, y_s, h_s, rows)

        @pl.when(ch == 0)
        def _():
            with scope("c_ready"):
                pl.semaphore_wait(ready, 3)

        ring_r.own(ch)
        return 0

    lax.fori_loop(0, n_tile, tile1, 0)
    with scope("c_svc"):
        lax.fori_loop(0, far * n_tile, lambda e, _: (ring_r.service(e // n_tile + 1, lax.rem(e, n_tile)), 0)[1], 0)

    def rest(i, _):
        for ch in range(n_tile):
            ring_r.wait(i * 2 + (1 - p.c), ch)
        return 0

    with scope("c_end"):
        lax.fori_loop(0, p.nz, rest, 0)
        ring_r.drain(xg.at[0:(n_tp - 1) * R, :])


def _main(n_dp, x, cond, pair_bias, mask_row, wq, bq, asc, aw, ab, zw, zb, wo, wup, wdn):
    S, T, D = x.shape
    C = cond.shape[-1]
    hd, hu = wq.shape[2], wdn.shape[1]
    n_tp = S * 2
    rows_w = hd + 3 * hu
    R = T // 2
    n_chunk = 3
    dma = pltpu.SemaphoreType.DMA
    v = pltpu.VMEM
    pair, blocks, each = dma((2,)), dma((S,)), dma((n_tp, n_chunk))
    n_tile = 4
    tiles = dma((n_tp, n_tile))
    return pl.pallas_call(
        functools.partial(_main_kernel, (S, T, D, C, n_tp, n_dp, hd, hu, n_chunk, n_tile)),
        out_shape=(v((n_tp * R, D), BF16), pltpu.HBM((n_tp, rows_w, D), BF16)),
        in_specs=[ANY, ANY, ANY, VMEM, ANY, VMEM, VMEM, ANY, VMEM, ANY, VMEM, ANY, ANY, ANY],
        out_specs=(VMEM, HBM),
        scratch_shapes=[
            v((T, T), BF16), v((T, T), F32), v((4 * HP, D), BF16), v((T, 2 * HP), BF16), v((2 * HP, T), BF16), v((HP, T), BF16),
            v((hd, T), F32), v((2, T, QT), F32), v((S, hd, T), BF16),
            v((2, R, D), BF16), v((2, R, C), BF16), v((2, T, D), BF16), v((4, C, 2, D), BF16), *[v((C, 2 * D), BF16)] * 2,
            *[v((rows_w, D), BF16)] * 2, v((R, C), BF16), v((R, D), BF16), v((R // n_tile, D), BF16), v((R // n_tile, n_tp * hu), BF16),
            v((n_tp, rows_w, D), BF16), *[v((R, 2 * D), F32)] * 3, *[v((n_tp, hd, R), BF16)] * 2,
            pair, pair, dma, dma((4,)), dma((4,)), dma((2, 4)), pair, dma, pair, pair, pltpu.SemaphoreType.REGULAR,
            dma((2, S, 2)), pair, dma, dma((n_tp, 1)), dma, blocks, each, dma, blocks, each, dma, tiles, dma, tiles, pltpu.SemaphoreType.REGULAR],
        cost_estimate=pl.CostEstimate(flops=S * T * T * D, bytes_accessed=S * T * D, transcendentals=S * T * T),
        compiler_params=pltpu.CompilerParams(collective_id=0, has_side_effects=True, vmem_limit_bytes=VM),
        name="blocks",
    )(x, cond, pair_bias, mask_row, wq, bq, asc, aw, ab, zw, zb, wo, wup, wdn)


def _store_kernel(src, dst, sem):
    cp = pltpu.make_async_copy(src, dst, sem)
    cp.start()
    cp.wait()


def _store(x):
    return pl.pallas_call(
        _store_kernel, out_shape=jax.ShapeDtypeStruct(x.shape, x.dtype), in_specs=[VMEM], out_specs=ANY,
        scratch_shapes=[pltpu.SemaphoreType.DMA], compiler_params=pltpu.CompilerParams(vmem_limit_bytes=1 << 20), name="store")(x)


def solution(mesh):
    n_dp = mesh.shape["dp"]

    def shard_body(token_act, token_cond, pair_bias, token_mask, ada_scale, ada_w, ada_bias, zero_w, zero_b, w_qkvg, b_q, w_o, w_up, w_down):
        S, T, D = token_act.shape
        mask_row = token_mask.reshape(1, T)
        wq = jnp.transpose(w_qkvg, (0, 2, 3, 1))
        wup = jnp.transpose(w_up, (0, 2, 3, 1))
        out, _ = _main(n_dp, token_act, token_cond, pair_bias, mask_row, wq, b_q, ada_scale, ada_w, ada_bias, zero_w, zero_b, w_o, wup, w_down)
        out = pltpu.with_memory_space_constraint(out, pltpu.VMEM)
        return _store(out).reshape(S, T, D)

    everywhere = P()
    rows, second, fourth = P('dp'), P(None, 'tp'), P(*[None] * 3, 'tp')
    in_specs = (rows, rows, second) + (everywhere,) * 6 + (fourth, second, second, fourth, second)
    return jax.shard_map(shard_body, mesh=mesh, in_specs=in_specs, out_specs=rows, check_vma=False)
```

```python
import functools
import math

import jax
import jax.numpy as jnp
from jax import lax
from jax.experimental import pallas as pl
from jax.experimental.pallas import tpu as pltpu
from jax.sharding import PartitionSpec as P

LN_EPS = 1e-5
LOG2E = 1.4426950408889634
MESH = pl.DeviceIdType.MESH
BF16 = jnp.bfloat16
F32 = jnp.float32
scope = jax.named_scope
HP = 64
QT = 256
ANY = pl.BlockSpec(memory_space=pl.ANY)
VMEM = pl.BlockSpec(memory_space=pltpu.VMEM)
HBM = pl.BlockSpec(memory_space=pltpu.HBM)
VM = 50 << 20


def _ln(x):
    mean = jnp.mean(x, axis=-1, keepdims=True)
    cen = x - mean
    var = jnp.mean(cen * cen, axis=-1, keepdims=True)
    return cen * lax.rsqrt(var + LN_EPS)


def _sig(x):
    return 0.5 * jnp.tanh(0.5 * x) + 0.5


def _dot(a, b, ca=1, cb=0):
    return lax.dot_general(a, b, (((ca,), (cb,)), ((), ())), preferred_element_type=F32)


def _ada(x_f32, cond_normed, scale, w, bias):
    d = x_f32.shape[-1]
    mod = _dot((cond_normed * scale).astype(BF16), w)
    return (_sig(mod[:, :d] + bias) * _ln(x_f32) + mod[:, d:]).astype(BF16)


class Place:
    def __init__(self, n_tp, n_dp):
        self.n = n_tp
        self.n_dp = n_dp
        self.col = lax.axis_index("dp")
        self.nz = n_tp // 2
        self.me = lax.axis_index("tp")
        self.z = self.me // 2
        self.c = lax.rem(self.me, 2)
        self.partner = self.z * 2 + (1 - self.c)

    def at(self, off):
        return lax.rem(self.z + off + self.nz, self.nz) * 2 + self.c

    def column(self, i):
        return lax.rem(self.col + i, self.n_dp)

    def enter(self):
        barrier = pltpu.get_barrier_semaphore()
        peers = [{"tp": lax.rem(self.me + i, self.n)} for i in range(1, self.n)]
        peers += [{"dp": self.column(i), "tp": self.me} for i in range(1, self.n_dp)]
        for peer in peers:
            pl.semaphore_signal(barrier, inc=1, device_id=peer, device_id_type=MESH)
        return lambda: pl.semaphore_wait(barrier, len(peers))


class Ring:
    def __init__(self, place, view, recv_sem, send_sem, right=None):
        self.p, self.view, self.recv, self.send = place, view, recv_sem, send_sem
        self.far = place.nz // 2
        self.right = right or (lambda ch: place.c == 0)

    def _push(self, b, ch, dst, src=None):
        v = self.view(b, ch)
        pltpu.make_async_remote_copy(
            src_ref=v if src is None else src, dst_ref=v, send_sem=self.send, recv_sem=self.recv.at[b, ch],
            device_id={"tp": dst}, device_id_type=MESH).start()

    def own(self, ch, src=None):
        p = self.p
        self._push(p.me, ch, p.at(1), src)
        self._push(p.me, ch, p.at(-1), src)
        self._push(p.me, ch, p.partner, src)

    def wait(self, b, ch):
        v = self.view(b, ch)
        pltpu.make_async_copy(v, v, self.recv.at[b, ch]).wait()

    def service(self, h, ch):
        p = self.p
        right = self.right(ch)
        for sign, far in ((1, right), (-1, jnp.logical_not(right))):
            b = p.at(-sign * h)

            @pl.when((h < self.far) | far)
            def _():
                self.wait(b, ch)

                @pl.when((h < self.far - 1) | ((h == self.far - 1) & far))
                def _():
                    self._push(b, ch, p.at(sign))

                self._push(b, ch, p.partner)

    def drain(self, whole):
        pltpu.make_async_copy(whole, whole, self.send).wait()


class Cross:
    def __init__(self, place, buf, lo, hi, n_chunk, recv_sem, near_sem, far_sem, spread=True):
        self.p, self.buf, self.lo, self.hi, self.n_chunk, self.spread = place, buf, lo, hi, n_chunk, spread
        self.recv, self.near, self.far_sem = recv_sem, near_sem, far_sem
        self.far = place.nz // 2
        self.size = (hi - lo) // n_chunk

    def _rows(self, ch):
        return pl.ds(self.lo + ch * self.size, self.size)

    def _push(self, b, ch, dst, sem, src=None):
        v = self.buf.at[b, self._rows(ch), :]
        pltpu.make_async_remote_copy(
            src_ref=v if src is None else src, dst_ref=v, send_sem=sem, recv_sem=self.recv.at[b, ch],
            device_id=dst, device_id_type=MESH).start()

    def _push_over(self, b, ch, plane):
        p = self.p

        @pl.when(plane)
        def _():
            for i in range(1, p.n_dp):
                self._push(b, ch, {"dp": p.column(i), "tp": p.me}, self.far_sem.at[b // 2])

        self._push(b, ch, {"tp": p.partner}, self.near)

    def _mine(self, b):
        return lax.rem(b, self.p.n_dp) == self.p.col

    def own(self, src):
        p = self.p
        for ch in range(self.n_chunk):
            part = src.at[self._rows(ch), :]

            @pl.when(self._mine(p.me))
            def _():
                for off in (1, -1):
                    self._push(p.me, ch, {"tp": p.at(off)}, self.far_sem.at[p.z], part)

            if self.spread:
                self._push(p.me, ch, {"tp": p.partner}, self.near, part)

    def wait(self, b, ch):
        v = self.buf.at[b, self._rows(ch), :]
        pltpu.make_async_copy(v, v, self.recv.at[b, ch]).wait()

    def _each(self, h, body):
        p = self.p
        for sign, core in ((1, 0), (-1, 1)):
            b = p.at(-sign * h)

            @pl.when((h < self.far) | (p.c == core))
            def _():
                body(b, sign, (h < self.far - 1) | ((h == self.far - 1) & (p.c == core)))

    def along(self, h, ch):
        p = self.p

        def body(b, sign, onward):
            @pl.when(self._mine(b))
            def _():
                self.wait(b, ch)

                @pl.when(onward)
                def _():
                    self._push(b, ch, {"tp": p.at(sign)}, self.far_sem.at[b // 2])

                if self.spread:
                    self._push_over(b, ch, True)

        self._each(h, body)

    def hand_on(self):
        p = self.p

        def block(i, _):
            b = i * 2 + p.c

            @pl.when(self._mine(b) | (i == p.z))
            def _():
                for ch in range(self.n_chunk):
                    self._push_over(b, ch, i != p.z)
            return 0

        lax.fori_loop(0, p.nz, block, 0)

    def across(self, h, ch):
        p = self.p

        def body(b, sign, onward):
            @pl.when(jnp.logical_not(self._mine(b)))
            def _():
                self.wait(b, ch)
                self._push(b, ch, {"tp": p.partner}, self.near)

        self._each(h, body)

    def _sent(self, k, sem):
        if k:
            v = self.buf.at[0:k, self.lo:self.hi, :]
            pltpu.make_async_copy(v, v, sem).wait()

    def finish_near(self):
        p = self.p

        def other(i, _):
            for ch in range(self.n_chunk):
                self.wait(i * 2 + (1 - p.c), ch)
            return 0

        lax.fori_loop(0, p.nz, other, 0)
        self._sent(p.nz, self.near)

    def finish_far(self, ring=True):
        p = self.p
        over = p.n_dp - 1 if self.spread else 0
        if ring:
            @pl.when(self._mine(p.me))
            def _():
                self._sent(2, self.far_sem.at[p.z])

        def body(b, sign, onward):
            sem = self.far_sem.at[b // 2]

            @pl.when(self._mine(b))
            def _():
                if not ring:
                    self._sent(over, sem)
                else:
                    @pl.when(onward)
                    def _():
                        self._sent(over + 1, sem)

                    @pl.when(jnp.logical_not(onward))
                    def _():
                        self._sent(over, sem)

        def hop(h, _):
            self._each(h, body)
            return 0

        lax.fori_loop(1, self.far + 1, hop, 0)


def _copy(src, dst, sem):
    cp = pltpu.make_async_copy(src, dst, sem)
    cp.start()
    return cp


def _stage(l, hd, hu, wo_hbm, wup_hbm, wdn_hbm, wst, sem):
    cps, lo = [], 0
    for src, rows in ((wo_hbm.at[l], hd), (wup_hbm.at[l, 0], hu), (wup_hbm.at[l, 1], hu), (wdn_hbm.at[l], hu)):
        cps.append(_copy(src, wst.at[pl.ds(lo, rows), :], sem.at[len(cps)]))
        lo += rows
    return cps


def _stage_qkvg(l, hd, wq_hbm, w_s, sem):
    return [_copy(wq_hbm.at[l, f], w_s.at[pl.ds(i * HP, hd), :], sem.at[i]) for i, f in enumerate((1, 0, 2, 3))]


class Attend:
    def __init__(self, n_tp, hd, w, brow, bt, k_s, qt_s, vt_s, gt_s, lg, o_s, x_rows):
        self.__dict__.update(locals())
        self.T = bt.shape[0]

    def project(self):
        T, hd = self.T, self.hd
        tile = QT
        for i in range(T // tile):
            rows = pl.ds(i * tile, tile)
            res = _dot(self.x_rows(i, tile), self.w[...], 1, 1) + self.brow
            self.k_s[rows, :] = res[:, :2 * HP].astype(BF16)
            rest = res.T
            self.qt_s[0:HP, rows] = rest[HP:2 * HP].astype(BF16)
            ones = lax.broadcasted_iota(jnp.int32, (HP, tile), 0) == hd
            self.vt_s[:, rows] = jnp.where(ones, 1.0, rest[2 * HP:3 * HP]).astype(BF16)
            self.gt_s[:, rows] = _sig(rest[3 * HP:3 * HP + hd])

    def attend(self, slot, hook=None):
        T, hd = self.T, self.hd
        n = T // QT
        c1 = LOG2E / math.sqrt(hd)

        def scores(i):
            cols = pl.ds(i * QT, QT)
            logits = _dot(self.k_s[...], self.qt_s[:, cols]) * c1 + self.bt[:, cols]
            self.lg[i % 2] = logits
            return jnp.max(logits, axis=0, keepdims=True)

        top = scores(0)
        if hook is not None:
            hook()
        for i in range(n):
            cols = pl.ds(i * QT, QT)
            nxt = scores(i + 1) if i + 1 < n else None
            probs = jnp.exp2(self.lg[i % 2] - top).astype(BF16)
            mixed = _dot(self.vt_s[...], probs)
            self.o_s[slot, :, cols] = (self.gt_s[:, cols] * (mixed[:hd] / mixed[hd:hd + 1])).astype(BF16)
            top = nxt


def _load_bias(bias_v, mask_ref, bt):
    T = bt.shape[0]
    mask_add = (mask_ref[...].astype(F32) - 1.0) * 1e9

    def step(i, _):
        r = pl.multiple_of(i * 128, 128)
        rows = (bias_v[pl.ds(r, 128), :].astype(F32) + mask_add) * LOG2E
        bt[:, pl.ds(r, 128)] = rows.T
        return 0

    lax.fori_loop(0, T // 128, step, 0)


class Exchange:
    def __init__(self, place, sample_of, o_s, o_out, send_sem, recv_sem):
        self.p, self.sample_of, self.o_s, self.o_out, self.send, self.recv = place, sample_of, o_s, o_out, send_sem, recv_sem
        self.half = o_s.shape[-1] // 2

    def _each(self, k, remote, local):
        p = self.p
        for c in range(2):
            dst = self.sample_of(k) * 2 + c
            src = self.o_s.at[k, :, pl.ds(c * self.half, self.half)]
            sem = self.send.at[k, c]
            cp = pltpu.make_async_remote_copy(
                src_ref=src, dst_ref=self.o_out.at[p.me], send_sem=sem, recv_sem=self.recv,
                device_id={"tp": dst}, device_id_type=MESH)

            @pl.when(dst != p.me)
            def _():
                remote(cp)

            @pl.when(dst == p.me)
            def _():
                local(pltpu.make_async_copy(src, self.o_out.at[p.me], sem))

    def start(self, k):
        self._each(k, lambda cp: cp.start(), lambda cp: cp.start())

    def sent(self):
        def one(k, _):
            self._each(k, lambda cp: cp.wait_send(), lambda cp: cp.wait())
            return 0

        lax.fori_loop(0, self.o_s.shape[0], one, 0)

    def arrived(self):
        rest = self.o_out.at[0:self.p.n - 1]
        pltpu.make_async_copy(rest, rest, self.recv).wait()


def _bias_row(bq, hd):
    return jnp.concatenate([jnp.zeros((1, HP), F32), bq, jnp.zeros((1, 3 * HP - hd), F32)], axis=1)


def _gates(out, cond, w, bias):
    d = bias.shape[-1]
    out[...] = _dot(cond, w)
    for j in range(bias.shape[0]):
        cols = pl.ds(j * d, d)
        out[:, cols] = _sig(out[:, cols] + bias[j:j + 1, :])


def _modulation(out, cond_normed, scale, w, bias):
    d = bias.shape[-1]
    out[...] = _dot((cond_normed * scale).astype(BF16), w)
    out[:, :d] = _sig(out[:, :d] + bias)


def _flat(raw):
    c, two, d = raw.shape
    return raw[...].reshape(c, two * d)


def _transition(dims, tile, gates, mod1, o_v, act, wall, y_s, h_s, rows):
    D, n_tp, hd, hu = dims
    w_o = wall[:, 0:hd, :].reshape(n_tp * hd, D)
    o_t = o_v[:, :, rows].reshape(n_tp * hd, tile)
    t = _dot(o_t, w_o, 0, 0).astype(BF16).astype(F32)
    mid = (act[rows, :].astype(F32) + gates[rows, :D] * t).astype(BF16).astype(F32)
    y_s[...] = (mod1[rows, :D] * _ln(mid) + mod1[rows, D:]).astype(BF16)
    step = 4 * hu
    for j in range(n_tp * hu // step):
        dv = slice(4 * j, 4 * j + 4)
        u1 = _dot(y_s[...], wall[dv, hd:hd + hu, :].reshape(step, D), 1, 1)
        u2 = _dot(y_s[...], wall[dv, hd + hu:hd + 2 * hu, :].reshape(step, D), 1, 1)
        h_s[:, j * step:(j + 1) * step] = (u1 * _sig(u1) * u2).astype(BF16)
    r = _dot(h_s[...], wall[:, hd + 2 * hu:hd + 3 * hu, :].reshape(n_tp * hu, D)).astype(BF16).astype(F32)
    return (mid + gates[rows, D:] * r).astype(BF16)


def _main_kernel(dims, x_hbm, cond_hbm, bias_hbm, mask_ref, wq_hbm, bq_ref, asc_ref, aw_hbm, ab_ref, zw_hbm, zb_ref, wo_hbm, wup_hbm, wdn_hbm,
                 xg, w1g,
                 bias_v, bt, w_s, k_s, qt_s, vt_s, gt_s, lg, o_s, xraw, craw, xn, raw, aw_s, flat_s, wst, wst1, cond, act, y_s, h_s,
                 wall, gate, mod, nxt, o0, o1,
                 ld_sem, cd_sem, b_sem, q_sem, a_sem, st_sem, own_sem, k_sem, n_send, n_recv, n_free,
                 o_send, o_recv, w_send, w_recv, c_near, c_far, c_recv, d_near, d_far, d_recv, x_send, x_recv, r_send, r_recv, ready):
    S, T, D, C, n_tp, n_dp, hd, hu, n_chunk, n_tile = dims
    p = Place(n_tp, n_dp)
    entered = p.enter()
    far = p.nz // 2
    rows_w = hd + 3 * hu
    cut = 2 * hd
    R = S * T // n_tp
    row0 = p.me * R
    tile = R // n_tile
    mine = pl.ds(p.c * R, R)
    stage = [_stage(l, hd, hu, wo_hbm, wup_hbm, wdn_hbm, w, st_sem.at[l]) for l, w in enumerate((wst, wst1))]

    def toward(k):
        late, own = (k + S - 2) // S, k // (S - 1)
        j = (1 - late) * (k + 1) + (late - own) * (S + 1 - k)
        return lax.rem(p.z + S + (1 - 2 * lax.rem(j, 2)) * ((j + 1) // 2), S)

    def outward(j):
        return lax.rem(p.z + S + (1 - 2 * p.c) * (1 - 2 * lax.rem(j, 2)) * ((j + 1) // 2), S)

    def loads(k, slot):
        s = toward(k)
        return [pltpu.make_async_copy(x_hbm.at[s, mine], xraw.at[slot], ld_sem.at[slot]),
                pltpu.make_async_copy(cond_hbm.at[s, mine], craw.at[slot], cd_sem.at[slot])]

    raw0 = _copy(aw_hbm.at[0, 0], raw.at[0], a_sem.at[0])
    for k in range(2):
        for cp in loads(k, k):
            cp.start()
    bias_cp = _copy(bias_hbm.at[0, 0], bias_v, b_sem)
    for cp in stage[0]:
        cp.wait()
    raws = [_copy(src, raw.at[i + 1], a_sem.at[i + 1]) for i, src in enumerate((zw_hbm.at[0], aw_hbm.at[0, 1], aw_hbm.at[1, 0]))]
    own = [_copy(cond_hbm.at[p.z, mine], cond, own_sem.at[0]), _copy(x_hbm.at[p.z, mine], act, own_sem.at[1])]
    entered()
    ring_o = Ring(p, lambda b, ch: wall.at[b, 0:cut, :], w_recv, w_send)
    cross = Cross(p, wall, cut, rows_w, n_chunk, c_recv, c_near, c_far)
    cross1 = Cross(p, w1g, 0, rows_w, n_chunk, d_recv, d_near, d_far)
    ring_x = Ring(p, lambda b, ch: xg.at[pl.ds(b * R + ch * tile, tile), :], x_recv, x_send)
    ring_r = Ring(p, lambda b, ch: xg.at[pl.ds(b * R + ch * tile, tile), :], r_recv, r_send)
    ring_o.own(0, wst.at[0:cut, :])
    cross.own(wst)
    w_s[...] = jnp.zeros_like(w_s)
    qt_s[HP:, :] = jnp.zeros((HP, T), BF16)
    wq = _stage_qkvg(0, hd, wq_hbm, w_s, q_sem)

    def half(slot):
        v = xn.at[slot, mine]
        return pltpu.make_async_remote_copy(src_ref=v, dst_ref=v, send_sem=n_send.at[slot], recv_sem=n_recv.at[slot],
                                            device_id={"tp": p.partner}, device_id_type=MESH)

    def normalise(slot):
        big = R // 2
        for i in range(2):
            rows = pl.ds(i * big, big)
            cn = _ln(craw[slot, rows, :].astype(F32))
            y = _ada(xraw[slot, rows, :].astype(F32), cn, asc_ref[0, 0:1, :], aw_s[...], ab_ref[0, 0:1, :])
            xn[slot, pl.ds(pl.multiple_of(p.c * R, R) + i * big, big), :] = y

    raw0.wait()
    aw_s[...] = _flat(raw.at[0])
    for cp in loads(0, 0):
        cp.wait()
    normalise(0)
    bias_cp.wait()
    half(0).start()
    _load_bias(bias_v, mask_ref, bt)
    bias_cp = _copy(bias_hbm.at[1, 0], bias_v, b_sem)
    for cp in stage[1] + wq:
        cp.wait()
    wall[p.me] = wst[...]
    keep = _copy(wst1, w1g.at[p.me], k_sem)

    def gates(l, i):
        raws[i].wait()
        flat_s[...] = _flat(raw.at[i + 1])
        _gates(gate, cond[...], flat_s[...], zb_ref.at[l])

    def modulation(out, l, j, i):
        raws[i].wait()
        flat_s[...] = _flat(raw.at[i + 1])
        cn = _ln(cond[...].astype(F32))
        _modulation(out, cn, asc_ref[l, j:j + 1, :], flat_s[...], ab_ref[l, j:j + 1, :])

    events = {}

    def plan(when, f, *args):
        events.setdefault(when, []).append((f, args))

    def take(step, k):
        for when in sorted(events):
            if when % 2 == step:
                @pl.when(k == when // 2)
                def _():
                    for f, args in events[when]:
                        f(*args)

    first, over, first1 = (0, 4, 7, 10), (4, 8, 11, 14), (10, 13)
    for h in range(1, far + 1):
        plan(first[h - 1] + 1, ring_o.service, h, 0)
        for ch in range(n_chunk):
            plan(first[h - 1] + ch, cross.along, h, ch)
            plan(over[h - 1] + ch, cross.across, h, ch)
    for h, when in enumerate(first1):
        for ch in range(n_chunk):
            plan(when + (ch + 1) // 2, cross1.along, h + 1, ch)
    plan(n_chunk + 1, cross1.own, wst1)
    for cp in own:
        plan(3, cp.wait)
    plan(5, gates, 0, 0)
    plan(7, modulation, mod, 0, 1, 1)
    plan(9, modulation, nxt, 1, 0, 2)
    ex = [Exchange(p, order, o_s, o, o_send.at[l], o_recv.at[l]) for l, (order, o) in enumerate(((toward, o0), (outward, o1)))]
    brow = [_bias_row(bq_ref[l:l + 1, :], hd) for l in range(2)]
    heads = (n_tp, hd, w_s)
    work = (bt, k_s, qt_s, vt_s, gt_s, lg, o_s)

    def step0(k, _):
        slot = lax.rem(k, 2)

        @pl.when(k + 2 < S)
        def _():
            for cp in loads(k + 2, slot):
                cp.start()

        with scope("a_half"):
            v = xn.at[slot, pl.ds((1 - p.c) * R, R)]
            pltpu.make_async_copy(v, v, n_recv.at[slot]).wait()
            half(slot).wait_send()
        at = Attend(*heads, brow[0], *work, lambda i, t: xn[slot, pl.ds(i * t, t), :])
        at.project()

        @pl.when(k + 2 < S)
        def _():
            pl.semaphore_signal(n_free, inc=1, device_id={"tp": p.partner}, device_id_type=MESH)

        @pl.when(k >= 1)
        def _():
            ex[0].start(k - 1)

        @pl.when(k + 1 < S)
        def _():
            for cp in loads(k + 1, 1 - slot):
                cp.wait()
            normalise(1 - slot)

            @pl.when(k >= 1)
            def _():
                pl.semaphore_wait(n_free, 1)

        with scope("a_ev0"):
            take(0, k)

        def hook():
            @pl.when(k + 1 < S)
            def _():
                half(1 - slot).start()

        with scope("a_att"):
            at.attend(k, hook)
        with scope("a_ev1"):
            take(1, k)
        return 0

    lax.fori_loop(0, S, step0, 0)
    ex[0].start(S - 1)
    wq = _stage_qkvg(1, hd, wq_hbm, w_s, q_sem)
    raws = [_copy(src, raw.at[i + 1], a_sem.at[i + 1]) for i, src in enumerate((zw_hbm.at[1], aw_hbm.at[1, 1]))]
    for when in sorted(events):
        if when >= 2 * S:
            for f, args in events[when]:
                f(*args)

    def other(i, _):
        ring_o.wait(i * 2 + (1 - p.c), 0)
        return 0

    with scope("b_w0"):
        lax.fori_loop(0, p.nz, other, 0)
        cross.finish_near()
    with scope("b_o0"):
        ex[0].sent()
        ex[0].arrived()
    size = (D, n_tp, hd, hu)

    def tile0(ch, _):
        rows = pl.ds(pl.multiple_of(ch * tile, tile), tile)
        with scope("b_mlp"):
            new = _transition(size, tile, gate, mod, o0, act, wall, y_s, h_s, rows)
            act[rows, :] = new
            xg[pl.ds(pl.multiple_of(row0 + ch * tile, tile), tile), :] = (nxt[rows, :D] * _ln(new.astype(F32)) + nxt[rows, D:]).astype(BF16)
        ring_x.own(ch)

        @pl.when(ch == 1)
        def _():
            with scope("b_along"):
                for i in range(n_chunk):
                    cross1.along(far - 1, i)
        return 0

    lax.fori_loop(0, n_tile, tile0, 0)
    bias_cp.wait()
    _load_bias(bias_v, mask_ref, bt)
    for cp in wq:
        cp.wait()
    ring_o.drain(wall.at[0:n_tp - 1, 0:cut, :])
    cross.finish_far()
    keep.wait()
    events = {}
    for ch in range(n_chunk):
        plan(5, cross1.along, far, ch)
        for h in range(1, far + 1):
            plan(2 * h + 5, cross1.across, h, ch)
    plan(1, gates, 1, 0)
    plan(5, modulation, mod, 1, 1, 1)

    def last_weights():
        cross1.finish_near()
        pltpu.make_async_copy(w1g, wall, k_sem).start()

    plan(2 * S - 3, last_weights)

    def step1(j, _):
        with scope("b_svc"):
            for i in range(n_tile // 2):
                ring_x.service(j // 2 + 1, lax.rem(j, 2) * (n_tile // 2) + i)

        @pl.when(j >= 1)
        def _():
            ex[1].start(j - 1)

        s = outward(j)
        with scope("b_half"):
            for ch in range(n_tile):
                ring_x.wait(s * 2 + (1 - p.c), ch)
        at = Attend(*heads, brow[1], *work, lambda i, t: xg[pl.ds(pl.multiple_of(s * T, T) + i * t, t), :])
        with scope("b_att"):
            at.project()
            at.attend(j)
        with scope("b_ev"):
            take(1, j)
        return 0

    lax.fori_loop(0, S, step1, 0)
    ex[1].start(S - 1)
    pltpu.make_async_copy(w1g, wall, k_sem).wait()
    cross1.finish_far()
    ring_x.drain(xg.at[0:(n_tp - 1) * R, :])
    for peer in (p.at(1), p.at(-1), p.partner):
        pl.semaphore_signal(ready, inc=1, device_id={"tp": peer}, device_id_type=MESH)
    with scope("c_o1"):
        ex[1].sent()
        ex[1].arrived()
    def tile1(ch, _):
        rows = pl.ds(pl.multiple_of(ch * tile, tile), tile)
        with scope("c_mlp"):
            xg[pl.ds(pl.multiple_of(row0 + ch * tile, tile), tile), :] = _transition(size, tile, gate, mod, o1, act, wall, y_s, h_s, rows)

        @pl.when(ch == 0)
        def _():
            with scope("c_ready"):
                pl.semaphore_wait(ready, 3)

        ring_r.own(ch)
        return 0

    lax.fori_loop(0, n_tile, tile1, 0)
    with scope("c_svc"):
        lax.fori_loop(0, far * n_tile, lambda e, _: (ring_r.service(e // n_tile + 1, lax.rem(e, n_tile)), 0)[1], 0)

    def rest(i, _):
        for ch in range(n_tile):
            ring_r.wait(i * 2 + (1 - p.c), ch)
        return 0

    with scope("c_end"):
        lax.fori_loop(0, p.nz, rest, 0)
        ring_r.drain(xg.at[0:(n_tp - 1) * R, :])


def _main(n_dp, x, cond, pair_bias, mask_row, wq, bq, asc, aw, ab, zw, zb, wo, wup, wdn):
    S, T, D = x.shape
    C = cond.shape[-1]
    hd, hu = wq.shape[2], wdn.shape[1]
    n_tp = S * 2
    rows_w = hd + 3 * hu
    R = T // 2
    n_chunk = 3
    dma = pltpu.SemaphoreType.DMA
    v = pltpu.VMEM
    pair, blocks, each = dma((2,)), dma((S,)), dma((n_tp, n_chunk))
    n_tile = 4
    tiles = dma((n_tp, n_tile))
    return pl.pallas_call(
        functools.partial(_main_kernel, (S, T, D, C, n_tp, n_dp, hd, hu, n_chunk, n_tile)),
        out_shape=(v((n_tp * R, D), BF16), pltpu.HBM((n_tp, rows_w, D), BF16)),
        in_specs=[ANY, ANY, ANY, VMEM, ANY, VMEM, VMEM, ANY, VMEM, ANY, VMEM, ANY, ANY, ANY],
        out_specs=(VMEM, HBM),
        scratch_shapes=[
            v((T, T), BF16), v((T, T), F32), v((4 * HP, D), BF16), v((T, 2 * HP), BF16), v((2 * HP, T), BF16), v((HP, T), BF16),
            v((hd, T), F32), v((2, T, QT), F32), v((S, hd, T), BF16),
            v((2, R, D), BF16), v((2, R, C), BF16), v((2, T, D), BF16), v((4, C, 2, D), BF16), *[v((C, 2 * D), BF16)] * 2,
            *[v((rows_w, D), BF16)] * 2, v((R, C), BF16), v((R, D), BF16), v((R // n_tile, D), BF16), v((R // n_tile, n_tp * hu), BF16),
            v((n_tp, rows_w, D), BF16), *[v((R, 2 * D), F32)] * 3, *[v((n_tp, hd, R), BF16)] * 2,
            pair, pair, dma, dma((4,)), dma((4,)), dma((2, 4)), pair, dma, pair, pair, pltpu.SemaphoreType.REGULAR,
            dma((2, S, 2)), pair, dma, dma((n_tp, 1)), dma, blocks, each, dma, blocks, each, dma, tiles, dma, tiles, pltpu.SemaphoreType.REGULAR],
        cost_estimate=pl.CostEstimate(flops=S * T * T * D, bytes_accessed=S * T * D, transcendentals=S * T * T),
        compiler_params=pltpu.CompilerParams(collective_id=0, has_side_effects=True, vmem_limit_bytes=VM),
        name="blocks",
    )(x, cond, pair_bias, mask_row, wq, bq, asc, aw, ab, zw, zb, wo, wup, wdn)


def _store_kernel(src, dst, sem):
    cp = pltpu.make_async_copy(src, dst, sem)
    cp.start()
    cp.wait()


def _store(x):
    return pl.pallas_call(
        _store_kernel, out_shape=jax.ShapeDtypeStruct(x.shape, x.dtype), in_specs=[VMEM], out_specs=ANY,
        scratch_shapes=[pltpu.SemaphoreType.DMA], compiler_params=pltpu.CompilerParams(vmem_limit_bytes=1 << 20), name="store")(x)


def solution(mesh):
    n_dp = mesh.shape["dp"]

    def shard_body(token_act, token_cond, pair_bias, token_mask, ada_scale, ada_w, ada_bias, zero_w, zero_b, w_qkvg, b_q, w_o, w_up, w_down):
        S, T, D = token_act.shape
        mask_row = token_mask.reshape(1, T)
        wq = jnp.transpose(w_qkvg, (0, 2, 3, 1))
        wup = jnp.transpose(w_up, (0, 2, 3, 1))
        out, _ = _main(n_dp, token_act, token_cond, pair_bias, mask_row, wq, b_q, ada_scale, ada_w, ada_bias, zero_w, zero_b, w_o, wup, w_down)
        out = pltpu.with_memory_space_constraint(out, pltpu.VMEM)
        return _store(out).reshape(S, T, D)

    everywhere = P()
    rows, second, fourth = P('dp'), P(None, 'tp'), P(*[None] * 3, 'tp')
    in_specs = (rows, rows, second) + (everywhere,) * 6 + (fourth, second, second, fourth, second)
    return jax.shard_map(shard_body, mesh=mesh, in_specs=in_specs, out_specs=rows, check_vma=False)
```

```python
import functools
import math

import jax
import jax.numpy as jnp
from jax import lax
from jax.experimental import pallas as pl
from jax.experimental.pallas import tpu as pltpu
from jax.sharding import PartitionSpec as P

LN_EPS = 1e-5
LOG2E = 1.4426950408889634
MESH = pl.DeviceIdType.MESH
BF16 = jnp.bfloat16
F32 = jnp.float32
scope = jax.named_scope
HP = 64
QT = 256
ANY = pl.BlockSpec(memory_space=pl.ANY)
VMEM = pl.BlockSpec(memory_space=pltpu.VMEM)
HBM = pl.BlockSpec(memory_space=pltpu.HBM)
VM = 50 << 20


def _ln(x):
    mean = jnp.mean(x, axis=-1, keepdims=True)
    cen = x - mean
    var = jnp.mean(cen * cen, axis=-1, keepdims=True)
    return cen * lax.rsqrt(var + LN_EPS)


def _sig(x):
    return 0.5 * jnp.tanh(0.5 * x) + 0.5


def _dot(a, b, ca=1, cb=0):
    return lax.dot_general(a, b, (((ca,), (cb,)), ((), ())), preferred_element_type=F32)


def _ada(x_f32, cond_normed, scale, w, bias):
    d = x_f32.shape[-1]
    mod = _dot((cond_normed * scale).astype(BF16), w)
    return (_sig(mod[:, :d] + bias) * _ln(x_f32) + mod[:, d:]).astype(BF16)


class Place:
    def __init__(self, n_tp, n_dp):
        self.n = n_tp
        self.n_dp = n_dp
        self.col = lax.axis_index("dp")
        self.nz = n_tp // 2
        self.me = lax.axis_index("tp")
        self.z = self.me // 2
        self.c = lax.rem(self.me, 2)
        self.partner = self.z * 2 + (1 - self.c)

    def at(self, off):
        return lax.rem(self.z + off + self.nz, self.nz) * 2 + self.c

    def column(self, i):
        return lax.rem(self.col + i, self.n_dp)

    def enter(self):
        barrier = pltpu.get_barrier_semaphore()
        peers = [{"tp": lax.rem(self.me + i, self.n)} for i in range(1, self.n)]
        peers += [{"dp": self.column(i), "tp": self.me} for i in range(1, self.n_dp)]
        for peer in peers:
            pl.semaphore_signal(barrier, inc=1, device_id=peer, device_id_type=MESH)
        return lambda: pl.semaphore_wait(barrier, len(peers))


class Ring:
    def __init__(self, place, view, recv_sem, send_sem, right=None):
        self.p, self.view, self.recv, self.send = place, view, recv_sem, send_sem
        self.far = place.nz // 2
        self.right = right or (lambda ch: place.c == 0)

    def _push(self, b, ch, dst, src=None):
        v = self.view(b, ch)
        pltpu.make_async_remote_copy(
            src_ref=v if src is None else src, dst_ref=v, send_sem=self.send, recv_sem=self.recv.at[b, ch],
            device_id={"tp": dst}, device_id_type=MESH).start()

    def own(self, ch, src=None):
        p = self.p
        self._push(p.me, ch, p.at(1), src)
        self._push(p.me, ch, p.at(-1), src)
        self._push(p.me, ch, p.partner, src)

    def wait(self, b, ch):
        v = self.view(b, ch)
        pltpu.make_async_copy(v, v, self.recv.at[b, ch]).wait()

    def service(self, h, ch):
        p = self.p
        right = self.right(ch)
        for sign, far in ((1, right), (-1, jnp.logical_not(right))):
            b = p.at(-sign * h)

            @pl.when((h < self.far) | far)
            def _():
                self.wait(b, ch)

                @pl.when((h < self.far - 1) | ((h == self.far - 1) & far))
                def _():
                    self._push(b, ch, p.at(sign))

                self._push(b, ch, p.partner)

    def drain(self, whole):
        pltpu.make_async_copy(whole, whole, self.send).wait()


class Cross:
    def __init__(self, place, buf, lo, hi, n_chunk, recv_sem, near_sem, far_sem, shift):
        self.p, self.buf, self.lo, self.hi, self.n_chunk, self.shift = place, buf, lo, hi, n_chunk, shift
        self.recv, self.near, self.far_sem = recv_sem, near_sem, far_sem
        self.far = place.nz // 2
        self.size = (hi - lo) // n_chunk

    def _rows(self, ch):
        return pl.ds(self.lo + ch * self.size, self.size)

    def _push(self, b, ch, dst, sem, src=None):
        v = self.buf.at[b, self._rows(ch), :]
        pltpu.make_async_remote_copy(
            src_ref=v if src is None else src, dst_ref=v, send_sem=sem, recv_sem=self.recv.at[b, ch],
            device_id=dst, device_id_type=MESH).start()

    def _push_over(self, b, ch):
        p = self.p
        for i in range(1, p.n_dp):
            self._push(b, ch, {"dp": p.column(i), "tp": p.me}, self.far_sem.at[b // 2])
        self._push(b, ch, {"tp": p.partner}, self.near)

    def _mine(self, b):
        return lax.rem(b + self.shift, self.p.n_dp) == self.p.col

    def own(self, src):
        p = self.p
        for ch in range(self.n_chunk):
            part = src.at[self._rows(ch), :]

            @pl.when(self._mine(p.me))
            def _():
                for off in (1, -1):
                    self._push(p.me, ch, {"tp": p.at(off)}, self.far_sem.at[p.z], part)

            self._push(p.me, ch, {"tp": p.partner}, self.near, part)

    def wait(self, b, ch):
        v = self.buf.at[b, self._rows(ch), :]
        pltpu.make_async_copy(v, v, self.recv.at[b, ch]).wait()

    def _each(self, h, body):
        p = self.p
        for sign, core in ((1, 0), (-1, 1)):
            b = p.at(-sign * h)

            @pl.when((h < self.far) | (p.c == core))
            def _():
                body(b, sign, (h < self.far - 1) | ((h == self.far - 1) & (p.c == core)))

    def along(self, h, ch):
        p = self.p

        def body(b, sign, onward):
            @pl.when(self._mine(b))
            def _():
                self.wait(b, ch)

                @pl.when(onward)
                def _():
                    self._push(b, ch, {"tp": p.at(sign)}, self.far_sem.at[b // 2])

                self._push_over(b, ch)

        self._each(h, body)

    def across(self, h, ch):
        p = self.p

        def body(b, sign, onward):
            @pl.when(jnp.logical_not(self._mine(b)))
            def _():
                self.wait(b, ch)
                self._push(b, ch, {"tp": p.partner}, self.near)

        self._each(h, body)

    def _sent(self, k, sem):
        if k:
            v = self.buf.at[0:k, self.lo:self.hi, :]
            pltpu.make_async_copy(v, v, sem).wait()

    def finish_near(self):
        p = self.p

        def other(i, _):
            for ch in range(self.n_chunk):
                self.wait(i * 2 + (1 - p.c), ch)
            return 0

        lax.fori_loop(0, p.nz, other, 0)
        self._sent(p.nz, self.near)

    def finish_far(self):
        p = self.p
        over = p.n_dp - 1

        @pl.when(self._mine(p.me))
        def _():
            self._sent(2, self.far_sem.at[p.z])

        def body(b, sign, onward):
            @pl.when(self._mine(b))
            def _():
                @pl.when(onward)
                def _():
                    self._sent(over + 1, self.far_sem.at[b // 2])

                @pl.when(jnp.logical_not(onward))
                def _():
                    self._sent(over, self.far_sem.at[b // 2])

        def hop(h, _):
            self._each(h, body)
            return 0

        lax.fori_loop(1, self.far + 1, hop, 0)


def _copy(src, dst, sem):
    cp = pltpu.make_async_copy(src, dst, sem)
    cp.start()
    return cp


def _stage(l, hd, hu, wo_hbm, wup_hbm, wdn_hbm, wst, sem):
    cps, lo = [], 0
    for src, rows in ((wo_hbm.at[l], hd), (wup_hbm.at[l, 0], hu), (wup_hbm.at[l, 1], hu), (wdn_hbm.at[l], hu)):
        cps.append(_copy(src, wst.at[pl.ds(lo, rows), :], sem.at[len(cps)]))
        lo += rows
    return cps


def _stage_qkvg(l, hd, wq_hbm, w_s, sem):
    return [_copy(wq_hbm.at[l, f], w_s.at[pl.ds(i * HP, hd), :], sem.at[i]) for i, f in enumerate((1, 0, 2, 3))]


class Attend:
    def __init__(self, n_tp, hd, w, brow, bt, k_s, qt_s, vt_s, gt_s, lg, o_s, x_rows):
        self.__dict__.update(locals())
        self.T = bt.shape[0]

    def project(self):
        T, hd = self.T, self.hd
        tile = QT
        for i in range(T // tile):
            rows = pl.ds(i * tile, tile)
            res = _dot(self.x_rows(i, tile), self.w[...], 1, 1) + self.brow
            self.k_s[rows, :] = res[:, :2 * HP].astype(BF16)
            rest = res.T
            self.qt_s[0:HP, rows] = rest[HP:2 * HP].astype(BF16)
            ones = lax.broadcasted_iota(jnp.int32, (HP, tile), 0) == hd
            self.vt_s[:, rows] = jnp.where(ones, 1.0, rest[2 * HP:3 * HP]).astype(BF16)
            self.gt_s[:, rows] = _sig(rest[3 * HP:3 * HP + hd])

    def attend(self, slot, hook=None):
        T, hd = self.T, self.hd
        n = T // QT
        c1 = LOG2E / math.sqrt(hd)

        def scores(i):
            cols = pl.ds(i * QT, QT)
            logits = _dot(self.k_s[...], self.qt_s[:, cols]) * c1 + self.bt[:, cols]
            self.lg[i % 2] = logits
            return jnp.max(logits, axis=0, keepdims=True)

        top = scores(0)
        if hook is not None:
            hook()
        for i in range(n):
            cols = pl.ds(i * QT, QT)
            nxt = scores(i + 1) if i + 1 < n else None
            probs = jnp.exp2(self.lg[i % 2] - top).astype(BF16)
            mixed = _dot(self.vt_s[...], probs)
            self.o_s[slot, :, cols] = (self.gt_s[:, cols] * (mixed[:hd] / mixed[hd:hd + 1])).astype(BF16)
            top = nxt


def _load_bias(bias_v, mask_ref, bt):
    T = bt.shape[0]
    mask_add = (mask_ref[...].astype(F32) - 1.0) * 1e9

    def step(i, _):
        r = pl.multiple_of(i * 128, 128)
        rows = (bias_v[pl.ds(r, 128), :].astype(F32) + mask_add) * LOG2E
        bt[:, pl.ds(r, 128)] = rows.T
        return 0

    lax.fori_loop(0, T // 128, step, 0)


class Exchange:
    def __init__(self, place, sample_of, o_s, o_out, send_sem, recv_sem):
        self.p, self.sample_of, self.o_s, self.o_out, self.send, self.recv = place, sample_of, o_s, o_out, send_sem, recv_sem
        self.half = o_s.shape[-1] // 2

    def _each(self, k, remote, local):
        p = self.p
        for c in range(2):
            dst = self.sample_of(k) * 2 + c
            src = self.o_s.at[k, :, pl.ds(c * self.half, self.half)]
            sem = self.send.at[k, c]
            cp = pltpu.make_async_remote_copy(
                src_ref=src, dst_ref=self.o_out.at[p.me], send_sem=sem, recv_sem=self.recv,
                device_id={"tp": dst}, device_id_type=MESH)

            @pl.when(dst != p.me)
            def _():
                remote(cp)

            @pl.when(dst == p.me)
            def _():
                local(pltpu.make_async_copy(src, self.o_out.at[p.me], sem))

    def start(self, k):
        self._each(k, lambda cp: cp.start(), lambda cp: cp.start())

    def sent(self):
        def one(k, _):
            self._each(k, lambda cp: cp.wait_send(), lambda cp: cp.wait())
            return 0

        lax.fori_loop(0, self.o_s.shape[0], one, 0)

    def arrived(self):
        rest = self.o_out.at[0:self.p.n - 1]
        pltpu.make_async_copy(rest, rest, self.recv).wait()


def _bias_row(bq, hd):
    return jnp.concatenate([jnp.zeros((1, HP), F32), bq, jnp.zeros((1, 3 * HP - hd), F32)], axis=1)


def _gates(out, cond, w, bias):
    d = bias.shape[-1]
    out[...] = _dot(cond, w)
    for j in range(bias.shape[0]):
        cols = pl.ds(j * d, d)
        out[:, cols] = _sig(out[:, cols] + bias[j:j + 1, :])


def _modulation(out, cond_normed, scale, w, bias):
    d = bias.shape[-1]
    out[...] = _dot((cond_normed * scale).astype(BF16), w)
    out[:, :d] = _sig(out[:, :d] + bias)


def _flat(raw):
    c, two, d = raw.shape
    return raw[...].reshape(c, two * d)


def _transition(dims, tile, gates, mod1, o_v, act, wall, y_s, h_s, rows):
    D, n_tp, hd, hu = dims
    w_o = wall[:, 0:hd, :].reshape(n_tp * hd, D)
    o_t = o_v[:, :, rows].reshape(n_tp * hd, tile)
    t = _dot(o_t, w_o, 0, 0).astype(BF16).astype(F32)
    mid = (act[rows, :].astype(F32) + gates[rows, :D] * t).astype(BF16).astype(F32)
    y_s[...] = (mod1[rows, :D] * _ln(mid) + mod1[rows, D:]).astype(BF16)
    step = 4 * hu
    for j in range(n_tp * hu // step):
        dv = slice(4 * j, 4 * j + 4)
        u1 = _dot(y_s[...], wall[dv, hd:hd + hu, :].reshape(step, D), 1, 1)
        u2 = _dot(y_s[...], wall[dv, hd + hu:hd + 2 * hu, :].reshape(step, D), 1, 1)
        h_s[:, j * step:(j + 1) * step] = (u1 * _sig(u1) * u2).astype(BF16)
    r = _dot(h_s[...], wall[:, hd + 2 * hu:hd + 3 * hu, :].reshape(n_tp * hu, D)).astype(BF16).astype(F32)
    return (mid + gates[rows, D:] * r).astype(BF16)


def _main_kernel(dims, x_hbm, cond_hbm, bias_hbm, mask_ref, wq_hbm, bq_ref, asc_ref, aw_hbm, ab_ref, zw_hbm, zb_ref, wo_hbm, wup_hbm, wdn_hbm,
                 xg, w1g,
                 bias_v, bt, w_s, k_s, qt_s, vt_s, gt_s, lg, o_s, xraw, craw, xn, raw, aw_s, flat_s, wst, wst1, cond, act, y_s, h_s,
                 wall, gate, mod, nxt, o0, o1,
                 ld_sem, cd_sem, b_sem, q_sem, a_sem, st_sem, own_sem, k_sem, n_send, n_recv, n_free,
                 o_send, o_recv, w_send, w_recv, c_near, c_far, c_recv, d_near, d_far, d_recv, x_send, x_recv, r_send, r_recv, ready):
    S, T, D, C, n_tp, n_dp, hd, hu, n_chunk, n_tile = dims
    p = Place(n_tp, n_dp)
    entered = p.enter()
    far = p.nz // 2
    rows_w = hd + 3 * hu
    cut = 2 * hd
    R = S * T // n_tp
    row0 = p.me * R
    tile = R // n_tile
    mine = pl.ds(p.c * R, R)
    stage = [_stage(l, hd, hu, wo_hbm, wup_hbm, wdn_hbm, w, st_sem.at[l]) for l, w in enumerate((wst, wst1))]

    def toward(k):
        j = S - 1 - k
        return lax.rem(p.z + S + (1 - 2 * lax.rem(j, 2)) * ((j + 1) // 2), S)

    def outward(j):
        return lax.rem(p.z + S + (1 - 2 * p.c) * (1 - 2 * lax.rem(j, 2)) * ((j + 1) // 2), S)

    def loads(k, slot):
        s = toward(k)
        return [pltpu.make_async_copy(x_hbm.at[s, mine], xraw.at[slot], ld_sem.at[slot]),
                pltpu.make_async_copy(cond_hbm.at[s, mine], craw.at[slot], cd_sem.at[slot])]

    raw0 = _copy(aw_hbm.at[0, 0], raw.at[0], a_sem.at[0])
    for k in range(2):
        for cp in loads(k, k):
            cp.start()
    bias_cp = _copy(bias_hbm.at[0, 0], bias_v, b_sem)
    for cp in stage[0]:
        cp.wait()
    raws = [_copy(src, raw.at[i + 1], a_sem.at[i + 1]) for i, src in enumerate((zw_hbm.at[0], aw_hbm.at[0, 1], aw_hbm.at[1, 0]))]
    own = [_copy(cond_hbm.at[p.z, mine], cond, own_sem.at[0]), _copy(x_hbm.at[p.z, mine], act, own_sem.at[1])]
    entered()
    ring_o = Ring(p, lambda b, ch: wall.at[b, 0:cut, :], w_recv, w_send)
    cross = Cross(p, wall, cut, rows_w, n_chunk, c_recv, c_near, c_far, 0)
    cross1 = Cross(p, w1g, 0, rows_w, n_chunk, d_recv, d_near, d_far, 1)
    ring_x = Ring(p, lambda b, ch: xg.at[pl.ds(b * R + ch * tile, tile), :], x_recv, x_send)
    ring_r = Ring(p, lambda b, ch: xg.at[pl.ds(b * R + ch * tile, tile), :], r_recv, r_send)
    ring_o.own(0, wst.at[0:cut, :])
    cross.own(wst)
    w_s[...] = jnp.zeros_like(w_s)
    qt_s[HP:, :] = jnp.zeros((HP, T), BF16)
    wq = _stage_qkvg(0, hd, wq_hbm, w_s, q_sem)

    def half(slot):
        v = xn.at[slot, mine]
        return pltpu.make_async_remote_copy(src_ref=v, dst_ref=v, send_sem=n_send.at[slot], recv_sem=n_recv.at[slot],
                                            device_id={"tp": p.partner}, device_id_type=MESH)

    def normalise(slot):
        big = R // 2
        for i in range(2):
            rows = pl.ds(i * big, big)
            cn = _ln(craw[slot, rows, :].astype(F32))
            y = _ada(xraw[slot, rows, :].astype(F32), cn, asc_ref[0, 0:1, :], aw_s[...], ab_ref[0, 0:1, :])
            xn[slot, pl.ds(pl.multiple_of(p.c * R, R) + i * big, big), :] = y

    raw0.wait()
    aw_s[...] = _flat(raw.at[0])
    for cp in loads(0, 0):
        cp.wait()
    normalise(0)
    bias_cp.wait()
    half(0).start()
    _load_bias(bias_v, mask_ref, bt)
    bias_cp = _copy(bias_hbm.at[1, 0], bias_v, b_sem)
    for cp in stage[1] + wq:
        cp.wait()
    wall[p.me] = wst[...]
    keep = _copy(wst1, w1g.at[p.me], k_sem)

    def gates(l, i):
        raws[i].wait()
        flat_s[...] = _flat(raw.at[i + 1])
        _gates(gate, cond[...], flat_s[...], zb_ref.at[l])

    def modulation(out, l, j, i):
        raws[i].wait()
        flat_s[...] = _flat(raw.at[i + 1])
        cn = _ln(cond[...].astype(F32))
        _modulation(out, cn, asc_ref[l, j:j + 1, :], flat_s[...], ab_ref[l, j:j + 1, :])

    events = {}

    def plan(when, f, *args):
        events.setdefault(when, []).append((f, args))

    def take(step, k):
        for when in sorted(events):
            if when % 2 == step:
                @pl.when(k == when // 2)
                def _():
                    for f, args in events[when]:
                        f(*args)

    first, over, first1 = (0, 4, 7, 10), (4, 8, 11, 14), (10, 13)
    for h in range(1, far + 1):
        plan(first[h - 1] + 1, ring_o.service, h, 0)
        for ch in range(n_chunk):
            plan(first[h - 1] + ch, cross.along, h, ch)
            plan(over[h - 1] + ch, cross.across, h, ch)
    for h, when in enumerate(first1):
        for ch in range(n_chunk):
            plan(when + (ch + 1) // 2, cross1.along, h + 1, ch)
    plan(6, cross1.own, wst1)
    for cp in own:
        plan(3, cp.wait)
    plan(5, gates, 0, 0)
    plan(7, modulation, mod, 0, 1, 1)
    plan(9, modulation, nxt, 1, 0, 2)
    ex = [Exchange(p, order, o_s, o, o_send.at[l], o_recv.at[l]) for l, (order, o) in enumerate(((toward, o0), (outward, o1)))]
    brow = [_bias_row(bq_ref[l:l + 1, :], hd) for l in range(2)]
    heads = (n_tp, hd, w_s)
    work = (bt, k_s, qt_s, vt_s, gt_s, lg, o_s)

    def step0(k, _):
        slot = lax.rem(k, 2)

        @pl.when(k + 2 < S)
        def _():
            for cp in loads(k + 2, slot):
                cp.start()

        with scope("a_half"):
            v = xn.at[slot, pl.ds((1 - p.c) * R, R)]
            pltpu.make_async_copy(v, v, n_recv.at[slot]).wait()
            half(slot).wait_send()
        at = Attend(*heads, brow[0], *work, lambda i, t: xn[slot, pl.ds(i * t, t), :])
        at.project()

        @pl.when(k + 2 < S)
        def _():
            pl.semaphore_signal(n_free, inc=1, device_id={"tp": p.partner}, device_id_type=MESH)

        @pl.when(k >= 1)
        def _():
            ex[0].start(k - 1)

        @pl.when(k + 1 < S)
        def _():
            for cp in loads(k + 1, 1 - slot):
                cp.wait()
            normalise(1 - slot)

            @pl.when(k >= 1)
            def _():
                pl.semaphore_wait(n_free, 1)

        with scope("a_ev0"):
            take(0, k)

        def hook():
            @pl.when(k + 1 < S)
            def _():
                half(1 - slot).start()

        with scope("a_att"):
            at.attend(k, hook)
        with scope("a_ev1"):
            take(1, k)
        return 0

    lax.fori_loop(0, S, step0, 0)
    ex[0].start(S - 1)
    wq = _stage_qkvg(1, hd, wq_hbm, w_s, q_sem)
    raws = [_copy(src, raw.at[i + 1], a_sem.at[i + 1]) for i, src in enumerate((zw_hbm.at[1], aw_hbm.at[1, 1]))]
    for when in sorted(events):
        if when >= 2 * S:
            for f, args in events[when]:
                f(*args)

    def other(i, _):
        ring_o.wait(i * 2 + (1 - p.c), 0)
        return 0

    with scope("b_w0"):
        lax.fori_loop(0, p.nz, other, 0)
        cross.finish_near()
    with scope("b_o0"):
        ex[0].sent()
        ex[0].arrived()
    size = (D, n_tp, hd, hu)

    def tile0(ch, _):
        rows = pl.ds(pl.multiple_of(ch * tile, tile), tile)
        with scope("b_mlp"):
            new = _transition(size, tile, gate, mod, o0, act, wall, y_s, h_s, rows)
            act[rows, :] = new
            xg[pl.ds(pl.multiple_of(row0 + ch * tile, tile), tile), :] = (nxt[rows, :D] * _ln(new.astype(F32)) + nxt[rows, D:]).astype(BF16)
        ring_x.own(ch)

        @pl.when(ch == 1)
        def _():
            with scope("b_along"):
                for i in range(n_chunk):
                    cross1.along(far - 1, i)
        return 0

    lax.fori_loop(0, n_tile, tile0, 0)
    bias_cp.wait()
    _load_bias(bias_v, mask_ref, bt)
    for cp in wq:
        cp.wait()
    ring_o.drain(wall.at[0:n_tp - 1, 0:cut, :])
    cross.finish_far()
    keep.wait()
    events = {}
    for ch in range(n_chunk):
        plan(5, cross1.along, far, ch)
        for h in range(1, far + 1):
            plan(2 * h + 5, cross1.across, h, ch)
    plan(1, gates, 1, 0)
    plan(5, modulation, mod, 1, 1, 1)

    def last_weights():
        cross1.finish_near()
        pltpu.make_async_copy(w1g, wall, k_sem).start()

    plan(2 * S - 3, last_weights)

    def step1(j, _):
        with scope("b_svc"):
            for i in range(n_tile // 2):
                ring_x.service(j // 2 + 1, lax.rem(j, 2) * (n_tile // 2) + i)

        @pl.when(j >= 1)
        def _():
            ex[1].start(j - 1)

        s = outward(j)
        with scope("b_half"):
            for ch in range(n_tile):
                ring_x.wait(s * 2 + (1 - p.c), ch)
        at = Attend(*heads, brow[1], *work, lambda i, t: xg[pl.ds(pl.multiple_of(s * T, T) + i * t, t), :])
        with scope("b_att"):
            at.project()
            at.attend(j)
        with scope("b_ev"):
            take(1, j)
        return 0

    lax.fori_loop(0, S, step1, 0)
    ex[1].start(S - 1)
    pltpu.make_async_copy(w1g, wall, k_sem).wait()
    cross1.finish_far()
    ring_x.drain(xg.at[0:(n_tp - 1) * R, :])
    for peer in (p.at(1), p.at(-1), p.partner):
        pl.semaphore_signal(ready, inc=1, device_id={"tp": peer}, device_id_type=MESH)
    with scope("c_o1"):
        ex[1].sent()
        ex[1].arrived()
    def tile1(ch, _):
        rows = pl.ds(pl.multiple_of(ch * tile, tile), tile)
        with scope("c_mlp"):
            xg[pl.ds(pl.multiple_of(row0 + ch * tile, tile), tile), :] = _transition(size, tile, gate, mod, o1, act, wall, y_s, h_s, rows)

        @pl.when(ch == 0)
        def _():
            with scope("c_ready"):
                pl.semaphore_wait(ready, 3)

        ring_r.own(ch)
        return 0

    lax.fori_loop(0, n_tile, tile1, 0)
    with scope("c_svc"):
        lax.fori_loop(0, far * n_tile, lambda e, _: (ring_r.service(e // n_tile + 1, lax.rem(e, n_tile)), 0)[1], 0)

    def rest(i, _):
        for ch in range(n_tile):
            ring_r.wait(i * 2 + (1 - p.c), ch)
        return 0

    with scope("c_end"):
        lax.fori_loop(0, p.nz, rest, 0)
        ring_r.drain(xg.at[0:(n_tp - 1) * R, :])


def _main(n_dp, x, cond, pair_bias, mask_row, wq, bq, asc, aw, ab, zw, zb, wo, wup, wdn):
    S, T, D = x.shape
    C = cond.shape[-1]
    hd, hu = wq.shape[2], wdn.shape[1]
    n_tp = S * 2
    rows_w = hd + 3 * hu
    R = T // 2
    n_chunk = 3
    dma = pltpu.SemaphoreType.DMA
    v = pltpu.VMEM
    pair, blocks, each = dma((2,)), dma((S,)), dma((n_tp, n_chunk))
    n_tile = 4
    tiles = dma((n_tp, n_tile))
    return pl.pallas_call(
        functools.partial(_main_kernel, (S, T, D, C, n_tp, n_dp, hd, hu, n_chunk, n_tile)),
        out_shape=(v((n_tp * R, D), BF16), pltpu.HBM((n_tp, rows_w, D), BF16)),
        in_specs=[ANY, ANY, ANY, VMEM, ANY, VMEM, VMEM, ANY, VMEM, ANY, VMEM, ANY, ANY, ANY],
        out_specs=(VMEM, HBM),
        scratch_shapes=[
            v((T, T), BF16), v((T, T), F32), v((4 * HP, D), BF16), v((T, 2 * HP), BF16), v((2 * HP, T), BF16), v((HP, T), BF16),
            v((hd, T), F32), v((2, T, QT), F32), v((S, hd, T), BF16),
            v((2, R, D), BF16), v((2, R, C), BF16), v((2, T, D), BF16), v((4, C, 2, D), BF16), *[v((C, 2 * D), BF16)] * 2,
            *[v((rows_w, D), BF16)] * 2, v((R, C), BF16), v((R, D), BF16), v((R // n_tile, D), BF16), v((R // n_tile, n_tp * hu), BF16),
            v((n_tp, rows_w, D), BF16), *[v((R, 2 * D), F32)] * 3, *[v((n_tp, hd, R), BF16)] * 2,
            pair, pair, dma, dma((4,)), dma((4,)), dma((2, 4)), pair, dma, pair, pair, pltpu.SemaphoreType.REGULAR,
            dma((2, S, 2)), pair, dma, dma((n_tp, 1)), dma, blocks, each, dma, blocks, each, dma, tiles, dma, tiles, pltpu.SemaphoreType.REGULAR],
        cost_estimate=pl.CostEstimate(flops=S * T * T * D, bytes_accessed=S * T * D, transcendentals=S * T * T),
        compiler_params=pltpu.CompilerParams(collective_id=0, has_side_effects=True, vmem_limit_bytes=VM),
        name="blocks",
    )(x, cond, pair_bias, mask_row, wq, bq, asc, aw, ab, zw, zb, wo, wup, wdn)


def _store_kernel(src, dst, sem):
    cp = pltpu.make_async_copy(src, dst, sem)
    cp.start()
    cp.wait()


def _store(x):
    return pl.pallas_call(
        _store_kernel, out_shape=jax.ShapeDtypeStruct(x.shape, x.dtype), in_specs=[VMEM], out_specs=ANY,
        scratch_shapes=[pltpu.SemaphoreType.DMA], compiler_params=pltpu.CompilerParams(vmem_limit_bytes=1 << 20), name="store")(x)


def solution(mesh):
    n_dp = mesh.shape["dp"]

    def shard_body(token_act, token_cond, pair_bias, token_mask, ada_scale, ada_w, ada_bias, zero_w, zero_b, w_qkvg, b_q, w_o, w_up, w_down):
        S, T, D = token_act.shape
        mask_row = token_mask.reshape(1, T)
        wq = jnp.transpose(w_qkvg, (0, 2, 3, 1))
        wup = jnp.transpose(w_up, (0, 2, 3, 1))
        out, _ = _main(n_dp, token_act, token_cond, pair_bias, mask_row, wq, b_q, ada_scale, ada_w, ada_bias, zero_w, zero_b, w_o, wup, w_down)
        out = pltpu.with_memory_space_constraint(out, pltpu.VMEM)
        return _store(out).reshape(S, T, D)

    everywhere = P()
    rows, second, fourth = P('dp'), P(None, 'tp'), P(*[None] * 3, 'tp')
    in_specs = (rows, rows, second) + (everywhere,) * 6 + (fourth, second, second, fourth, second)
    return jax.shard_map(shard_body, mesh=mesh, in_specs=in_specs, out_specs=rows, check_vma=False)
```

```python
import functools
import math

import jax
import jax.numpy as jnp
from jax import lax
from jax.experimental import pallas as pl
from jax.experimental.pallas import tpu as pltpu
from jax.sharding import PartitionSpec as P

LN_EPS = 1e-5
LOG2E = 1.4426950408889634
MESH = pl.DeviceIdType.MESH
BF16 = jnp.bfloat16
F32 = jnp.float32
scope = jax.named_scope
HP = 64
QT = 256
ANY = pl.BlockSpec(memory_space=pl.ANY)
VMEM = pl.BlockSpec(memory_space=pltpu.VMEM)
HBM = pl.BlockSpec(memory_space=pltpu.HBM)
VM = 50 << 20


def _ln(x):
    mean = jnp.mean(x, axis=-1, keepdims=True)
    cen = x - mean
    var = jnp.mean(cen * cen, axis=-1, keepdims=True)
    return cen * lax.rsqrt(var + LN_EPS)


def _sig(x):
    return 0.5 * jnp.tanh(0.5 * x) + 0.5


def _dot(a, b, ca=1, cb=0):
    return lax.dot_general(a, b, (((ca,), (cb,)), ((), ())), preferred_element_type=F32)


def _ada(x_f32, cond_normed, scale, w, bias):
    d = x_f32.shape[-1]
    mod = _dot((cond_normed * scale).astype(BF16), w)
    return (_sig(mod[:, :d] + bias) * _ln(x_f32) + mod[:, d:]).astype(BF16)


class Place:
    def __init__(self, n_tp, n_dp):
        self.n = n_tp
        self.n_dp = n_dp
        self.col = lax.axis_index("dp")
        self.nz = n_tp // 2
        self.me = lax.axis_index("tp")
        self.z = self.me // 2
        self.c = lax.rem(self.me, 2)
        self.partner = self.z * 2 + (1 - self.c)

    def at(self, off):
        return lax.rem(self.z + off + self.nz, self.nz) * 2 + self.c

    def column(self, i):
        return lax.rem(self.col + i, self.n_dp)

    def enter(self):
        barrier = pltpu.get_barrier_semaphore()
        peers = [{"tp": lax.rem(self.me + i, self.n)} for i in range(1, self.n)]
        peers += [{"dp": self.column(i), "tp": self.me} for i in range(1, self.n_dp)]
        for peer in peers:
            pl.semaphore_signal(barrier, inc=1, device_id=peer, device_id_type=MESH)
        return lambda: pl.semaphore_wait(barrier, len(peers))


class Ring:
    def __init__(self, place, view, recv_sem, send_sem, right=None):
        self.p, self.view, self.recv, self.send = place, view, recv_sem, send_sem
        self.far = place.nz // 2
        self.right = right or (lambda ch: place.c == 0)

    def _push(self, b, ch, dst, src=None):
        v = self.view(b, ch)
        pltpu.make_async_remote_copy(
            src_ref=v if src is None else src, dst_ref=v, send_sem=self.send, recv_sem=self.recv.at[b, ch],
            device_id={"tp": dst}, device_id_type=MESH).start()

    def own(self, ch, src=None):
        p = self.p
        self._push(p.me, ch, p.at(1), src)
        self._push(p.me, ch, p.at(-1), src)
        self._push(p.me, ch, p.partner, src)

    def wait(self, b, ch):
        v = self.view(b, ch)
        pltpu.make_async_copy(v, v, self.recv.at[b, ch]).wait()

    def service(self, h, ch):
        p = self.p
        right = self.right(ch)
        for sign, far in ((1, right), (-1, jnp.logical_not(right))):
            b = p.at(-sign * h)

            @pl.when((h < self.far) | far)
            def _():
                self.wait(b, ch)

                @pl.when((h < self.far - 1) | ((h == self.far - 1) & far))
                def _():
                    self._push(b, ch, p.at(sign))

                self._push(b, ch, p.partner)

    def drain(self, whole):
        pltpu.make_async_copy(whole, whole, self.send).wait()


class Cross:
    def __init__(self, place, buf, lo, hi, n_chunk, recv_sem, near_sem, far_sem, shift):
        self.p, self.buf, self.lo, self.hi, self.n_chunk, self.shift = place, buf, lo, hi, n_chunk, shift
        self.recv, self.near, self.far_sem = recv_sem, near_sem, far_sem
        self.far = place.nz // 2
        self.size = (hi - lo) // n_chunk

    def _rows(self, ch):
        return pl.ds(self.lo + ch * self.size, self.size)

    def _push(self, b, ch, dst, sem, src=None):
        v = self.buf.at[b, self._rows(ch), :]
        pltpu.make_async_remote_copy(
            src_ref=v if src is None else src, dst_ref=v, send_sem=sem, recv_sem=self.recv.at[b, ch],
            device_id=dst, device_id_type=MESH).start()

    def _push_over(self, b, ch):
        p = self.p
        for i in range(1, p.n_dp):
            self._push(b, ch, {"dp": p.column(i), "tp": p.me}, self.far_sem.at[b // 2])
        self._push(b, ch, {"tp": p.partner}, self.near)

    def _mine(self, b):
        return lax.rem(b + self.shift, self.p.n_dp) == self.p.col

    def own(self, src):
        p = self.p
        for ch in range(self.n_chunk):
            part = src.at[self._rows(ch), :]

            @pl.when(self._mine(p.me))
            def _():
                for off in (1, -1):
                    self._push(p.me, ch, {"tp": p.at(off)}, self.far_sem.at[p.z], part)

            self._push(p.me, ch, {"tp": p.partner}, self.near, part)

    def wait(self, b, ch):
        v = self.buf.at[b, self._rows(ch), :]
        pltpu.make_async_copy(v, v, self.recv.at[b, ch]).wait()

    def _each(self, h, body):
        p = self.p
        for sign, core in ((1, 0), (-1, 1)):
            b = p.at(-sign * h)

            @pl.when((h < self.far) | (p.c == core))
            def _():
                body(b, sign, (h < self.far - 1) | ((h == self.far - 1) & (p.c == core)))

    def along(self, h, ch):
        p = self.p

        def body(b, sign, onward):
            @pl.when(self._mine(b))
            def _():
                self.wait(b, ch)

                @pl.when(onward)
                def _():
                    self._push(b, ch, {"tp": p.at(sign)}, self.far_sem.at[b // 2])

                self._push_over(b, ch)

        self._each(h, body)

    def across(self, h, ch):
        p = self.p

        def body(b, sign, onward):
            @pl.when(jnp.logical_not(self._mine(b)))
            def _():
                self.wait(b, ch)
                self._push(b, ch, {"tp": p.partner}, self.near)

        self._each(h, body)

    def _sent(self, k, sem):
        if k:
            v = self.buf.at[0:k, self.lo:self.hi, :]
            pltpu.make_async_copy(v, v, sem).wait()

    def finish_near(self):
        p = self.p

        def other(i, _):
            for ch in range(self.n_chunk):
                self.wait(i * 2 + (1 - p.c), ch)
            return 0

        lax.fori_loop(0, p.nz, other, 0)
        self._sent(p.nz, self.near)

    def finish_far(self):
        p = self.p
        over = p.n_dp - 1

        @pl.when(self._mine(p.me))
        def _():
            self._sent(2, self.far_sem.at[p.z])

        def body(b, sign, onward):
            @pl.when(self._mine(b))
            def _():
                @pl.when(onward)
                def _():
                    self._sent(over + 1, self.far_sem.at[b // 2])

                @pl.when(jnp.logical_not(onward))
                def _():
                    self._sent(over, self.far_sem.at[b // 2])

        def hop(h, _):
            self._each(h, body)
            return 0

        lax.fori_loop(1, self.far + 1, hop, 0)


def _copy(src, dst, sem):
    cp = pltpu.make_async_copy(src, dst, sem)
    cp.start()
    return cp


def _stage(l, hd, hu, wo_hbm, wup_hbm, wdn_hbm, wst, sem):
    cps, lo = [], 0
    for src, rows in ((wo_hbm.at[l], hd), (wup_hbm.at[l, 0], hu), (wup_hbm.at[l, 1], hu), (wdn_hbm.at[l], hu)):
        cps.append(_copy(src, wst.at[pl.ds(lo, rows), :], sem.at[len(cps)]))
        lo += rows
    return cps


def _stage_qkvg(l, hd, wq_hbm, w_s, sem):
    return [_copy(wq_hbm.at[l, f], w_s.at[pl.ds(i * HP, hd), :], sem.at[i]) for i, f in enumerate((1, 0, 2, 3))]


class Attend:
    def __init__(self, n_tp, hd, w, brow, bt, k_s, qt_s, vt_s, gt_s, lg, o_s, x_rows):
        self.__dict__.update(locals())
        self.T = bt.shape[0]

    def project(self):
        T, hd = self.T, self.hd
        tile = QT
        for i in range(T // tile):
            rows = pl.ds(i * tile, tile)
            res = _dot(self.x_rows(i, tile), self.w[...], 1, 1) + self.brow
            self.k_s[rows, :] = res[:, :2 * HP].astype(BF16)
            rest = res.T
            self.qt_s[0:HP, rows] = rest[HP:2 * HP].astype(BF16)
            ones = lax.broadcasted_iota(jnp.int32, (HP, tile), 0) == hd
            self.vt_s[:, rows] = jnp.where(ones, 1.0, rest[2 * HP:3 * HP]).astype(BF16)
            self.gt_s[:, rows] = _sig(rest[3 * HP:3 * HP + hd])

    def attend(self, slot, hook=None):
        T, hd = self.T, self.hd
        n = T // QT
        c1 = LOG2E / math.sqrt(hd)

        def scores(i):
            cols = pl.ds(i * QT, QT)
            logits = _dot(self.k_s[...], self.qt_s[:, cols]) * c1 + self.bt[:, cols]
            self.lg[i % 2] = logits
            return jnp.max(logits, axis=0, keepdims=True)

        top = scores(0)
        if hook is not None:
            hook()
        for i in range(n):
            cols = pl.ds(i * QT, QT)
            nxt = scores(i + 1) if i + 1 < n else None
            probs = jnp.exp2(self.lg[i % 2] - top).astype(BF16)
            mixed = _dot(self.vt_s[...], probs)
            self.o_s[slot, :, cols] = (self.gt_s[:, cols] * (mixed[:hd] / mixed[hd:hd + 1])).astype(BF16)
            top = nxt


def _load_bias(bias_v, mask_ref, bt):
    T = bt.shape[0]
    mask_add = (mask_ref[...].astype(F32) - 1.0) * 1e9

    def step(i, _):
        r = pl.multiple_of(i * 128, 128)
        rows = (bias_v[pl.ds(r, 128), :].astype(F32) + mask_add) * LOG2E
        bt[:, pl.ds(r, 128)] = rows.T
        return 0

    lax.fori_loop(0, T // 128, step, 0)


class Exchange:
    def __init__(self, place, sample_of, o_s, o_out, send_sem, recv_sem):
        self.p, self.sample_of, self.o_s, self.o_out, self.send, self.recv = place, sample_of, o_s, o_out, send_sem, recv_sem
        self.half = o_s.shape[-1] // 2

    def _each(self, k, remote, local):
        p = self.p
        for c in range(2):
            dst = self.sample_of(k) * 2 + c
            src = self.o_s.at[k, :, pl.ds(c * self.half, self.half)]
            sem = self.send.at[k, c]
            cp = pltpu.make_async_remote_copy(
                src_ref=src, dst_ref=self.o_out.at[p.me], send_sem=sem, recv_sem=self.recv,
                device_id={"tp": dst}, device_id_type=MESH)

            @pl.when(dst != p.me)
            def _():
                remote(cp)

            @pl.when(dst == p.me)
            def _():
                local(pltpu.make_async_copy(src, self.o_out.at[p.me], sem))

    def start(self, k):
        self._each(k, lambda cp: cp.start(), lambda cp: cp.start())

    def sent(self):
        def one(k, _):
            self._each(k, lambda cp: cp.wait_send(), lambda cp: cp.wait())
            return 0

        lax.fori_loop(0, self.o_s.shape[0], one, 0)

    def arrived(self):
        rest = self.o_out.at[0:self.p.n - 1]
        pltpu.make_async_copy(rest, rest, self.recv).wait()


def _bias_row(bq, hd):
    return jnp.concatenate([jnp.zeros((1, HP), F32), bq, jnp.zeros((1, 3 * HP - hd), F32)], axis=1)


def _gates(out, cond, w, bias):
    d = bias.shape[-1]
    out[...] = _dot(cond, w)
    for j in range(bias.shape[0]):
        cols = pl.ds(j * d, d)
        out[:, cols] = _sig(out[:, cols] + bias[j:j + 1, :])


def _modulation(out, cond_normed, scale, w, bias):
    d = bias.shape[-1]
    out[...] = _dot((cond_normed * scale).astype(BF16), w)
    out[:, :d] = _sig(out[:, :d] + bias)


def _flat(raw):
    c, two, d = raw.shape
    return raw[...].reshape(c, two * d)


def _transition(dims, tile, gates, mod1, o_v, act, wall, y_s, h_s, rows):
    D, n_tp, hd, hu = dims
    w_o = wall[:, 0:hd, :].reshape(n_tp * hd, D)
    o_t = o_v[:, :, rows].reshape(n_tp * hd, tile)
    t = _dot(o_t, w_o, 0, 0).astype(BF16).astype(F32)
    mid = (act[rows, :].astype(F32) + gates[rows, :D] * t).astype(BF16).astype(F32)
    y_s[...] = (mod1[rows, :D] * _ln(mid) + mod1[rows, D:]).astype(BF16)
    step = 4 * hu
    for j in range(n_tp * hu // step):
        dv = slice(4 * j, 4 * j + 4)
        u1 = _dot(y_s[...], wall[dv, hd:hd + hu, :].reshape(step, D), 1, 1)
        u2 = _dot(y_s[...], wall[dv, hd + hu:hd + 2 * hu, :].reshape(step, D), 1, 1)
        h_s[:, j * step:(j + 1) * step] = (u1 * _sig(u1) * u2).astype(BF16)
    r = _dot(h_s[...], wall[:, hd + 2 * hu:hd + 3 * hu, :].reshape(n_tp * hu, D)).astype(BF16).astype(F32)
    return (mid + gates[rows, D:] * r).astype(BF16)


def _main_kernel(dims, x_hbm, cond_hbm, bias_hbm, mask_ref, wq_hbm, bq_ref, asc_ref, aw_hbm, ab_ref, zw_hbm, zb_ref, wo_hbm, wup_hbm, wdn_hbm,
                 xg, w1g,
                 bias_v, bt, w_s, k_s, qt_s, vt_s, gt_s, lg, o_s, xraw, craw, xn, raw, aw_s, flat_s, wst, wst1, cond, act, y_s, h_s,
                 wall, gate, mod, nxt, o0, o1,
                 ld_sem, cd_sem, b_sem, q_sem, a_sem, st_sem, own_sem, k_sem, n_send, n_recv, n_free,
                 o_send, o_recv, w_send, w_recv, c_near, c_far, c_recv, d_near, d_far, d_recv, x_send, x_recv, r_send, r_recv, ready):
    S, T, D, C, n_tp, n_dp, hd, hu, n_chunk, n_tile = dims
    p = Place(n_tp, n_dp)
    entered = p.enter()
    far = p.nz // 2
    rows_w = hd + 3 * hu
    cut = 2 * hd
    R = S * T // n_tp
    row0 = p.me * R
    tile = R // n_tile
    mine = pl.ds(p.c * R, R)
    stage = [_stage(l, hd, hu, wo_hbm, wup_hbm, wdn_hbm, w, st_sem.at[l]) for l, w in enumerate((wst, wst1))]

    def toward(k):
        j = S - 1 - k
        return lax.rem(p.z + S + (1 - 2 * lax.rem(j, 2)) * ((j + 1) // 2), S)

    def outward(j):
        return lax.rem(p.z + S + (1 - 2 * p.c) * (1 - 2 * lax.rem(j, 2)) * ((j + 1) // 2), S)

    def loads(k, slot):
        s = toward(k)
        return [pltpu.make_async_copy(x_hbm.at[s, mine], xraw.at[slot], ld_sem.at[slot]),
                pltpu.make_async_copy(cond_hbm.at[s, mine], craw.at[slot], cd_sem.at[slot])]

    raw0 = _copy(aw_hbm.at[0, 0], raw.at[0], a_sem.at[0])
    for k in range(2):
        for cp in loads(k, k):
            cp.start()
    bias_cp = _copy(bias_hbm.at[0, 0], bias_v, b_sem)
    for cp in stage[0]:
        cp.wait()
    raws = [_copy(src, raw.at[i + 1], a_sem.at[i + 1]) for i, src in enumerate((zw_hbm.at[0], aw_hbm.at[0, 1], aw_hbm.at[1, 0]))]
    own = [_copy(cond_hbm.at[p.z, mine], cond, own_sem.at[0]), _copy(x_hbm.at[p.z, mine], act, own_sem.at[1])]
    entered()
    ring_o = Ring(p, lambda b, ch: wall.at[b, 0:cut, :], w_recv, w_send)
    cross = Cross(p, wall, cut, rows_w, n_chunk, c_recv, c_near, c_far, 0)
    cross1 = Cross(p, w1g, 0, rows_w, n_chunk, d_recv, d_near, d_far, 0)
    ring_x = Ring(p, lambda b, ch: xg.at[pl.ds(b * R + ch * tile, tile), :], x_recv, x_send)
    ring_r = Ring(p, lambda b, ch: xg.at[pl.ds(b * R + ch * tile, tile), :], r_recv, r_send)
    ring_o.own(0, wst.at[0:cut, :])
    cross.own(wst)
    w_s[...] = jnp.zeros_like(w_s)
    qt_s[HP:, :] = jnp.zeros((HP, T), BF16)
    wq = _stage_qkvg(0, hd, wq_hbm, w_s, q_sem)

    def half(slot):
        v = xn.at[slot, mine]
        return pltpu.make_async_remote_copy(src_ref=v, dst_ref=v, send_sem=n_send.at[slot], recv_sem=n_recv.at[slot],
                                            device_id={"tp": p.partner}, device_id_type=MESH)

    def normalise(slot):
        big = R // 2
        for i in range(2):
            rows = pl.ds(i * big, big)
            cn = _ln(craw[slot, rows, :].astype(F32))
            y = _ada(xraw[slot, rows, :].astype(F32), cn, asc_ref[0, 0:1, :], aw_s[...], ab_ref[0, 0:1, :])
            xn[slot, pl.ds(pl.multiple_of(p.c * R, R) + i * big, big), :] = y

    raw0.wait()
    aw_s[...] = _flat(raw.at[0])
    for cp in loads(0, 0):
        cp.wait()
    normalise(0)
    bias_cp.wait()
    half(0).start()
    _load_bias(bias_v, mask_ref, bt)
    bias_cp = _copy(bias_hbm.at[1, 0], bias_v, b_sem)
    for cp in stage[1] + wq:
        cp.wait()
    wall[p.me] = wst[...]
    keep = _copy(wst1, w1g.at[p.me], k_sem)

    def gates(l, i):
        raws[i].wait()
        flat_s[...] = _flat(raw.at[i + 1])
        _gates(gate, cond[...], flat_s[...], zb_ref.at[l])

    def modulation(out, l, j, i):
        raws[i].wait()
        flat_s[...] = _flat(raw.at[i + 1])
        cn = _ln(cond[...].astype(F32))
        _modulation(out, cn, asc_ref[l, j:j + 1, :], flat_s[...], ab_ref[l, j:j + 1, :])

    events = {}

    def plan(when, f, *args):
        events.setdefault(when, []).append((f, args))

    def take(step, k):
        for when in sorted(events):
            if when % 2 == step:
                @pl.when(k == when // 2)
                def _():
                    for f, args in events[when]:
                        f(*args)

    first, over = (0, 7, 9, 12), (5, 10, 13, 16)
    for h in range(1, far + 1):
        plan(first[h - 1] + 1, ring_o.service, h, 0)
        for ch in range(n_chunk):
            plan(first[h - 1] + ch, cross.along, h, ch)
            plan(over[h - 1] + ch, cross.across, h, ch)
    for ch in range(n_chunk):
        plan(2 * S + n_chunk, cross1.along, 1, ch)
    plan(13, cross1.own, wst1)
    for cp in own:
        plan(3, cp.wait)
    plan(5, gates, 0, 0)
    plan(7, modulation, mod, 0, 1, 1)
    plan(9, modulation, nxt, 1, 0, 2)
    ex = [Exchange(p, order, o_s, o, o_send.at[l], o_recv.at[l]) for l, (order, o) in enumerate(((toward, o0), (outward, o1)))]
    brow = [_bias_row(bq_ref[l:l + 1, :], hd) for l in range(2)]
    heads = (n_tp, hd, w_s)
    work = (bt, k_s, qt_s, vt_s, gt_s, lg, o_s)

    def step0(k, _):
        slot = lax.rem(k, 2)

        @pl.when(k + 2 < S)
        def _():
            for cp in loads(k + 2, slot):
                cp.start()

        with scope("a_half"):
            v = xn.at[slot, pl.ds((1 - p.c) * R, R)]
            pltpu.make_async_copy(v, v, n_recv.at[slot]).wait()
            half(slot).wait_send()
        at = Attend(*heads, brow[0], *work, lambda i, t: xn[slot, pl.ds(i * t, t), :])
        at.project()

        @pl.when(k + 2 < S)
        def _():
            pl.semaphore_signal(n_free, inc=1, device_id={"tp": p.partner}, device_id_type=MESH)

        @pl.when(k >= 1)
        def _():
            ex[0].start(k - 1)

        @pl.when(k + 1 < S)
        def _():
            for cp in loads(k + 1, 1 - slot):
                cp.wait()
            normalise(1 - slot)

            @pl.when(k >= 1)
            def _():
                pl.semaphore_wait(n_free, 1)

        with scope("a_ev0"):
            take(0, k)

        def hook():
            @pl.when(k + 1 < S)
            def _():
                half(1 - slot).start()

        with scope("a_att"):
            at.attend(k, hook)
        with scope("a_ev1"):
            take(1, k)
        return 0

    lax.fori_loop(0, S, step0, 0)
    ex[0].start(S - 1)
    wq = _stage_qkvg(1, hd, wq_hbm, w_s, q_sem)
    raws = [_copy(src, raw.at[i + 1], a_sem.at[i + 1]) for i, src in enumerate((zw_hbm.at[1], aw_hbm.at[1, 1]))]
    for when in sorted(events):
        if when >= 2 * S:
            for f, args in events[when]:
                f(*args)

    def other(i, _):
        ring_o.wait(i * 2 + (1 - p.c), 0)
        return 0

    with scope("b_w0"):
        lax.fori_loop(0, p.nz, other, 0)
        cross.finish_near()
    with scope("b_o0"):
        ex[0].sent()
        ex[0].arrived()
    size = (D, n_tp, hd, hu)

    def tile0(ch, _):
        rows = pl.ds(pl.multiple_of(ch * tile, tile), tile)
        with scope("b_mlp"):
            new = _transition(size, tile, gate, mod, o0, act, wall, y_s, h_s, rows)
            act[rows, :] = new
            xg[pl.ds(pl.multiple_of(row0 + ch * tile, tile), tile), :] = (nxt[rows, :D] * _ln(new.astype(F32)) + nxt[rows, D:]).astype(BF16)
        ring_x.own(ch)

        @pl.when(ch == n_tile - 1)
        def _():
            with scope("b_along"):
                for i in range(n_chunk):
                    cross1.along(2, i)
        return 0

    lax.fori_loop(0, n_tile, tile0, 0)
    bias_cp.wait()
    _load_bias(bias_v, mask_ref, bt)
    for cp in wq:
        cp.wait()
    ring_o.drain(wall.at[0:n_tp - 1, 0:cut, :])
    cross.finish_far()
    keep.wait()
    events = {}
    for ch in range(n_chunk):
        plan(3, cross1.along, far - 1, ch)
        plan(9, cross1.along, far, ch)
        for h in range(1, far + 1):
            plan(2 * h + 5, cross1.across, h, ch)
    plan(1, gates, 1, 0)
    plan(5, modulation, mod, 1, 1, 1)

    def last_weights():
        cross1.finish_near()
        pltpu.make_async_copy(w1g, wall, k_sem).start()

    plan(2 * S - 3, last_weights)

    def step1(j, _):
        with scope("b_svc"):
            for i in range(n_tile // 2):
                ring_x.service(j // 2 + 1, lax.rem(j, 2) * (n_tile // 2) + i)

        @pl.when(j >= 1)
        def _():
            ex[1].start(j - 1)

        s = outward(j)
        with scope("b_half"):
            for ch in range(n_tile):
                ring_x.wait(s * 2 + (1 - p.c), ch)
        at = Attend(*heads, brow[1], *work, lambda i, t: xg[pl.ds(pl.multiple_of(s * T, T) + i * t, t), :])
        with scope("b_att"):
            at.project()
            at.attend(j)
        with scope("b_ev"):
            take(1, j)
        return 0

    lax.fori_loop(0, S, step1, 0)
    ex[1].start(S - 1)
    pltpu.make_async_copy(w1g, wall, k_sem).wait()
    cross1.finish_far()
    ring_x.drain(xg.at[0:(n_tp - 1) * R, :])
    for peer in (p.at(1), p.at(-1), p.partner):
        pl.semaphore_signal(ready, inc=1, device_id={"tp": peer}, device_id_type=MESH)
    with scope("c_o1"):
        ex[1].sent()
        ex[1].arrived()
    def tile1(ch, _):
        rows = pl.ds(pl.multiple_of(ch * tile, tile), tile)
        with scope("c_mlp"):
            xg[pl.ds(pl.multiple_of(row0 + ch * tile, tile), tile), :] = _transition(size, tile, gate, mod, o1, act, wall, y_s, h_s, rows)

        @pl.when(ch == 0)
        def _():
            with scope("c_ready"):
                pl.semaphore_wait(ready, 3)

        ring_r.own(ch)
        return 0

    lax.fori_loop(0, n_tile, tile1, 0)
    with scope("c_svc"):
        lax.fori_loop(0, far * n_tile, lambda e, _: (ring_r.service(e // n_tile + 1, lax.rem(e, n_tile)), 0)[1], 0)

    def rest(i, _):
        for ch in range(n_tile):
            ring_r.wait(i * 2 + (1 - p.c), ch)
        return 0

    with scope("c_end"):
        lax.fori_loop(0, p.nz, rest, 0)
        ring_r.drain(xg.at[0:(n_tp - 1) * R, :])


def _main(n_dp, x, cond, pair_bias, mask_row, wq, bq, asc, aw, ab, zw, zb, wo, wup, wdn):
    S, T, D = x.shape
    C = cond.shape[-1]
    hd, hu = wq.shape[2], wdn.shape[1]
    n_tp = S * 2
    rows_w = hd + 3 * hu
    R = T // 2
    n_chunk = 3
    dma = pltpu.SemaphoreType.DMA
    v = pltpu.VMEM
    pair, blocks, each = dma((2,)), dma((S,)), dma((n_tp, n_chunk))
    n_tile = 4
    tiles = dma((n_tp, n_tile))
    return pl.pallas_call(
        functools.partial(_main_kernel, (S, T, D, C, n_tp, n_dp, hd, hu, n_chunk, n_tile)),
        out_shape=(v((n_tp * R, D), BF16), pltpu.HBM((n_tp, rows_w, D), BF16)),
        in_specs=[ANY, ANY, ANY, VMEM, ANY, VMEM, VMEM, ANY, VMEM, ANY, VMEM, ANY, ANY, ANY],
        out_specs=(VMEM, HBM),
        scratch_shapes=[
            v((T, T), BF16), v((T, T), F32), v((4 * HP, D), BF16), v((T, 2 * HP), BF16), v((2 * HP, T), BF16), v((HP, T), BF16),
            v((hd, T), F32), v((2, T, QT), F32), v((S, hd, T), BF16),
            v((2, R, D), BF16), v((2, R, C), BF16), v((2, T, D), BF16), v((4, C, 2, D), BF16), *[v((C, 2 * D), BF16)] * 2,
            *[v((rows_w, D), BF16)] * 2, v((R, C), BF16), v((R, D), BF16), v((R // n_tile, D), BF16), v((R // n_tile, n_tp * hu), BF16),
            v((n_tp, rows_w, D), BF16), *[v((R, 2 * D), F32)] * 3, *[v((n_tp, hd, R), BF16)] * 2,
            pair, pair, dma, dma((4,)), dma((4,)), dma((2, 4)), pair, dma, pair, pair, pltpu.SemaphoreType.REGULAR,
            dma((2, S, 2)), pair, dma, dma((n_tp, 1)), dma, blocks, each, dma, blocks, each, dma, tiles, dma, tiles, pltpu.SemaphoreType.REGULAR],
        cost_estimate=pl.CostEstimate(flops=S * T * T * D, bytes_accessed=S * T * D, transcendentals=S * T * T),
        compiler_params=pltpu.CompilerParams(collective_id=0, has_side_effects=True, vmem_limit_bytes=VM),
        name="blocks",
    )(x, cond, pair_bias, mask_row, wq, bq, asc, aw, ab, zw, zb, wo, wup, wdn)


def _store_kernel(src, dst, sem):
    cp = pltpu.make_async_copy(src, dst, sem)
    cp.start()
    cp.wait()


def _store(x):
    return pl.pallas_call(
        _store_kernel, out_shape=jax.ShapeDtypeStruct(x.shape, x.dtype), in_specs=[VMEM], out_specs=ANY,
        scratch_shapes=[pltpu.SemaphoreType.DMA], compiler_params=pltpu.CompilerParams(vmem_limit_bytes=1 << 20), name="store")(x)


def solution(mesh):
    n_dp = mesh.shape["dp"]

    def shard_body(token_act, token_cond, pair_bias, token_mask, ada_scale, ada_w, ada_bias, zero_w, zero_b, w_qkvg, b_q, w_o, w_up, w_down):
        S, T, D = token_act.shape
        mask_row = token_mask.reshape(1, T)
        wq = jnp.transpose(w_qkvg, (0, 2, 3, 1))
        wup = jnp.transpose(w_up, (0, 2, 3, 1))
        out, _ = _main(n_dp, token_act, token_cond, pair_bias, mask_row, wq, b_q, ada_scale, ada_w, ada_bias, zero_w, zero_b, w_o, wup, w_down)
        out = pltpu.with_memory_space_constraint(out, pltpu.VMEM)
        return _store(out).reshape(S, T, D)

    everywhere = P()
    rows, second, fourth = P('dp'), P(None, 'tp'), P(*[None] * 3, 'tp')
    in_specs = (rows, rows, second) + (everywhere,) * 6 + (fourth, second, second, fourth, second)
    return jax.shard_map(shard_body, mesh=mesh, in_specs=in_specs, out_specs=rows, check_vma=False)
```

```python
import functools
import math

import jax
import jax.numpy as jnp
from jax import lax
from jax.experimental import pallas as pl
from jax.experimental.pallas import tpu as pltpu
from jax.sharding import PartitionSpec as P

LN_EPS = 1e-5
LOG2E = 1.4426950408889634
MESH = pl.DeviceIdType.MESH
BF16 = jnp.bfloat16
F32 = jnp.float32
scope = jax.named_scope
HP = 64
QT = 256
ANY = pl.BlockSpec(memory_space=pl.ANY)
VMEM = pl.BlockSpec(memory_space=pltpu.VMEM)
HBM = pl.BlockSpec(memory_space=pltpu.HBM)
VM = 50 << 20


def _ln(x):
    mean = jnp.mean(x, axis=-1, keepdims=True)
    cen = x - mean
    var = jnp.mean(cen * cen, axis=-1, keepdims=True)
    return cen * lax.rsqrt(var + LN_EPS)


def _sig(x):
    return 0.5 * jnp.tanh(0.5 * x) + 0.5


def _dot(a, b, ca=1, cb=0):
    return lax.dot_general(a, b, (((ca,), (cb,)), ((), ())), preferred_element_type=F32)


def _ada(x_f32, cond_normed, scale, w, bias):
    d = x_f32.shape[-1]
    mod = _dot((cond_normed * scale).astype(BF16), w)
    return (_sig(mod[:, :d] + bias) * _ln(x_f32) + mod[:, d:]).astype(BF16)


class Place:
    def __init__(self, n_tp, n_dp):
        self.n = n_tp
        self.n_dp = n_dp
        self.col = lax.axis_index("dp")
        self.nz = n_tp // 2
        self.me = lax.axis_index("tp")
        self.z = self.me // 2
        self.c = lax.rem(self.me, 2)
        self.partner = self.z * 2 + (1 - self.c)

    def at(self, off):
        return lax.rem(self.z + off + self.nz, self.nz) * 2 + self.c

    def column(self, i):
        return lax.rem(self.col + i, self.n_dp)

    def enter(self):
        barrier = pltpu.get_barrier_semaphore()
        peers = [{"tp": lax.rem(self.me + i, self.n)} for i in range(1, self.n)]
        peers += [{"dp": self.column(i), "tp": self.me} for i in range(1, self.n_dp)]
        for peer in peers:
            pl.semaphore_signal(barrier, inc=1, device_id=peer, device_id_type=MESH)
        return lambda: pl.semaphore_wait(barrier, len(peers))


class Ring:
    def __init__(self, place, view, recv_sem, send_sem, right=None):
        self.p, self.view, self.recv, self.send = place, view, recv_sem, send_sem
        self.far = place.nz // 2
        self.right = right or (lambda ch: place.c == 0)

    def _push(self, b, ch, dst, src=None):
        v = self.view(b, ch)
        pltpu.make_async_remote_copy(
            src_ref=v if src is None else src, dst_ref=v, send_sem=self.send, recv_sem=self.recv.at[b, ch],
            device_id={"tp": dst}, device_id_type=MESH).start()

    def own(self, ch, src=None):
        p = self.p
        self._push(p.me, ch, p.at(1), src)
        self._push(p.me, ch, p.at(-1), src)
        self._push(p.me, ch, p.partner, src)

    def wait(self, b, ch):
        v = self.view(b, ch)
        pltpu.make_async_copy(v, v, self.recv.at[b, ch]).wait()

    def service(self, h, ch):
        p = self.p
        right = self.right(ch)
        for sign, far in ((1, right), (-1, jnp.logical_not(right))):
            b = p.at(-sign * h)

            @pl.when((h < self.far) | far)
            def _():
                self.wait(b, ch)

                @pl.when((h < self.far - 1) | ((h == self.far - 1) & far))
                def _():
                    self._push(b, ch, p.at(sign))

                self._push(b, ch, p.partner)

    def drain(self, whole):
        pltpu.make_async_copy(whole, whole, self.send).wait()


class Cross:
    def __init__(self, place, buf, lo, hi, n_chunk, recv_sem, near_sem, far_sem, shift):
        self.p, self.buf, self.lo, self.hi, self.n_chunk, self.shift = place, buf, lo, hi, n_chunk, shift
        self.recv, self.near, self.far_sem = recv_sem, near_sem, far_sem
        self.far = place.nz // 2
        self.size = (hi - lo) // n_chunk

    def _rows(self, ch):
        return pl.ds(self.lo + ch * self.size, self.size)

    def _push(self, b, ch, dst, sem, src=None):
        v = self.buf.at[b, self._rows(ch), :]
        pltpu.make_async_remote_copy(
            src_ref=v if src is None else src, dst_ref=v, send_sem=sem, recv_sem=self.recv.at[b, ch],
            device_id=dst, device_id_type=MESH).start()

    def _push_over(self, b, ch):
        p = self.p
        for i in range(1, p.n_dp):
            self._push(b, ch, {"dp": p.column(i), "tp": p.me}, self.far_sem.at[b // 2])
        self._push(b, ch, {"tp": p.partner}, self.near)

    def _mine(self, b):
        return lax.rem(b + self.shift, self.p.n_dp) == self.p.col

    def own(self, src):
        p = self.p
        for ch in range(self.n_chunk):
            part = src.at[self._rows(ch), :]

            @pl.when(self._mine(p.me))
            def _():
                for off in (1, -1):
                    self._push(p.me, ch, {"tp": p.at(off)}, self.far_sem.at[p.z], part)

            self._push(p.me, ch, {"tp": p.partner}, self.near, part)

    def wait(self, b, ch):
        v = self.buf.at[b, self._rows(ch), :]
        pltpu.make_async_copy(v, v, self.recv.at[b, ch]).wait()

    def _each(self, h, body):
        p = self.p
        for sign, core in ((1, 0), (-1, 1)):
            b = p.at(-sign * h)

            @pl.when((h < self.far) | (p.c == core))
            def _():
                body(b, sign, (h < self.far - 1) | ((h == self.far - 1) & (p.c == core)))

    def along(self, h, ch):
        p = self.p

        def body(b, sign, onward):
            @pl.when(self._mine(b))
            def _():
                self.wait(b, ch)

                @pl.when(onward)
                def _():
                    self._push(b, ch, {"tp": p.at(sign)}, self.far_sem.at[b // 2])

                self._push_over(b, ch)

        self._each(h, body)

    def across(self, h, ch):
        p = self.p

        def body(b, sign, onward):
            @pl.when(jnp.logical_not(self._mine(b)))
            def _():
                self.wait(b, ch)
                self._push(b, ch, {"tp": p.partner}, self.near)

        self._each(h, body)

    def _sent(self, k, sem):
        if k:
            v = self.buf.at[0:k, self.lo:self.hi, :]
            pltpu.make_async_copy(v, v, sem).wait()

    def finish_near(self):
        p = self.p

        def other(i, _):
            for ch in range(self.n_chunk):
                self.wait(i * 2 + (1 - p.c), ch)
            return 0

        lax.fori_loop(0, p.nz, other, 0)
        self._sent(p.nz, self.near)

    def finish_far(self):
        p = self.p
        over = p.n_dp - 1

        @pl.when(self._mine(p.me))
        def _():
            self._sent(2, self.far_sem.at[p.z])

        def body(b, sign, onward):
            @pl.when(self._mine(b))
            def _():
                @pl.when(onward)
                def _():
                    self._sent(over + 1, self.far_sem.at[b // 2])

                @pl.when(jnp.logical_not(onward))
                def _():
                    self._sent(over, self.far_sem.at[b // 2])

        def hop(h, _):
            self._each(h, body)
            return 0

        lax.fori_loop(1, self.far + 1, hop, 0)


def _copy(src, dst, sem):
    cp = pltpu.make_async_copy(src, dst, sem)
    cp.start()
    return cp


def _stage(l, hd, hu, wo_hbm, wup_hbm, wdn_hbm, wst, sem):
    cps, lo = [], 0
    for src, rows in ((wo_hbm.at[l], hd), (wup_hbm.at[l, 0], hu), (wup_hbm.at[l, 1], hu), (wdn_hbm.at[l], hu)):
        cps.append(_copy(src, wst.at[pl.ds(lo, rows), :], sem.at[len(cps)]))
        lo += rows
    return cps


def _stage_qkvg(l, hd, wq_hbm, w_s, sem):
    return [_copy(wq_hbm.at[l, f], w_s.at[pl.ds(i * HP, hd), :], sem.at[i]) for i, f in enumerate((1, 0, 2, 3))]


class Attend:
    def __init__(self, n_tp, hd, w, brow, bt, k_s, qt_s, vt_s, gt_s, lg, o_s, x_rows):
        self.__dict__.update(locals())
        self.T = bt.shape[0]

    def project(self):
        T, hd = self.T, self.hd
        tile = QT
        for i in range(T // tile):
            rows = pl.ds(i * tile, tile)
            res = _dot(self.x_rows(i, tile), self.w[...], 1, 1) + self.brow
            self.k_s[rows, :] = res[:, :2 * HP].astype(BF16)
            rest = res.T
            self.qt_s[0:HP, rows] = rest[HP:2 * HP].astype(BF16)
            ones = lax.broadcasted_iota(jnp.int32, (HP, tile), 0) == hd
            self.vt_s[:, rows] = jnp.where(ones, 1.0, rest[2 * HP:3 * HP]).astype(BF16)
            self.gt_s[:, rows] = _sig(rest[3 * HP:3 * HP + hd])

    def attend(self, slot, hook=None):
        T, hd = self.T, self.hd
        n = T // QT
        c1 = LOG2E / math.sqrt(hd)

        def scores(i):
            cols = pl.ds(i * QT, QT)
            logits = _dot(self.k_s[...], self.qt_s[:, cols]) * c1 + self.bt[:, cols]
            self.lg[i % 2] = logits
            return jnp.max(logits, axis=0, keepdims=True)

        top = scores(0)
        if hook is not None:
            hook()
        for i in range(n):
            cols = pl.ds(i * QT, QT)
            nxt = scores(i + 1) if i + 1 < n else None
            probs = jnp.exp2(self.lg[i % 2] - top).astype(BF16)
            mixed = _dot(self.vt_s[...], probs)
            self.o_s[slot, :, cols] = (self.gt_s[:, cols] * (mixed[:hd] / mixed[hd:hd + 1])).astype(BF16)
            top = nxt


def _load_bias(bias_v, mask_ref, bt):
    T = bt.shape[0]
    mask_add = (mask_ref[...].astype(F32) - 1.0) * 1e9

    def step(i, _):
        r = pl.multiple_of(i * 128, 128)
        rows = (bias_v[pl.ds(r, 128), :].astype(F32) + mask_add) * LOG2E
        bt[:, pl.ds(r, 128)] = rows.T
        return 0

    lax.fori_loop(0, T // 128, step, 0)


class Exchange:
    def __init__(self, place, sample_of, o_s, o_out, send_sem, recv_sem):
        self.p, self.sample_of, self.o_s, self.o_out, self.send, self.recv = place, sample_of, o_s, o_out, send_sem, recv_sem
        self.half = o_s.shape[-1] // 2

    def _each(self, k, remote, local):
        p = self.p
        for c in range(2):
            dst = self.sample_of(k) * 2 + c
            src = self.o_s.at[k, :, pl.ds(c * self.half, self.half)]
            sem = self.send.at[k, c]
            cp = pltpu.make_async_remote_copy(
                src_ref=src, dst_ref=self.o_out.at[p.me], send_sem=sem, recv_sem=self.recv,
                device_id={"tp": dst}, device_id_type=MESH)

            @pl.when(dst != p.me)
            def _():
                remote(cp)

            @pl.when(dst == p.me)
            def _():
                local(pltpu.make_async_copy(src, self.o_out.at[p.me], sem))

    def start(self, k):
        self._each(k, lambda cp: cp.start(), lambda cp: cp.start())

    def sent(self):
        def one(k, _):
            self._each(k, lambda cp: cp.wait_send(), lambda cp: cp.wait())
            return 0

        lax.fori_loop(0, self.o_s.shape[0], one, 0)

    def arrived(self):
        rest = self.o_out.at[0:self.p.n - 1]
        pltpu.make_async_copy(rest, rest, self.recv).wait()


def _bias_row(bq, hd):
    return jnp.concatenate([jnp.zeros((1, HP), F32), bq, jnp.zeros((1, 3 * HP - hd), F32)], axis=1)


def _gates(out, cond, w, bias):
    d = bias.shape[-1]
    out[...] = _dot(cond, w)
    for j in range(bias.shape[0]):
        cols = pl.ds(j * d, d)
        out[:, cols] = _sig(out[:, cols] + bias[j:j + 1, :])


def _modulation(out, cond_normed, scale, w, bias):
    d = bias.shape[-1]
    out[...] = _dot((cond_normed * scale).astype(BF16), w)
    out[:, :d] = _sig(out[:, :d] + bias)


def _flat(raw):
    c, two, d = raw.shape
    return raw[...].reshape(c, two * d)


def _transition(dims, tile, gates, mod1, o_v, act, wall, y_s, h_s, rows):
    D, n_tp, hd, hu = dims
    w_o = wall[:, 0:hd, :].reshape(n_tp * hd, D)
    o_t = o_v[:, :, rows].reshape(n_tp * hd, tile)
    t = _dot(o_t, w_o, 0, 0).astype(BF16).astype(F32)
    mid = (act[rows, :].astype(F32) + gates[rows, :D] * t).astype(BF16).astype(F32)
    y_s[...] = (mod1[rows, :D] * _ln(mid) + mod1[rows, D:]).astype(BF16)
    step = 4 * hu
    for j in range(n_tp * hu // step):
        dv = slice(4 * j, 4 * j + 4)
        u1 = _dot(y_s[...], wall[dv, hd:hd + hu, :].reshape(step, D), 1, 1)
        u2 = _dot(y_s[...], wall[dv, hd + hu:hd + 2 * hu, :].reshape(step, D), 1, 1)
        h_s[:, j * step:(j + 1) * step] = (u1 * _sig(u1) * u2).astype(BF16)
    r = _dot(h_s[...], wall[:, hd + 2 * hu:hd + 3 * hu, :].reshape(n_tp * hu, D)).astype(BF16).astype(F32)
    return (mid + gates[rows, D:] * r).astype(BF16)


def _main_kernel(dims, x_hbm, cond_hbm, bias_hbm, mask_ref, wq_hbm, bq_ref, asc_ref, aw_hbm, ab_ref, zw_hbm, zb_ref, wo_hbm, wup_hbm, wdn_hbm,
                 xg, w1g,
                 bias_v, bt, w_s, k_s, qt_s, vt_s, gt_s, lg, o_s, xraw, craw, xn, raw, aw_s, flat_s, wst, wst1, cond, act, y_s, h_s,
                 wall, gate, mod, nxt, o0, o1,
                 ld_sem, cd_sem, b_sem, q_sem, a_sem, st_sem, own_sem, k_sem, n_send, n_recv, n_free,
                 o_send, o_recv, w_send, w_recv, c_near, c_far, c_recv, d_near, d_far, d_recv, x_send, x_recv, r_send, r_recv, ready):
    S, T, D, C, n_tp, n_dp, hd, hu, n_chunk, n_tile = dims
    p = Place(n_tp, n_dp)
    entered = p.enter()
    far = p.nz // 2
    rows_w = hd + 3 * hu
    cut = 2 * hd
    R = S * T // n_tp
    row0 = p.me * R
    tile = R // n_tile
    mine = pl.ds(p.c * R, R)
    stage = [_stage(l, hd, hu, wo_hbm, wup_hbm, wdn_hbm, w, st_sem.at[l]) for l, w in enumerate((wst, wst1))]

    def toward(k):
        j = S - 1 - k
        return lax.rem(p.z + S + (1 - 2 * lax.rem(j, 2)) * ((j + 1) // 2), S)

    def outward(j):
        return lax.rem(p.z + S + (1 - 2 * p.c) * (1 - 2 * lax.rem(j, 2)) * ((j + 1) // 2), S)

    def loads(k, slot):
        s = toward(k)
        return [pltpu.make_async_copy(x_hbm.at[s, mine], xraw.at[slot], ld_sem.at[slot]),
                pltpu.make_async_copy(cond_hbm.at[s, mine], craw.at[slot], cd_sem.at[slot])]

    raw0 = _copy(aw_hbm.at[0, 0], raw.at[0], a_sem.at[0])
    for k in range(2):
        for cp in loads(k, k):
            cp.start()
    bias_cp = _copy(bias_hbm.at[0, 0], bias_v, b_sem)
    for cp in stage[0]:
        cp.wait()
    raws = [_copy(src, raw.at[i + 1], a_sem.at[i + 1]) for i, src in enumerate((zw_hbm.at[0], aw_hbm.at[0, 1], aw_hbm.at[1, 0]))]
    own = [_copy(cond_hbm.at[p.z, mine], cond, own_sem.at[0]), _copy(x_hbm.at[p.z, mine], act, own_sem.at[1])]
    entered()
    ring_o = Ring(p, lambda b, ch: wall.at[b, 0:cut, :], w_recv, w_send)
    cross = Cross(p, wall, cut, rows_w, n_chunk, c_recv, c_near, c_far, 0)
    cross1 = Cross(p, w1g, 0, rows_w, n_chunk, d_recv, d_near, d_far, 0)
    ring_x = Ring(p, lambda b, ch: xg.at[pl.ds(b * R + ch * tile, tile), :], x_recv, x_send)
    ring_r = Ring(p, lambda b, ch: xg.at[pl.ds(b * R + ch * tile, tile), :], r_recv, r_send)
    ring_o.own(0, wst.at[0:cut, :])
    cross.own(wst)
    w_s[...] = jnp.zeros_like(w_s)
    qt_s[HP:, :] = jnp.zeros((HP, T), BF16)
    wq = _stage_qkvg(0, hd, wq_hbm, w_s, q_sem)

    def half(slot):
        v = xn.at[slot, mine]
        return pltpu.make_async_remote_copy(src_ref=v, dst_ref=v, send_sem=n_send.at[slot], recv_sem=n_recv.at[slot],
                                            device_id={"tp": p.partner}, device_id_type=MESH)

    def normalise(slot):
        big = R // 2
        for i in range(2):
            rows = pl.ds(i * big, big)
            cn = _ln(craw[slot, rows, :].astype(F32))
            y = _ada(xraw[slot, rows, :].astype(F32), cn, asc_ref[0, 0:1, :], aw_s[...], ab_ref[0, 0:1, :])
            xn[slot, pl.ds(pl.multiple_of(p.c * R, R) + i * big, big), :] = y

    raw0.wait()
    aw_s[...] = _flat(raw.at[0])
    for cp in loads(0, 0):
        cp.wait()
    normalise(0)
    bias_cp.wait()
    half(0).start()
    _load_bias(bias_v, mask_ref, bt)
    bias_cp = _copy(bias_hbm.at[1, 0], bias_v, b_sem)
    for cp in stage[1] + wq:
        cp.wait()
    wall[p.me] = wst[...]
    keep = _copy(wst1, w1g.at[p.me], k_sem)

    def gates(l, i):
        raws[i].wait()
        flat_s[...] = _flat(raw.at[i + 1])
        _gates(gate, cond[...], flat_s[...], zb_ref.at[l])

    def modulation(out, l, j, i):
        raws[i].wait()
        flat_s[...] = _flat(raw.at[i + 1])
        cn = _ln(cond[...].astype(F32))
        _modulation(out, cn, asc_ref[l, j:j + 1, :], flat_s[...], ab_ref[l, j:j + 1, :])

    events = {}

    def plan(when, f, *args):
        events.setdefault(when, []).append((f, args))

    def take(step, k):
        for when in sorted(events):
            if when % 2 == step:
                @pl.when(k == when // 2)
                def _():
                    for f, args in events[when]:
                        f(*args)

    first, over, whole = (0, 7, 9, 12), (5, 10, 13, 16), (1, 8, 12, 15)
    for h in range(1, far + 1):
        plan(whole[h - 1], ring_o.service, h, 0)
        for ch in range(n_chunk):
            plan(first[h - 1] + ch, cross.along, h, ch)
            plan(over[h - 1] + ch, cross.across, h, ch)
    for ch in range(n_chunk):
        plan(2 * S + n_chunk, cross1.along, 1, ch)
    plan(13, cross1.own, wst1)
    for cp in own:
        plan(3, cp.wait)
    plan(5, gates, 0, 0)
    plan(7, modulation, mod, 0, 1, 1)
    plan(9, modulation, nxt, 1, 0, 2)
    ex = [Exchange(p, order, o_s, o, o_send.at[l], o_recv.at[l]) for l, (order, o) in enumerate(((toward, o0), (outward, o1)))]
    brow = [_bias_row(bq_ref[l:l + 1, :], hd) for l in range(2)]
    heads = (n_tp, hd, w_s)
    work = (bt, k_s, qt_s, vt_s, gt_s, lg, o_s)

    def step0(k, _):
        slot = lax.rem(k, 2)

        @pl.when(k + 2 < S)
        def _():
            for cp in loads(k + 2, slot):
                cp.start()

        with scope("a_half"):
            v = xn.at[slot, pl.ds((1 - p.c) * R, R)]
            pltpu.make_async_copy(v, v, n_recv.at[slot]).wait()
            half(slot).wait_send()
        at = Attend(*heads, brow[0], *work, lambda i, t: xn[slot, pl.ds(i * t, t), :])
        at.project()

        @pl.when(k + 2 < S)
        def _():
            pl.semaphore_signal(n_free, inc=1, device_id={"tp": p.partner}, device_id_type=MESH)

        @pl.when(k >= 1)
        def _():
            ex[0].start(k - 1)

        @pl.when(k + 1 < S)
        def _():
            for cp in loads(k + 1, 1 - slot):
                cp.wait()
            normalise(1 - slot)

            @pl.when(k >= 1)
            def _():
                pl.semaphore_wait(n_free, 1)

        with scope("a_ev0"):
            take(0, k)

        def hook():
            @pl.when(k + 1 < S)
            def _():
                half(1 - slot).start()

        with scope("a_att"):
            at.attend(k, hook)
        with scope("a_ev1"):
            take(1, k)
        return 0

    lax.fori_loop(0, S, step0, 0)
    ex[0].start(S - 1)
    wq = _stage_qkvg(1, hd, wq_hbm, w_s, q_sem)
    raws = [_copy(src, raw.at[i + 1], a_sem.at[i + 1]) for i, src in enumerate((zw_hbm.at[1], aw_hbm.at[1, 1]))]
    for when in sorted(events):
        if when >= 2 * S:
            for f, args in events[when]:
                f(*args)

    def other(i, _):
        ring_o.wait(i * 2 + (1 - p.c), 0)
        return 0

    with scope("b_w0"):
        lax.fori_loop(0, p.nz, other, 0)
        cross.finish_near()
    with scope("b_o0"):
        ex[0].sent()
        ex[0].arrived()
    size = (D, n_tp, hd, hu)

    def tile0(ch, _):
        rows = pl.ds(pl.multiple_of(ch * tile, tile), tile)
        with scope("b_mlp"):
            new = _transition(size, tile, gate, mod, o0, act, wall, y_s, h_s, rows)
            act[rows, :] = new
            xg[pl.ds(pl.multiple_of(row0 + ch * tile, tile), tile), :] = (nxt[rows, :D] * _ln(new.astype(F32)) + nxt[rows, D:]).astype(BF16)
        ring_x.own(ch)

        @pl.when(ch == n_tile - 1)
        def _():
            with scope("b_along"):
                for i in range(n_chunk):
                    cross1.along(2, i)
        return 0

    lax.fori_loop(0, n_tile, tile0, 0)
    bias_cp.wait()
    _load_bias(bias_v, mask_ref, bt)
    for cp in wq:
        cp.wait()
    ring_o.drain(wall.at[0:n_tp - 1, 0:cut, :])
    cross.finish_far()
    keep.wait()
    events = {}
    for ch in range(n_chunk):
        plan(5, cross1.along, far - 1, ch)
        plan(9, cross1.along, far, ch)
        for h in range(1, far + 1):
            plan(2 * h + 5, cross1.across, h, ch)
    plan(1, gates, 1, 0)
    plan(5, modulation, mod, 1, 1, 1)

    def last_weights():
        cross1.finish_near()
        pltpu.make_async_copy(w1g, wall, k_sem).start()

    plan(2 * S - 3, last_weights)

    def step1(j, _):
        with scope("b_svc"):
            for i in range(n_tile // 2):
                ring_x.service(j // 2 + 1, lax.rem(j, 2) * (n_tile // 2) + i)

        @pl.when(j >= 1)
        def _():
            ex[1].start(j - 1)

        s = outward(j)
        with scope("b_half"):
            for ch in range(n_tile):
                ring_x.wait(s * 2 + (1 - p.c), ch)
        at = Attend(*heads, brow[1], *work, lambda i, t: xg[pl.ds(pl.multiple_of(s * T, T) + i * t, t), :])
        with scope("b_att"):
            at.project()
            at.attend(j)
        with scope("b_ev"):
            take(1, j)
        return 0

    lax.fori_loop(0, S, step1, 0)
    ex[1].start(S - 1)
    pltpu.make_async_copy(w1g, wall, k_sem).wait()
    cross1.finish_far()
    ring_x.drain(xg.at[0:(n_tp - 1) * R, :])
    for peer in (p.at(1), p.at(-1), p.partner):
        pl.semaphore_signal(ready, inc=1, device_id={"tp": peer}, device_id_type=MESH)
    with scope("c_o1"):
        ex[1].sent()
        ex[1].arrived()
    def tile1(ch, _):
        rows = pl.ds(pl.multiple_of(ch * tile, tile), tile)
        with scope("c_mlp"):
            xg[pl.ds(pl.multiple_of(row0 + ch * tile, tile), tile), :] = _transition(size, tile, gate, mod, o1, act, wall, y_s, h_s, rows)

        @pl.when(ch == 0)
        def _():
            with scope("c_ready"):
                pl.semaphore_wait(ready, 3)

        ring_r.own(ch)
        return 0

    lax.fori_loop(0, n_tile, tile1, 0)
    with scope("c_svc"):
        lax.fori_loop(0, far * n_tile, lambda e, _: (ring_r.service(e // n_tile + 1, lax.rem(e, n_tile)), 0)[1], 0)

    def rest(i, _):
        for ch in range(n_tile):
            ring_r.wait(i * 2 + (1 - p.c), ch)
        return 0

    with scope("c_end"):
        lax.fori_loop(0, p.nz, rest, 0)
        ring_r.drain(xg.at[0:(n_tp - 1) * R, :])


def _main(n_dp, x, cond, pair_bias, mask_row, wq, bq, asc, aw, ab, zw, zb, wo, wup, wdn):
    S, T, D = x.shape
    C = cond.shape[-1]
    hd, hu = wq.shape[2], wdn.shape[1]
    n_tp = S * 2
    rows_w = hd + 3 * hu
    R = T // 2
    n_chunk = 3
    dma = pltpu.SemaphoreType.DMA
    v = pltpu.VMEM
    pair, blocks, each = dma((2,)), dma((S,)), dma((n_tp, n_chunk))
    n_tile = 4
    tiles = dma((n_tp, n_tile))
    return pl.pallas_call(
        functools.partial(_main_kernel, (S, T, D, C, n_tp, n_dp, hd, hu, n_chunk, n_tile)),
        out_shape=(v((n_tp * R, D), BF16), pltpu.HBM((n_tp, rows_w, D), BF16)),
        in_specs=[ANY, ANY, ANY, VMEM, ANY, VMEM, VMEM, ANY, VMEM, ANY, VMEM, ANY, ANY, ANY],
        out_specs=(VMEM, HBM),
        scratch_shapes=[
            v((T, T), BF16), v((T, T), F32), v((4 * HP, D), BF16), v((T, 2 * HP), BF16), v((2 * HP, T), BF16), v((HP, T), BF16),
            v((hd, T), F32), v((2, T, QT), F32), v((S, hd, T), BF16),
            v((2, R, D), BF16), v((2, R, C), BF16), v((2, T, D), BF16), v((4, C, 2, D), BF16), *[v((C, 2 * D), BF16)] * 2,
            *[v((rows_w, D), BF16)] * 2, v((R, C), BF16), v((R, D), BF16), v((R // n_tile, D), BF16), v((R // n_tile, n_tp * hu), BF16),
            v((n_tp, rows_w, D), BF16), *[v((R, 2 * D), F32)] * 3, *[v((n_tp, hd, R), BF16)] * 2,
            pair, pair, dma, dma((4,)), dma((4,)), dma((2, 4)), pair, dma, pair, pair, pltpu.SemaphoreType.REGULAR,
            dma((2, S, 2)), pair, dma, dma((n_tp, 1)), dma, blocks, each, dma, blocks, each, dma, tiles, dma, tiles, pltpu.SemaphoreType.REGULAR],
        cost_estimate=pl.CostEstimate(flops=S * T * T * D, bytes_accessed=S * T * D, transcendentals=S * T * T),
        compiler_params=pltpu.CompilerParams(collective_id=0, has_side_effects=True, vmem_limit_bytes=VM),
        name="blocks",
    )(x, cond, pair_bias, mask_row, wq, bq, asc, aw, ab, zw, zb, wo, wup, wdn)


def _store_kernel(src, dst, sem):
    cp = pltpu.make_async_copy(src, dst, sem)
    cp.start()
    cp.wait()


def _store(x):
    return pl.pallas_call(
        _store_kernel, out_shape=jax.ShapeDtypeStruct(x.shape, x.dtype), in_specs=[VMEM], out_specs=ANY,
        scratch_shapes=[pltpu.SemaphoreType.DMA], compiler_params=pltpu.CompilerParams(vmem_limit_bytes=1 << 20), name="store")(x)


def solution(mesh):
    n_dp = mesh.shape["dp"]

    def shard_body(token_act, token_cond, pair_bias, token_mask, ada_scale, ada_w, ada_bias, zero_w, zero_b, w_qkvg, b_q, w_o, w_up, w_down):
        S, T, D = token_act.shape
        mask_row = token_mask.reshape(1, T)
        wq = jnp.transpose(w_qkvg, (0, 2, 3, 1))
        wup = jnp.transpose(w_up, (0, 2, 3, 1))
        out, _ = _main(n_dp, token_act, token_cond, pair_bias, mask_row, wq, b_q, ada_scale, ada_w, ada_bias, zero_w, zero_b, w_o, wup, w_down)
        out = pltpu.with_memory_space_constraint(out, pltpu.VMEM)
        return _store(out).reshape(S, T, D)

    everywhere = P()
    rows, second, fourth = P('dp'), P(None, 'tp'), P(*[None] * 3, 'tp')
    in_specs = (rows, rows, second) + (everywhere,) * 6 + (fourth, second, second, fourth, second)
    return jax.shard_map(shard_body, mesh=mesh, in_specs=in_specs, out_specs=rows, check_vma=False)
```

```python
import functools
import math

import jax
import jax.numpy as jnp
from jax import lax
from jax.experimental import pallas as pl
from jax.experimental.pallas import tpu as pltpu
from jax.sharding import PartitionSpec as P

LN_EPS = 1e-5
LOG2E = 1.4426950408889634
MESH = pl.DeviceIdType.MESH
BF16 = jnp.bfloat16
F32 = jnp.float32
scope = jax.named_scope
HP = 64
QT = 256
ANY = pl.BlockSpec(memory_space=pl.ANY)
VMEM = pl.BlockSpec(memory_space=pltpu.VMEM)
HBM = pl.BlockSpec(memory_space=pltpu.HBM)
VM = 50 << 20


def _ln(x):
    mean = jnp.mean(x, axis=-1, keepdims=True)
    cen = x - mean
    var = jnp.mean(cen * cen, axis=-1, keepdims=True)
    return cen * lax.rsqrt(var + LN_EPS)


def _sig(x):
    return 0.5 * jnp.tanh(0.5 * x) + 0.5


def _dot(a, b, ca=1, cb=0):
    return lax.dot_general(a, b, (((ca,), (cb,)), ((), ())), preferred_element_type=F32)


def _ada(x_f32, cond_normed, scale, w, bias):
    d = x_f32.shape[-1]
    mod = _dot((cond_normed * scale).astype(BF16), w)
    return (_sig(mod[:, :d] + bias) * _ln(x_f32) + mod[:, d:]).astype(BF16)


class Place:
    def __init__(self, n_tp, n_dp):
        self.n = n_tp
        self.n_dp = n_dp
        self.col = lax.axis_index("dp")
        self.nz = n_tp // 2
        self.me = lax.axis_index("tp")
        self.z = self.me // 2
        self.c = lax.rem(self.me, 2)
        self.partner = self.z * 2 + (1 - self.c)

    def at(self, off):
        return lax.rem(self.z + off + self.nz, self.nz) * 2 + self.c

    def column(self, i):
        return lax.rem(self.col + i, self.n_dp)

    def enter(self):
        barrier = pltpu.get_barrier_semaphore()
        peers = [{"tp": lax.rem(self.me + i, self.n)} for i in range(1, self.n)]
        peers += [{"dp": self.column(i), "tp": self.me} for i in range(1, self.n_dp)]
        for peer in peers:
            pl.semaphore_signal(barrier, inc=1, device_id=peer, device_id_type=MESH)
        return lambda: pl.semaphore_wait(barrier, len(peers))


class Ring:
    def __init__(self, place, view, recv_sem, send_sem, right=None):
        self.p, self.view, self.recv, self.send = place, view, recv_sem, send_sem
        self.far = place.nz // 2
        self.right = right or (lambda ch: place.c == 0)

    def _push(self, b, ch, dst, src=None):
        v = self.view(b, ch)
        pltpu.make_async_remote_copy(
            src_ref=v if src is None else src, dst_ref=v, send_sem=self.send, recv_sem=self.recv.at[b, ch],
            device_id={"tp": dst}, device_id_type=MESH).start()

    def own(self, ch, src=None):
        p = self.p
        self._push(p.me, ch, p.at(1), src)
        self._push(p.me, ch, p.at(-1), src)
        self._push(p.me, ch, p.partner, src)

    def wait(self, b, ch):
        v = self.view(b, ch)
        pltpu.make_async_copy(v, v, self.recv.at[b, ch]).wait()

    def service(self, h, ch):
        p = self.p
        right = self.right(ch)
        for sign, far in ((1, right), (-1, jnp.logical_not(right))):
            b = p.at(-sign * h)

            @pl.when((h < self.far) | far)
            def _():
                self.wait(b, ch)

                @pl.when((h < self.far - 1) | ((h == self.far - 1) & far))
                def _():
                    self._push(b, ch, p.at(sign))

                self._push(b, ch, p.partner)

    def drain(self, whole):
        pltpu.make_async_copy(whole, whole, self.send).wait()


class Cross:
    def __init__(self, place, buf, lo, hi, n_chunk, recv_sem, near_sem, far_sem):
        self.p, self.buf, self.lo, self.hi, self.n_chunk = place, buf, lo, hi, n_chunk
        self.recv, self.near, self.far_sem = recv_sem, near_sem, far_sem
        self.far = place.nz // 2
        self.size = (hi - lo) // n_chunk

    def _rows(self, ch):
        return pl.ds(self.lo + ch * self.size, self.size)

    def _push(self, b, ch, dst, sem, src=None):
        v = self.buf.at[b, self._rows(ch), :]
        pltpu.make_async_remote_copy(
            src_ref=v if src is None else src, dst_ref=v, send_sem=sem, recv_sem=self.recv.at[b, ch],
            device_id=dst, device_id_type=MESH).start()

    def _push_over(self, b, ch):
        p = self.p
        for i in range(1, p.n_dp):
            self._push(b, ch, {"dp": p.column(i), "tp": p.me}, self.far_sem.at[b // 2, ch])
        self._push(b, ch, {"tp": p.partner}, self.near)

    def _mine(self, b, ch):
        return lax.rem(b + ch, self.p.n_dp) == self.p.col

    def own(self, src):
        p = self.p
        for ch in range(self.n_chunk):
            part = src.at[self._rows(ch), :]

            @pl.when(self._mine(p.me, ch))
            def _():
                for off in (1, -1):
                    self._push(p.me, ch, {"tp": p.at(off)}, self.far_sem.at[p.z, ch], part)

            self._push(p.me, ch, {"tp": p.partner}, self.near, part)

    def wait(self, b, ch):
        v = self.buf.at[b, self._rows(ch), :]
        pltpu.make_async_copy(v, v, self.recv.at[b, ch]).wait()

    def _each(self, h, body):
        p = self.p
        for sign, core in ((1, 0), (-1, 1)):
            b = p.at(-sign * h)

            @pl.when((h < self.far) | (p.c == core))
            def _():
                body(b, sign, (h < self.far - 1) | ((h == self.far - 1) & (p.c == core)))

    def along(self, h, ch):
        p = self.p

        def body(b, sign, onward):
            @pl.when(self._mine(b, ch))
            def _():
                self.wait(b, ch)

                @pl.when(onward)
                def _():
                    self._push(b, ch, {"tp": p.at(sign)}, self.far_sem.at[b // 2, ch])

                self._push_over(b, ch)

        self._each(h, body)

    def across(self, h, ch):
        p = self.p

        def body(b, sign, onward):
            @pl.when(jnp.logical_not(self._mine(b, ch)))
            def _():
                self.wait(b, ch)
                self._push(b, ch, {"tp": p.partner}, self.near)

        self._each(h, body)

    def _sent(self, k, rows, sem):
        if k:
            v = self.buf.at[0:k, rows, :]
            pltpu.make_async_copy(v, v, sem).wait()

    def finish_near(self):
        p = self.p

        def other(i, _):
            for ch in range(self.n_chunk):
                self.wait(i * 2 + (1 - p.c), ch)
            return 0

        lax.fori_loop(0, p.nz, other, 0)
        self._sent(p.nz, pl.ds(self.lo, self.hi - self.lo), self.near)

    def finish_far(self):
        p = self.p
        over = p.n_dp - 1
        for ch in range(self.n_chunk):
            @pl.when(self._mine(p.me, ch))
            def _():
                self._sent(2, self._rows(ch), self.far_sem.at[p.z, ch])

        def body(b, sign, onward):
            for ch in range(self.n_chunk):
                sent = functools.partial(self._sent, rows=self._rows(ch), sem=self.far_sem.at[b // 2, ch])

                @pl.when(self._mine(b, ch) & onward)
                def _():
                    sent(over + 1)

                @pl.when(self._mine(b, ch) & jnp.logical_not(onward))
                def _():
                    sent(over)

        def hop(h, _):
            self._each(h, body)
            return 0

        lax.fori_loop(1, self.far + 1, hop, 0)


def _copy(src, dst, sem):
    cp = pltpu.make_async_copy(src, dst, sem)
    cp.start()
    return cp


def _stage(l, hd, hu, wo_hbm, wup_hbm, wdn_hbm, wst, sem):
    cps, lo = [], 0
    for src, rows in ((wo_hbm.at[l], hd), (wup_hbm.at[l, 0], hu), (wup_hbm.at[l, 1], hu), (wdn_hbm.at[l], hu)):
        cps.append(_copy(src, wst.at[pl.ds(lo, rows), :], sem.at[len(cps)]))
        lo += rows
    return cps


def _stage_qkvg(l, hd, wq_hbm, w_s, sem):
    return [_copy(wq_hbm.at[l, f], w_s.at[pl.ds(i * HP, hd), :], sem.at[i]) for i, f in enumerate((1, 0, 2, 3))]


class Attend:
    def __init__(self, n_tp, hd, w, brow, bt, k_s, qt_s, vt_s, gt_s, lg, o_s, x_rows):
        self.__dict__.update(locals())
        self.T = bt.shape[0]

    def project(self):
        T, hd = self.T, self.hd
        tile = QT
        for i in range(T // tile):
            rows = pl.ds(i * tile, tile)
            res = _dot(self.x_rows(i, tile), self.w[...], 1, 1) + self.brow
            self.k_s[rows, :] = res[:, :2 * HP].astype(BF16)
            rest = res.T
            self.qt_s[0:HP, rows] = rest[HP:2 * HP].astype(BF16)
            ones = lax.broadcasted_iota(jnp.int32, (HP, tile), 0) == hd
            self.vt_s[:, rows] = jnp.where(ones, 1.0, rest[2 * HP:3 * HP]).astype(BF16)
            self.gt_s[:, rows] = _sig(rest[3 * HP:3 * HP + hd])

    def attend(self, slot, hook=None):
        T, hd = self.T, self.hd
        n = T // QT
        c1 = LOG2E / math.sqrt(hd)

        def scores(i):
            cols = pl.ds(i * QT, QT)
            logits = _dot(self.k_s[...], self.qt_s[:, cols]) * c1 + self.bt[:, cols]
            self.lg[i % 2] = logits
            return jnp.max(logits, axis=0, keepdims=True)

        top = scores(0)
        if hook is not None:
            hook()
        for i in range(n):
            cols = pl.ds(i * QT, QT)
            nxt = scores(i + 1) if i + 1 < n else None
            probs = jnp.exp2(self.lg[i % 2] - top).astype(BF16)
            mixed = _dot(self.vt_s[...], probs)
            self.o_s[slot, :, cols] = (self.gt_s[:, cols] * (mixed[:hd] / mixed[hd:hd + 1])).astype(BF16)
            top = nxt


def _load_bias(bias_v, mask_ref, bt):
    T = bt.shape[0]
    mask_add = (mask_ref[...].astype(F32) - 1.0) * 1e9

    def step(i, _):
        r = pl.multiple_of(i * 128, 128)
        rows = (bias_v[pl.ds(r, 128), :].astype(F32) + mask_add) * LOG2E
        bt[:, pl.ds(r, 128)] = rows.T
        return 0

    lax.fori_loop(0, T // 128, step, 0)


class Exchange:
    def __init__(self, place, sample_of, o_s, o_out, send_sem, recv_sem):
        self.p, self.sample_of, self.o_s, self.o_out, self.send, self.recv = place, sample_of, o_s, o_out, send_sem, recv_sem
        self.half = o_s.shape[-1] // 2

    def _each(self, k, remote, local):
        p = self.p
        for c in range(2):
            dst = self.sample_of(k) * 2 + c
            src = self.o_s.at[k, :, pl.ds(c * self.half, self.half)]
            sem = self.send.at[k, c]
            cp = pltpu.make_async_remote_copy(
                src_ref=src, dst_ref=self.o_out.at[p.me], send_sem=sem, recv_sem=self.recv,
                device_id={"tp": dst}, device_id_type=MESH)

            @pl.when(dst != p.me)
            def _():
                remote(cp)

            @pl.when(dst == p.me)
            def _():
                local(pltpu.make_async_copy(src, self.o_out.at[p.me], sem))

    def start(self, k):
        self._each(k, lambda cp: cp.start(), lambda cp: cp.start())

    def sent(self):
        def one(k, _):
            self._each(k, lambda cp: cp.wait_send(), lambda cp: cp.wait())
            return 0

        lax.fori_loop(0, self.o_s.shape[0], one, 0)

    def arrived(self):
        rest = self.o_out.at[0:self.p.n - 1]
        pltpu.make_async_copy(rest, rest, self.recv).wait()


def _bias_row(bq, hd):
    return jnp.concatenate([jnp.zeros((1, HP), F32), bq, jnp.zeros((1, 3 * HP - hd), F32)], axis=1)


def _gates(out, cond, w, bias):
    d = bias.shape[-1]
    out[...] = _dot(cond, w)
    for j in range(bias.shape[0]):
        cols = pl.ds(j * d, d)
        out[:, cols] = _sig(out[:, cols] + bias[j:j + 1, :])


def _modulation(out, cond_normed, scale, w, bias):
    d = bias.shape[-1]
    out[...] = _dot((cond_normed * scale).astype(BF16), w)
    out[:, :d] = _sig(out[:, :d] + bias)


def _flat(raw):
    c, two, d = raw.shape
    return raw[...].reshape(c, two * d)


def _transition(dims, tile, gates, mod1, o_v, act, wall, y_s, h_s, rows):
    D, n_tp, hd, hu = dims
    w_o = wall[:, 0:hd, :].reshape(n_tp * hd, D)
    o_t = o_v[:, :, rows].reshape(n_tp * hd, tile)
    t = _dot(o_t, w_o, 0, 0).astype(BF16).astype(F32)
    mid = (act[rows, :].astype(F32) + gates[rows, :D] * t).astype(BF16).astype(F32)
    y_s[...] = (mod1[rows, :D] * _ln(mid) + mod1[rows, D:]).astype(BF16)
    step = 4 * hu
    for j in range(n_tp * hu // step):
        dv = slice(4 * j, 4 * j + 4)
        u1 = _dot(y_s[...], wall[dv, hd:hd + hu, :].reshape(step, D), 1, 1)
        u2 = _dot(y_s[...], wall[dv, hd + hu:hd + 2 * hu, :].reshape(step, D), 1, 1)
        h_s[:, j * step:(j + 1) * step] = (u1 * _sig(u1) * u2).astype(BF16)
    r = _dot(h_s[...], wall[:, hd + 2 * hu:hd + 3 * hu, :].reshape(n_tp * hu, D)).astype(BF16).astype(F32)
    return (mid + gates[rows, D:] * r).astype(BF16)


def _main_kernel(dims, x_hbm, cond_hbm, bias_hbm, mask_ref, wq_hbm, bq_ref, asc_ref, aw_hbm, ab_ref, zw_hbm, zb_ref, wo_hbm, wup_hbm, wdn_hbm,
                 xg, w1g,
                 bias_v, bt, w_s, k_s, qt_s, vt_s, gt_s, lg, o_s, xraw, craw, xn, raw, aw_s, flat_s, wst, wst1, cond, act, y_s, h_s,
                 wall, gate, mod, nxt, o0, o1,
                 ld_sem, cd_sem, b_sem, q_sem, a_sem, st_sem, own_sem, k_sem, n_send, n_recv, n_free,
                 o_send, o_recv, w_send, w_recv, c_near, c_far, c_recv, d_near, d_far, d_recv, x_send, x_recv, r_send, r_recv, ready):
    S, T, D, C, n_tp, n_dp, hd, hu, n_chunk, n_tile = dims
    p = Place(n_tp, n_dp)
    entered = p.enter()
    far = p.nz // 2
    rows_w = hd + 3 * hu
    cut = 2 * hd
    R = S * T // n_tp
    row0 = p.me * R
    tile = R // n_tile
    mine = pl.ds(p.c * R, R)
    stage = [_stage(l, hd, hu, wo_hbm, wup_hbm, wdn_hbm, w, st_sem.at[l]) for l, w in enumerate((wst, wst1))]

    def toward(k):
        j = S - 1 - k
        return lax.rem(p.z + S + (1 - 2 * lax.rem(j, 2)) * ((j + 1) // 2), S)

    def outward(j):
        return lax.rem(p.z + S + (1 - 2 * p.c) * (1 - 2 * lax.rem(j, 2)) * ((j + 1) // 2), S)

    def loads(k, slot):
        s = toward(k)
        return [pltpu.make_async_copy(x_hbm.at[s, mine], xraw.at[slot], ld_sem.at[slot]),
                pltpu.make_async_copy(cond_hbm.at[s, mine], craw.at[slot], cd_sem.at[slot])]

    raw0 = _copy(aw_hbm.at[0, 0], raw.at[0], a_sem.at[0])
    for k in range(2):
        for cp in loads(k, k):
            cp.start()
    bias_cp = _copy(bias_hbm.at[0, 0], bias_v, b_sem)
    for cp in stage[0]:
        cp.wait()
    raws = [_copy(src, raw.at[i + 1], a_sem.at[i + 1]) for i, src in enumerate((zw_hbm.at[0], aw_hbm.at[0, 1], aw_hbm.at[1, 0]))]
    own = [_copy(cond_hbm.at[p.z, mine], cond, own_sem.at[0]), _copy(x_hbm.at[p.z, mine], act, own_sem.at[1])]
    entered()
    ring_o = Ring(p, lambda b, ch: wall.at[b, 0:cut, :], w_recv, w_send)
    cross = Cross(p, wall, cut, rows_w, n_chunk, c_recv, c_near, c_far)
    cross1 = Cross(p, w1g, 0, rows_w, n_chunk, d_recv, d_near, d_far)
    ring_x = Ring(p, lambda b, ch: xg.at[pl.ds(b * R + ch * tile, tile), :], x_recv, x_send)
    ring_r = Ring(p, lambda b, ch: xg.at[pl.ds(b * R + ch * tile, tile), :], r_recv, r_send)
    ring_o.own(0, wst.at[0:cut, :])
    cross.own(wst)
    w_s[...] = jnp.zeros_like(w_s)
    qt_s[HP:, :] = jnp.zeros((HP, T), BF16)
    wq = _stage_qkvg(0, hd, wq_hbm, w_s, q_sem)

    def half(slot):
        v = xn.at[slot, mine]
        return pltpu.make_async_remote_copy(src_ref=v, dst_ref=v, send_sem=n_send.at[slot], recv_sem=n_recv.at[slot],
                                            device_id={"tp": p.partner}, device_id_type=MESH)

    def normalise(slot):
        big = R // 2
        for i in range(2):
            rows = pl.ds(i * big, big)
            cn = _ln(craw[slot, rows, :].astype(F32))
            y = _ada(xraw[slot, rows, :].astype(F32), cn, asc_ref[0, 0:1, :], aw_s[...], ab_ref[0, 0:1, :])
            xn[slot, pl.ds(pl.multiple_of(p.c * R, R) + i * big, big), :] = y

    raw0.wait()
    aw_s[...] = _flat(raw.at[0])
    for cp in loads(0, 0):
        cp.wait()
    normalise(0)
    bias_cp.wait()
    half(0).start()
    _load_bias(bias_v, mask_ref, bt)
    bias_cp = _copy(bias_hbm.at[1, 0], bias_v, b_sem)
    for cp in stage[1] + wq:
        cp.wait()
    wall[p.me] = wst[...]
    keep = _copy(wst1, w1g.at[p.me], k_sem)

    def gates(l, i):
        raws[i].wait()
        flat_s[...] = _flat(raw.at[i + 1])
        _gates(gate, cond[...], flat_s[...], zb_ref.at[l])

    def modulation(out, l, j, i):
        raws[i].wait()
        flat_s[...] = _flat(raw.at[i + 1])
        cn = _ln(cond[...].astype(F32))
        _modulation(out, cn, asc_ref[l, j:j + 1, :], flat_s[...], ab_ref[l, j:j + 1, :])

    events = {}

    def plan(when, f, *args):
        events.setdefault(when, []).append((f, args))

    def take(step, k):
        for when in sorted(events):
            if when % 2 == step:
                @pl.when(k == when // 2)
                def _():
                    for f, args in events[when]:
                        f(*args)

    first, over, whole = (0, 7, 9, 12), (5, 10, 13, 16), (1, 8, 12, 15)
    for h in range(1, far + 1):
        plan(whole[h - 1], ring_o.service, h, 0)
        for ch in range(n_chunk):
            plan(first[h - 1] + ch, cross.along, h, ch)
            plan(over[h - 1] + ch, cross.across, h, ch)
    for ch in range(n_chunk):
        plan(2 * S + n_chunk, cross1.along, 1, ch)
    plan(13, cross1.own, wst1)
    for cp in own:
        plan(3, cp.wait)
    plan(5, gates, 0, 0)
    plan(7, modulation, mod, 0, 1, 1)
    plan(9, modulation, nxt, 1, 0, 2)
    ex = [Exchange(p, order, o_s, o, o_send.at[l], o_recv.at[l]) for l, (order, o) in enumerate(((toward, o0), (outward, o1)))]
    brow = [_bias_row(bq_ref[l:l + 1, :], hd) for l in range(2)]
    heads = (n_tp, hd, w_s)
    work = (bt, k_s, qt_s, vt_s, gt_s, lg, o_s)

    def step0(k, _):
        slot = lax.rem(k, 2)

        @pl.when(k + 2 < S)
        def _():
            for cp in loads(k + 2, slot):
                cp.start()

        with scope("a_half"):
            v = xn.at[slot, pl.ds((1 - p.c) * R, R)]
            pltpu.make_async_copy(v, v, n_recv.at[slot]).wait()
            half(slot).wait_send()
        at = Attend(*heads, brow[0], *work, lambda i, t: xn[slot, pl.ds(i * t, t), :])
        at.project()

        @pl.when(k + 2 < S)
        def _():
            pl.semaphore_signal(n_free, inc=1, device_id={"tp": p.partner}, device_id_type=MESH)

        @pl.when(k >= 1)
        def _():
            ex[0].start(k - 1)

        @pl.when(k + 1 < S)
        def _():
            for cp in loads(k + 1, 1 - slot):
                cp.wait()
            normalise(1 - slot)

            @pl.when(k >= 1)
            def _():
                pl.semaphore_wait(n_free, 1)

        with scope("a_ev0"):
            take(0, k)

        def hook():
            @pl.when(k + 1 < S)
            def _():
                half(1 - slot).start()

        with scope("a_att"):
            at.attend(k, hook)
        with scope("a_ev1"):
            take(1, k)
        return 0

    lax.fori_loop(0, S, step0, 0)
    ex[0].start(S - 1)
    wq = _stage_qkvg(1, hd, wq_hbm, w_s, q_sem)
    raws = [_copy(src, raw.at[i + 1], a_sem.at[i + 1]) for i, src in enumerate((zw_hbm.at[1], aw_hbm.at[1, 1]))]
    for when in sorted(events):
        if when >= 2 * S:
            for f, args in events[when]:
                f(*args)

    def other(i, _):
        ring_o.wait(i * 2 + (1 - p.c), 0)
        return 0

    with scope("b_w0"):
        lax.fori_loop(0, p.nz, other, 0)
        cross.finish_near()
    with scope("b_o0"):
        ex[0].sent()
        ex[0].arrived()
    size = (D, n_tp, hd, hu)

    def tile0(ch, _):
        rows = pl.ds(pl.multiple_of(ch * tile, tile), tile)
        with scope("b_mlp"):
            new = _transition(size, tile, gate, mod, o0, act, wall, y_s, h_s, rows)
            act[rows, :] = new
            xg[pl.ds(pl.multiple_of(row0 + ch * tile, tile), tile), :] = (nxt[rows, :D] * _ln(new.astype(F32)) + nxt[rows, D:]).astype(BF16)
        ring_x.own(ch)

        @pl.when(ch == n_tile - 1)
        def _():
            with scope("b_along"):
                for i in range(n_chunk):
                    cross1.along(2, i)
        return 0

    lax.fori_loop(0, n_tile, tile0, 0)
    bias_cp.wait()
    _load_bias(bias_v, mask_ref, bt)
    for cp in wq:
        cp.wait()
    ring_o.drain(wall.at[0:n_tp - 1, 0:cut, :])
    cross.finish_far()
    keep.wait()
    events = {}
    for ch in range(n_chunk):
        plan(5, cross1.along, far - 1, ch)
        plan(9, cross1.along, far, ch)
        for h in range(1, far + 1):
            plan(2 * h + 5, cross1.across, h, ch)
    plan(1, gates, 1, 0)
    plan(5, modulation, mod, 1, 1, 1)

    def last_weights():
        cross1.finish_near()
        pltpu.make_async_copy(w1g, wall, k_sem).start()

    plan(2 * S - 3, last_weights)

    def step1(j, _):
        with scope("b_svc"):
            for i in range(n_tile // 2):
                ring_x.service(j // 2 + 1, lax.rem(j, 2) * (n_tile // 2) + i)

        @pl.when(j >= 1)
        def _():
            ex[1].start(j - 1)

        s = outward(j)
        with scope("b_half"):
            for ch in range(n_tile):
                ring_x.wait(s * 2 + (1 - p.c), ch)
        at = Attend(*heads, brow[1], *work, lambda i, t: xg[pl.ds(pl.multiple_of(s * T, T) + i * t, t), :])
        with scope("b_att"):
            at.project()
            at.attend(j)
        with scope("b_ev"):
            take(1, j)
        return 0

    lax.fori_loop(0, S, step1, 0)
    ex[1].start(S - 1)
    pltpu.make_async_copy(w1g, wall, k_sem).wait()
    cross1.finish_far()
    ring_x.drain(xg.at[0:(n_tp - 1) * R, :])
    for peer in (p.at(1), p.at(-1), p.partner):
        pl.semaphore_signal(ready, inc=1, device_id={"tp": peer}, device_id_type=MESH)
    with scope("c_o1"):
        ex[1].sent()
        ex[1].arrived()
    def tile1(ch, _):
        rows = pl.ds(pl.multiple_of(ch * tile, tile), tile)
        with scope("c_mlp"):
            xg[pl.ds(pl.multiple_of(row0 + ch * tile, tile), tile), :] = _transition(size, tile, gate, mod, o1, act, wall, y_s, h_s, rows)

        @pl.when(ch == 0)
        def _():
            with scope("c_ready"):
                pl.semaphore_wait(ready, 3)

        ring_r.own(ch)
        return 0

    lax.fori_loop(0, n_tile, tile1, 0)
    with scope("c_svc"):
        lax.fori_loop(0, far * n_tile, lambda e, _: (ring_r.service(e // n_tile + 1, lax.rem(e, n_tile)), 0)[1], 0)

    def rest(i, _):
        for ch in range(n_tile):
            ring_r.wait(i * 2 + (1 - p.c), ch)
        return 0

    with scope("c_end"):
        lax.fori_loop(0, p.nz, rest, 0)
        ring_r.drain(xg.at[0:(n_tp - 1) * R, :])


def _main(n_dp, x, cond, pair_bias, mask_row, wq, bq, asc, aw, ab, zw, zb, wo, wup, wdn):
    S, T, D = x.shape
    C = cond.shape[-1]
    hd, hu = wq.shape[2], wdn.shape[1]
    n_tp = S * 2
    rows_w = hd + 3 * hu
    R = T // 2
    n_chunk = 3
    dma = pltpu.SemaphoreType.DMA
    v = pltpu.VMEM
    pair, pieces, each = dma((2,)), dma((S, n_chunk)), dma((n_tp, n_chunk))
    n_tile = 4
    tiles = dma((n_tp, n_tile))
    return pl.pallas_call(
        functools.partial(_main_kernel, (S, T, D, C, n_tp, n_dp, hd, hu, n_chunk, n_tile)),
        out_shape=(v((n_tp * R, D), BF16), pltpu.HBM((n_tp, rows_w, D), BF16)),
        in_specs=[ANY, ANY, ANY, VMEM, ANY, VMEM, VMEM, ANY, VMEM, ANY, VMEM, ANY, ANY, ANY],
        out_specs=(VMEM, HBM),
        scratch_shapes=[
            v((T, T), BF16), v((T, T), F32), v((4 * HP, D), BF16), v((T, 2 * HP), BF16), v((2 * HP, T), BF16), v((HP, T), BF16),
            v((hd, T), F32), v((2, T, QT), F32), v((S, hd, T), BF16),
            v((2, R, D), BF16), v((2, R, C), BF16), v((2, T, D), BF16), v((4, C, 2, D), BF16), *[v((C, 2 * D), BF16)] * 2,
            *[v((rows_w, D), BF16)] * 2, v((R, C), BF16), v((R, D), BF16), v((R // n_tile, D), BF16), v((R // n_tile, n_tp * hu), BF16),
            v((n_tp, rows_w, D), BF16), *[v((R, 2 * D), F32)] * 3, *[v((n_tp, hd, R), BF16)] * 2,
            pair, pair, dma, dma((4,)), dma((4,)), dma((2, 4)), pair, dma, pair, pair, pltpu.SemaphoreType.REGULAR,
            dma((2, S, 2)), pair, dma, dma((n_tp, 1)), dma, pieces, each, dma, pieces, each, dma, tiles, dma, tiles, pltpu.SemaphoreType.REGULAR],
        cost_estimate=pl.CostEstimate(flops=S * T * T * D, bytes_accessed=S * T * D, transcendentals=S * T * T),
        compiler_params=pltpu.CompilerParams(collective_id=0, has_side_effects=True, vmem_limit_bytes=VM),
        name="blocks",
    )(x, cond, pair_bias, mask_row, wq, bq, asc, aw, ab, zw, zb, wo, wup, wdn)


def _store_kernel(src, dst, sem):
    cp = pltpu.make_async_copy(src, dst, sem)
    cp.start()
    cp.wait()


def _store(x):
    return pl.pallas_call(
        _store_kernel, out_shape=jax.ShapeDtypeStruct(x.shape, x.dtype), in_specs=[VMEM], out_specs=ANY,
        scratch_shapes=[pltpu.SemaphoreType.DMA], compiler_params=pltpu.CompilerParams(vmem_limit_bytes=1 << 20), name="store")(x)


def solution(mesh):
    n_dp = mesh.shape["dp"]

    def shard_body(token_act, token_cond, pair_bias, token_mask, ada_scale, ada_w, ada_bias, zero_w, zero_b, w_qkvg, b_q, w_o, w_up, w_down):
        S, T, D = token_act.shape
        mask_row = token_mask.reshape(1, T)
        wq = jnp.transpose(w_qkvg, (0, 2, 3, 1))
        wup = jnp.transpose(w_up, (0, 2, 3, 1))
        out, _ = _main(n_dp, token_act, token_cond, pair_bias, mask_row, wq, b_q, ada_scale, ada_w, ada_bias, zero_w, zero_b, w_o, wup, w_down)
        out = pltpu.with_memory_space_constraint(out, pltpu.VMEM)
        return _store(out).reshape(S, T, D)

    everywhere = P()
    rows, second, fourth = P('dp'), P(None, 'tp'), P(*[None] * 3, 'tp')
    in_specs = (rows, rows, second) + (everywhere,) * 6 + (fourth, second, second, fourth, second)
    return jax.shard_map(shard_body, mesh=mesh, in_specs=in_specs, out_specs=rows, check_vma=False)
```

```python
import functools
import math

import jax
import jax.numpy as jnp
from jax import lax
from jax.experimental import pallas as pl
from jax.experimental.pallas import tpu as pltpu
from jax.sharding import PartitionSpec as P

LN_EPS = 1e-5
LOG2E = 1.4426950408889634
MESH = pl.DeviceIdType.MESH
BF16 = jnp.bfloat16
F32 = jnp.float32
scope = jax.named_scope
HP = 64
QT = 256
ANY = pl.BlockSpec(memory_space=pl.ANY)
VMEM = pl.BlockSpec(memory_space=pltpu.VMEM)
HBM = pl.BlockSpec(memory_space=pltpu.HBM)
VM = 50 << 20


def _ln(x):
    mean = jnp.mean(x, axis=-1, keepdims=True)
    cen = x - mean
    var = jnp.mean(cen * cen, axis=-1, keepdims=True)
    return cen * lax.rsqrt(var + LN_EPS)


def _sig(x):
    return 0.5 * jnp.tanh(0.5 * x) + 0.5


def _dot(a, b, ca=1, cb=0):
    return lax.dot_general(a, b, (((ca,), (cb,)), ((), ())), preferred_element_type=F32)


def _ada(x_f32, cond_normed, scale, w, bias):
    d = x_f32.shape[-1]
    mod = _dot((cond_normed * scale).astype(BF16), w)
    return (_sig(mod[:, :d] + bias) * _ln(x_f32) + mod[:, d:]).astype(BF16)


class Place:
    def __init__(self, n_tp, n_dp):
        self.n = n_tp
        self.n_dp = n_dp
        self.col = lax.axis_index("dp")
        self.nz = n_tp // 2
        self.me = lax.axis_index("tp")
        self.z = self.me // 2
        self.c = lax.rem(self.me, 2)
        self.partner = self.z * 2 + (1 - self.c)

    def at(self, off):
        return lax.rem(self.z + off + self.nz, self.nz) * 2 + self.c

    def column(self, i):
        return lax.rem(self.col + i, self.n_dp)

    def enter(self):
        barrier = pltpu.get_barrier_semaphore()
        peers = [{"tp": lax.rem(self.me + i, self.n)} for i in range(1, self.n)]
        peers += [{"dp": self.column(i), "tp": self.me} for i in range(1, self.n_dp)]
        for peer in peers:
            pl.semaphore_signal(barrier, inc=1, device_id=peer, device_id_type=MESH)
        return lambda: pl.semaphore_wait(barrier, len(peers))


class Ring:
    def __init__(self, place, view, recv_sem, send_sem, right=None):
        self.p, self.view, self.recv, self.send = place, view, recv_sem, send_sem
        self.far = place.nz // 2
        self.right = right or (lambda ch: place.c == 0)

    def _push(self, b, ch, dst, src=None):
        v = self.view(b, ch)
        pltpu.make_async_remote_copy(
            src_ref=v if src is None else src, dst_ref=v, send_sem=self.send, recv_sem=self.recv.at[b, ch],
            device_id={"tp": dst}, device_id_type=MESH).start()

    def own(self, ch, src=None):
        p = self.p
        self._push(p.me, ch, p.at(1), src)
        self._push(p.me, ch, p.at(-1), src)
        self._push(p.me, ch, p.partner, src)

    def wait(self, b, ch):
        v = self.view(b, ch)
        pltpu.make_async_copy(v, v, self.recv.at[b, ch]).wait()

    def service(self, h, ch):
        p = self.p
        right = self.right(ch)
        for sign, far in ((1, right), (-1, jnp.logical_not(right))):
            b = p.at(-sign * h)

            @pl.when((h < self.far) | far)
            def _():
                self.wait(b, ch)

                @pl.when((h < self.far - 1) | ((h == self.far - 1) & far))
                def _():
                    self._push(b, ch, p.at(sign))

                self._push(b, ch, p.partner)

    def drain(self, whole):
        pltpu.make_async_copy(whole, whole, self.send).wait()


class Cross:
    def __init__(self, place, buf, lo, hi, n_chunk, recv_sem, near_sem, far_sem, shift):
        self.p, self.buf, self.lo, self.hi, self.n_chunk, self.shift = place, buf, lo, hi, n_chunk, shift
        self.recv, self.near, self.far_sem = recv_sem, near_sem, far_sem
        self.far = place.nz // 2
        self.size = (hi - lo) // n_chunk

    def _rows(self, ch):
        return pl.ds(self.lo + ch * self.size, self.size)

    def _push(self, b, ch, dst, sem, src=None):
        v = self.buf.at[b, self._rows(ch), :]
        pltpu.make_async_remote_copy(
            src_ref=v if src is None else src, dst_ref=v, send_sem=sem, recv_sem=self.recv.at[b, ch],
            device_id=dst, device_id_type=MESH).start()

    def _push_over(self, b, ch):
        p = self.p
        for i in range(1, p.n_dp):
            self._push(b, ch, {"dp": p.column(i), "tp": p.me}, self.far_sem.at[b // 2])
        self._push(b, ch, {"tp": p.partner}, self.near)

    def _mine(self, b):
        return lax.rem(b + self.shift, self.p.n_dp) == self.p.col

    def own(self, src):
        p = self.p
        for ch in range(self.n_chunk):
            part = src.at[self._rows(ch), :]

            @pl.when(self._mine(p.me))
            def _():
                for off in (1, -1):
                    self._push(p.me, ch, {"tp": p.at(off)}, self.far_sem.at[p.z], part)

            self._push(p.me, ch, {"tp": p.partner}, self.near, part)

    def wait(self, b, ch):
        v = self.buf.at[b, self._rows(ch), :]
        pltpu.make_async_copy(v, v, self.recv.at[b, ch]).wait()

    def _each(self, h, body):
        p = self.p
        for sign, core in ((1, 0), (-1, 1)):
            b = p.at(-sign * h)

            @pl.when((h < self.far) | (p.c == core))
            def _():
                body(b, sign, (h < self.far - 1) | ((h == self.far - 1) & (p.c == core)))

    def along(self, h, ch):
        p = self.p

        def body(b, sign, onward):
            @pl.when(self._mine(b))
            def _():
                self.wait(b, ch)

                @pl.when(onward)
                def _():
                    self._push(b, ch, {"tp": p.at(sign)}, self.far_sem.at[b // 2])

                self._push_over(b, ch)

        self._each(h, body)

    def across(self, h, ch):
        p = self.p

        def body(b, sign, onward):
            @pl.when(jnp.logical_not(self._mine(b)))
            def _():
                self.wait(b, ch)
                self._push(b, ch, {"tp": p.partner}, self.near)

        self._each(h, body)

    def _sent(self, k, sem):
        if k:
            v = self.buf.at[0:k, self.lo:self.hi, :]
            pltpu.make_async_copy(v, v, sem).wait()

    def finish_near(self):
        p = self.p

        def other(i, _):
            for ch in range(self.n_chunk):
                self.wait(i * 2 + (1 - p.c), ch)
            return 0

        lax.fori_loop(0, p.nz, other, 0)
        self._sent(p.nz, self.near)

    def finish_far(self):
        p = self.p
        over = p.n_dp - 1

        @pl.when(self._mine(p.me))
        def _():
            self._sent(2, self.far_sem.at[p.z])

        def body(b, sign, onward):
            @pl.when(self._mine(b))
            def _():
                @pl.when(onward)
                def _():
                    self._sent(over + 1, self.far_sem.at[b // 2])

                @pl.when(jnp.logical_not(onward))
                def _():
                    self._sent(over, self.far_sem.at[b // 2])

        def hop(h, _):
            self._each(h, body)
            return 0

        lax.fori_loop(1, self.far + 1, hop, 0)


def _copy(src, dst, sem):
    cp = pltpu.make_async_copy(src, dst, sem)
    cp.start()
    return cp


def _stage(l, hd, hu, wo_hbm, wup_hbm, wdn_hbm, wst, sem):
    cps, lo = [], 0
    for src, rows in ((wo_hbm.at[l], hd), (wup_hbm.at[l, 0], hu), (wup_hbm.at[l, 1], hu), (wdn_hbm.at[l], hu)):
        cps.append(_copy(src, wst.at[pl.ds(lo, rows), :], sem.at[len(cps)]))
        lo += rows
    return cps


def _stage_qkvg(l, hd, wq_hbm, w_s, sem):
    return [_copy(wq_hbm.at[l, f], w_s.at[pl.ds(i * HP, hd), :], sem.at[i]) for i, f in enumerate((1, 0, 2, 3))]


class Attend:
    def __init__(self, n_tp, hd, w, brow, bt, k_s, qt_s, vt_s, gt_s, lg, o_s, x_rows):
        self.__dict__.update(locals())
        self.T = bt.shape[0]

    def project(self):
        T, hd = self.T, self.hd
        tile = QT
        for i in range(T // tile):
            rows = pl.ds(i * tile, tile)
            res = _dot(self.x_rows(i, tile), self.w[...], 1, 1) + self.brow
            self.k_s[rows, :] = res[:, :2 * HP].astype(BF16)
            rest = res.T
            self.qt_s[0:HP, rows] = rest[HP:2 * HP].astype(BF16)
            ones = lax.broadcasted_iota(jnp.int32, (HP, tile), 0) == hd
            self.vt_s[:, rows] = jnp.where(ones, 1.0, rest[2 * HP:3 * HP]).astype(BF16)
            self.gt_s[:, rows] = _sig(rest[3 * HP:3 * HP + hd])

    def attend(self, slot, hook=None):
        T, hd = self.T, self.hd
        n = T // QT
        c1 = LOG2E / math.sqrt(hd)

        def scores(i):
            cols = pl.ds(i * QT, QT)
            logits = _dot(self.k_s[...], self.qt_s[:, cols]) * c1 + self.bt[:, cols]
            self.lg[i % 2] = logits
            return jnp.max(logits, axis=0, keepdims=True)

        top = scores(0)
        if hook is not None:
            hook()
        for i in range(n):
            cols = pl.ds(i * QT, QT)
            nxt = scores(i + 1) if i + 1 < n else None
            probs = jnp.exp2(self.lg[i % 2] - top).astype(BF16)
            mixed = _dot(self.vt_s[...], probs)
            self.o_s[slot, :, cols] = (self.gt_s[:, cols] * (mixed[:hd] / mixed[hd:hd + 1])).astype(BF16)
            top = nxt


def _load_bias(bias_v, mask_ref, bt):
    T = bt.shape[0]
    mask_add = (mask_ref[...].astype(F32) - 1.0) * 1e9

    def step(i, _):
        r = pl.multiple_of(i * 128, 128)
        rows = (bias_v[pl.ds(r, 128), :].astype(F32) + mask_add) * LOG2E
        bt[:, pl.ds(r, 128)] = rows.T
        return 0

    lax.fori_loop(0, T // 128, step, 0)


class Exchange:
    def __init__(self, place, sample_of, o_s, o_out, send_sem, recv_sem):
        self.p, self.sample_of, self.o_s, self.o_out, self.send, self.recv = place, sample_of, o_s, o_out, send_sem, recv_sem
        self.half = o_s.shape[-1] // 2

    def _each(self, k, remote, local):
        p = self.p
        for c in range(2):
            dst = self.sample_of(k) * 2 + c
            src = self.o_s.at[k, :, pl.ds(c * self.half, self.half)]
            sem = self.send.at[k, c]
            cp = pltpu.make_async_remote_copy(
                src_ref=src, dst_ref=self.o_out.at[p.me], send_sem=sem, recv_sem=self.recv,
                device_id={"tp": dst}, device_id_type=MESH)

            @pl.when(dst != p.me)
            def _():
                remote(cp)

            @pl.when(dst == p.me)
            def _():
                local(pltpu.make_async_copy(src, self.o_out.at[p.me], sem))

    def start(self, k):
        self._each(k, lambda cp: cp.start(), lambda cp: cp.start())

    def sent(self):
        def one(k, _):
            self._each(k, lambda cp: cp.wait_send(), lambda cp: cp.wait())
            return 0

        lax.fori_loop(0, self.o_s.shape[0], one, 0)

    def arrived(self):
        rest = self.o_out.at[0:self.p.n - 1]
        pltpu.make_async_copy(rest, rest, self.recv).wait()


def _bias_row(bq, hd):
    return jnp.concatenate([jnp.zeros((1, HP), F32), bq, jnp.zeros((1, 3 * HP - hd), F32)], axis=1)


def _gates(out, cond, w, bias):
    d = bias.shape[-1]
    out[...] = _dot(cond, w)
    for j in range(bias.shape[0]):
        cols = pl.ds(j * d, d)
        out[:, cols] = _sig(out[:, cols] + bias[j:j + 1, :])


def _modulation(out, cond_normed, scale, w, bias):
    d = bias.shape[-1]
    out[...] = _dot((cond_normed * scale).astype(BF16), w)
    out[:, :d] = _sig(out[:, :d] + bias)


def _flat(raw):
    c, two, d = raw.shape
    return raw[...].reshape(c, two * d)


def _transition(dims, tile, gates, mod1, o_v, act, wall, y_s, h_s, rows):
    D, n_tp, hd, hu = dims
    w_o = wall[:, 0:hd, :].reshape(n_tp * hd, D)
    o_t = o_v[:, :, rows].reshape(n_tp * hd, tile)
    t = _dot(o_t, w_o, 0, 0).astype(BF16).astype(F32)
    mid = (act[rows, :].astype(F32) + gates[rows, :D] * t).astype(BF16).astype(F32)
    y_s[...] = (mod1[rows, :D] * _ln(mid) + mod1[rows, D:]).astype(BF16)
    step = 4 * hu
    for j in range(n_tp * hu // step):
        dv = slice(4 * j, 4 * j + 4)
        u1 = _dot(y_s[...], wall[dv, hd:hd + hu, :].reshape(step, D), 1, 1)
        u2 = _dot(y_s[...], wall[dv, hd + hu:hd + 2 * hu, :].reshape(step, D), 1, 1)
        h_s[:, j * step:(j + 1) * step] = (u1 * _sig(u1) * u2).astype(BF16)
    r = _dot(h_s[...], wall[:, hd + 2 * hu:hd + 3 * hu, :].reshape(n_tp * hu, D)).astype(BF16).astype(F32)
    return (mid + gates[rows, D:] * r).astype(BF16)


def _main_kernel(dims, x_hbm, cond_hbm, bias_hbm, mask_ref, wq_hbm, bq_ref, asc_ref, aw_hbm, ab_ref, zw_hbm, zb_ref, wo_hbm, wup_hbm, wdn_hbm,
                 xg, w1g,
                 bias_v, bt, w_s, k_s, qt_s, vt_s, gt_s, lg, o_s, xraw, craw, xn, raw, aw_s, flat_s, wst, wst1, cond, act, y_s, h_s,
                 wall, gate, mod, nxt, o0, o1,
                 ld_sem, cd_sem, b_sem, q_sem, a_sem, st_sem, own_sem, k_sem, n_send, n_recv, n_free,
                 o_send, o_recv, w_send, w_recv, c_near, c_far, c_recv, d_near, d_far, d_recv, x_send, x_recv, r_send, r_recv, ready):
    S, T, D, C, n_tp, n_dp, hd, hu, n_chunk, n_tile = dims
    p = Place(n_tp, n_dp)
    entered = p.enter()
    far = p.nz // 2
    rows_w = hd + 3 * hu
    cut = 2 * hd
    R = S * T // n_tp
    row0 = p.me * R
    tile = R // n_tile
    mine = pl.ds(p.c * R, R)
    stage = [_stage(l, hd, hu, wo_hbm, wup_hbm, wdn_hbm, w, st_sem.at[l]) for l, w in enumerate((wst, wst1))]

    def toward(k):
        j = S - 1 - k
        return lax.rem(p.z + S + (1 - 2 * lax.rem(j, 2)) * ((j + 1) // 2), S)

    def outward(j):
        return lax.rem(p.z + S + (1 - 2 * p.c) * (1 - 2 * lax.rem(j, 2)) * ((j + 1) // 2), S)

    def loads(k, slot):
        s = toward(k)
        return [pltpu.make_async_copy(x_hbm.at[s, mine], xraw.at[slot], ld_sem.at[slot]),
                pltpu.make_async_copy(cond_hbm.at[s, mine], craw.at[slot], cd_sem.at[slot])]

    raw0 = _copy(aw_hbm.at[0, 0], raw.at[0], a_sem.at[0])
    for k in range(2):
        for cp in loads(k, k):
            cp.start()
    bias_cp = _copy(bias_hbm.at[0, 0], bias_v, b_sem)
    for cp in stage[0]:
        cp.wait()
    raws = [_copy(src, raw.at[i + 1], a_sem.at[i + 1]) for i, src in enumerate((zw_hbm.at[0], aw_hbm.at[0, 1], aw_hbm.at[1, 0]))]
    own = [_copy(cond_hbm.at[p.z, mine], cond, own_sem.at[0]), _copy(x_hbm.at[p.z, mine], act, own_sem.at[1])]
    entered()
    ring_o = Ring(p, lambda b, ch: wall.at[b, 0:cut, :], w_recv, w_send)
    cross = Cross(p, wall, cut, rows_w, n_chunk, c_recv, c_near, c_far, 0)
    cross1 = Cross(p, w1g, 0, rows_w, n_chunk, d_recv, d_near, d_far, 0)
    ring_x = Ring(p, lambda b, ch: xg.at[pl.ds(b * R + ch * tile, tile), :], x_recv, x_send)
    ring_r = Ring(p, lambda b, ch: xg.at[pl.ds(b * R + ch * tile, tile), :], r_recv, r_send)
    ring_o.own(0, wst.at[0:cut, :])
    cross.own(wst)
    w_s[...] = jnp.zeros_like(w_s)
    qt_s[HP:, :] = jnp.zeros((HP, T), BF16)
    wq = _stage_qkvg(0, hd, wq_hbm, w_s, q_sem)

    def half(slot):
        v = xn.at[slot, mine]
        return pltpu.make_async_remote_copy(src_ref=v, dst_ref=v, send_sem=n_send.at[slot], recv_sem=n_recv.at[slot],
                                            device_id={"tp": p.partner}, device_id_type=MESH)

    def normalise(slot):
        big = R // 2
        for i in range(2):
            rows = pl.ds(i * big, big)
            cn = _ln(craw[slot, rows, :].astype(F32))
            y = _ada(xraw[slot, rows, :].astype(F32), cn, asc_ref[0, 0:1, :], aw_s[...], ab_ref[0, 0:1, :])
            xn[slot, pl.ds(pl.multiple_of(p.c * R, R) + i * big, big), :] = y

    raw0.wait()
    aw_s[...] = _flat(raw.at[0])
    for cp in loads(0, 0):
        cp.wait()
    normalise(0)
    bias_cp.wait()
    half(0).start()
    _load_bias(bias_v, mask_ref, bt)
    bias_cp = _copy(bias_hbm.at[1, 0], bias_v, b_sem)
    for cp in stage[1] + wq:
        cp.wait()
    wall[p.me] = wst[...]
    keep = _copy(wst1, w1g.at[p.me], k_sem)

    def gates(l, i):
        raws[i].wait()
        flat_s[...] = _flat(raw.at[i + 1])
        _gates(gate, cond[...], flat_s[...], zb_ref.at[l])

    def modulation(out, l, j, i):
        raws[i].wait()
        flat_s[...] = _flat(raw.at[i + 1])
        cn = _ln(cond[...].astype(F32))
        _modulation(out, cn, asc_ref[l, j:j + 1, :], flat_s[...], ab_ref[l, j:j + 1, :])

    events = {}

    def plan(when, f, *args):
        events.setdefault(when, []).append((f, args))

    def take(step, k):
        for when in sorted(events):
            if when % 2 == step:
                @pl.when(k == when // 2)
                def _():
                    for f, args in events[when]:
                        f(*args)

    first, over, whole = (0, 7, 9, 12), (5, 10, 13, 16), (1, 8, 12, 15)
    for h in range(1, far + 1):
        plan(whole[h - 1], ring_o.service, h, 0)
        for ch in range(n_chunk):
            plan(first[h - 1] + ch, cross.along, h, ch)
            plan(over[h - 1] + ch, cross.across, h, ch)
    for ch in range(n_chunk):
        plan(2 * S + n_chunk, cross1.along, 1, ch)
    plan(13, cross1.own, wst1)
    for cp in own:
        plan(3, cp.wait)
    plan(5, gates, 0, 0)
    plan(7, modulation, mod, 0, 1, 1)
    plan(9, modulation, nxt, 1, 0, 2)
    ex = [Exchange(p, order, o_s, o, o_send.at[l], o_recv.at[l]) for l, (order, o) in enumerate(((toward, o0), (outward, o1)))]
    brow = [_bias_row(bq_ref[l:l + 1, :], hd) for l in range(2)]
    heads = (n_tp, hd, w_s)
    work = (bt, k_s, qt_s, vt_s, gt_s, lg, o_s)

    def step0(k, _):
        slot = lax.rem(k, 2)

        @pl.when(k + 2 < S)
        def _():
            for cp in loads(k + 2, slot):
                cp.start()

        with scope("a_half"):
            v = xn.at[slot, pl.ds((1 - p.c) * R, R)]
            pltpu.make_async_copy(v, v, n_recv.at[slot]).wait()
            half(slot).wait_send()
        at = Attend(*heads, brow[0], *work, lambda i, t: xn[slot, pl.ds(i * t, t), :])
        at.project()

        @pl.when(k + 2 < S)
        def _():
            pl.semaphore_signal(n_free, inc=1, device_id={"tp": p.partner}, device_id_type=MESH)

        @pl.when(k >= 1)
        def _():
            ex[0].start(k - 1)

        @pl.when(k + 1 < S)
        def _():
            for cp in loads(k + 1, 1 - slot):
                cp.wait()
            normalise(1 - slot)

            @pl.when(k >= 1)
            def _():
                pl.semaphore_wait(n_free, 1)

        with scope("a_ev0"):
            take(0, k)

        def hook():
            @pl.when(k + 1 < S)
            def _():
                half(1 - slot).start()

        with scope("a_att"):
            at.attend(k, hook)
        with scope("a_ev1"):
            take(1, k)
        return 0

    lax.fori_loop(0, S, step0, 0)
    ex[0].start(S - 1)
    wq = _stage_qkvg(1, hd, wq_hbm, w_s, q_sem)
    raws = [_copy(src, raw.at[i + 1], a_sem.at[i + 1]) for i, src in enumerate((zw_hbm.at[1], aw_hbm.at[1, 1]))]
    for when in sorted(events):
        if when >= 2 * S:
            for f, args in events[when]:
                f(*args)

    def other(i, _):
        ring_o.wait(i * 2 + (1 - p.c), 0)
        return 0

    with scope("b_w0"):
        lax.fori_loop(0, p.nz, other, 0)
        cross.finish_near()
    with scope("b_o0"):
        ex[0].sent()
        ex[0].arrived()
    size = (D, n_tp, hd, hu)

    def tile0(ch, _):
        rows = pl.ds(pl.multiple_of(ch * tile, tile), tile)
        with scope("b_mlp"):
            new = _transition(size, tile, gate, mod, o0, act, wall, y_s, h_s, rows)
            act[rows, :] = new
            xg[pl.ds(pl.multiple_of(row0 + ch * tile, tile), tile), :] = (nxt[rows, :D] * _ln(new.astype(F32)) + nxt[rows, D:]).astype(BF16)
        ring_x.own(ch)

        @pl.when(ch == n_tile - 1)
        def _():
            with scope("b_along"):
                for i in range(n_chunk):
                    cross1.along(2, i)
        return 0

    lax.fori_loop(0, n_tile, tile0, 0)
    bias_cp.wait()
    _load_bias(bias_v, mask_ref, bt)
    for cp in wq:
        cp.wait()
    ring_o.drain(wall.at[0:n_tp - 1, 0:cut, :])
    cross.finish_far()
    keep.wait()
    events = {}
    for ch in range(n_chunk):
        plan(5, cross1.along, far - 1, ch)
        plan(9, cross1.along, far, ch)
        for h in range(1, far + 1):
            plan(2 * h + 5, cross1.across, h, ch)
    plan(1, gates, 1, 0)
    plan(5, modulation, mod, 1, 1, 1)

    def last_weights():
        cross1.finish_near()
        pltpu.make_async_copy(w1g, wall, k_sem).start()

    plan(2 * S - 3, last_weights)

    def step1(j, _):
        with scope("b_svc"):
            for i in range(n_tile // 2):
                ring_x.service(j // 2 + 1, lax.rem(j, 2) * (n_tile // 2) + i)

        s = outward(j)
        with scope("b_half"):
            for ch in range(n_tile):
                ring_x.wait(s * 2 + (1 - p.c), ch)
        at = Attend(*heads, brow[1], *work, lambda i, t: xg[pl.ds(pl.multiple_of(s * T, T) + i * t, t), :])
        with scope("b_att"):
            at.project()
            at.attend(j)
        ex[1].start(j)
        with scope("b_ev"):
            take(1, j)
        return 0

    lax.fori_loop(0, S, step1, 0)
    pltpu.make_async_copy(w1g, wall, k_sem).wait()
    cross1.finish_far()
    ring_x.drain(xg.at[0:(n_tp - 1) * R, :])
    for peer in (p.at(1), p.at(-1), p.partner):
        pl.semaphore_signal(ready, inc=1, device_id={"tp": peer}, device_id_type=MESH)
    with scope("c_o1"):
        ex[1].sent()
        ex[1].arrived()
    def tile1(ch, _):
        rows = pl.ds(pl.multiple_of(ch * tile, tile), tile)
        with scope("c_mlp"):
            xg[pl.ds(pl.multiple_of(row0 + ch * tile, tile), tile), :] = _transition(size, tile, gate, mod, o1, act, wall, y_s, h_s, rows)

        @pl.when(ch == 0)
        def _():
            with scope("c_ready"):
                pl.semaphore_wait(ready, 3)

        ring_r.own(ch)
        return 0

    lax.fori_loop(0, n_tile, tile1, 0)
    with scope("c_svc"):
        lax.fori_loop(0, far * n_tile, lambda e, _: (ring_r.service(e // n_tile + 1, lax.rem(e, n_tile)), 0)[1], 0)

    def rest(i, _):
        for ch in range(n_tile):
            ring_r.wait(i * 2 + (1 - p.c), ch)
        return 0

    with scope("c_end"):
        lax.fori_loop(0, p.nz, rest, 0)
        ring_r.drain(xg.at[0:(n_tp - 1) * R, :])


def _main(n_dp, x, cond, pair_bias, mask_row, wq, bq, asc, aw, ab, zw, zb, wo, wup, wdn):
    S, T, D = x.shape
    C = cond.shape[-1]
    hd, hu = wq.shape[2], wdn.shape[1]
    n_tp = S * 2
    rows_w = hd + 3 * hu
    R = T // 2
    n_chunk = 3
    dma = pltpu.SemaphoreType.DMA
    v = pltpu.VMEM
    pair, blocks, each = dma((2,)), dma((S,)), dma((n_tp, n_chunk))
    n_tile = 4
    tiles = dma((n_tp, n_tile))
    return pl.pallas_call(
        functools.partial(_main_kernel, (S, T, D, C, n_tp, n_dp, hd, hu, n_chunk, n_tile)),
        out_shape=(v((n_tp * R, D), BF16), pltpu.HBM((n_tp, rows_w, D), BF16)),
        in_specs=[ANY, ANY, ANY, VMEM, ANY, VMEM, VMEM, ANY, VMEM, ANY, VMEM, ANY, ANY, ANY],
        out_specs=(VMEM, HBM),
        scratch_shapes=[
            v((T, T), BF16), v((T, T), F32), v((4 * HP, D), BF16), v((T, 2 * HP), BF16), v((2 * HP, T), BF16), v((HP, T), BF16),
            v((hd, T), F32), v((2, T, QT), F32), v((S, hd, T), BF16),
            v((2, R, D), BF16), v((2, R, C), BF16), v((2, T, D), BF16), v((4, C, 2, D), BF16), *[v((C, 2 * D), BF16)] * 2,
            *[v((rows_w, D), BF16)] * 2, v((R, C), BF16), v((R, D), BF16), v((R // n_tile, D), BF16), v((R // n_tile, n_tp * hu), BF16),
            v((n_tp, rows_w, D), BF16), *[v((R, 2 * D), F32)] * 3, *[v((n_tp, hd, R), BF16)] * 2,
            pair, pair, dma, dma((4,)), dma((4,)), dma((2, 4)), pair, dma, pair, pair, pltpu.SemaphoreType.REGULAR,
            dma((2, S, 2)), pair, dma, dma((n_tp, 1)), dma, blocks, each, dma, blocks, each, dma, tiles, dma, tiles, pltpu.SemaphoreType.REGULAR],
        cost_estimate=pl.CostEstimate(flops=S * T * T * D, bytes_accessed=S * T * D, transcendentals=S * T * T),
        compiler_params=pltpu.CompilerParams(collective_id=0, has_side_effects=True, vmem_limit_bytes=VM),
        name="blocks",
    )(x, cond, pair_bias, mask_row, wq, bq, asc, aw, ab, zw, zb, wo, wup, wdn)


def _store_kernel(src, dst, sem):
    cp = pltpu.make_async_copy(src, dst, sem)
    cp.start()
    cp.wait()


def _store(x):
    return pl.pallas_call(
        _store_kernel, out_shape=jax.ShapeDtypeStruct(x.shape, x.dtype), in_specs=[VMEM], out_specs=ANY,
        scratch_shapes=[pltpu.SemaphoreType.DMA], compiler_params=pltpu.CompilerParams(vmem_limit_bytes=1 << 20), name="store")(x)


def solution(mesh):
    n_dp = mesh.shape["dp"]

    def shard_body(token_act, token_cond, pair_bias, token_mask, ada_scale, ada_w, ada_bias, zero_w, zero_b, w_qkvg, b_q, w_o, w_up, w_down):
        S, T, D = token_act.shape
        mask_row = token_mask.reshape(1, T)
        wq = jnp.transpose(w_qkvg, (0, 2, 3, 1))
        wup = jnp.transpose(w_up, (0, 2, 3, 1))
        out, _ = _main(n_dp, token_act, token_cond, pair_bias, mask_row, wq, b_q, ada_scale, ada_w, ada_bias, zero_w, zero_b, w_o, wup, w_down)
        out = pltpu.with_memory_space_constraint(out, pltpu.VMEM)
        return _store(out).reshape(S, T, D)

    everywhere = P()
    rows, second, fourth = P('dp'), P(None, 'tp'), P(*[None] * 3, 'tp')
    in_specs = (rows, rows, second) + (everywhere,) * 6 + (fourth, second, second, fourth, second)
    return jax.shard_map(shard_body, mesh=mesh, in_specs=in_specs, out_specs=rows, check_vma=False)
```
